32 devices in a mesh: dp: 4 (over y, core), expert: 8 (over z, x).
Axes of the slice: x: 2, y: 2, z: 4, core: 2. Of those that a mesh axis runs over, the one named last changes fastest.
Arguments:
- tokens: bfloat16 [16, 1024, 768], P('dp', 'expert'), may hold values from -6 to 6
- segments: int32 [16, 1024], P('dp'), may hold values from 0 to 3, never falling along the last dimension, each value on 1 to 800 neighbouring positions
- routes: int32 [16, 1024, 2], P('dp', 'expert'), may hold values from 0 to 7, as said below
- slots: int32 [16, 1024, 2], P('dp', 'expert'), may hold values from -1 to 191, as said below
- cotangent: bfloat16 [16, 1024, 768], P('dp', 'expert'), may hold values from -6 to 6
- attn_gain: bfloat16 [768], replicated, may hold values from 0.25 to 1.75
- w_qkv: bfloat16 [768, 2304], replicated, may hold values from -0.21875 to 0.21875
- w_out: bfloat16 [768, 768], replicated, may hold values from -0.875 to 0.875
- ffn_gain: bfloat16 [768], replicated, may hold values from 0.25 to 1.75
- w_router: bfloat16 [768, 8], replicated, may hold values from -0.14941406 to 0.14941406
- shared_gate: bfloat16 [768, 2048], replicated, may hold values from -0.21875 to 0.21875
- shared_up: bfloat16 [768, 2048], replicated, may hold values from -0.21875 to 0.21875
- shared_down: bfloat16 [2048, 768], replicated, may hold values from -0.125 to 0.125
- expert_gate: bfloat16 [8, 768, 2048], P('expert'), may hold values from -0.21875 to 0.21875
- expert_up: bfloat16 [8, 768, 2048], P('expert'), may hold values from -0.21875 to 0.21875
- expert_down: bfloat16 [8, 2048, 768], P('expert'), may hold values from -0.125 to 0.125
Outputs:
- layer_out: bfloat16 [16, 1024, 768], P('dp', 'expert')
- token_grad: bfloat16 [16, 1024, 768], P('dp', 'expert')
- grad_attn_gain: float32 [768], P(('dp', 'expert'))
- grad_w_qkv: float32 [768, 2304], P(('dp', 'expert'))
- grad_w_out: float32 [768, 768], P(('dp', 'expert'))
- grad_ffn_gain: float32 [768], P(('dp', 'expert'))
- grad_w_router: float32 [768, 8], P(('dp', 'expert'))
- grad_shared_gate: float32 [768, 2048], P(('dp', 'expert'))
- grad_shared_up: float32 [768, 2048], P(('dp', 'expert'))
- grad_shared_down: float32 [2048, 768], P(None, ('dp', 'expert'))
- grad_expert_gate: float32 [8, 768, 2048], P('expert', None, 'dp')
- grad_expert_up: float32 [8, 768, 2048], P('expert', None, 'dp')
- grad_expert_down: float32 [8, 2048, 768], P('expert', 'dp')
The draws below stay inside these ranges and needn't reach their ends.
Inputs may be any that keep to these rules, and one draw needn't show every extreme that they name: `segments`: documents are numbered from 0 in order along each sequence, 4 of them, each of at most 800 tokens. `routes`: the 2 experts of a token differ; among the tokens of one device (positions r * 128 to (r + 1) * 128 - 1 of the 4 sequences of one index of dp), exactly 256 name as first choice one expert, the same for all devices of that index of dp. On one device, taking its tokens in order of sequence, then position, then choice, the routes to one expert get slots 0, 1, 2, ... and those from 192 on get -1; in every index of dp one expert takes 192 slots from every device.
All inputs are finite; a program needn't handle non-finite values.
Results may differ from the reference program's by a relative error of at most 0.015.
Values may be sent and summed in bfloat16 or wider, within the bound.
No kernel may reach another device: no remote copies, remote signals or barrier semaphores. Data moves between devices by JAX's collectives and lax.ppermute only.
A program may use at most 320 MiB of HBM per device.

```python
import math
import jax
import jax.numpy as jnp
import numpy as np
from jax import lax

D = 768
HEADS = 12
HEAD_DIM = 64
FF = 2048
FS = 2048
EXPERTS = 8
TOP = 2
SPAN = 128
SEQ_GRP = 4
LEN = 1024
SEQS = 16
DOC_MOST = 800
DOCS = 4
CAP_DEV = 192
HOT_ROWS = 256


def route_table(key):
    group_count = SEQS // SEQ_GRP
    rank_count = LEN // SPAN
    per_device = SEQ_GRP * SPAN
    device_count = group_count * rank_count
    hottest = jax.random.randint(jax.random.fold_in(key, 101), (group_count,), 0, EXPERTS)
    hot_device = jnp.repeat(hottest, rank_count)[:, None]
    device_keys = jax.random.split(jax.random.fold_in(key, 102), device_count)
    ordering = jax.vmap(lambda device_key: jax.random.permutation(device_key, per_device))(device_keys)
    others = jax.random.randint(jax.random.fold_in(key, 103), (device_count, per_device), 0, EXPERTS - 1)
    stepping = jax.random.randint(jax.random.fold_in(key, 104), (device_count, per_device), 0, EXPERTS - 1)
    leading = jnp.where(ordering < HOT_ROWS, hot_device, (hot_device + 1 + others) % EXPERTS)
    trailing = (leading + 1 + stepping) % EXPERTS
    chosen = jnp.stack([leading, trailing], axis=-1).reshape(device_count, 2 * per_device)
    onehot = (chosen[:, :, None] == jnp.arange(EXPERTS)[None, None, :]).astype(jnp.int32)
    earlier = jnp.cumsum(onehot, axis=1) - onehot
    slot_all = jnp.sum(earlier * onehot, axis=-1)
    kept = jnp.where(slot_all < CAP_DEV, slot_all, -1)

    def arrange(table):
        table = table.reshape(group_count, rank_count, SEQ_GRP, SPAN, 2)
        return jnp.transpose(table, (0, 2, 1, 3, 4)).reshape(SEQS, LEN, 2)
    return (arrange(chosen).astype(jnp.int32), arrange(kept).astype(jnp.int32))


def draw_routes(key, part):
    return route_table(key)[0]


def draw_slots(key, part):
    return route_table(key)[1]


def level_of(key, extent, pieces, least, high):
    level = 1.0
    for axis_at, blocks in pieces:
        heights = jax.random.uniform(jax.random.fold_in(jax.random.fold_in(key, 6), axis_at), (blocks,), jnp.float32, least / len(pieces), high / len(pieces))
        level = level * jnp.repeat(jnp.exp(heights), extent[axis_at] // blocks).reshape((-1,) + (1,) * (len(extent) - 1 - axis_at))
    return level


def length_profile(number_of, total, reach, slope):
    loads = [(1 << 20) // math.isqrt(grade ** slope) + 1 for grade in range(2, number_of + 1)]
    spare, holding = total - reach - (number_of - 1), [1] * (number_of - 1)
    while spare > 0:
        movable = [i for i in range(number_of - 1) if holding[i] < reach]
        pool, left = sum([loads[i] for i in movable]), spare
        for i in movable:
            extra = min(reach - holding[i], max(1, left * loads[i] // pool), spare)
            holding[i] = holding[i] + extra
            spare = spare - extra
    return np.array([reach] + holding)


def ragged_sizes(stream_key, amount, total, bound, lean):
    if amount == 2:
        one = jax.random.randint(stream_key, (), max(1, total - bound), min(bound, total - 1) + 1)
        return jnp.stack([one, total - one])
    lengths = jnp.asarray(length_profile(amount, total, bound, lean), jnp.int32)
    pairs = (amount - 1) // 2
    source_of, taker = lengths[1:1 + 2 * pairs:2], lengths[2:2 + 2 * pairs:2]
    room = jnp.minimum(source_of - 1, bound - taker)
    passed = jax.random.randint(jax.random.fold_in(stream_key, 1), (pairs,), 0, 1 << 20) % (room + 1)
    lengths = lengths.at[1:1 + 2 * pairs:2].set(source_of - passed).at[2:2 + 2 * pairs:2].set(taker + passed)
    return lengths[jax.random.permutation(jax.random.fold_in(stream_key, 2), amount)]


def bell_draw(key, extent, scale, limit, pieces=(), kind=jnp.bfloat16):
    result = scale * jax.random.normal(key, extent, jnp.float32)
    if pieces:
        result = result * level_of(key, extent, pieces, -0.22, 0.18)
    return jnp.clip(result, -limit, limit).astype(kind)


def setup_inputs(seed: int = 0) -> dict:
    key_list = jax.random.split(jax.random.key(seed), 17)
    tokens = bell_draw(key_list[0], (SEQS, LEN, D), 1.0, 6.0, ((0, 4), (1, 8)))
    segments = jax.vmap(lambda own: jnp.searchsorted(jnp.cumsum(ragged_sizes(own, DOCS, LEN, DOC_MOST, 2)), jnp.arange(LEN), side="right"))(jax.random.split(key_list[1], SEQS)).reshape((SEQS, LEN)).astype(jnp.int32)
    routes = draw_routes(jax.random.fold_in(key_list[16], 71), 0)
    slots = draw_slots(jax.random.fold_in(key_list[16], 71), 0)
    cotangent = bell_draw(key_list[4], (SEQS, LEN, D), 1.0, 6.0, ((0, 4), (1, 8)))
    attn_gain = jnp.clip(1.0 + 0.15 * jax.random.normal(key_list[5], (D,), jnp.float32), 0.25, 1.75).astype(jnp.bfloat16)
    w_qkv = bell_draw(key_list[6], (D, 3 * D), D ** -0.5, 0.21875)
    w_out = bell_draw(key_list[7], (D, D), (D // 16) ** -0.5, 0.875)
    ffn_gain = jnp.clip(1.0 + 0.15 * jax.random.normal(key_list[8], (D,), jnp.float32), 0.25, 1.75).astype(jnp.bfloat16)
    w_router = bell_draw(key_list[9], (D, EXPERTS), 0.025, 0.14941406)
    shared_gate = bell_draw(key_list[10], (D, FS), D ** -0.5, 0.21875)
    shared_up = bell_draw(key_list[11], (D, FS), D ** -0.5, 0.21875)
    shared_down = bell_draw(key_list[12], (FS, D), FS ** -0.5, 0.125)
    expert_gate = bell_draw(key_list[13], (EXPERTS, D, FF), D ** -0.5, 0.21875, ((0, 8),))
    expert_up = bell_draw(key_list[14], (EXPERTS, D, FF), D ** -0.5, 0.21875, ((0, 8),))
    expert_down = bell_draw(key_list[15], (EXPERTS, FF, D), FF ** -0.5, 0.125, ((0, 8),))
    return {"tokens": tokens, "segments": segments, "routes": routes, "slots": slots, "cotangent": cotangent, "attn_gain": attn_gain, "w_qkv": w_qkv, "w_out": w_out, "ffn_gain": ffn_gain, "w_router": w_router, "shared_gate": shared_gate, "shared_up": shared_up, "shared_down": shared_down, "expert_gate": expert_gate, "expert_up": expert_up, "expert_down": expert_down}


eps = 1e-06
HIGH = lax.Precision.HIGHEST

@jax.custom_vjp
def low(v):
    return lax.optimization_barrier(v.astype(jnp.bfloat16)).astype(jnp.float32)

@jax.custom_vjp
def low_back(v):
    return v

def low_keep(v):
    return (low(v), None)

def low_pass(kept, grad):
    return (grad,)

def back_keep(v):
    return (v, None)

def back_low(kept, grad):
    return (low(grad),)
low.defvjp(low_keep, low_pass)
low_back.defvjp(back_keep, back_low)

def rms_scale(values):
    return lax.rsqrt(lax.optimization_barrier(jnp.mean(values * values, axis=-1, keepdims=True)) + eps)

def rotate(tensor, cosine, sine_table):
    middle = tensor.shape[-1] // 2
    leading = tensor[..., :middle]
    trailing = tensor[..., middle:]
    return jnp.concatenate([leading * cosine - trailing * sine_table, trailing * cosine + leading * sine_table], axis=-1)

def attend_one(queries, key_rows, values, segment):
    scores = jnp.einsum('qhd,khd->hqk', queries, key_rows, precision=HIGH) * (1.0 / math.sqrt(HEAD_DIM))
    scores = low_back(scores)
    position = jnp.arange(LEN, dtype=jnp.int32)
    allowed = (segment[:, None] == segment[None, :]) & (position[None, :] <= position[:, None])
    scores = jnp.where(allowed[None], scores, -1e+30)
    weights = jax.nn.softmax(scores, axis=-1)
    return jnp.einsum('hqk,khd->qhd', low(weights), values, precision=HIGH)

def attend_block(inputs):
    queries, key_rows, values, segment = inputs
    return attend_one(queries, key_rows, values, segment)

def forward(params, tokens_in, segment, cosine, sine_table, buffer_token, row_place, route_hot):
    attn_gain, w_qkv, w_out, ffn_gain, w_router, shared_gate, shared_up, shared_down, expert_gate, expert_up, expert_down = params
    token_rows = tokens_in.reshape(-1, D)
    normed = low(token_rows * rms_scale(token_rows) * attn_gain)
    projected = low_back(jnp.dot(normed, w_qkv, precision=HIGH))
    head_shape = (SEQ_GRP, LEN, HEADS, HEAD_DIM)
    queries = low(rotate(projected[:, :D].reshape(head_shape), cosine, sine_table))
    key_rows = low(rotate(projected[:, D:2 * D].reshape(head_shape), cosine, sine_table))
    values = low(projected[:, 2 * D:].reshape(head_shape))
    attended = lax.map(jax.checkpoint(attend_block), (queries, key_rows, values, segment))
    attended = low(low_back(attended.reshape(-1, D)))
    attn_out = low_back(jnp.dot(attended, w_out, precision=HIGH))
    hidden = token_rows + attn_out
    branch_in = low(hidden * rms_scale(hidden) * ffn_gain)
    logits = low_back(jnp.dot(branch_in, w_router, precision=HIGH))
    chosen = lax.optimization_barrier(jnp.sum(logits[:, None, :] * route_hot, axis=-1))
    gates = jax.nn.softmax(chosen, axis=-1)
    shared_gval = low_back(jnp.dot(branch_in, shared_gate, precision=HIGH))
    shared_uval = low_back(jnp.dot(branch_in, shared_up, precision=HIGH))
    shared_hid = low(jax.nn.silu(shared_gval) * shared_uval)
    shared_out = low_back(jnp.dot(shared_hid, shared_down, precision=HIGH))
    padded_in = jnp.concatenate([branch_in, jnp.zeros((1, D), jnp.float32)], axis=0)
    expert_in = low_back(padded_in[buffer_token]).reshape(EXPERTS, -1, D)
    expert_gval = low_back(jnp.einsum('erd,edf->erf', expert_in, expert_gate, precision=HIGH))
    expert_uval = low_back(jnp.einsum('erd,edf->erf', expert_in, expert_up, precision=HIGH))
    expert_hid = low(jax.nn.silu(expert_gval) * expert_uval)
    expert_out = low(low_back(jnp.einsum('erf,efd->erd', expert_hid, expert_down, precision=HIGH)))
    padded_out = jnp.concatenate([expert_out.reshape(-1, D), jnp.zeros((1, D), jnp.float32)], axis=0)
    returned = padded_out[row_place]
    routed = lax.optimization_barrier(jnp.sum(gates[:, :, None] * returned, axis=1))
    return (hidden + shared_out + routed).reshape(tokens_in.shape)

def place_rows(group_routes, group_slots):
    row_total = SEQ_GRP * LEN
    per_expert = LEN // SPAN * CAP_DEV
    owner = (jnp.arange(LEN, dtype=jnp.int32) // SPAN)[None, :, None]
    target = group_routes * per_expert + owner * CAP_DEV + group_slots
    target = jnp.where(group_slots >= 0, target, EXPERTS * per_expert).reshape(row_total, TOP).astype(jnp.int32)
    row_ids = (jnp.arange(row_total * TOP, dtype=jnp.int32) // TOP).astype(jnp.int32)
    buffer_token = jnp.full((EXPERTS * per_expert,), row_total, jnp.int32).at[target.reshape(-1)].set(row_ids, mode='drop')
    route_hot = (group_routes.reshape(row_total, TOP)[:, :, None] == jnp.arange(EXPERTS, dtype=jnp.int32)[None, None, :]).astype(jnp.float32)
    return (buffer_token, target, route_hot)

def reference(tokens, segments, routes, slots, cotangent, attn_gain, w_qkv, w_out, ffn_gain, w_router, shared_gate, shared_up, shared_down, expert_gate, expert_up, expert_down):
    params = tuple((weight.astype(jnp.float32) for weight in (attn_gain, w_qkv, w_out, ffn_gain, w_router, shared_gate, shared_up, shared_down, expert_gate, expert_up, expert_down)))
    group_count = SEQS // SEQ_GRP
    frequency = jnp.power(10000.0, -2.0 * jnp.arange(HEAD_DIM // 2, dtype=jnp.float32) / HEAD_DIM)
    angles = jnp.arange(LEN, dtype=jnp.int32).astype(jnp.float32)[:, None] * frequency[None, :]
    cosine = jnp.cos(angles)[None, :, None, :]
    sine_table = jnp.sin(angles)[None, :, None, :]

    def one_group(totals, inputs):
        group_tokens, group_segments, group_routes, group_slots, group_cotangent = inputs
        buffer_token, row_place, route_hot = place_rows(group_routes, group_slots)

        def apply_layer(weights_in, tokens_in):
            return forward(weights_in, tokens_in, group_segments, cosine, sine_table, buffer_token, row_place, route_hot)
        output, pullback = jax.vjp(apply_layer, params, group_tokens.astype(jnp.float32))
        weight_grads, token_grads = pullback(group_cotangent.astype(jnp.float32))
        totals = jax.tree.map(jnp.add, totals, weight_grads)
        return (totals, (output.astype(jnp.bfloat16), token_grads.astype(jnp.bfloat16)))
    zeros = jax.tree.map(jnp.zeros_like, params)
    stacked = (tokens.reshape(group_count, SEQ_GRP, LEN, D), segments.reshape(group_count, SEQ_GRP, LEN), routes.reshape(group_count, SEQ_GRP, LEN, TOP), slots.reshape(group_count, SEQ_GRP, LEN, TOP), cotangent.reshape(group_count, SEQ_GRP, LEN, D))
    totals, (outputs, token_grads) = lax.scan(one_group, zeros, stacked)
    return (outputs.reshape(SEQS, LEN, D), token_grads.reshape(SEQS, LEN, D), totals[0], totals[1], totals[2], totals[3], totals[4], totals[5], totals[6], totals[7], totals[8], totals[9], totals[10])
```

```python
import jax
import jax.numpy as jnp
from jax import lax
from jax.experimental import pallas as pl
from jax.experimental.pallas import tpu as pltpu
from jax.sharding import Mesh
from jax.sharding import PartitionSpec as P

HEAD_DIM = 64
EPS = 1e-06
BF = jnp.bfloat16
F32 = jnp.float32
NEG = -1e30
NN = (((1,), (0,)), ((), ()))
NT = (((1,), (1,)), ((), ()))
TN = (((0,), (0,)), ((), ()))
VMEM_MOST = 60 << 20


def mm(left, right, dims=NN):
    return lax.dot_general(left, right, dims, preferred_element_type=F32)


def sds(shape, dtype):
    return jax.ShapeDtypeStruct(shape, dtype)


def call(body, grid, in_specs, out_specs, out_shape, args, scratch=(), prefetch=0, flops=0):
    leaves = jax.tree.leaves(out_shape)
    moved = sum(a.size * a.dtype.itemsize for a in args) + sum(
        a.size * a.dtype.itemsize for a in leaves
    )
    return pl.pallas_call(
        body,
        out_shape=out_shape,
        grid_spec=pltpu.PrefetchScalarGridSpec(
            num_scalar_prefetch=prefetch,
            grid=grid,
            in_specs=in_specs,
            out_specs=out_specs,
            scratch_shapes=list(scratch),
        ),
        compiler_params=pltpu.CompilerParams(
            dimension_semantics=("arbitrary",) * len(grid), vmem_limit_bytes=VMEM_MOST
        ),
        cost_estimate=pl.CostEstimate(
            flops=int(flops), transcendentals=0, bytes_accessed=int(moved)
        ),
    )(*args)


def whole(shape):
    rank = len(shape)
    return pl.BlockSpec(tuple(shape), lambda *_: (0,) * rank)


def swap_halves(value):
    lane = lax.broadcasted_iota(jnp.int32, value.shape, 1)
    return jnp.where(lane % 64 < 32, pltpu.roll(value, 96, 1), pltpu.roll(value, 32, 1))


def rms(values):
    return lax.rsqrt(jnp.mean(values * values, axis=1, keepdims=True) + EPS)


def project(rows, gain, weight, cosine, sine):
    parts, blocks, span, width = rows.shape
    cols = weight.shape[1]
    group = cols // 3
    height = parts * span
    length = height * blocks

    def body(r_ref, g_ref, w_ref, c_ref, s_ref, qkv_ref, n_ref):
        tok = r_ref[...].reshape(height, width).astype(F32)
        normed = (tok * rms(tok) * g_ref[...]).astype(BF)
        n_ref[...] = normed
        proj = mm(normed, w_ref[...])
        for at in range(0, 2 * group, 128):
            part = proj[:, at : at + 128]
            lane = lax.broadcasted_iota(jnp.int32, part.shape, 1) + at
            turned = part * c_ref[...] + swap_halves(part) * s_ref[...]
            turned = turned * jnp.where(lane < group, HEAD_DIM**-0.5, 1.0)
            qkv_ref[:, at : at + 128] = turned.astype(BF)
        qkv_ref[:, 2 * group :] = proj[:, 2 * group :].astype(BF)

    return call(
        body,
        (blocks,),
        [
            pl.BlockSpec((parts, 1, span, width), lambda i: (0, i, 0, 0)),
            whole((1, width)),
            whole((width, cols)),
            pl.BlockSpec((height, 128), lambda i: (i, 0)),
            pl.BlockSpec((height, 128), lambda i: (i, 0)),
        ],
        [
            pl.BlockSpec((height, cols), lambda i: (i, 0)),
            pl.BlockSpec((height, width), lambda i: (i, 0)),
        ],
        [sds((length, cols), BF), sds((length, width), BF)],
        (rows, gain, weight, cosine, sine),
        flops=2 * length * width * cols,
    )


def project_back(grads, weight, rows, gain):
    parts, blocks, span, width = rows.shape
    group = grads[0].shape[1]
    height = parts * span
    length = height * blocks

    def body(q_ref, k_ref, v_ref, w_ref, r_ref, out_ref, gain_ref, acc_ref):
        step = pl.program_id(0)
        back = mm(q_ref[...], w_ref[:, :group], NT)
        back += mm(k_ref[...], w_ref[:, group : 2 * group], NT)
        back += mm(v_ref[...], w_ref[:, 2 * group :], NT)
        tok = r_ref[...].reshape(height, width).astype(F32)
        part = jnp.sum(back * tok * rms(tok), axis=0, keepdims=True)

        @pl.when(step == 0)
        def _():
            acc_ref[...] = jnp.zeros_like(acc_ref)

        acc_ref[...] += jnp.broadcast_to(part, acc_ref.shape)
        out_ref[...] = back.astype(BF).reshape(parts, 1, span, width)

        @pl.when(step == blocks - 1)
        def _():
            column = jnp.transpose(acc_ref[...])
            gain_ref[...] = jnp.broadcast_to(column[:, :1], gain_ref.shape)

    block = pl.BlockSpec((height, group), lambda i: (i, 0))
    return call(
        body,
        (blocks,),
        [
            block,
            block,
            block,
            whole(weight.shape),
            pl.BlockSpec((parts, 1, span, width), lambda i: (0, i, 0, 0)),
        ],
        [
            pl.BlockSpec((parts, 1, span, width), lambda i: (0, i, 0, 0)),
            whole((width, 128)),
        ],
        [sds((parts, blocks, span, width), BF), sds((width, 128), F32)],
        (*grads, weight, rows),
        scratch=[pltpu.VMEM((8, width), F32)],
        flops=6 * length * width * group,
    )


def attend(qkv, seg_row, seg_col):
    length, cols = qkv.shape
    group = cols // 3
    pairs = group // 128
    high = min(256, length)

    def body(q_ref, k_ref, v_ref, sr_ref, sc_ref, o_ref, l_ref):
        lane = lax.broadcasted_iota(jnp.int32, (high, 128), 1)
        for at in range(0, length, high):
            end = at + high
            query = q_ref[at:end, :]
            keys = k_ref[:end, :]
            vals = v_ref[:end, :]
            q_pos = lax.broadcasted_iota(jnp.int32, (high, end), 0) + at
            k_pos = lax.broadcasted_iota(jnp.int32, (high, end), 1)
            allowed = (sc_ref[at:end, :] == sr_ref[:, :end]) & (k_pos <= q_pos)
            outs = []
            for head in range(2):
                mine = (lane // 64) == head
                scores = mm(jnp.where(mine, query, jnp.zeros_like(query)), keys, NT)
                scores = jnp.where(allowed, scores, NEG)
                most = jnp.max(scores, axis=1, keepdims=True)
                expo = jnp.exp(scores - most)
                total = jnp.sum(expo, axis=1, keepdims=True)
                outs.append(mm(expo.astype(BF), vals) / total)
                lse = jnp.broadcast_to(most + jnp.log(total), (high, 128))
                l_ref[0, head : head + 1, at:end] = jnp.transpose(lse)[:1, :]
            o_ref[at:end, :] = jnp.where(lane < 64, outs[0], outs[1]).astype(BF)

    def col(offset):
        return pl.BlockSpec((length, 128), lambda i: (0, offset * pairs + i))

    return call(
        body,
        (pairs,),
        [col(0), col(1), col(2), whole((1, length)), whole((length, 1))],
        [col(0), pl.BlockSpec((1, 2, length), lambda i: (i, 0, 0))],
        [sds((length, group), BF), sds((pairs, 2, length), F32)],
        (qkv, qkv, qkv, seg_row, seg_col),
        flops=4 * length * length * group,
    )


def attend_back(qkv, grad, lse, seg_row, seg_col, cosine, sine):
    length, cols = qkv.shape
    group = cols // 3
    pairs = group // 128
    high = min(256, length)

    def body(
        q_ref, k_ref, v_ref, g_ref, l_ref, sr_ref, sc_ref, c_ref, s_ref, dq_ref, dk_ref, dv_ref,
        ka_ref, va_ref,
    ):
        lane = lax.broadcasted_iota(jnp.int32, (high, 128), 1)
        ka_ref[...] = jnp.zeros_like(ka_ref)
        va_ref[...] = jnp.zeros_like(va_ref)
        for at in range(0, length, high):
            end = at + high
            query = q_ref[at:end, :]
            grads = g_ref[at:end, :]
            keys = k_ref[:end, :]
            vals = v_ref[:end, :]
            k_pos = lax.broadcasted_iota(jnp.int32, (end, high), 0)
            q_pos = lax.broadcasted_iota(jnp.int32, (end, high), 1) + at
            allowed = (sc_ref[:end, :] == sr_ref[:, at:end]) & (k_pos <= q_pos)
            outs = []
            for head in range(2):
                mine = (lane // 64) == head
                q_own = jnp.where(mine, query, jnp.zeros_like(query))
                g_own = jnp.where(mine, grads, jnp.zeros_like(grads))
                scores = jnp.where(allowed, mm(keys, q_own, NT), NEG)
                probs = jnp.exp(scores - l_ref[0, head : head + 1, at:end])
                grad_probs = mm(vals, g_own, NT)
                delta = jnp.sum(probs * grad_probs, axis=0, keepdims=True)
                grad_scores = (probs * (grad_probs - delta)).astype(BF)
                va_ref[:end, :] += mm(probs.astype(BF), g_own)
                ka_ref[:end, :] += mm(grad_scores, q_own)
                outs.append(mm(grad_scores, keys, TN))
            found = jnp.where(lane < 64, outs[0], outs[1]) * HEAD_DIM**-0.5
            back = found * c_ref[at:end, :] - swap_halves(found) * s_ref[at:end, :]
            dq_ref[at:end, :] = back.astype(BF)
        found = ka_ref[...]
        dk_ref[...] = (found * c_ref[...] - swap_halves(found) * s_ref[...]).astype(BF)
        dv_ref[...] = va_ref[...].astype(BF)

    def col(offset):
        return pl.BlockSpec((length, 128), lambda i: (0, offset * pairs + i))

    return call(
        body,
        (pairs,),
        [
            col(0),
            col(1),
            col(2),
            col(0),
            pl.BlockSpec((1, 2, length), lambda i: (i, 0, 0)),
            whole((1, length)),
            whole((length, 1)),
            whole((length, 128)),
            whole((length, 128)),
        ],
        [col(0), col(0), col(0)],
        [sds((length, group), BF)] * 3,
        (qkv, qkv, qkv, grad, lse, seg_row, seg_col, cosine, sine),
        scratch=[pltpu.VMEM((length, 128), F32)] * 2,
        flops=10 * length * length * group,
    )


def heads_of(flat):
    return flat.reshape(flat.shape[0], -1, HEAD_DIM)


def plain_mask(seg_row, seg_col):
    length = seg_col.shape[0]
    spots = jnp.arange(length, dtype=jnp.int32)
    return (seg_row == seg_col) & (spots[None, :] <= spots[:, None])


def plain_attend(qkv, seg_row, seg_col):
    query, keys, vals = (heads_of(part) for part in jnp.split(qkv, 3, axis=1))
    scores = jnp.einsum("qhd,khd->hqk", query, keys, preferred_element_type=F32)
    scores = jnp.where(plain_mask(seg_row, seg_col)[None], scores, NEG)
    lse = jax.nn.logsumexp(scores, axis=-1, keepdims=True)
    probs = jnp.exp(scores - lse).astype(BF)
    found = jnp.einsum("hqk,khd->qhd", probs, vals, preferred_element_type=F32)
    return found.astype(BF).reshape(qkv.shape[0], -1), lse


def plain_turn_back(grads, cosine, sine):
    table_c, table_s = cosine[:, None, :HEAD_DIM], sine[:, None, :HEAD_DIM]
    swapped = jnp.roll(grads, HEAD_DIM // 2, axis=-1)
    return (grads * table_c - swapped * table_s).astype(BF).reshape(grads.shape[0], -1)


def plain_attend_back(qkv, grad, lse, seg_row, seg_col, cosine, sine):
    query, keys, vals = (heads_of(part) for part in jnp.split(qkv, 3, axis=1))
    grad = heads_of(grad)
    scores = jnp.einsum("qhd,khd->hqk", query, keys, preferred_element_type=F32)
    scores = jnp.where(plain_mask(seg_row, seg_col)[None], scores, NEG)
    probs = jnp.exp(scores - lse)
    grad_probs = jnp.einsum("qhd,khd->hqk", grad, vals, preferred_element_type=F32)
    delta = jnp.sum(probs * grad_probs, axis=-1, keepdims=True)
    grad_scores = (probs * (grad_probs - delta)).astype(BF)
    gq = jnp.einsum("hqk,khd->qhd", grad_scores, keys, preferred_element_type=F32)
    gk = jnp.einsum("hqk,qhd->khd", grad_scores, query, preferred_element_type=F32)
    gv = jnp.einsum("hqk,qhd->khd", probs.astype(BF), grad, preferred_element_type=F32)
    return (
        plain_turn_back(gq * HEAD_DIM**-0.5, cosine, sine),
        plain_turn_back(gk, cosine, sine),
        gv.astype(BF).reshape(qkv.shape[0], -1),
    )


def after_attention(tokens, attended, w_out, gain):
    seqs, parts, span, group = attended.shape
    count, width = tokens.shape

    def body(t_ref, a_ref, w_ref, g_ref, h_ref, b_ref):
        hidden = t_ref[...].astype(F32)
        for part in range(parts):
            rows = a_ref[:, part].reshape(count, group)
            hidden += mm(rows, w_ref[part * group : (part + 1) * group, :])
        h_ref[...] = hidden
        b_ref[...] = (hidden * rms(hidden) * g_ref[...]).astype(BF)

    return call(
        body,
        (1,),
        [whole(a.shape) for a in (tokens, attended, w_out, gain)],
        [whole(tokens.shape)] * 2,
        [sds(tokens.shape, F32), sds(tokens.shape, BF)],
        (tokens, attended, w_out, gain),
        flops=2 * count * width * width,
    )


def dispatch(rows, target_rows, experts, capacity):
    count, width = rows.shape

    def body(r_ref, t_ref, o_ref):
        slot = lax.broadcasted_iota(jnp.int32, (capacity, count), 0)
        slot += pl.program_id(0) * capacity
        hit = (slot == t_ref[0:1, :]) | (slot == t_ref[1:2, :])
        o_ref[0] = mm(hit.astype(F32).astype(BF), r_ref[...]).astype(BF)

    return call(
        body,
        (experts,),
        [whole(rows.shape), whole(target_rows.shape)],
        pl.BlockSpec((1, capacity, width), lambda i: (i, 0, 0)),
        sds((experts, capacity, width), BF),
        (rows, target_rows),
        flops=2 * experts * capacity * count * width,
    )


def pick(target, rows):
    spot = lax.broadcasted_iota(jnp.int32, (target.shape[0], rows.shape[0]), 1)
    hit = (spot == target[:, 0:1]) | (spot == target[:, 1:2])
    return mm(hit.astype(F32).astype(BF), rows)


def layer_end(hidden, shared_out, rows, target):
    count, width = hidden.shape
    high = count // 2

    def body(h_ref, s_ref, r_ref, t_ref, o_ref):
        o_ref[...] = (h_ref[...] + s_ref[...] + pick(t_ref[...], r_ref[...])).astype(BF)

    block = pl.BlockSpec((high, width), lambda i: (i, 0))
    return call(
        body,
        (2,),
        [block, block, whole(rows.shape), pl.BlockSpec((high, 2), lambda i: (i, 0))],
        block,
        sds(hidden.shape, BF),
        (hidden, shared_out, rows, target),
        flops=2 * count * width * rows.shape[0],
    )


def middle_back(hidden, grad_shared, rows, target, cotangent, gain, w_out, parts, span):
    count, width = hidden.shape
    seqs = count // span
    each = 2 if seqs % 2 == 0 else 1
    high = each * span
    steps = count // high
    group = width // parts

    def body(h_ref, s_ref, r_ref, t_ref, c_ref, g_ref, w_ref, gh_ref, ga_ref, d_ref, n_ref, acc_ref):
        step = pl.program_id(0)
        branch = s_ref[...] + pick(t_ref[...], r_ref[...])
        hidden = h_ref[...]
        scale = rms(hidden)
        weighted = branch * g_ref[...]
        inner = jnp.mean(weighted * hidden, axis=1, keepdims=True)
        part = jnp.sum(branch * hidden * scale, axis=0, keepdims=True)
        out = c_ref[...].astype(F32) + scale * weighted - hidden * (scale * scale * scale * inner)
        gh_ref[...] = out
        out = out.astype(BF)
        ga_ref[...] = out
        for at in range(parts):
            sent = mm(out, w_ref[at * group : (at + 1) * group, :], NT).astype(BF)
            d_ref[:, at] = sent.reshape(each, span, group)

        @pl.when(step == 0)
        def _():
            acc_ref[...] = jnp.zeros_like(acc_ref)

        acc_ref[...] += jnp.broadcast_to(part, acc_ref.shape)

        @pl.when(step == steps - 1)
        def _():
            column = jnp.transpose(acc_ref[...])
            n_ref[...] = jnp.broadcast_to(column[:, :1], n_ref.shape)

    block = pl.BlockSpec((high, width), lambda i: (i, 0))
    return call(
        body,
        (steps,),
        [
            block,
            block,
            whole(rows.shape),
            pl.BlockSpec((high, 2), lambda i: (i, 0)),
            block,
            whole(gain.shape),
            whole(w_out.shape),
        ],
        [
            block,
            block,
            pl.BlockSpec((each, parts, span, group), lambda i: (i, 0, 0, 0)),
            whole((width, 128)),
        ],
        [
            sds(hidden.shape, F32),
            sds(hidden.shape, BF),
            sds((seqs, parts, span, group), BF),
            sds((width, 128), F32),
        ],
        (hidden, grad_shared, rows, target, cotangent, gain, w_out),
        scratch=[pltpu.VMEM((8, width), F32)],
        flops=2 * count * width * (rows.shape[0] + width),
    )


def first_norm_back(tokens, gain, grad_normed, grad_hidden):
    count, width = tokens.shape
    high = count // 2

    def body(t_ref, g_ref, n_ref, h_ref, o_ref):
        tok = t_ref[...].astype(F32)
        scale = rms(tok)
        weighted = n_ref[...].astype(F32) * g_ref[...]
        inner = jnp.mean(weighted * tok, axis=1, keepdims=True)
        out = h_ref[...] + scale * weighted - tok * (scale * scale * scale * inner)
        o_ref[...] = out.astype(BF)

    block = pl.BlockSpec((high, width), lambda i: (i, 0))
    return call(
        body,
        (2,),
        [block, whole(gain.shape), block, block],
        block,
        sds(tokens.shape, BF),
        (tokens, gain, grad_normed, grad_hidden),
    )


def feed_forward(rows, grads, w_gate, w_up, w_down, router=None, other=None, own=None):
    count, width = rows.shape
    units = w_gate.shape[1]
    wide = 512
    steps = units // wide
    high = 256
    gated = router is not None
    kind = BF if gated else F32

    def body(*refs):
        if gated:
            (own_ref, x_ref, g_ref, wg_ref, wu_ref, wd_ref, wr_ref, ot_ref,
             y_ref, gi_ref, hid_ref, dg_ref, du_ref, eo_ref, gl_ref, ya_ref, ga_ref, gate_ref) = refs
        else:
            (x_ref, g_ref, wg_ref, wu_ref, wd_ref,
             y_ref, gi_ref, hid_ref, dg_ref, du_ref, ya_ref, ga_ref) = refs
        step = pl.program_id(0)

        if gated:

            @pl.when(step == 0)
            def _():
                logits = mm(x_ref[...], wr_ref[...])
                lane = lax.broadcasted_iota(jnp.int32, logits.shape, 1)
                mine = jnp.sum(jnp.where(lane == own_ref[0], logits, 0.0), axis=1, keepdims=True)
                theirs = jnp.sum(jnp.where(lane == ot_ref[...], logits, 0.0), axis=1, keepdims=True)
                gate = 1.0 / (1.0 + jnp.exp(theirs - mine))
                rest = 1.0 / (1.0 + jnp.exp(mine - theirs))
                gate_ref[:, 0:1] = gate
                gate_ref[:, 1:2] = rest
                eo_ref[...] = (g_ref[...].astype(F32) * gate).astype(BF)

        def rows_at(index, carry):
            at = pl.ds(pl.multiple_of(index * high, high), high)
            row = x_ref[at, :]
            grad = eo_ref[at, :] if gated else g_ref[at, :]
            gval = mm(row, wg_ref[...])
            uval = mm(row, wu_ref[...])
            sigma = 1.0 / (1.0 + jnp.exp(-gval))
            silu = gval * sigma
            hid = (silu * uval).astype(BF)
            hid_ref[at, :] = hid
            grad_hid = mm(grad, wd_ref[...], NT)
            du = (grad_hid * silu).astype(BF)
            dg = (grad_hid * uval * sigma * (1.0 + gval * (1.0 - sigma))).astype(BF)
            du_ref[at, :] = du
            dg_ref[at, :] = dg
            out = mm(hid, wd_ref[...])
            back = mm(dg, wg_ref[...], NT) + mm(du, wu_ref[...], NT)

            @pl.when(step == 0)
            def _():
                ya_ref[at, :] = out
                ga_ref[at, :] = back

            @pl.when(step > 0)
            def _():
                ya_ref[at, :] += out
                ga_ref[at, :] += back

            return carry

        lax.fori_loop(0, count // high, rows_at, 0)

        @pl.when(step == steps - 1)
        def _():
            if gated:
                out = ya_ref[...]
                gate = gate_ref[:, 0:1]
                lean = jnp.sum(out * g_ref[...].astype(F32), axis=1, keepdims=True)
                lean = lean * gate * gate_ref[:, 1:2]
                lane = lax.broadcasted_iota(jnp.int32, (count, 128), 1)
                sign = (lane == own_ref[0]).astype(F32) - (lane == ot_ref[...]).astype(F32)
                grad_logits = (lean * sign).astype(BF)
                gl_ref[...] = grad_logits
                y_ref[...] = (out * gate).astype(BF)
                gi_ref[...] = (ga_ref[...] + mm(grad_logits, wr_ref[...], NT)).astype(BF)
            else:
                y_ref[...] = ya_ref[...]
                gi_ref[...] = ga_ref[...]

    full = whole((count, width))
    hidden = pl.BlockSpec((count, wide), lambda i, *_: (0, i))
    in_specs = [
        full,
        full,
        pl.BlockSpec((width, wide), lambda i, *_: (0, i)),
        pl.BlockSpec((width, wide), lambda i, *_: (0, i)),
        pl.BlockSpec((wide, width), lambda i, *_: (i, 0)),
    ]
    out_specs = [full, full, hidden, hidden, hidden]
    out_shape = [sds((count, width), kind)] * 2 + [sds((count, units), BF)] * 3
    scratch = [pltpu.VMEM((count, width), F32)] * 2
    args = [rows, grads, w_gate, w_up, w_down]
    if gated:
        in_specs += [whole(router.shape), whole(other.shape)]
        out_specs += [full, whole((count, 128))]
        out_shape += [sds((count, width), BF), sds((count, 128), BF)]
        scratch += [pltpu.VMEM((count, 128), F32)]
        args = [own, *args, router, other]
    return call(
        body,
        (steps,),
        in_specs,
        out_specs,
        out_shape,
        tuple(args),
        scratch=scratch,
        prefetch=1 if gated else 0,
        flops=12 * count * width * units,
    )


def expert_weight_grads(rows, grads, dg, du, hid, grad_logits, sizes):
    outer, cores = sizes["y"], sizes["core"]
    count, width = rows.shape
    units = dg.shape[1]
    wide = units // (outer * cores)

    def body(x_ref, g_ref, dg_ref, du_ref, hid_ref, gl_ref, o_ref, r_ref):
        o_ref[0, 0, 0] = mm(x_ref[...], dg_ref[...], TN).astype(BF)
        o_ref[0, 0, 1] = mm(x_ref[...], du_ref[...], TN).astype(BF)
        o_ref[0, 0, 2] = mm(g_ref[...], hid_ref[...], TN).astype(BF)

        @pl.when(pl.program_id(0) == 0)
        def _():
            r_ref[...] = mm(x_ref[...], gl_ref[...], TN)

    hidden = pl.BlockSpec((count, wide), lambda i: (0, i))
    return call(
        body,
        (outer * cores,),
        [whole(rows.shape), whole(grads.shape), hidden, hidden, hidden, whole(grad_logits.shape)],
        [
            pl.BlockSpec((1, 1, 3, width, wide), lambda i: (i % cores, i // cores, 0, 0, 0)),
            whole((width, 128)),
        ],
        [sds((cores, outer, 3, width, wide), BF), sds((width, 128), F32)],
        (rows, grads, dg, du, hid, grad_logits),
        flops=6 * count * width * units,
    )


def spread(value, sizes, names):
    order = ("y", "core", "z", "x")
    split = value.reshape(*(sizes[n] for n in order), -1, value.shape[-1])
    return jnp.transpose(split, (*(order.index(n) for n in names), 4, 5))


def spread_places(sizes, names):
    found = []
    for y in range(sizes["y"]):
        for core in range(sizes["core"]):
            for z in range(sizes["z"]):
                for x in range(sizes["x"]):
                    at = {"y": y, "core": core, "z": z, "x": x}
                    found.append(tuple(at[n] for n in names))
    return found


def spread_shape(sizes, names):
    return tuple(sizes[n] for n in names)


def shared_weight_grads(rows, grads, dg, du, hid, sizes):
    names = ("core", "y", "x", "z")
    lead = spread_shape(sizes, names)
    places = spread_places(sizes, names)
    count, width = rows.shape
    units = dg.shape[1]
    wide = 512
    each = width // len(places)
    direct = each % 8 == 0

    def body(x_ref, g_ref, dg_ref, du_ref, hid_ref, o_ref):
        pairs = ((x_ref, dg_ref), (x_ref, du_ref), (g_ref, hid_ref))
        for index, (left, right) in enumerate(pairs):
            found = mm(left[...], right[...], TN)
            if direct:
                for at, place in enumerate(places):
                    o_ref[(*place, index)] = found[at * each : (at + 1) * each].astype(BF)
            else:
                o_ref[index] = found.astype(BF)

    hidden = pl.BlockSpec((count, wide), lambda i: (0, i))
    if direct:
        shape = (*lead, 3, each, units)
        spec = pl.BlockSpec((*lead, 3, each, wide), lambda i: (0,) * 6 + (i,))
    else:
        shape = (3, width, units)
        spec = pl.BlockSpec((3, width, wide), lambda i: (0, 0, i))
    out = call(
        body,
        (units // wide,),
        [whole(rows.shape), whole(grads.shape), hidden, hidden, hidden],
        spec,
        sds(shape, BF),
        (rows, grads, dg, du, hid),
        flops=6 * count * width * units,
    )
    if direct:
        return out
    return jnp.stack([spread(out[i], sizes, names) for i in range(3)], axis=4)


def tall_weight_grads(lefts, rights, extras, sizes, names):
    lead = spread_shape(sizes, names)
    places = spread_places(sizes, names)
    width = sum(left.shape[1] for left in lefts)
    cols = sum(right.shape[1] for right in rights)
    each = width // len(places)
    direct = each % 8 == 0
    flops = 2 * lefts[0].shape[0] * width * cols

    def body(*refs):
        left_refs = refs[: len(lefts)]
        right_refs = refs[len(lefts) : len(lefts) + len(rights)]
        extra_refs = refs[len(lefts) + len(rights) : -1]
        out_ref = refs[-1]

        def store(row, found, col):
            span = found.shape[1]
            if not direct:
                out_ref[row : row + found.shape[0], col : col + span] = found.astype(BF)
                return
            for at in range(found.shape[0] // each):
                place = places[row // each + at]
                piece = found[at * each : (at + 1) * each].astype(BF)
                out_ref[(*place, slice(None), slice(col, col + span))] = piece

        row = 0
        for left in left_refs:
            col = 0
            for right in right_refs:
                store(row, mm(left[...], right[...], TN), col)
                col += right.shape[1]
            row += left.shape[1]
        more = extra_refs[0][...]
        for extra in extra_refs[1:]:
            more = more + extra[...]
        store(0, more, cols)

    args = (*lefts, *rights, *extras)
    shape = (*lead, each, cols + 128) if direct else (width, cols + 128)
    out = call(
        body,
        (1,),
        [whole(a.shape) for a in args],
        whole(shape),
        sds(shape, BF),
        args,
        flops=flops,
    )
    return out if direct else spread(out, sizes, names)


def scatter_sum(value, name):
    return lax.psum_scatter(value, name, scatter_dimension=0, tiled=False)


def swap_all(value, names):
    return lax.all_to_all(value, names, 0, 0, tiled=True)


def on_device(
    tokens,
    segments,
    routes,
    slots,
    cotangent,
    attn_gain,
    w_qkv,
    w_out,
    ffn_gain,
    w_router,
    shared_gate,
    shared_up,
    shared_down,
    expert_gate,
    expert_up,
    expert_down,
):
    sizes = {name: lax.axis_size(name) for name in ("y", "core", "z", "x")}
    ranks = ("z", "x")
    seqs, span, width = tokens.shape
    blocks, parts = sizes["z"], sizes["x"]
    experts = blocks * parts
    count = seqs * span
    capacity = 3 * count // experts
    length = span * experts
    group = width // parts
    z_at, x_at = lax.axis_index("z"), lax.axis_index("x")
    own = (z_at * parts + x_at).astype(jnp.int32).reshape(1)
    attn_scale = attn_gain.astype(F32).reshape(1, width)
    ffn_scale = ffn_gain.astype(F32).reshape(1, width)
    flat_tokens = tokens.reshape(count, width)
    flat_cot = cotangent.reshape(count, width)

    by_seq = swap_all(tokens, "z")
    if parts == 2:
        theirs = lax.ppermute(by_seq, "x", [(0, 1), (1, 0)])
        first = x_at == 0
        rows = jnp.stack([jnp.where(first, by_seq, theirs), jnp.where(first, theirs, by_seq)])
    else:
        rows = lax.all_gather(by_seq, "x", axis=0, tiled=False)

    route_rows = routes.reshape(count, 2)
    slot_rows = slots.reshape(count, 2)
    target = jnp.where(slot_rows >= 0, route_rows * capacity + slot_rows, -1)
    target_rows = jnp.transpose(target)
    grad_sent = dispatch(flat_cot, target_rows, experts, capacity)
    spots = jnp.where(target >= 0, target, experts * capacity).reshape(-1)
    other = (
        jnp.zeros((experts * capacity,), F32)
        .at[spots]
        .set(route_rows[:, ::-1].reshape(-1).astype(F32), mode="drop")
    )
    other = swap_all(other.reshape(experts, capacity), ranks)
    other = other.reshape(-1, 1).astype(jnp.int32)
    grad_rows = swap_all(grad_sent, ranks).reshape(-1, width)

    frequency = jnp.power(10000.0, -2.0 * jnp.arange(32, dtype=F32) / HEAD_DIM)
    angles = jnp.arange(length, dtype=jnp.int32).astype(F32)[:, None] * jnp.tile(frequency, 4)
    sign = jnp.where(jnp.arange(128) % 64 < 32, -1.0, 1.0)
    cosine, sine = jnp.cos(angles), jnp.sin(angles) * sign
    w_group = lax.dynamic_index_in_dim(
        w_qkv.reshape(width, 3, parts, group), x_at, 2, keepdims=False
    ).reshape(width, 3 * group)
    seg_row = lax.dynamic_slice_in_dim(segments, z_at, 1, 0)
    seg_col = seg_row.reshape(length, 1)
    qkv, normed = project(rows, attn_scale, w_group, cosine, sine)
    fused = group % 128 == 0
    attended, lse = (attend if fused else plain_attend)(qkv, seg_row, seg_col)
    attended = swap_all(attended.reshape(experts, span, group), ranks)
    attended = attended.reshape(seqs, parts, span, group)

    hidden, branch_in = after_attention(flat_tokens, attended, w_out, ffn_scale)
    sent = dispatch(branch_in, target_rows, experts, capacity)
    received = swap_all(sent, ranks).reshape(-1, width)

    shared_out, shared_back, hid, dg, du = feed_forward(
        branch_in, flat_cot, shared_gate, shared_up, shared_down
    )
    shared_sums = shared_weight_grads(branch_in, flat_cot, dg, du, hid, sizes)
    for name in ("core", "y", "x", "z"):
        shared_sums = scatter_sum(shared_sums, name)

    router = jnp.pad(w_router, ((0, 0), (0, 128 - experts)))
    made, made_back, hid, dg, du, gated_grads, grad_logits = feed_forward(
        received, grad_rows, expert_gate[0], expert_up[0], expert_down[0], router, other, own
    )
    back_rows = swap_all(made_back.reshape(experts, capacity, width), ranks).reshape(-1, width)
    made_rows = swap_all(made.reshape(experts, capacity, width), ranks).reshape(-1, width)
    expert_sums, grad_router = expert_weight_grads(
        received, gated_grads, dg, du, hid, grad_logits, sizes
    )
    for name in ("core", "y"):
        expert_sums = scatter_sum(expert_sums, name)
    layer_out = layer_end(hidden, shared_out, made_rows, target).reshape(tokens.shape)

    grad_hidden, grad_attn, grad_att, grad_ffn = middle_back(
        hidden, shared_back, back_rows, target, flat_cot, ffn_scale, w_out, parts, span
    )
    grad_att = swap_all(grad_att.reshape(experts, span, group), ranks).reshape(length, group)

    column = lax.broadcasted_iota(jnp.int32, (width, 128), 1)
    small = jnp.where(column < experts, grad_router, jnp.where(column == experts, grad_ffn, 0.0))
    out_sums = tall_weight_grads(
        [attended[:, part].reshape(count, group) for part in range(parts)],
        [grad_attn],
        [small],
        sizes,
        ("core", "y", "x", "z"),
    )
    for name in ("core", "y", "x", "z"):
        out_sums = scatter_sum(out_sums, name)

    grads = (attend_back if fused else plain_attend_back)(
        qkv, grad_att, lse, seg_row, seg_col, cosine, sine
    )
    normed_back, grad_gain = project_back(grads, w_group, rows, attn_scale)
    if parts == 2:
        keep = lax.dynamic_index_in_dim(normed_back, x_at, 0, keepdims=False)
        give = lax.dynamic_index_in_dim(normed_back, 1 - x_at, 0, keepdims=False)
        got = lax.ppermute(give, "x", [(0, 1), (1, 0)])
        normed_back = (keep.astype(F32) + got.astype(F32)).astype(BF)
    else:
        normed_back = scatter_sum(normed_back, "x")
    normed_back = swap_all(normed_back, "z").reshape(count, width)
    token_grad = first_norm_back(flat_tokens, attn_scale, normed_back, grad_hidden)

    qkv_sums = tall_weight_grads([normed], list(grads), [grad_gain], sizes, ("core", "y", "z", "x"))
    for name in ("core", "y", "z"):
        qkv_sums = scatter_sum(qkv_sums, name)
    qkv_sums = swap_all(qkv_sums, "x").astype(F32)
    grad_attn_gain = jnp.sum(qkv_sums[:, :, 3 * group], axis=0)
    each = qkv_sums.shape[1]
    grad_w_qkv = qkv_sums[:, :, : 3 * group].reshape(parts, each, 3, group)
    grad_w_qkv = jnp.transpose(grad_w_qkv, (1, 2, 0, 3)).reshape(each, 3 * width)

    out_sums = out_sums.astype(F32)
    shared_sums = shared_sums.astype(F32)
    expert_sums = expert_sums.astype(F32)
    return (
        layer_out,
        token_grad.reshape(tokens.shape),
        grad_attn_gain,
        grad_w_qkv,
        out_sums[:, :width],
        out_sums[:, width + experts],
        out_sums[:, width : width + experts],
        shared_sums[0],
        shared_sums[1],
        jnp.transpose(shared_sums[2]),
        expert_sums[0][None],
        expert_sums[1][None],
        jnp.transpose(expert_sums[2])[None],
    )


def solution(mesh):
    dp, experts = mesh.shape["dp"], mesh.shape["expert"]

    def step(*args):
        seqs = args[0].shape[0] // dp
        cores = 2 if dp % 2 == 0 else 1
        fine = Mesh(
            mesh.devices.reshape(dp // cores, cores, seqs, experts // seqs),
            ("y", "core", "z", "x"),
        )
        data, ranks, every = ("y", "core"), ("z", "x"), ("y", "core", "z", "x")
        placed = (
            P(data, ranks, None),
            P(data, None),
            P(data, ranks, None),
            P(data, ranks, None),
            P(data, ranks, None),
            *([P()] * 8),
            P(ranks, None, None),
            P(ranks, None, None),
            P(ranks, None, None),
        )
        return jax.shard_map(
            on_device,
            mesh=fine,
            in_specs=placed,
            out_specs=(
                P(data, ranks, None),
                P(data, ranks, None),
                P(every),
                P(every, None),
                P(every, None),
                P(every),
                P(every, None),
                P(every, None),
                P(every, None),
                P(None, every),
                P(ranks, None, data),
                P(ranks, None, data),
                P(ranks, data, None),
            ),
            check_vma=False,
        )(*args)

    return step
```

```python
import jax
import jax.numpy as jnp
from jax import lax
from jax.experimental import pallas as pl
from jax.experimental.pallas import tpu as pltpu
from jax.sharding import Mesh
from jax.sharding import PartitionSpec as P

HEAD_DIM = 64
EPS = 1e-06
BF = jnp.bfloat16
F32 = jnp.float32
NEG = -1e30
NN = (((1,), (0,)), ((), ()))
NT = (((1,), (1,)), ((), ()))
TN = (((0,), (0,)), ((), ()))
VMEM_MOST = 60 << 20


def mm(left, right, dims=NN):
    return lax.dot_general(left, right, dims, preferred_element_type=F32)


def sds(shape, dtype):
    return jax.ShapeDtypeStruct(shape, dtype)


def call(body, grid, in_specs, out_specs, out_shape, args, scratch=(), prefetch=0, flops=0):
    leaves = jax.tree.leaves(out_shape)
    moved = sum(a.size * a.dtype.itemsize for a in args) + sum(
        a.size * a.dtype.itemsize for a in leaves
    )
    return pl.pallas_call(
        body,
        out_shape=out_shape,
        grid_spec=pltpu.PrefetchScalarGridSpec(
            num_scalar_prefetch=prefetch,
            grid=grid,
            in_specs=in_specs,
            out_specs=out_specs,
            scratch_shapes=list(scratch),
        ),
        compiler_params=pltpu.CompilerParams(
            dimension_semantics=("arbitrary",) * len(grid), vmem_limit_bytes=VMEM_MOST
        ),
        cost_estimate=pl.CostEstimate(
            flops=int(flops), transcendentals=0, bytes_accessed=int(moved)
        ),
    )(*args)


def whole(shape):
    rank = len(shape)
    return pl.BlockSpec(tuple(shape), lambda *_: (0,) * rank)


def swap_halves(value):
    lane = lax.broadcasted_iota(jnp.int32, value.shape, 1)
    return jnp.where(lane % 64 < 32, pltpu.roll(value, 96, 1), pltpu.roll(value, 32, 1))


def rms(values):
    return lax.rsqrt(jnp.mean(values * values, axis=1, keepdims=True) + EPS)


def row_specs(rows):
    if len(rows) == 2:
        _, span, width = rows[0].shape
        return [pl.BlockSpec((1, span, width), lambda i, *_: (i, 0, 0))] * 2
    parts, _, span, width = rows[0].shape
    return [pl.BlockSpec((parts, 1, span, width), lambda i, *_: (0, i, 0, 0))]


def load_rows(refs, at_ref):
    if len(refs) == 2:
        mine, theirs = refs[0][0].astype(F32), refs[1][0].astype(F32)
        first = at_ref[0] == 0
        pair = [jnp.where(first, mine, theirs), jnp.where(first, theirs, mine)]
        return jnp.concatenate(pair, axis=0)
    value = refs[0][...]
    return value.reshape(value.shape[0] * value.shape[2], value.shape[3]).astype(F32)


def weight_specs(weights, group):
    if len(weights) == 1:
        return [whole(weights[0].shape)]
    width, cols = weights[0].shape
    parts = cols // (3 * group)

    def spec(index):
        return pl.BlockSpec((width, group), lambda i, at: (0, index * parts + at[0]))

    return [spec(index) for index in range(3)]


def load_weights(refs, group):
    if len(refs) == 3:
        return [ref[...] for ref in refs]
    return [refs[0][:, at * group : (at + 1) * group] for at in range(3)]


def project(rows, gain, weights, group, cosine, sine, x_at, parts):
    blocks, span, width = rows[0].shape[-3:]
    height = parts * span
    length = height * blocks
    cut = len(rows)

    def body(at_ref, *refs):
        r_refs, (g_ref, c_ref, s_ref) = refs[:cut], refs[cut : cut + 3]
        w_refs, (qkv_ref, n_ref) = refs[cut + 3 : -2], refs[-2:]
        tok = load_rows(r_refs, at_ref)
        normed = (tok * rms(tok) * g_ref[...]).astype(BF)
        n_ref[...] = normed
        if len(w_refs) == 3:
            found = [mm(normed, ref[...]) for ref in w_refs]
            turning = [(found[0], 0), (found[1], group)]
            last = found[2]
        else:
            found = mm(normed, w_refs[0][...])
            turning, last = [(found[:, : 2 * group], 0)], found[:, 2 * group :]
        for value, base in turning:
            for at in range(0, value.shape[1], 128):
                part = value[:, at : at + 128]
                lane = lax.broadcasted_iota(jnp.int32, part.shape, 1) + (base + at)
                turned = part * c_ref[...] + swap_halves(part) * s_ref[...]
                turned = turned * jnp.where(lane < group, HEAD_DIM**-0.5, 1.0)
                qkv_ref[:, base + at : base + at + 128] = turned.astype(BF)
        qkv_ref[:, 2 * group :] = last.astype(BF)

    return call(
        body,
        (blocks,),
        [
            *row_specs(rows),
            whole((1, width)),
            pl.BlockSpec((height, 128), lambda i, *_: (i, 0)),
            pl.BlockSpec((height, 128), lambda i, *_: (i, 0)),
            *weight_specs(weights, group),
        ],
        [
            pl.BlockSpec((height, 3 * group), lambda i, *_: (i, 0)),
            pl.BlockSpec((height, width), lambda i, *_: (i, 0)),
        ],
        [sds((length, 3 * group), BF), sds((length, width), BF)],
        (x_at, *rows, gain, cosine, sine, *weights),
        prefetch=1,
        flops=6 * length * width * group,
    )


def project_back(grads, weights, rows, x_at, parts):
    blocks, span, width = rows[0].shape[-3:]
    group = grads[0].shape[1]
    height = parts * span
    length = height * blocks
    cut = len(rows)

    def body(at_ref, q_ref, k_ref, v_ref, *refs):
        r_refs, w_refs, (out_ref, gain_ref, acc_ref) = refs[:cut], refs[cut:-3], refs[-3:]
        step = pl.program_id(0)
        w_q, w_k, w_v = load_weights(w_refs, group)
        back = mm(q_ref[...], w_q, NT) + mm(k_ref[...], w_k, NT) + mm(v_ref[...], w_v, NT)
        tok = load_rows(r_refs, at_ref)
        part = jnp.sum(back * tok * rms(tok), axis=0, keepdims=True)

        @pl.when(step == 0)
        def _():
            acc_ref[...] = jnp.zeros_like(acc_ref)

        acc_ref[...] += jnp.broadcast_to(part, acc_ref.shape)
        out_ref[...] = back.astype(BF).reshape(parts, 1, span, width)

        @pl.when(step == blocks - 1)
        def _():
            column = jnp.transpose(acc_ref[...])
            gain_ref[...] = jnp.broadcast_to(column[:, :1], gain_ref.shape)

    block = pl.BlockSpec((height, group), lambda i, *_: (i, 0))
    return call(
        body,
        (blocks,),
        [block, block, block, *row_specs(rows), *weight_specs(weights, group)],
        [
            pl.BlockSpec((parts, 1, span, width), lambda i, *_: (0, i, 0, 0)),
            whole((width, 128)),
        ],
        [sds((parts, blocks, span, width), BF), sds((width, 128), F32)],
        (x_at, *grads, *rows, *weights),
        scratch=[pltpu.VMEM((8, width), F32)],
        prefetch=1,
        flops=6 * length * width * group,
    )


def attend(qkv, seg_row, seg_col):
    length, cols = qkv.shape
    group = cols // 3
    pairs = group // 128
    high = min(256, length)

    def body(q_ref, k_ref, v_ref, sr_ref, sc_ref, o_ref, l_ref):
        lane = lax.broadcasted_iota(jnp.int32, (high, 128), 1)
        for at in range(0, length, high):
            end = at + high
            query = q_ref[at:end, :]
            keys = k_ref[:end, :]
            vals = v_ref[:end, :]
            q_pos = lax.broadcasted_iota(jnp.int32, (high, end), 0) + at
            k_pos = lax.broadcasted_iota(jnp.int32, (high, end), 1)
            allowed = (sc_ref[at:end, :] == sr_ref[:, :end]) & (k_pos <= q_pos)
            outs = []
            for head in range(2):
                mine = (lane // 64) == head
                scores = mm(jnp.where(mine, query, jnp.zeros_like(query)), keys, NT)
                scores = jnp.where(allowed, scores, NEG)
                most = jnp.max(scores, axis=1, keepdims=True)
                expo = jnp.exp(scores - most)
                total = jnp.sum(expo, axis=1, keepdims=True)
                outs.append(mm(expo.astype(BF), vals) / total)
                lse = jnp.broadcast_to(most + jnp.log(total), (high, 128))
                l_ref[0, head : head + 1, at:end] = jnp.transpose(lse)[:1, :]
            o_ref[at:end, :] = jnp.where(lane < 64, outs[0], outs[1]).astype(BF)

    def col(offset):
        return pl.BlockSpec((length, 128), lambda i: (0, offset * pairs + i))

    return call(
        body,
        (pairs,),
        [col(0), col(1), col(2), whole((1, length)), whole((length, 1))],
        [col(0), pl.BlockSpec((1, 2, length), lambda i: (i, 0, 0))],
        [sds((length, group), BF), sds((pairs, 2, length), F32)],
        (qkv, qkv, qkv, seg_row, seg_col),
        flops=4 * length * length * group,
    )


def attend_back(qkv, grad, lse, seg_row, seg_col, cosine, sine):
    length, cols = qkv.shape
    group = cols // 3
    pairs = group // 128
    high = min(256, length)

    def body(
        q_ref, k_ref, v_ref, g_ref, l_ref, sr_ref, sc_ref, c_ref, s_ref, dq_ref, dk_ref, dv_ref,
        ka_ref, va_ref,
    ):
        lane = lax.broadcasted_iota(jnp.int32, (high, 128), 1)
        ka_ref[...] = jnp.zeros_like(ka_ref)
        va_ref[...] = jnp.zeros_like(va_ref)
        for at in range(0, length, high):
            end = at + high
            query = q_ref[at:end, :]
            grads = g_ref[at:end, :]
            keys = k_ref[:end, :]
            vals = v_ref[:end, :]
            k_pos = lax.broadcasted_iota(jnp.int32, (end, high), 0)
            q_pos = lax.broadcasted_iota(jnp.int32, (end, high), 1) + at
            allowed = (sc_ref[:end, :] == sr_ref[:, at:end]) & (k_pos <= q_pos)
            outs = []
            for head in range(2):
                mine = (lane // 64) == head
                q_own = jnp.where(mine, query, jnp.zeros_like(query))
                g_own = jnp.where(mine, grads, jnp.zeros_like(grads))
                scores = jnp.where(allowed, mm(keys, q_own, NT), NEG)
                probs = jnp.exp(scores - l_ref[0, head : head + 1, at:end])
                grad_probs = mm(vals, g_own, NT)
                delta = jnp.sum(probs * grad_probs, axis=0, keepdims=True)
                grad_scores = (probs * (grad_probs - delta)).astype(BF)
                va_ref[:end, :] += mm(probs.astype(BF), g_own)
                ka_ref[:end, :] += mm(grad_scores, q_own)
                outs.append(mm(grad_scores, keys, TN))
            found = jnp.where(lane < 64, outs[0], outs[1]) * HEAD_DIM**-0.5
            back = found * c_ref[at:end, :] - swap_halves(found) * s_ref[at:end, :]
            dq_ref[at:end, :] = back.astype(BF)
        found = ka_ref[...]
        dk_ref[...] = (found * c_ref[...] - swap_halves(found) * s_ref[...]).astype(BF)
        dv_ref[...] = va_ref[...].astype(BF)

    def col(offset):
        return pl.BlockSpec((length, 128), lambda i: (0, offset * pairs + i))

    return call(
        body,
        (pairs,),
        [
            col(0),
            col(1),
            col(2),
            col(0),
            pl.BlockSpec((1, 2, length), lambda i: (i, 0, 0)),
            whole((1, length)),
            whole((length, 1)),
            whole((length, 128)),
            whole((length, 128)),
        ],
        [col(0), col(0), col(0)],
        [sds((length, group), BF)] * 3,
        (qkv, qkv, qkv, grad, lse, seg_row, seg_col, cosine, sine),
        scratch=[pltpu.VMEM((length, 128), F32)] * 2,
        flops=10 * length * length * group,
    )


def heads_of(flat):
    return flat.reshape(flat.shape[0], -1, HEAD_DIM)


def plain_mask(seg_row, seg_col):
    length = seg_col.shape[0]
    spots = jnp.arange(length, dtype=jnp.int32)
    return (seg_row == seg_col) & (spots[None, :] <= spots[:, None])


def plain_attend(qkv, seg_row, seg_col):
    query, keys, vals = (heads_of(part) for part in jnp.split(qkv, 3, axis=1))
    scores = jnp.einsum("qhd,khd->hqk", query, keys, preferred_element_type=F32)
    scores = jnp.where(plain_mask(seg_row, seg_col)[None], scores, NEG)
    lse = jax.nn.logsumexp(scores, axis=-1, keepdims=True)
    probs = jnp.exp(scores - lse).astype(BF)
    found = jnp.einsum("hqk,khd->qhd", probs, vals, preferred_element_type=F32)
    return found.astype(BF).reshape(qkv.shape[0], -1), lse


def plain_turn_back(grads, cosine, sine):
    table_c, table_s = cosine[:, None, :HEAD_DIM], sine[:, None, :HEAD_DIM]
    swapped = jnp.roll(grads, HEAD_DIM // 2, axis=-1)
    return (grads * table_c - swapped * table_s).astype(BF).reshape(grads.shape[0], -1)


def plain_attend_back(qkv, grad, lse, seg_row, seg_col, cosine, sine):
    query, keys, vals = (heads_of(part) for part in jnp.split(qkv, 3, axis=1))
    grad = heads_of(grad)
    scores = jnp.einsum("qhd,khd->hqk", query, keys, preferred_element_type=F32)
    scores = jnp.where(plain_mask(seg_row, seg_col)[None], scores, NEG)
    probs = jnp.exp(scores - lse)
    grad_probs = jnp.einsum("qhd,khd->hqk", grad, vals, preferred_element_type=F32)
    delta = jnp.sum(probs * grad_probs, axis=-1, keepdims=True)
    grad_scores = (probs * (grad_probs - delta)).astype(BF)
    gq = jnp.einsum("hqk,khd->qhd", grad_scores, keys, preferred_element_type=F32)
    gk = jnp.einsum("hqk,qhd->khd", grad_scores, query, preferred_element_type=F32)
    gv = jnp.einsum("hqk,qhd->khd", probs.astype(BF), grad, preferred_element_type=F32)
    return (
        plain_turn_back(gq * HEAD_DIM**-0.5, cosine, sine),
        plain_turn_back(gk, cosine, sine),
        gv.astype(BF).reshape(qkv.shape[0], -1),
    )


def after_attention(tokens, attended, w_out, gain):
    seqs, parts, span, group = attended.shape
    count, width = tokens.shape

    def body(t_ref, a_ref, w_ref, g_ref, h_ref, b_ref):
        hidden = t_ref[...].astype(F32)
        for part in range(parts):
            rows = a_ref[:, part].reshape(count, group)
            hidden += mm(rows, w_ref[part * group : (part + 1) * group, :])
        h_ref[...] = hidden
        b_ref[...] = (hidden * rms(hidden) * g_ref[...]).astype(BF)

    return call(
        body,
        (1,),
        [whole(a.shape) for a in (tokens, attended, w_out, gain)],
        [whole(tokens.shape)] * 2,
        [sds(tokens.shape, F32), sds(tokens.shape, BF)],
        (tokens, attended, w_out, gain),
        flops=2 * count * width * width,
    )


def dispatch(rows, target_rows, experts, capacity, route_rows=None):
    count, width = rows.shape
    more = 0 if route_rows is None else 16
    tables = () if route_rows is None else (route_rows,)

    def body(r_ref, t_ref, *refs):
        o_ref = refs[-1]
        slot = lax.broadcasted_iota(jnp.int32, (capacity, count), 0)
        slot += pl.program_id(0) * capacity
        hits = [slot == t_ref[k : k + 1, :] for k in range(2)]
        hot = (hits[0] | hits[1]).astype(F32).astype(BF)
        o_ref[0, :capacity, :] = mm(hot, r_ref[...]).astype(BF)
        if more:
            o_ref[0, capacity:, :] = jnp.zeros((more, width), BF)
            other = jnp.zeros((8, capacity), F32)
            for k in range(2):
                route = jnp.broadcast_to(refs[0][1 - k : 2 - k, :].astype(F32), (8, count))
                other += mm(route.astype(BF), hits[k].astype(F32).astype(BF), NT)
            o_ref[0, capacity : capacity + 8, :capacity] = other.astype(BF)

    return call(
        body,
        (experts,),
        [whole(a.shape) for a in (rows, target_rows, *tables)],
        pl.BlockSpec((1, capacity + more, width), lambda i: (i, 0, 0)),
        sds((experts, capacity + more, width), BF),
        (rows, target_rows, *tables),
        flops=2 * experts * capacity * count * width,
    )


def pick(target, rows):
    spot = lax.broadcasted_iota(jnp.int32, (target.shape[0], rows.shape[0]), 1)
    hit = (spot == target[:, 0:1]) | (spot == target[:, 1:2])
    return mm(hit.astype(F32).astype(BF), rows)


def layer_end(hidden, shared_out, rows, target):
    count, width = hidden.shape
    high = count // 2

    def body(h_ref, s_ref, r_ref, t_ref, o_ref):
        o_ref[...] = (h_ref[...] + s_ref[...] + pick(t_ref[...], r_ref[...])).astype(BF)

    block = pl.BlockSpec((high, width), lambda i: (i, 0))
    return call(
        body,
        (2,),
        [block, block, whole(rows.shape), pl.BlockSpec((high, 2), lambda i: (i, 0))],
        block,
        sds(hidden.shape, BF),
        (hidden, shared_out, rows, target),
        flops=2 * count * width * rows.shape[0],
    )


def middle_back(hidden, grad_shared, rows, target, cotangent, gain, w_out, parts, span):
    count, width = hidden.shape
    seqs = count // span
    each = 2 if seqs % 2 == 0 else 1
    high = each * span
    steps = count // high
    group = width // parts

    def body(h_ref, s_ref, r_ref, t_ref, c_ref, g_ref, w_ref, gh_ref, ga_ref, d_ref, n_ref, acc_ref):
        step = pl.program_id(0)
        branch = s_ref[...] + pick(t_ref[...], r_ref[...])
        hidden = h_ref[...]
        scale = rms(hidden)
        weighted = branch * g_ref[...]
        inner = jnp.mean(weighted * hidden, axis=1, keepdims=True)
        part = jnp.sum(branch * hidden * scale, axis=0, keepdims=True)
        out = c_ref[...].astype(F32) + scale * weighted - hidden * (scale * scale * scale * inner)
        gh_ref[...] = out
        out = out.astype(BF)
        ga_ref[...] = out
        for at in range(parts):
            sent = mm(out, w_ref[at * group : (at + 1) * group, :], NT).astype(BF)
            d_ref[:, at] = sent.reshape(each, span, group)

        @pl.when(step == 0)
        def _():
            acc_ref[...] = jnp.zeros_like(acc_ref)

        acc_ref[...] += jnp.broadcast_to(part, acc_ref.shape)

        @pl.when(step == steps - 1)
        def _():
            column = jnp.transpose(acc_ref[...])
            n_ref[...] = jnp.broadcast_to(column[:, :1], n_ref.shape)

    block = pl.BlockSpec((high, width), lambda i: (i, 0))
    return call(
        body,
        (steps,),
        [
            block,
            block,
            whole(rows.shape),
            pl.BlockSpec((high, 2), lambda i: (i, 0)),
            block,
            whole(gain.shape),
            whole(w_out.shape),
        ],
        [
            block,
            block,
            pl.BlockSpec((each, parts, span, group), lambda i: (i, 0, 0, 0)),
            whole((width, 128)),
        ],
        [
            sds(hidden.shape, F32),
            sds(hidden.shape, BF),
            sds((seqs, parts, span, group), BF),
            sds((width, 128), F32),
        ],
        (hidden, grad_shared, rows, target, cotangent, gain, w_out),
        scratch=[pltpu.VMEM((8, width), F32)],
        flops=2 * count * width * (rows.shape[0] + width),
    )


def first_norm_back(tokens, gain, pieces, grad_hidden, z_at):
    count, width = tokens.shape
    blocks = len(pieces)
    span = count // blocks

    def body(at_ref, t_ref, g_ref, h_ref, *refs):
        o_ref = refs[-1]
        for index in range(blocks):
            seq = (at_ref[0] + blocks - index) % blocks
            spot = pl.ds(pl.multiple_of(seq * span, span), span)
            tok = t_ref[spot, :].astype(F32)
            scale = rms(tok)
            weighted = refs[index][...].astype(F32) * g_ref[...]
            inner = jnp.mean(weighted * tok, axis=1, keepdims=True)
            out = h_ref[spot, :] + scale * weighted - tok * (scale * scale * scale * inner)
            o_ref[spot, :] = out.astype(BF)

    return call(
        body,
        (1,),
        [whole(a.shape) for a in (tokens, gain, grad_hidden, *pieces)],
        whole(tokens.shape),
        sds(tokens.shape, BF),
        (z_at, tokens, gain, grad_hidden, *pieces),
        prefetch=1,
    )


def feed_forward(rows, grads, w_gate, w_up, w_down, router=None, other=None, own=None):
    count, width = rows.shape
    units = w_gate.shape[1]
    wide = 512
    steps = units // wide
    high = 256
    gated = router is not None
    kind = BF if gated else F32

    def body(*refs):
        if gated:
            (own_ref, x_ref, g_ref, wg_ref, wu_ref, wd_ref, wr_ref, ot_ref,
             y_ref, gi_ref, hid_ref, dg_ref, du_ref, eo_ref, gl_ref, ya_ref, ga_ref, gate_ref) = refs
        else:
            (x_ref, g_ref, wg_ref, wu_ref, wd_ref,
             y_ref, gi_ref, hid_ref, dg_ref, du_ref, ya_ref, ga_ref) = refs
        step = pl.program_id(0)

        if gated:

            @pl.when(step == 0)
            def _():
                logits = mm(x_ref[...], wr_ref[...])
                lane = lax.broadcasted_iota(jnp.int32, logits.shape, 1)
                mine = jnp.sum(jnp.where(lane == own_ref[0], logits, 0.0), axis=1, keepdims=True)
                theirs = jnp.sum(jnp.where(lane == ot_ref[...], logits, 0.0), axis=1, keepdims=True)
                gate = 1.0 / (1.0 + jnp.exp(theirs - mine))
                rest = 1.0 / (1.0 + jnp.exp(mine - theirs))
                gate_ref[:, 0:1] = gate
                gate_ref[:, 1:2] = rest
                eo_ref[...] = (g_ref[...].astype(F32) * gate).astype(BF)

        def rows_at(index, carry):
            at = pl.ds(pl.multiple_of(index * high, high), high)
            row = x_ref[at, :]
            grad = eo_ref[at, :] if gated else g_ref[at, :]
            gval = mm(row, wg_ref[...])
            uval = mm(row, wu_ref[...])
            sigma = 1.0 / (1.0 + jnp.exp(-gval))
            silu = gval * sigma
            hid = (silu * uval).astype(BF)
            hid_ref[at, :] = hid
            grad_hid = mm(grad, wd_ref[...], NT)
            du = (grad_hid * silu).astype(BF)
            dg = (grad_hid * uval * sigma * (1.0 + gval * (1.0 - sigma))).astype(BF)
            du_ref[at, :] = du
            dg_ref[at, :] = dg
            out = mm(hid, wd_ref[...])
            back = mm(dg, wg_ref[...], NT) + mm(du, wu_ref[...], NT)

            @pl.when(step == 0)
            def _():
                ya_ref[at, :] = out
                ga_ref[at, :] = back

            @pl.when(step > 0)
            def _():
                ya_ref[at, :] += out
                ga_ref[at, :] += back

            return carry

        lax.fori_loop(0, count // high, rows_at, 0)

        @pl.when(step == steps - 1)
        def _():
            if gated:
                out = ya_ref[...]
                gate = gate_ref[:, 0:1]
                lean = jnp.sum(out * g_ref[...].astype(F32), axis=1, keepdims=True)
                lean = lean * gate * gate_ref[:, 1:2]
                lane = lax.broadcasted_iota(jnp.int32, (count, 128), 1)
                sign = (lane == own_ref[0]).astype(F32) - (lane == ot_ref[...]).astype(F32)
                grad_logits = (lean * sign).astype(BF)
                gl_ref[...] = grad_logits
                y_ref[...] = (out * gate).astype(BF)
                gi_ref[...] = (ga_ref[...] + mm(grad_logits, wr_ref[...], NT)).astype(BF)
            else:
                y_ref[...] = ya_ref[...]
                gi_ref[...] = ga_ref[...]

    full = whole((count, width))
    hidden = pl.BlockSpec((count, wide), lambda i, *_: (0, i))
    in_specs = [
        full,
        full,
        pl.BlockSpec((width, wide), lambda i, *_: (0, i)),
        pl.BlockSpec((width, wide), lambda i, *_: (0, i)),
        pl.BlockSpec((wide, width), lambda i, *_: (i, 0)),
    ]
    out_specs = [full, full, hidden, hidden, hidden]
    out_shape = [sds((count, width), kind)] * 2 + [sds((count, units), BF)] * 3
    scratch = [pltpu.VMEM((count, width), F32)] * 2
    args = [rows, grads, w_gate, w_up, w_down]
    if gated:
        in_specs += [whole(router.shape), whole(other.shape)]
        out_specs += [full, whole((count, 128))]
        out_shape += [sds((count, width), BF), sds((count, 128), BF)]
        scratch += [pltpu.VMEM((count, 128), F32)]
        args = [own, *args, router, other]
    return call(
        body,
        (steps,),
        in_specs,
        out_specs,
        out_shape,
        tuple(args),
        scratch=scratch,
        prefetch=1 if gated else 0,
        flops=12 * count * width * units,
    )


def expert_weight_grads(rows, grads, dg, du, hid, grad_logits, sizes, core_at):
    outer, cores = sizes["y"], sizes["core"]
    count, width = rows.shape
    units = dg.shape[1]
    wide = units // (outer * cores)

    def body(at_ref, x_ref, g_ref, dg_ref, du_ref, hid_ref, gl_ref, keep_ref, give_ref, r_ref):
        step = pl.program_id(0)
        found = [
            mm(x_ref[...], dg_ref[...], TN).astype(BF),
            mm(x_ref[...], du_ref[...], TN).astype(BF),
            mm(g_ref[...], hid_ref[...], TN).astype(BF),
        ]

        @pl.when(step < outer)
        def _():
            for index in range(3):
                give_ref[0, index] = found[index]

        @pl.when(step >= outer)
        def _():
            for index in range(3):
                keep_ref[0, index] = found[index]

        @pl.when(step == 0)
        def _():
            r_ref[...] = mm(x_ref[...], gl_ref[...], TN)

    def taken(i, at):
        core = jnp.where(i < outer, 1 - at[0], at[0])
        return (0, (i % outer) * cores + core)

    hidden = pl.BlockSpec((count, wide), taken)
    part = (1, 3, width, wide)
    return call(
        body,
        (outer * cores,),
        [whole(rows.shape), whole(grads.shape), hidden, hidden, hidden, whole(grad_logits.shape)],
        [
            pl.BlockSpec(part, lambda i, *_: (jnp.maximum(i - outer, 0), 0, 0, 0)),
            pl.BlockSpec(part, lambda i, *_: (jnp.minimum(i, outer - 1), 0, 0, 0)),
            whole((width, 128)),
        ],
        [sds((outer, *part[1:]), BF)] * 2 + [sds((width, 128), F32)],
        (core_at, rows, grads, dg, du, hid, grad_logits),
        prefetch=1,
        flops=6 * count * width * units,
    )


def spread_places(sizes, names):
    found = []
    for y in range(sizes["y"]):
        for core in range(sizes["core"]):
            for z in range(sizes["z"]):
                for x in range(sizes["x"]):
                    at = {"y": y, "core": core, "z": z, "x": x}
                    found.append((core, tuple(at[n] for n in names)))
    return found


def spread(value, sizes, names, core_at):
    order = ("y", "core", "z", "x")
    split = value.reshape(*(sizes[n] for n in order), -1, value.shape[-1])
    split = jnp.transpose(split, (1, *(order.index(n) for n in names), 4, 5))
    return at_index(split, core_at[0]), at_index(split, 1 - core_at[0])


def store_spread(places, each, core_at, found, row, keep, give):
    first = row // each
    for core in range(2):
        todo = [at for at in range(found.shape[0] // each) if places[first + at][0] == core]

        def put(store, todo=todo):
            for at in todo:
                store(places[first + at][1], found[at * each : (at + 1) * each].astype(BF))

        pl.when(core_at == core)(lambda put=put: put(keep))
        pl.when(core_at != core)(lambda put=put: put(give))


def shared_weight_grads(rows, grads, dg, du, hid, sizes, core_at):
    names = ("y", "x", "z")
    lead = tuple(sizes[n] for n in names)
    places = spread_places(sizes, names)
    count, width = rows.shape
    units = dg.shape[1]
    wide = 512
    each = width // len(places)
    direct = each % 8 == 0

    def body(at_ref, x_ref, g_ref, dg_ref, du_ref, hid_ref, *outs):
        pairs = ((x_ref, dg_ref), (x_ref, du_ref), (g_ref, hid_ref))
        for index, (left, right) in enumerate(pairs):
            found = mm(left[...], right[...], TN)
            if not direct:
                outs[0][index] = found.astype(BF)
                continue

            def into(ref, index=index):
                def store(place, piece):
                    ref[(*place, index)] = piece

                return store

            store_spread(places, each, at_ref[0], found, 0, into(outs[0]), into(outs[1]))

    hidden = pl.BlockSpec((count, wide), lambda i, *_: (0, i))
    if direct:
        shapes = [(*lead, 3, each, units)] * 2
        spec = [pl.BlockSpec((*lead, 3, each, wide), lambda i, *_: (0,) * 5 + (i,))] * 2
    else:
        shapes = [(3, width, units)]
        spec = [pl.BlockSpec((3, width, wide), lambda i, *_: (0, 0, i))]
    out = call(
        body,
        (units // wide,),
        [whole(rows.shape), whole(grads.shape), hidden, hidden, hidden],
        spec,
        [sds(shape, BF) for shape in shapes],
        (core_at, rows, grads, dg, du, hid),
        prefetch=1,
        flops=6 * count * width * units,
    )
    if direct:
        return out
    found = [spread(out[0][i], sizes, names, core_at) for i in range(3)]
    return [jnp.stack([part[side] for part in found], axis=3) for side in range(2)]


def tall_weight_grads(lefts, rights, extras, sizes, core_at):
    names = ("y", "z", "x")
    lead = tuple(sizes[n] for n in names)
    places = spread_places(sizes, names)
    width = sum(left.shape[1] for left in lefts)
    cols = sum(right.shape[1] for right in rights)
    each = width // len(places)
    direct = each % 8 == 0
    flops = 2 * lefts[0].shape[0] * width * cols

    def body(at_ref, *refs):
        left_refs = refs[: len(lefts)]
        right_refs = refs[len(lefts) : len(lefts) + len(rights)]
        rest = refs[len(lefts) + len(rights) :]
        extra_refs, outs = rest[: len(extras)], rest[len(extras) :]

        def save(row, found, col):
            span = found.shape[1]
            if not direct:
                outs[0][row : row + found.shape[0], col : col + span] = found.astype(BF)
                return

            def into(ref):
                def store(place, piece):
                    ref[(*place, slice(None), slice(col, col + span))] = piece

                return store

            store_spread(places, each, at_ref[0], found, row, into(outs[0]), into(outs[1]))

        row = 0
        for left in left_refs:
            col = 0
            for right in right_refs:
                save(row, mm(left[...], right[...], TN), col)
                col += right.shape[1]
            row += left.shape[1]
        more = extra_refs[0][...]
        for extra in extra_refs[1:]:
            more = more + extra[...]
        save(0, more, cols)

    args = (*lefts, *rights, *extras)
    shapes = [(*lead, each, cols + 128)] * 2 if direct else [(width, cols + 128)]
    out = call(
        body,
        (1,),
        [whole(a.shape) for a in args],
        [whole(shape) for shape in shapes],
        [sds(shape, BF) for shape in shapes],
        (core_at, *args),
        prefetch=1,
        flops=flops,
    )
    return out if direct else spread(out[0], sizes, names, core_at)


def scatter_sum(value, name):
    return lax.psum_scatter(value, name, scatter_dimension=0, tiled=False)


def swap_all(value, names):
    return lax.all_to_all(value, names, 0, 0, tiled=True)


def at_index(value, index):
    return lax.dynamic_index_in_dim(value, index, 0, keepdims=False)


def fold(value, name):
    if lax.axis_size(name) != 2:
        return scatter_sum(value, name)
    at = lax.axis_index(name)
    got = lax.ppermute(at_index(value, 1 - at), name, [(0, 1), (1, 0)])
    return (at_index(value, at).astype(F32) + got.astype(F32)).astype(BF)


def join(keep, give, name):
    got = lax.ppermute(give, name, [(0, 1), (1, 0)])
    return (keep.astype(F32) + got.astype(F32)).astype(BF)


def swap_by_steps(value, name):
    size, at = value.shape[0], lax.axis_index(name)
    found = [at_index(value, at)]
    for step in range(1, size):
        sent = at_index(value, (at + step) % size)
        found.append(lax.ppermute(sent, name, [(i, (i + step) % size) for i in range(size)]))
    return found


def after(value, *others):
    return lax.optimization_barrier((value, *others))[0]


def on_device(
    tokens,
    segments,
    routes,
    slots,
    cotangent,
    attn_gain,
    w_qkv,
    w_out,
    ffn_gain,
    w_router,
    shared_gate,
    shared_up,
    shared_down,
    expert_gate,
    expert_up,
    expert_down,
):
    sizes = {name: lax.axis_size(name) for name in ("y", "core", "z", "x")}
    ranks = ("z", "x")
    seqs, span, width = tokens.shape
    blocks, parts = sizes["z"], sizes["x"]
    experts = blocks * parts
    count = seqs * span
    capacity = 3 * count // experts
    length = span * experts
    group = width // parts
    z_at, x_at = lax.axis_index("z"), lax.axis_index("x")
    own = (z_at * parts + x_at).astype(jnp.int32).reshape(1)
    z_ref, x_ref = z_at.astype(jnp.int32).reshape(1), x_at.astype(jnp.int32).reshape(1)
    core_ref = lax.axis_index("core").astype(jnp.int32).reshape(1)
    attn_scale = attn_gain.astype(F32).reshape(1, width)
    ffn_scale = ffn_gain.astype(F32).reshape(1, width)
    flat_tokens = tokens.reshape(count, width)
    flat_cot = cotangent.reshape(count, width)

    route_rows = routes.reshape(count, 2)
    slot_rows = slots.reshape(count, 2)
    target = jnp.where(slot_rows >= 0, route_rows * capacity + slot_rows, -1)
    target_rows = jnp.transpose(target)
    grad_sent = dispatch(flat_cot, target_rows, experts, capacity, jnp.transpose(route_rows))

    frequency = jnp.power(10000.0, -2.0 * jnp.arange(32, dtype=F32) / HEAD_DIM)
    angles = jnp.arange(length, dtype=jnp.int32).astype(F32)[:, None] * jnp.tile(frequency, 4)
    sign = jnp.where(jnp.arange(128) % 64 < 32, -1.0, 1.0)
    cosine, sine = jnp.cos(angles), jnp.sin(angles) * sign
    seg_row = lax.dynamic_slice_in_dim(segments, z_at, 1, 0)
    seg_col = seg_row.reshape(length, 1)
    fused = group % 128 == 0
    if fused:
        weights = [w_qkv] * 3
    else:
        picked = w_qkv.reshape(width, 3, parts, group)
        picked = lax.dynamic_index_in_dim(picked, x_at, 2, keepdims=False)
        weights = [picked.reshape(width, 3 * group)]

    by_seq = swap_all(tokens, "z")
    by_seq, cosine, sine, seg_col, grad_sent = lax.optimization_barrier(
        (by_seq, cosine, sine, seg_col, grad_sent)
    )
    grad_came = swap_all(grad_sent, ranks)
    if parts == 2:
        rows = [by_seq, lax.ppermute(by_seq, "x", [(0, 1), (1, 0)])]
    else:
        rows = [lax.all_gather(by_seq, "x", axis=0, tiled=False)]

    qkv, normed = project(rows, attn_scale, weights, group, cosine, sine, x_ref, parts)
    attended, lse = (attend if fused else plain_attend)(qkv, seg_row, seg_col)
    attended = after(attended, grad_came)
    attended = swap_all(attended.reshape(experts, span, group), ranks)
    attended = attended.reshape(seqs, parts, span, group)

    hidden, branch_in = after_attention(flat_tokens, attended, w_out, ffn_scale)
    sent = dispatch(branch_in, target_rows, experts, capacity)
    received = swap_all(sent, ranks).reshape(-1, width)

    shared_out, shared_back, hid, dg, du = feed_forward(
        branch_in, flat_cot, shared_gate, shared_up, shared_down
    )
    keep, give = shared_weight_grads(branch_in, flat_cot, dg, du, hid, sizes, core_ref)
    shared_sums = fold(join(keep, give, "core"), "y")
    grad_rows = grad_came[:, :capacity, :].reshape(-1, width)
    other = grad_came[:, capacity, :capacity].astype(jnp.int32).reshape(-1, 1)
    received = after(received, give, grad_rows, other)

    router = jnp.pad(w_router, ((0, 0), (0, 128 - experts)))
    made, made_back, hid, dg, du, gated_grads, grad_logits = feed_forward(
        received, grad_rows, expert_gate[0], expert_up[0], expert_down[0], router, other, own
    )
    back_rows = swap_all(made_back.reshape(experts, capacity, width), ranks).reshape(-1, width)
    keep, give, grad_router = expert_weight_grads(
        received, gated_grads, dg, du, hid, grad_logits, sizes, core_ref
    )
    back_rows = after(back_rows, give)
    expert_sums = fold(join(keep, give, "core"), "y")
    shared_sums = swap_by_steps(fold(shared_sums, "x"), "z")

    grad_hidden, grad_attn, grad_att, grad_ffn = middle_back(
        hidden, shared_back, back_rows, target, flat_cot, ffn_scale, w_out, parts, span
    )
    grad_att = swap_all(grad_att.reshape(experts, span, group), ranks).reshape(length, group)

    column = lax.broadcasted_iota(jnp.int32, (width, 128), 1)
    small = jnp.where(column < experts, grad_router, jnp.where(column == experts, grad_ffn, 0.0))
    out_sums = tall_weight_grads(
        [attended[:, part].reshape(count, group) for part in range(parts)],
        [grad_attn],
        [small],
        sizes,
        core_ref,
    )
    out_sums = fold(join(*out_sums, "core"), "y")

    made = after(made, grad_att)
    made_rows = swap_all(made.reshape(experts, capacity, width), ranks).reshape(-1, width)
    grads = (attend_back if fused else plain_attend_back)(
        qkv, grad_att, lse, seg_row, seg_col, cosine, sine
    )
    normed_back, grad_gain = project_back(grads, weights, rows, x_ref, parts)
    normed_back = fold(normed_back, "x")
    pieces = swap_by_steps(normed_back, "z")

    qkv_sums = tall_weight_grads([normed], list(grads), [grad_gain], sizes, core_ref)
    qkv_sums = fold(join(*qkv_sums, "core"), "y")
    token_grad = first_norm_back(flat_tokens, attn_scale, pieces, grad_hidden, z_ref)
    layer_out = layer_end(hidden, shared_out, made_rows, target).reshape(tokens.shape)

    last = after(jnp.concatenate([out_sums, qkv_sums], axis=-1), made_rows)
    each, cols = last.shape[-2:]
    last = swap_all(last.reshape(experts, each, cols), ranks).astype(F32)
    last = jnp.sum(last.reshape(blocks, parts, each, cols), axis=0)
    out_sums = jnp.sum(last[:, :, : width + 128], axis=0)
    qkv_sums = last[:, :, width + 128 :]
    grad_attn_gain = jnp.sum(qkv_sums[:, :, 3 * group], axis=0)
    grad_w_qkv = qkv_sums[:, :, : 3 * group].reshape(parts, each, 3, group)
    grad_w_qkv = jnp.transpose(grad_w_qkv, (1, 2, 0, 3)).reshape(each, 3 * width)

    shared_sums = sum(part.astype(F32) for part in shared_sums)
    expert_sums = expert_sums.astype(F32)
    return (
        layer_out,
        token_grad.reshape(tokens.shape),
        grad_attn_gain,
        grad_w_qkv,
        out_sums[:, :width],
        out_sums[:, width + experts],
        out_sums[:, width : width + experts],
        shared_sums[0],
        shared_sums[1],
        jnp.transpose(shared_sums[2]),
        expert_sums[0][None],
        expert_sums[1][None],
        jnp.transpose(expert_sums[2])[None],
    )


def solution(mesh):
    dp, experts = mesh.shape["dp"], mesh.shape["expert"]

    def step(*args):
        seqs = args[0].shape[0] // dp
        cores = 2 if dp % 2 == 0 else 1
        fine = Mesh(
            mesh.devices.reshape(dp // cores, cores, seqs, experts // seqs),
            ("y", "core", "z", "x"),
        )
        data, ranks, every = ("y", "core"), ("z", "x"), ("y", "core", "z", "x")
        placed = (
            P(data, ranks, None),
            P(data, None),
            P(data, ranks, None),
            P(data, ranks, None),
            P(data, ranks, None),
            *([P()] * 8),
            P(ranks, None, None),
            P(ranks, None, None),
            P(ranks, None, None),
        )
        return jax.shard_map(
            on_device,
            mesh=fine,
            in_specs=placed,
            out_specs=(
                P(data, ranks, None),
                P(data, ranks, None),
                P(every),
                P(every, None),
                P(every, None),
                P(every),
                P(every, None),
                P(every, None),
                P(every, None),
                P(None, every),
                P(ranks, None, data),
                P(ranks, None, data),
                P(ranks, data, None),
            ),
            check_vma=False,
        )(*args)

    return step
```

```python
import jax
import jax.numpy as jnp
from jax import lax
from jax.experimental import pallas as pl
from jax.experimental.pallas import tpu as pltpu
from jax.sharding import Mesh
from jax.sharding import PartitionSpec as P

HEAD_DIM = 64
EPS = 1e-06
BF = jnp.bfloat16
F32 = jnp.float32
NEG = -1e30
NN = (((1,), (0,)), ((), ()))
NT = (((1,), (1,)), ((), ()))
TN = (((0,), (0,)), ((), ()))
VMEM_MOST = 60 << 20


def mm(left, right, dims=NN):
    return lax.dot_general(left, right, dims, preferred_element_type=F32)


def sds(shape, dtype):
    return jax.ShapeDtypeStruct(shape, dtype)


def call(body, grid, in_specs, out_specs, out_shape, args, scratch=(), prefetch=0, flops=0):
    leaves = jax.tree.leaves(out_shape)
    moved = sum(a.size * a.dtype.itemsize for a in args) + sum(
        a.size * a.dtype.itemsize for a in leaves
    )
    return pl.pallas_call(
        body,
        out_shape=out_shape,
        grid_spec=pltpu.PrefetchScalarGridSpec(
            num_scalar_prefetch=prefetch,
            grid=grid,
            in_specs=in_specs,
            out_specs=out_specs,
            scratch_shapes=list(scratch),
        ),
        compiler_params=pltpu.CompilerParams(
            dimension_semantics=("arbitrary",) * len(grid), vmem_limit_bytes=VMEM_MOST
        ),
        cost_estimate=pl.CostEstimate(
            flops=int(flops), transcendentals=0, bytes_accessed=int(moved)
        ),
    )(*args)


def whole(shape):
    rank = len(shape)
    return pl.BlockSpec(tuple(shape), lambda *_: (0,) * rank)


def swap_halves(value):
    lane = lax.broadcasted_iota(jnp.int32, value.shape, 1)
    return jnp.where(lane % 64 < 32, pltpu.roll(value, 96, 1), pltpu.roll(value, 32, 1))


def rms(values):
    return lax.rsqrt(jnp.mean(values * values, axis=1, keepdims=True) + EPS)


def row_specs(rows):
    if len(rows) == 2:
        _, span, width = rows[0].shape
        return [pl.BlockSpec((1, span, width), lambda i, *_: (i, 0, 0))] * 2
    parts, _, span, width = rows[0].shape
    return [pl.BlockSpec((parts, 1, span, width), lambda i, *_: (0, i, 0, 0))]


def load_rows(refs, at_ref):
    if len(refs) == 2:
        mine, theirs = refs[0][0].astype(F32), refs[1][0].astype(F32)
        first = at_ref[0] == 0
        pair = [jnp.where(first, mine, theirs), jnp.where(first, theirs, mine)]
        return jnp.concatenate(pair, axis=0)
    value = refs[0][...]
    return value.reshape(value.shape[0] * value.shape[2], value.shape[3]).astype(F32)


def weight_specs(weights, group):
    if len(weights) == 1:
        return [whole(weights[0].shape)]
    width, cols = weights[0].shape
    parts = cols // (3 * group)

    def spec(index):
        return pl.BlockSpec((width, group), lambda i, at: (0, index * parts + at[0]))

    return [spec(index) for index in range(3)]


def load_weights(refs, group):
    if len(refs) == 3:
        return [ref[...] for ref in refs]
    return [refs[0][:, at * group : (at + 1) * group] for at in range(3)]


def project(rows, gain, weights, group, cosine, sine, x_at, parts):
    blocks, span, width = rows[0].shape[-3:]
    height = parts * span
    length = height * blocks
    cut = len(rows)

    def body(at_ref, *refs):
        r_refs, (g_ref, c_ref, s_ref) = refs[:cut], refs[cut : cut + 3]
        w_refs, (qkv_ref, n_ref) = refs[cut + 3 : -2], refs[-2:]
        tok = load_rows(r_refs, at_ref)
        normed = (tok * rms(tok) * g_ref[...]).astype(BF)
        n_ref[...] = normed
        if len(w_refs) == 3:
            found = [mm(normed, ref[...]) for ref in w_refs]
            turning = [(found[0], 0), (found[1], group)]
            last = found[2]
        else:
            found = mm(normed, w_refs[0][...])
            turning, last = [(found[:, : 2 * group], 0)], found[:, 2 * group :]
        for value, base in turning:
            for at in range(0, value.shape[1], 128):
                part = value[:, at : at + 128]
                lane = lax.broadcasted_iota(jnp.int32, part.shape, 1) + (base + at)
                turned = part * c_ref[...] + swap_halves(part) * s_ref[...]
                turned = turned * jnp.where(lane < group, HEAD_DIM**-0.5, 1.0)
                qkv_ref[:, base + at : base + at + 128] = turned.astype(BF)
        qkv_ref[:, 2 * group :] = last.astype(BF)

    return call(
        body,
        (blocks,),
        [
            *row_specs(rows),
            whole((1, width)),
            pl.BlockSpec((height, 128), lambda i, *_: (i, 0)),
            pl.BlockSpec((height, 128), lambda i, *_: (i, 0)),
            *weight_specs(weights, group),
        ],
        [
            pl.BlockSpec((height, 3 * group), lambda i, *_: (i, 0)),
            pl.BlockSpec((height, width), lambda i, *_: (i, 0)),
        ],
        [sds((length, 3 * group), BF), sds((length, width), BF)],
        (x_at, *rows, gain, cosine, sine, *weights),
        prefetch=1,
        flops=6 * length * width * group,
    )


def project_back(grads, weights, rows, x_at, parts):
    blocks, span, width = rows[0].shape[-3:]
    group = grads[0].shape[1]
    height = parts * span
    length = height * blocks
    cut = len(rows)

    def body(at_ref, q_ref, k_ref, v_ref, *refs):
        r_refs, w_refs, (out_ref, gain_ref, acc_ref) = refs[:cut], refs[cut:-3], refs[-3:]
        step = pl.program_id(0)
        w_q, w_k, w_v = load_weights(w_refs, group)
        back = mm(q_ref[...], w_q, NT) + mm(k_ref[...], w_k, NT) + mm(v_ref[...], w_v, NT)
        tok = load_rows(r_refs, at_ref)
        part = jnp.sum(back * tok * rms(tok), axis=0, keepdims=True)

        @pl.when(step == 0)
        def _():
            acc_ref[...] = jnp.zeros_like(acc_ref)

        acc_ref[...] += jnp.broadcast_to(part, acc_ref.shape)
        out_ref[...] = back.astype(BF).reshape(parts, 1, span, width)

        @pl.when(step == blocks - 1)
        def _():
            column = jnp.transpose(acc_ref[...])
            gain_ref[...] = jnp.broadcast_to(column[:, :1], gain_ref.shape)

    block = pl.BlockSpec((height, group), lambda i, *_: (i, 0))
    return call(
        body,
        (blocks,),
        [block, block, block, *row_specs(rows), *weight_specs(weights, group)],
        [
            pl.BlockSpec((parts, 1, span, width), lambda i, *_: (0, i, 0, 0)),
            whole((width, 128)),
        ],
        [sds((parts, blocks, span, width), BF), sds((width, 128), F32)],
        (x_at, *grads, *rows, *weights),
        scratch=[pltpu.VMEM((8, width), F32)],
        prefetch=1,
        flops=6 * length * width * group,
    )


def attend(qkv, seg_row, seg_col):
    length, cols = qkv.shape
    group = cols // 3
    pairs = group // 128
    high = min(256, length)

    def body(q_ref, k_ref, v_ref, sr_ref, sc_ref, o_ref, l_ref):
        lane = lax.broadcasted_iota(jnp.int32, (high, 128), 1)
        for at in range(0, length, high):
            end = at + high
            query = q_ref[at:end, :]
            keys = k_ref[:end, :]
            vals = v_ref[:end, :]
            q_pos = lax.broadcasted_iota(jnp.int32, (high, end), 0) + at
            k_pos = lax.broadcasted_iota(jnp.int32, (high, end), 1)
            allowed = (sc_ref[at:end, :] == sr_ref[:, :end]) & (k_pos <= q_pos)
            outs = []
            for head in range(2):
                mine = (lane // 64) == head
                scores = mm(jnp.where(mine, query, jnp.zeros_like(query)), keys, NT)
                scores = jnp.where(allowed, scores, NEG)
                most = jnp.max(scores, axis=1, keepdims=True)
                expo = jnp.exp(scores - most)
                total = jnp.sum(expo, axis=1, keepdims=True)
                outs.append(mm(expo.astype(BF), vals) / total)
                lse = jnp.broadcast_to(most + jnp.log(total), (high, 128))
                l_ref[0, head : head + 1, at:end] = jnp.transpose(lse)[:1, :]
            o_ref[at:end, :] = jnp.where(lane < 64, outs[0], outs[1]).astype(BF)

    def col(offset):
        return pl.BlockSpec((length, 128), lambda i: (0, offset * pairs + i))

    return call(
        body,
        (pairs,),
        [col(0), col(1), col(2), whole((1, length)), whole((length, 1))],
        [col(0), pl.BlockSpec((1, 2, length), lambda i: (i, 0, 0))],
        [sds((length, group), BF), sds((pairs, 2, length), F32)],
        (qkv, qkv, qkv, seg_row, seg_col),
        flops=4 * length * length * group,
    )


def attend_back(qkv, grad, lse, seg_row, seg_col, cosine, sine):
    length, cols = qkv.shape
    group = cols // 3
    pairs = group // 128
    high = min(256, length)

    def body(
        q_ref, k_ref, v_ref, g_ref, l_ref, sr_ref, sc_ref, c_ref, s_ref, dq_ref, dk_ref, dv_ref,
        ka_ref, va_ref,
    ):
        lane = lax.broadcasted_iota(jnp.int32, (high, 128), 1)
        ka_ref[...] = jnp.zeros_like(ka_ref)
        va_ref[...] = jnp.zeros_like(va_ref)
        for at in range(0, length, high):
            end = at + high
            query = q_ref[at:end, :]
            grads = g_ref[at:end, :]
            keys = k_ref[:end, :]
            vals = v_ref[:end, :]
            k_pos = lax.broadcasted_iota(jnp.int32, (end, high), 0)
            q_pos = lax.broadcasted_iota(jnp.int32, (end, high), 1) + at
            allowed = (sc_ref[:end, :] == sr_ref[:, at:end]) & (k_pos <= q_pos)
            outs = []
            for head in range(2):
                mine = (lane // 64) == head
                q_own = jnp.where(mine, query, jnp.zeros_like(query))
                g_own = jnp.where(mine, grads, jnp.zeros_like(grads))
                scores = jnp.where(allowed, mm(keys, q_own, NT), NEG)
                probs = jnp.exp(scores - l_ref[0, head : head + 1, at:end])
                grad_probs = mm(vals, g_own, NT)
                delta = jnp.sum(probs * grad_probs, axis=0, keepdims=True)
                grad_scores = (probs * (grad_probs - delta)).astype(BF)
                va_ref[:end, :] += mm(probs.astype(BF), g_own)
                ka_ref[:end, :] += mm(grad_scores, q_own)
                outs.append(mm(grad_scores, keys, TN))
            found = jnp.where(lane < 64, outs[0], outs[1]) * HEAD_DIM**-0.5
            back = found * c_ref[at:end, :] - swap_halves(found) * s_ref[at:end, :]
            dq_ref[at:end, :] = back.astype(BF)
        found = ka_ref[...]
        dk_ref[...] = (found * c_ref[...] - swap_halves(found) * s_ref[...]).astype(BF)
        dv_ref[...] = va_ref[...].astype(BF)

    def col(offset):
        return pl.BlockSpec((length, 128), lambda i: (0, offset * pairs + i))

    return call(
        body,
        (pairs,),
        [
            col(0),
            col(1),
            col(2),
            col(0),
            pl.BlockSpec((1, 2, length), lambda i: (i, 0, 0)),
            whole((1, length)),
            whole((length, 1)),
            whole((length, 128)),
            whole((length, 128)),
        ],
        [col(0), col(0), col(0)],
        [sds((length, group), BF)] * 3,
        (qkv, qkv, qkv, grad, lse, seg_row, seg_col, cosine, sine),
        scratch=[pltpu.VMEM((length, 128), F32)] * 2,
        flops=10 * length * length * group,
    )


def heads_of(flat):
    return flat.reshape(flat.shape[0], -1, HEAD_DIM)


def plain_mask(seg_row, seg_col):
    length = seg_col.shape[0]
    spots = jnp.arange(length, dtype=jnp.int32)
    return (seg_row == seg_col) & (spots[None, :] <= spots[:, None])


def plain_attend(qkv, seg_row, seg_col):
    query, keys, vals = (heads_of(part) for part in jnp.split(qkv, 3, axis=1))
    scores = jnp.einsum("qhd,khd->hqk", query, keys, preferred_element_type=F32)
    scores = jnp.where(plain_mask(seg_row, seg_col)[None], scores, NEG)
    lse = jax.nn.logsumexp(scores, axis=-1, keepdims=True)
    probs = jnp.exp(scores - lse).astype(BF)
    found = jnp.einsum("hqk,khd->qhd", probs, vals, preferred_element_type=F32)
    return found.astype(BF).reshape(qkv.shape[0], -1), lse


def plain_turn_back(grads, cosine, sine):
    table_c, table_s = cosine[:, None, :HEAD_DIM], sine[:, None, :HEAD_DIM]
    swapped = jnp.roll(grads, HEAD_DIM // 2, axis=-1)
    return (grads * table_c - swapped * table_s).astype(BF).reshape(grads.shape[0], -1)


def plain_attend_back(qkv, grad, lse, seg_row, seg_col, cosine, sine):
    query, keys, vals = (heads_of(part) for part in jnp.split(qkv, 3, axis=1))
    grad = heads_of(grad)
    scores = jnp.einsum("qhd,khd->hqk", query, keys, preferred_element_type=F32)
    scores = jnp.where(plain_mask(seg_row, seg_col)[None], scores, NEG)
    probs = jnp.exp(scores - lse)
    grad_probs = jnp.einsum("qhd,khd->hqk", grad, vals, preferred_element_type=F32)
    delta = jnp.sum(probs * grad_probs, axis=-1, keepdims=True)
    grad_scores = (probs * (grad_probs - delta)).astype(BF)
    gq = jnp.einsum("hqk,khd->qhd", grad_scores, keys, preferred_element_type=F32)
    gk = jnp.einsum("hqk,qhd->khd", grad_scores, query, preferred_element_type=F32)
    gv = jnp.einsum("hqk,qhd->khd", probs.astype(BF), grad, preferred_element_type=F32)
    return (
        plain_turn_back(gq * HEAD_DIM**-0.5, cosine, sine),
        plain_turn_back(gk, cosine, sine),
        gv.astype(BF).reshape(qkv.shape[0], -1),
    )


def after_attention(tokens, attended, w_out, gain):
    seqs, parts, span, group = attended.shape
    count, width = tokens.shape

    def body(t_ref, a_ref, w_ref, g_ref, h_ref, b_ref):
        hidden = t_ref[...].astype(F32)
        for part in range(parts):
            rows = a_ref[:, part].reshape(count, group)
            hidden += mm(rows, w_ref[part * group : (part + 1) * group, :])
        h_ref[...] = hidden
        b_ref[...] = (hidden * rms(hidden) * g_ref[...]).astype(BF)

    return call(
        body,
        (1,),
        [whole(a.shape) for a in (tokens, attended, w_out, gain)],
        [whole(tokens.shape)] * 2,
        [sds(tokens.shape, F32), sds(tokens.shape, BF)],
        (tokens, attended, w_out, gain),
        flops=2 * count * width * width,
    )


def dispatch(rows, target_rows, experts, capacity, route_rows=None):
    count, width = rows.shape
    more = 0 if route_rows is None else 16
    tables = () if route_rows is None else (route_rows,)

    def body(r_ref, t_ref, *refs):
        o_ref = refs[-1]
        slot = lax.broadcasted_iota(jnp.int32, (capacity, count), 0)
        slot += pl.program_id(0) * capacity
        hits = [slot == t_ref[k : k + 1, :] for k in range(2)]
        hot = (hits[0] | hits[1]).astype(F32).astype(BF)
        o_ref[0, :capacity, :] = mm(hot, r_ref[...]).astype(BF)
        if more:
            o_ref[0, capacity:, :] = jnp.zeros((more, width), BF)
            other = jnp.zeros((8, capacity), F32)
            for k in range(2):
                route = jnp.broadcast_to(refs[0][1 - k : 2 - k, :].astype(F32), (8, count))
                other += mm(route.astype(BF), hits[k].astype(F32).astype(BF), NT)
            o_ref[0, capacity : capacity + 8, :capacity] = other.astype(BF)

    return call(
        body,
        (experts,),
        [whole(a.shape) for a in (rows, target_rows, *tables)],
        pl.BlockSpec((1, capacity + more, width), lambda i: (i, 0, 0)),
        sds((experts, capacity + more, width), BF),
        (rows, target_rows, *tables),
        flops=2 * experts * capacity * count * width,
    )


def pick(target, rows):
    spot = lax.broadcasted_iota(jnp.int32, (target.shape[0], rows.shape[0]), 1)
    hit = (spot == target[:, 0:1]) | (spot == target[:, 1:2])
    return mm(hit.astype(F32).astype(BF), rows)


def layer_end(hidden, shared_out, rows, target):
    count, width = hidden.shape
    high = count // 2

    def body(h_ref, s_ref, r_ref, t_ref, o_ref):
        o_ref[...] = (h_ref[...] + s_ref[...] + pick(t_ref[...], r_ref[...])).astype(BF)

    block = pl.BlockSpec((high, width), lambda i: (i, 0))
    return call(
        body,
        (2,),
        [block, block, whole(rows.shape), pl.BlockSpec((high, 2), lambda i: (i, 0))],
        block,
        sds(hidden.shape, BF),
        (hidden, shared_out, rows, target),
        flops=2 * count * width * rows.shape[0],
    )


def middle_back(hidden, grad_shared, rows, target, cotangent, gain, w_out, parts, span):
    count, width = hidden.shape
    seqs = count // span
    each = 2 if seqs % 2 == 0 else 1
    high = each * span
    steps = count // high
    group = width // parts

    def body(h_ref, s_ref, r_ref, t_ref, c_ref, g_ref, w_ref, gh_ref, ga_ref, d_ref, n_ref, acc_ref):
        step = pl.program_id(0)
        branch = s_ref[...] + pick(t_ref[...], r_ref[...])
        hidden = h_ref[...]
        scale = rms(hidden)
        weighted = branch * g_ref[...]
        inner = jnp.mean(weighted * hidden, axis=1, keepdims=True)
        part = jnp.sum(branch * hidden * scale, axis=0, keepdims=True)
        out = c_ref[...].astype(F32) + scale * weighted - hidden * (scale * scale * scale * inner)
        gh_ref[...] = out
        out = out.astype(BF)
        ga_ref[...] = out
        for at in range(parts):
            sent = mm(out, w_ref[at * group : (at + 1) * group, :], NT).astype(BF)
            d_ref[:, at] = sent.reshape(each, span, group)

        @pl.when(step == 0)
        def _():
            acc_ref[...] = jnp.zeros_like(acc_ref)

        acc_ref[...] += jnp.broadcast_to(part, acc_ref.shape)

        @pl.when(step == steps - 1)
        def _():
            column = jnp.transpose(acc_ref[...])
            n_ref[...] = jnp.broadcast_to(column[:, :1], n_ref.shape)

    block = pl.BlockSpec((high, width), lambda i: (i, 0))
    return call(
        body,
        (steps,),
        [
            block,
            block,
            whole(rows.shape),
            pl.BlockSpec((high, 2), lambda i: (i, 0)),
            block,
            whole(gain.shape),
            whole(w_out.shape),
        ],
        [
            block,
            block,
            pl.BlockSpec((each, parts, span, group), lambda i: (i, 0, 0, 0)),
            whole((width, 128)),
        ],
        [
            sds(hidden.shape, F32),
            sds(hidden.shape, BF),
            sds((seqs, parts, span, group), BF),
            sds((width, 128), F32),
        ],
        (hidden, grad_shared, rows, target, cotangent, gain, w_out),
        scratch=[pltpu.VMEM((8, width), F32)],
        flops=2 * count * width * (rows.shape[0] + width),
    )


def first_norm_back(tokens, gain, pieces, grad_hidden, z_at):
    count, width = tokens.shape
    blocks = len(pieces)
    span = count // blocks

    def body(at_ref, t_ref, g_ref, h_ref, *refs):
        o_ref = refs[-1]
        for index in range(blocks):
            seq = (at_ref[0] + blocks - index) % blocks
            spot = pl.ds(pl.multiple_of(seq * span, span), span)
            tok = t_ref[spot, :].astype(F32)
            scale = rms(tok)
            weighted = refs[index][...].astype(F32) * g_ref[...]
            inner = jnp.mean(weighted * tok, axis=1, keepdims=True)
            out = h_ref[spot, :] + scale * weighted - tok * (scale * scale * scale * inner)
            o_ref[spot, :] = out.astype(BF)

    return call(
        body,
        (1,),
        [whole(a.shape) for a in (tokens, gain, grad_hidden, *pieces)],
        whole(tokens.shape),
        sds(tokens.shape, BF),
        (z_at, tokens, gain, grad_hidden, *pieces),
        prefetch=1,
    )


def feed_forward(rows, grads, w_gate, w_up, w_down, router=None, other=None, own=None):
    count, width = rows.shape
    units = w_gate.shape[1]
    wide = 512
    steps = units // wide
    high = 256
    gated = router is not None
    kind = BF if gated else F32

    def body(*refs):
        if gated:
            (own_ref, x_ref, g_ref, wg_ref, wu_ref, wd_ref, wr_ref, ot_ref,
             y_ref, gi_ref, hid_ref, dg_ref, du_ref, eo_ref, gl_ref, ya_ref, ga_ref, gate_ref) = refs
        else:
            (x_ref, g_ref, wg_ref, wu_ref, wd_ref,
             y_ref, gi_ref, hid_ref, dg_ref, du_ref, ya_ref, ga_ref) = refs
        step = pl.program_id(0)

        if gated:

            @pl.when(step == 0)
            def _():
                logits = mm(x_ref[...], wr_ref[...])
                lane = lax.broadcasted_iota(jnp.int32, logits.shape, 1)
                mine = jnp.sum(jnp.where(lane == own_ref[0], logits, 0.0), axis=1, keepdims=True)
                theirs = jnp.sum(jnp.where(lane == ot_ref[...], logits, 0.0), axis=1, keepdims=True)
                gate = 1.0 / (1.0 + jnp.exp(theirs - mine))
                rest = 1.0 / (1.0 + jnp.exp(mine - theirs))
                gate_ref[:, 0:1] = gate
                gate_ref[:, 1:2] = rest
                eo_ref[...] = (g_ref[...].astype(F32) * gate).astype(BF)

        def rows_at(index, carry):
            at = pl.ds(pl.multiple_of(index * high, high), high)
            row = x_ref[at, :]
            grad = eo_ref[at, :] if gated else g_ref[at, :]
            gval = mm(row, wg_ref[...])
            uval = mm(row, wu_ref[...])
            sigma = 1.0 / (1.0 + jnp.exp(-gval))
            silu = gval * sigma
            hid = (silu * uval).astype(BF)
            hid_ref[at, :] = hid
            grad_hid = mm(grad, wd_ref[...], NT)
            du = (grad_hid * silu).astype(BF)
            dg = (grad_hid * uval * sigma * (1.0 + gval * (1.0 - sigma))).astype(BF)
            du_ref[at, :] = du
            dg_ref[at, :] = dg
            out = mm(hid, wd_ref[...])
            back = mm(dg, wg_ref[...], NT) + mm(du, wu_ref[...], NT)

            @pl.when(step == 0)
            def _():
                ya_ref[at, :] = out
                ga_ref[at, :] = back

            @pl.when(step > 0)
            def _():
                ya_ref[at, :] += out
                ga_ref[at, :] += back

            return carry

        lax.fori_loop(0, count // high, rows_at, 0)

        @pl.when(step == steps - 1)
        def _():
            if gated:
                out = ya_ref[...]
                gate = gate_ref[:, 0:1]
                lean = jnp.sum(out * g_ref[...].astype(F32), axis=1, keepdims=True)
                lean = lean * gate * gate_ref[:, 1:2]
                lane = lax.broadcasted_iota(jnp.int32, (count, 128), 1)
                sign = (lane == own_ref[0]).astype(F32) - (lane == ot_ref[...]).astype(F32)
                grad_logits = (lean * sign).astype(BF)
                gl_ref[...] = grad_logits
                y_ref[...] = (out * gate).astype(BF)
                gi_ref[...] = (ga_ref[...] + mm(grad_logits, wr_ref[...], NT)).astype(BF)
            else:
                y_ref[...] = ya_ref[...]
                gi_ref[...] = ga_ref[...]

    full = whole((count, width))
    hidden = pl.BlockSpec((count, wide), lambda i, *_: (0, i))
    in_specs = [
        full,
        full,
        pl.BlockSpec((width, wide), lambda i, *_: (0, i)),
        pl.BlockSpec((width, wide), lambda i, *_: (0, i)),
        pl.BlockSpec((wide, width), lambda i, *_: (i, 0)),
    ]
    out_specs = [full, full, hidden, hidden, hidden]
    out_shape = [sds((count, width), kind)] * 2 + [sds((count, units), BF)] * 3
    scratch = [pltpu.VMEM((count, width), F32)] * 2
    args = [rows, grads, w_gate, w_up, w_down]
    if gated:
        in_specs += [whole(router.shape), whole(other.shape)]
        out_specs += [full, whole((count, 128))]
        out_shape += [sds((count, width), BF), sds((count, 128), BF)]
        scratch += [pltpu.VMEM((count, 128), F32)]
        args = [own, *args, router, other]
    return call(
        body,
        (steps,),
        in_specs,
        out_specs,
        out_shape,
        tuple(args),
        scratch=scratch,
        prefetch=1 if gated else 0,
        flops=12 * count * width * units,
    )


def expert_weight_grads(rows, grads, dg, du, hid, grad_logits, sizes, core_at):
    outer, cores = sizes["y"], sizes["core"]
    count, width = rows.shape
    units = dg.shape[1]
    wide = units // (outer * cores)

    def body(at_ref, x_ref, g_ref, dg_ref, du_ref, hid_ref, gl_ref, keep_ref, give_ref, r_ref):
        step = pl.program_id(0)
        found = [
            mm(x_ref[...], dg_ref[...], TN).astype(BF),
            mm(x_ref[...], du_ref[...], TN).astype(BF),
            mm(g_ref[...], hid_ref[...], TN).astype(BF),
        ]

        @pl.when(step < outer)
        def _():
            for index in range(3):
                give_ref[0, index] = found[index]

        @pl.when(step >= outer)
        def _():
            for index in range(3):
                keep_ref[0, index] = found[index]

        @pl.when(step == 0)
        def _():
            r_ref[...] = mm(x_ref[...], gl_ref[...], TN)

    def taken(i, at):
        core = jnp.where(i < outer, 1 - at[0], at[0])
        return (0, (i % outer) * cores + core)

    hidden = pl.BlockSpec((count, wide), taken)
    part = (1, 3, width, wide)
    return call(
        body,
        (outer * cores,),
        [whole(rows.shape), whole(grads.shape), hidden, hidden, hidden, whole(grad_logits.shape)],
        [
            pl.BlockSpec(part, lambda i, *_: (jnp.maximum(i - outer, 0), 0, 0, 0)),
            pl.BlockSpec(part, lambda i, *_: (jnp.minimum(i, outer - 1), 0, 0, 0)),
            whole((width, 128)),
        ],
        [sds((outer, *part[1:]), BF)] * 2 + [sds((width, 128), F32)],
        (core_at, rows, grads, dg, du, hid, grad_logits),
        prefetch=1,
        flops=6 * count * width * units,
    )


def spread_places(sizes, names):
    found = []
    for y in range(sizes["y"]):
        for core in range(sizes["core"]):
            for z in range(sizes["z"]):
                for x in range(sizes["x"]):
                    at = {"y": y, "core": core, "z": z, "x": x}
                    found.append((core, tuple(at[n] for n in names)))
    return found


def spread(value, sizes, names, core_at):
    order = ("y", "core", "z", "x")
    split = value.reshape(*(sizes[n] for n in order), -1, value.shape[-1])
    split = jnp.transpose(split, (1, *(order.index(n) for n in names), 4, 5))
    return at_index(split, core_at[0]), at_index(split, 1 - core_at[0])


def store_spread(places, each, core_at, found, row, keep, give):
    first = row // each
    for core in range(2):
        todo = [at for at in range(found.shape[0] // each) if places[first + at][0] == core]

        def put(store, todo=todo):
            for at in todo:
                store(places[first + at][1], found[at * each : (at + 1) * each].astype(BF))

        pl.when(core_at == core)(lambda put=put: put(keep))
        pl.when(core_at != core)(lambda put=put: put(give))


def shared_weight_grads(rows, grads, dg, du, hid, sizes, core_at):
    names = ("y", "x", "z")
    lead = tuple(sizes[n] for n in names)
    places = spread_places(sizes, names)
    count, width = rows.shape
    units = dg.shape[1]
    wide = 512
    each = width // len(places)
    direct = each % 8 == 0

    def body(at_ref, x_ref, g_ref, dg_ref, du_ref, hid_ref, *outs):
        pairs = ((x_ref, dg_ref), (x_ref, du_ref), (g_ref, hid_ref))
        for index, (left, right) in enumerate(pairs):
            found = mm(left[...], right[...], TN)
            if not direct:
                outs[0][index] = found.astype(BF)
                continue

            def into(ref, index=index):
                def store(place, piece):
                    ref[(*place, index)] = piece

                return store

            store_spread(places, each, at_ref[0], found, 0, into(outs[0]), into(outs[1]))

    hidden = pl.BlockSpec((count, wide), lambda i, *_: (0, i))
    if direct:
        shapes = [(*lead, 3, each, units)] * 2
        spec = [pl.BlockSpec((*lead, 3, each, wide), lambda i, *_: (0,) * 5 + (i,))] * 2
    else:
        shapes = [(3, width, units)]
        spec = [pl.BlockSpec((3, width, wide), lambda i, *_: (0, 0, i))]
    out = call(
        body,
        (units // wide,),
        [whole(rows.shape), whole(grads.shape), hidden, hidden, hidden],
        spec,
        [sds(shape, BF) for shape in shapes],
        (core_at, rows, grads, dg, du, hid),
        prefetch=1,
        flops=6 * count * width * units,
    )
    if direct:
        return out
    found = [spread(out[0][i], sizes, names, core_at) for i in range(3)]
    return [jnp.stack([part[side] for part in found], axis=3) for side in range(2)]


def tall_weight_grads(lefts, rights, extras, sizes, core_at):
    names = ("y", "z", "x")
    lead = tuple(sizes[n] for n in names)
    places = spread_places(sizes, names)
    width = sum(left.shape[1] for left in lefts)
    cols = sum(right.shape[1] for right in rights)
    each = width // len(places)
    direct = each % 8 == 0
    flops = 2 * lefts[0].shape[0] * width * cols

    def body(at_ref, *refs):
        left_refs = refs[: len(lefts)]
        right_refs = refs[len(lefts) : len(lefts) + len(rights)]
        rest = refs[len(lefts) + len(rights) :]
        extra_refs, outs = rest[: len(extras)], rest[len(extras) :]

        def save(row, found, col):
            span = found.shape[1]
            if not direct:
                outs[0][row : row + found.shape[0], col : col + span] = found.astype(BF)
                return

            def into(ref):
                def store(place, piece):
                    ref[(*place, slice(None), slice(col, col + span))] = piece

                return store

            store_spread(places, each, at_ref[0], found, row, into(outs[0]), into(outs[1]))

        row = 0
        for left in left_refs:
            col = 0
            for right in right_refs:
                save(row, mm(left[...], right[...], TN), col)
                col += right.shape[1]
            row += left.shape[1]
        more = extra_refs[0][...]
        for extra in extra_refs[1:]:
            more = more + extra[...]
        save(0, more, cols)

    args = (*lefts, *rights, *extras)
    shapes = [(*lead, each, cols + 128)] * 2 if direct else [(width, cols + 128)]
    out = call(
        body,
        (1,),
        [whole(a.shape) for a in args],
        [whole(shape) for shape in shapes],
        [sds(shape, BF) for shape in shapes],
        (core_at, *args),
        prefetch=1,
        flops=flops,
    )
    return out if direct else spread(out[0], sizes, names, core_at)


def scatter_sum(value, name):
    return lax.psum_scatter(value, name, scatter_dimension=0, tiled=False)


def swap_all(value, names):
    return lax.all_to_all(value, names, 0, 0, tiled=True)


def at_index(value, index):
    return lax.dynamic_index_in_dim(value, index, 0, keepdims=False)


def fold(value, name):
    if lax.axis_size(name) != 2:
        return scatter_sum(value, name)
    at = lax.axis_index(name)
    got = lax.ppermute(at_index(value, 1 - at), name, [(0, 1), (1, 0)])
    return (at_index(value, at).astype(F32) + got.astype(F32)).astype(BF)


def join(keep, give, name):
    got = lax.ppermute(give, name, [(0, 1), (1, 0)])
    return (keep.astype(F32) + got.astype(F32)).astype(BF)


def swap_by_steps(value, name):
    size, at = value.shape[0], lax.axis_index(name)
    found = [at_index(value, at)]
    for step in range(1, size):
        sent = at_index(value, (at + step) % size)
        found.append(lax.ppermute(sent, name, [(i, (i + step) % size) for i in range(size)]))
    return found


def after(value, *others):
    return lax.optimization_barrier((value, *others))[0]


def on_device(
    tokens,
    segments,
    routes,
    slots,
    cotangent,
    attn_gain,
    w_qkv,
    w_out,
    ffn_gain,
    w_router,
    shared_gate,
    shared_up,
    shared_down,
    expert_gate,
    expert_up,
    expert_down,
):
    sizes = {name: lax.axis_size(name) for name in ("y", "core", "z", "x")}
    ranks = ("z", "x")
    seqs, span, width = tokens.shape
    blocks, parts = sizes["z"], sizes["x"]
    experts = blocks * parts
    count = seqs * span
    capacity = 3 * count // experts
    length = span * experts
    group = width // parts
    z_at, x_at = lax.axis_index("z"), lax.axis_index("x")
    own = (z_at * parts + x_at).astype(jnp.int32).reshape(1)
    z_ref, x_ref = z_at.astype(jnp.int32).reshape(1), x_at.astype(jnp.int32).reshape(1)
    core_ref = lax.axis_index("core").astype(jnp.int32).reshape(1)
    attn_scale = attn_gain.astype(F32).reshape(1, width)
    ffn_scale = ffn_gain.astype(F32).reshape(1, width)
    flat_tokens = tokens.reshape(count, width)
    flat_cot = cotangent.reshape(count, width)

    route_rows = routes.reshape(count, 2)
    slot_rows = slots.reshape(count, 2)
    target = jnp.where(slot_rows >= 0, route_rows * capacity + slot_rows, -1)
    target_rows = jnp.transpose(target)
    grad_sent = dispatch(flat_cot, target_rows, experts, capacity, jnp.transpose(route_rows))

    frequency = jnp.power(10000.0, -2.0 * jnp.arange(32, dtype=F32) / HEAD_DIM)
    angles = jnp.arange(length, dtype=jnp.int32).astype(F32)[:, None] * jnp.tile(frequency, 4)
    sign = jnp.where(jnp.arange(128) % 64 < 32, -1.0, 1.0)
    cosine, sine = jnp.cos(angles), jnp.sin(angles) * sign
    seg_row = lax.dynamic_slice_in_dim(segments, z_at, 1, 0)
    seg_col = seg_row.reshape(length, 1)
    fused = group % 128 == 0
    if fused:
        weights = [w_qkv] * 3
    else:
        picked = w_qkv.reshape(width, 3, parts, group)
        picked = lax.dynamic_index_in_dim(picked, x_at, 2, keepdims=False)
        weights = [picked.reshape(width, 3 * group)]

    by_seq = swap_all(tokens, "z")
    by_seq, cosine, sine, seg_col, grad_sent = lax.optimization_barrier(
        (by_seq, cosine, sine, seg_col, grad_sent)
    )
    if parts == 2:
        rows = [by_seq, lax.ppermute(by_seq, "x", [(0, 1), (1, 0)])]
    else:
        rows = [lax.all_gather(by_seq, "x", axis=0, tiled=False)]
    *rows, grad_sent = lax.optimization_barrier((*rows, grad_sent))
    grad_came = swap_all(grad_sent, ranks)

    qkv, normed = project(rows, attn_scale, weights, group, cosine, sine, x_ref, parts)
    attended, lse = (attend if fused else plain_attend)(qkv, seg_row, seg_col)
    attended = after(attended, grad_came)
    attended = swap_all(attended.reshape(experts, span, group), ranks)
    attended = attended.reshape(seqs, parts, span, group)

    hidden, branch_in = after_attention(flat_tokens, attended, w_out, ffn_scale)
    sent = dispatch(branch_in, target_rows, experts, capacity)
    received = swap_all(sent, ranks).reshape(-1, width)

    shared_out, shared_back, hid, dg, du = feed_forward(
        after(branch_in, sent), flat_cot, shared_gate, shared_up, shared_down
    )
    keep, give = shared_weight_grads(branch_in, flat_cot, dg, du, hid, sizes, core_ref)
    shared_sums = fold(join(keep, give, "core"), "y")
    grad_rows = grad_came[:, :capacity, :].reshape(-1, width)
    other = grad_came[:, capacity, :capacity].astype(jnp.int32).reshape(-1, 1)
    received = after(received, give, grad_rows, other)

    router = jnp.pad(w_router, ((0, 0), (0, 128 - experts)))
    made, made_back, hid, dg, du, gated_grads, grad_logits = feed_forward(
        received, grad_rows, expert_gate[0], expert_up[0], expert_down[0], router, other, own
    )
    back_rows = swap_all(made_back.reshape(experts, capacity, width), ranks).reshape(-1, width)
    keep, give, grad_router = expert_weight_grads(
        received, gated_grads, dg, du, hid, grad_logits, sizes, core_ref
    )
    back_rows = after(back_rows, give)
    expert_sums = fold(join(keep, give, "core"), "y")
    shared_sums = fold(shared_sums, "x")

    grad_hidden, grad_attn, grad_att, grad_ffn = middle_back(
        hidden, shared_back, back_rows, target, flat_cot, ffn_scale, w_out, parts, span
    )
    grad_att = swap_all(grad_att.reshape(experts, span, group), ranks).reshape(length, group)

    column = lax.broadcasted_iota(jnp.int32, (width, 128), 1)
    small = jnp.where(column < experts, grad_router, jnp.where(column == experts, grad_ffn, 0.0))
    out_sums = tall_weight_grads(
        [attended[:, part].reshape(count, group) for part in range(parts)],
        [grad_attn],
        [small],
        sizes,
        core_ref,
    )
    out_sums = fold(join(*out_sums, "core"), "y")

    made = after(made, grad_att)
    made_rows = swap_all(made.reshape(experts, capacity, width), ranks).reshape(-1, width)
    grads = (attend_back if fused else plain_attend_back)(
        qkv, grad_att, lse, seg_row, seg_col, cosine, sine
    )
    normed_back, grad_gain = project_back(grads, weights, rows, x_ref, parts)
    normed_back = fold(normed_back, "x")
    pieces = swap_by_steps(normed_back, "z")

    qkv_sums = tall_weight_grads([normed], list(grads), [grad_gain], sizes, core_ref)
    qkv_sums = fold(join(*qkv_sums, "core"), "y")
    token_grad = first_norm_back(flat_tokens, attn_scale, pieces, grad_hidden, z_ref)
    layer_out = layer_end(hidden, shared_out, made_rows, target).reshape(tokens.shape)

    shared_sums = swap_by_steps(after(shared_sums, *pieces), "z")
    last = after(jnp.concatenate([out_sums, qkv_sums], axis=-1), made_rows)
    each, cols = last.shape[-2:]
    last = swap_all(last.reshape(experts, each, cols), ranks).astype(F32)
    last = jnp.sum(last.reshape(blocks, parts, each, cols), axis=0)
    out_sums = jnp.sum(last[:, :, : width + 128], axis=0)
    qkv_sums = last[:, :, width + 128 :]
    grad_attn_gain = jnp.sum(qkv_sums[:, :, 3 * group], axis=0)
    grad_w_qkv = qkv_sums[:, :, : 3 * group].reshape(parts, each, 3, group)
    grad_w_qkv = jnp.transpose(grad_w_qkv, (1, 2, 0, 3)).reshape(each, 3 * width)

    shared_sums = sum(part.astype(F32) for part in shared_sums)
    expert_sums = expert_sums.astype(F32)
    return (
        layer_out,
        token_grad.reshape(tokens.shape),
        grad_attn_gain,
        grad_w_qkv,
        out_sums[:, :width],
        out_sums[:, width + experts],
        out_sums[:, width : width + experts],
        shared_sums[0],
        shared_sums[1],
        jnp.transpose(shared_sums[2]),
        expert_sums[0][None],
        expert_sums[1][None],
        jnp.transpose(expert_sums[2])[None],
    )


def solution(mesh):
    dp, experts = mesh.shape["dp"], mesh.shape["expert"]

    def step(*args):
        seqs = args[0].shape[0] // dp
        cores = 2 if dp % 2 == 0 else 1
        fine = Mesh(
            mesh.devices.reshape(dp // cores, cores, seqs, experts // seqs),
            ("y", "core", "z", "x"),
        )
        data, ranks, every = ("y", "core"), ("z", "x"), ("y", "core", "z", "x")
        placed = (
            P(data, ranks, None),
            P(data, None),
            P(data, ranks, None),
            P(data, ranks, None),
            P(data, ranks, None),
            *([P()] * 8),
            P(ranks, None, None),
            P(ranks, None, None),
            P(ranks, None, None),
        )
        return jax.shard_map(
            on_device,
            mesh=fine,
            in_specs=placed,
            out_specs=(
                P(data, ranks, None),
                P(data, ranks, None),
                P(every),
                P(every, None),
                P(every, None),
                P(every),
                P(every, None),
                P(every, None),
                P(every, None),
                P(None, every),
                P(ranks, None, data),
                P(ranks, None, data),
                P(ranks, data, None),
            ),
            check_vma=False,
        )(*args)

    return step
```

```python
import jax
import jax.numpy as jnp
from jax import lax
from jax.experimental import pallas as pl
from jax.experimental.pallas import tpu as pltpu
from jax.sharding import Mesh
from jax.sharding import PartitionSpec as P

HEAD_DIM = 64
EPS = 1e-06
BF = jnp.bfloat16
F32 = jnp.float32
NEG = -1e30
NN = (((1,), (0,)), ((), ()))
NT = (((1,), (1,)), ((), ()))
TN = (((0,), (0,)), ((), ()))
VMEM_MOST = 60 << 20


def mm(left, right, dims=NN):
    return lax.dot_general(left, right, dims, preferred_element_type=F32)


def sds(shape, dtype):
    return jax.ShapeDtypeStruct(shape, dtype)


def call(body, grid, in_specs, out_specs, out_shape, args, scratch=(), prefetch=0, flops=0):
    leaves = jax.tree.leaves(out_shape)
    moved = sum(a.size * a.dtype.itemsize for a in args) + sum(
        a.size * a.dtype.itemsize for a in leaves
    )
    return pl.pallas_call(
        body,
        out_shape=out_shape,
        grid_spec=pltpu.PrefetchScalarGridSpec(
            num_scalar_prefetch=prefetch,
            grid=grid,
            in_specs=in_specs,
            out_specs=out_specs,
            scratch_shapes=list(scratch),
        ),
        compiler_params=pltpu.CompilerParams(
            dimension_semantics=("arbitrary",) * len(grid), vmem_limit_bytes=VMEM_MOST
        ),
        cost_estimate=pl.CostEstimate(
            flops=int(flops), transcendentals=0, bytes_accessed=int(moved)
        ),
    )(*args)


def whole(shape):
    rank = len(shape)
    return pl.BlockSpec(tuple(shape), lambda *_: (0,) * rank)


def swap_halves(value):
    lane = lax.broadcasted_iota(jnp.int32, value.shape, 1)
    return jnp.where(lane % 64 < 32, pltpu.roll(value, 96, 1), pltpu.roll(value, 32, 1))


def rms(values):
    return lax.rsqrt(jnp.mean(values * values, axis=1, keepdims=True) + EPS)


def row_specs(rows):
    if len(rows) == 2:
        _, span, width = rows[0].shape
        return [pl.BlockSpec((1, span, width), lambda i, *_: (i, 0, 0))] * 2
    parts, _, span, width = rows[0].shape
    return [pl.BlockSpec((parts, 1, span, width), lambda i, *_: (0, i, 0, 0))]


def load_rows(refs, at_ref):
    if len(refs) == 2:
        mine, theirs = refs[0][0].astype(F32), refs[1][0].astype(F32)
        first = at_ref[0] == 0
        pair = [jnp.where(first, mine, theirs), jnp.where(first, theirs, mine)]
        return jnp.concatenate(pair, axis=0)
    value = refs[0][...]
    return value.reshape(value.shape[0] * value.shape[2], value.shape[3]).astype(F32)


def weight_specs(weights, group):
    if len(weights) == 1:
        return [whole(weights[0].shape)]
    width, cols = weights[0].shape
    parts = cols // (3 * group)

    def spec(index):
        return pl.BlockSpec((width, group), lambda i, at: (0, index * parts + at[0]))

    return [spec(index) for index in range(3)]


def load_weights(refs, group):
    if len(refs) == 3:
        return [ref[...] for ref in refs]
    return [refs[0][:, at * group : (at + 1) * group] for at in range(3)]


def project(rows, gain, weights, group, cosine, sine, x_at, parts):
    blocks, span, width = rows[0].shape[-3:]
    height = parts * span
    length = height * blocks
    cut = len(rows)

    def body(at_ref, *refs):
        r_refs, (g_ref, c_ref, s_ref) = refs[:cut], refs[cut : cut + 3]
        w_refs, (qkv_ref, n_ref) = refs[cut + 3 : -2], refs[-2:]
        tok = load_rows(r_refs, at_ref)
        normed = (tok * rms(tok) * g_ref[...]).astype(BF)
        n_ref[...] = normed
        if len(w_refs) == 3:
            found = [mm(normed, ref[...]) for ref in w_refs]
            turning = [(found[0], 0), (found[1], group)]
            last = found[2]
        else:
            found = mm(normed, w_refs[0][...])
            turning, last = [(found[:, : 2 * group], 0)], found[:, 2 * group :]
        for value, base in turning:
            for at in range(0, value.shape[1], 128):
                part = value[:, at : at + 128]
                lane = lax.broadcasted_iota(jnp.int32, part.shape, 1) + (base + at)
                turned = part * c_ref[...] + swap_halves(part) * s_ref[...]
                turned = turned * jnp.where(lane < group, HEAD_DIM**-0.5, 1.0)
                qkv_ref[:, base + at : base + at + 128] = turned.astype(BF)
        qkv_ref[:, 2 * group :] = last.astype(BF)

    return call(
        body,
        (blocks,),
        [
            *row_specs(rows),
            whole((1, width)),
            pl.BlockSpec((height, 128), lambda i, *_: (i, 0)),
            pl.BlockSpec((height, 128), lambda i, *_: (i, 0)),
            *weight_specs(weights, group),
        ],
        [
            pl.BlockSpec((height, 3 * group), lambda i, *_: (i, 0)),
            pl.BlockSpec((height, width), lambda i, *_: (i, 0)),
        ],
        [sds((length, 3 * group), BF), sds((length, width), BF)],
        (x_at, *rows, gain, cosine, sine, *weights),
        prefetch=1,
        flops=6 * length * width * group,
    )


def project_back(grads, weights, rows, x_at, parts):
    blocks, span, width = rows[0].shape[-3:]
    group = grads[0].shape[1]
    height = parts * span
    length = height * blocks
    cut = len(rows)

    def body(at_ref, q_ref, k_ref, v_ref, *refs):
        r_refs, w_refs, (out_ref, gain_ref, acc_ref) = refs[:cut], refs[cut:-3], refs[-3:]
        step = pl.program_id(0)
        w_q, w_k, w_v = load_weights(w_refs, group)
        back = mm(q_ref[...], w_q, NT) + mm(k_ref[...], w_k, NT) + mm(v_ref[...], w_v, NT)
        tok = load_rows(r_refs, at_ref)
        part = jnp.sum(back * tok * rms(tok), axis=0, keepdims=True)

        @pl.when(step == 0)
        def _():
            acc_ref[...] = jnp.zeros_like(acc_ref)

        acc_ref[...] += jnp.broadcast_to(part, acc_ref.shape)
        out_ref[...] = back.astype(BF).reshape(parts, 1, span, width)

        @pl.when(step == blocks - 1)
        def _():
            column = jnp.transpose(acc_ref[...])
            gain_ref[...] = jnp.broadcast_to(column[:, :1], gain_ref.shape)

    block = pl.BlockSpec((height, group), lambda i, *_: (i, 0))
    return call(
        body,
        (blocks,),
        [block, block, block, *row_specs(rows), *weight_specs(weights, group)],
        [
            pl.BlockSpec((parts, 1, span, width), lambda i, *_: (0, i, 0, 0)),
            whole((width, 128)),
        ],
        [sds((parts, blocks, span, width), BF), sds((width, 128), F32)],
        (x_at, *grads, *rows, *weights),
        scratch=[pltpu.VMEM((8, width), F32)],
        prefetch=1,
        flops=6 * length * width * group,
    )


def attend(qkv, seg_row, seg_col):
    length, cols = qkv.shape
    group = cols // 3
    pairs = group // 128
    high = min(256, length)

    def body(q_ref, k_ref, v_ref, sr_ref, sc_ref, o_ref, l_ref):
        lane = lax.broadcasted_iota(jnp.int32, (high, 128), 1)
        for at in range(0, length, high):
            end = at + high
            query = q_ref[at:end, :]
            keys = k_ref[:end, :]
            vals = v_ref[:end, :]
            q_pos = lax.broadcasted_iota(jnp.int32, (high, end), 0) + at
            k_pos = lax.broadcasted_iota(jnp.int32, (high, end), 1)
            allowed = (sc_ref[at:end, :] == sr_ref[:, :end]) & (k_pos <= q_pos)
            outs = []
            for head in range(2):
                mine = (lane // 64) == head
                scores = mm(jnp.where(mine, query, jnp.zeros_like(query)), keys, NT)
                scores = jnp.where(allowed, scores, NEG)
                most = jnp.max(scores, axis=1, keepdims=True)
                expo = jnp.exp(scores - most)
                total = jnp.sum(expo, axis=1, keepdims=True)
                outs.append(mm(expo.astype(BF), vals) / total)
                lse = jnp.broadcast_to(most + jnp.log(total), (high, 128))
                l_ref[0, head : head + 1, at:end] = jnp.transpose(lse)[:1, :]
            o_ref[at:end, :] = jnp.where(lane < 64, outs[0], outs[1]).astype(BF)

    def col(offset):
        return pl.BlockSpec((length, 128), lambda i: (0, offset * pairs + i))

    return call(
        body,
        (pairs,),
        [col(0), col(1), col(2), whole((1, length)), whole((length, 1))],
        [col(0), pl.BlockSpec((1, 2, length), lambda i: (i, 0, 0))],
        [sds((length, group), BF), sds((pairs, 2, length), F32)],
        (qkv, qkv, qkv, seg_row, seg_col),
        flops=4 * length * length * group,
    )


def attend_back(qkv, grad, lse, seg_row, seg_col, cosine, sine):
    length, cols = qkv.shape
    group = cols // 3
    pairs = group // 128
    high = min(256, length)

    def body(
        q_ref, k_ref, v_ref, g_ref, l_ref, sr_ref, sc_ref, c_ref, s_ref, dq_ref, dk_ref, dv_ref,
        ka_ref, va_ref,
    ):
        lane = lax.broadcasted_iota(jnp.int32, (high, 128), 1)
        ka_ref[...] = jnp.zeros_like(ka_ref)
        va_ref[...] = jnp.zeros_like(va_ref)
        for at in range(0, length, high):
            end = at + high
            query = q_ref[at:end, :]
            grads = g_ref[at:end, :]
            keys = k_ref[:end, :]
            vals = v_ref[:end, :]
            k_pos = lax.broadcasted_iota(jnp.int32, (end, high), 0)
            q_pos = lax.broadcasted_iota(jnp.int32, (end, high), 1) + at
            allowed = (sc_ref[:end, :] == sr_ref[:, at:end]) & (k_pos <= q_pos)
            outs = []
            for head in range(2):
                mine = (lane // 64) == head
                q_own = jnp.where(mine, query, jnp.zeros_like(query))
                g_own = jnp.where(mine, grads, jnp.zeros_like(grads))
                scores = jnp.where(allowed, mm(keys, q_own, NT), NEG)
                probs = jnp.exp(scores - l_ref[0, head : head + 1, at:end])
                grad_probs = mm(vals, g_own, NT)
                delta = jnp.sum(probs * grad_probs, axis=0, keepdims=True)
                grad_scores = (probs * (grad_probs - delta)).astype(BF)
                va_ref[:end, :] += mm(probs.astype(BF), g_own)
                ka_ref[:end, :] += mm(grad_scores, q_own)
                outs.append(mm(grad_scores, keys, TN))
            found = jnp.where(lane < 64, outs[0], outs[1]) * HEAD_DIM**-0.5
            back = found * c_ref[at:end, :] - swap_halves(found) * s_ref[at:end, :]
            dq_ref[at:end, :] = back.astype(BF)
        found = ka_ref[...]
        dk_ref[...] = (found * c_ref[...] - swap_halves(found) * s_ref[...]).astype(BF)
        dv_ref[...] = va_ref[...].astype(BF)

    def col(offset):
        return pl.BlockSpec((length, 128), lambda i: (0, offset * pairs + i))

    return call(
        body,
        (pairs,),
        [
            col(0),
            col(1),
            col(2),
            col(0),
            pl.BlockSpec((1, 2, length), lambda i: (i, 0, 0)),
            whole((1, length)),
            whole((length, 1)),
            whole((length, 128)),
            whole((length, 128)),
        ],
        [col(0), col(0), col(0)],
        [sds((length, group), BF)] * 3,
        (qkv, qkv, qkv, grad, lse, seg_row, seg_col, cosine, sine),
        scratch=[pltpu.VMEM((length, 128), F32)] * 2,
        flops=10 * length * length * group,
    )


def heads_of(flat):
    return flat.reshape(flat.shape[0], -1, HEAD_DIM)


def plain_mask(seg_row, seg_col):
    length = seg_col.shape[0]
    spots = jnp.arange(length, dtype=jnp.int32)
    return (seg_row == seg_col) & (spots[None, :] <= spots[:, None])


def plain_attend(qkv, seg_row, seg_col):
    query, keys, vals = (heads_of(part) for part in jnp.split(qkv, 3, axis=1))
    scores = jnp.einsum("qhd,khd->hqk", query, keys, preferred_element_type=F32)
    scores = jnp.where(plain_mask(seg_row, seg_col)[None], scores, NEG)
    lse = jax.nn.logsumexp(scores, axis=-1, keepdims=True)
    probs = jnp.exp(scores - lse).astype(BF)
    found = jnp.einsum("hqk,khd->qhd", probs, vals, preferred_element_type=F32)
    return found.astype(BF).reshape(qkv.shape[0], -1), lse


def plain_turn_back(grads, cosine, sine):
    table_c, table_s = cosine[:, None, :HEAD_DIM], sine[:, None, :HEAD_DIM]
    swapped = jnp.roll(grads, HEAD_DIM // 2, axis=-1)
    return (grads * table_c - swapped * table_s).astype(BF).reshape(grads.shape[0], -1)


def plain_attend_back(qkv, grad, lse, seg_row, seg_col, cosine, sine):
    query, keys, vals = (heads_of(part) for part in jnp.split(qkv, 3, axis=1))
    grad = heads_of(grad)
    scores = jnp.einsum("qhd,khd->hqk", query, keys, preferred_element_type=F32)
    scores = jnp.where(plain_mask(seg_row, seg_col)[None], scores, NEG)
    probs = jnp.exp(scores - lse)
    grad_probs = jnp.einsum("qhd,khd->hqk", grad, vals, preferred_element_type=F32)
    delta = jnp.sum(probs * grad_probs, axis=-1, keepdims=True)
    grad_scores = (probs * (grad_probs - delta)).astype(BF)
    gq = jnp.einsum("hqk,khd->qhd", grad_scores, keys, preferred_element_type=F32)
    gk = jnp.einsum("hqk,qhd->khd", grad_scores, query, preferred_element_type=F32)
    gv = jnp.einsum("hqk,qhd->khd", probs.astype(BF), grad, preferred_element_type=F32)
    return (
        plain_turn_back(gq * HEAD_DIM**-0.5, cosine, sine),
        plain_turn_back(gk, cosine, sine),
        gv.astype(BF).reshape(qkv.shape[0], -1),
    )


def after_attention(tokens, attended, w_out, gain):
    seqs, parts, span, group = attended.shape
    count, width = tokens.shape

    def body(t_ref, a_ref, w_ref, g_ref, h_ref, b_ref):
        hidden = t_ref[...].astype(F32)
        for part in range(parts):
            rows = a_ref[:, part].reshape(count, group)
            hidden += mm(rows, w_ref[part * group : (part + 1) * group, :])
        h_ref[...] = hidden
        b_ref[...] = (hidden * rms(hidden) * g_ref[...]).astype(BF)

    return call(
        body,
        (1,),
        [whole(a.shape) for a in (tokens, attended, w_out, gain)],
        [whole(tokens.shape)] * 2,
        [sds(tokens.shape, F32), sds(tokens.shape, BF)],
        (tokens, attended, w_out, gain),
        flops=2 * count * width * width,
    )


def dispatch(rows, target_rows, experts, capacity, route_rows=None):
    count, width = rows.shape
    more = 0 if route_rows is None else 16
    tables = () if route_rows is None else (route_rows,)

    def body(r_ref, t_ref, *refs):
        o_ref = refs[-1]
        slot = lax.broadcasted_iota(jnp.int32, (capacity, count), 0)
        slot += pl.program_id(0) * capacity
        hits = [slot == t_ref[k : k + 1, :] for k in range(2)]
        hot = (hits[0] | hits[1]).astype(F32).astype(BF)
        o_ref[0, :capacity, :] = mm(hot, r_ref[...]).astype(BF)
        if more:
            o_ref[0, capacity:, :] = jnp.zeros((more, width), BF)
            other = jnp.zeros((8, capacity), F32)
            for k in range(2):
                route = jnp.broadcast_to(refs[0][1 - k : 2 - k, :].astype(F32), (8, count))
                other += mm(route.astype(BF), hits[k].astype(F32).astype(BF), NT)
            o_ref[0, capacity : capacity + 8, :capacity] = other.astype(BF)

    return call(
        body,
        (experts,),
        [whole(a.shape) for a in (rows, target_rows, *tables)],
        pl.BlockSpec((1, capacity + more, width), lambda i: (i, 0, 0)),
        sds((experts, capacity + more, width), BF),
        (rows, target_rows, *tables),
        flops=2 * experts * capacity * count * width,
    )


def pick(target, row_refs):
    total = None
    for index, ref in enumerate(row_refs):
        rows = ref[...]
        spot = lax.broadcasted_iota(jnp.int32, (target.shape[0], rows.shape[0]), 1)
        one, two = target[:, 2 * index : 2 * index + 1], target[:, 2 * index + 1 : 2 * index + 2]
        found = mm(((spot == one) | (spot == two)).astype(F32).astype(BF), rows)
        total = found if total is None else total + found
    return total


def layer_end(hidden, shared_out, rows, target):
    count, width = hidden.shape
    high = count // 2

    def body(h_ref, s_ref, t_ref, *refs):
        refs[-1][...] = (h_ref[...] + s_ref[...] + pick(t_ref[...], refs[:-1])).astype(BF)

    block = pl.BlockSpec((high, width), lambda i: (i, 0))
    return call(
        body,
        (2,),
        [
            block,
            block,
            pl.BlockSpec((high, target.shape[1]), lambda i: (i, 0)),
            *[whole(part.shape) for part in rows],
        ],
        block,
        sds(hidden.shape, BF),
        (hidden, shared_out, target, *rows),
        flops=2 * count * width * rows[0].shape[0] * len(rows),
    )


def middle_back(hidden, grad_shared, rows, target, cotangent, gain, w_out, parts, span):
    count, width = hidden.shape
    seqs = count // span
    each = 2 if seqs % 2 == 0 else 1
    high = each * span
    steps = count // high
    group = width // parts

    def body(h_ref, s_ref, t_ref, c_ref, g_ref, w_ref, *refs):
        gh_ref, ga_ref, d_ref, n_ref, acc_ref = refs[len(rows) :]
        step = pl.program_id(0)
        branch = s_ref[...] + pick(t_ref[...], refs[: len(rows)])
        hidden = h_ref[...]
        scale = rms(hidden)
        weighted = branch * g_ref[...]
        inner = jnp.mean(weighted * hidden, axis=1, keepdims=True)
        part = jnp.sum(branch * hidden * scale, axis=0, keepdims=True)
        out = c_ref[...].astype(F32) + scale * weighted - hidden * (scale * scale * scale * inner)
        gh_ref[...] = out
        out = out.astype(BF)
        ga_ref[...] = out
        for at in range(parts):
            sent = mm(out, w_ref[at * group : (at + 1) * group, :], NT).astype(BF)
            d_ref[:, at] = sent.reshape(each, span, group)

        @pl.when(step == 0)
        def _():
            acc_ref[...] = jnp.zeros_like(acc_ref)

        acc_ref[...] += jnp.broadcast_to(part, acc_ref.shape)

        @pl.when(step == steps - 1)
        def _():
            column = jnp.transpose(acc_ref[...])
            n_ref[...] = jnp.broadcast_to(column[:, :1], n_ref.shape)

    block = pl.BlockSpec((high, width), lambda i: (i, 0))
    return call(
        body,
        (steps,),
        [
            block,
            block,
            pl.BlockSpec((high, target.shape[1]), lambda i: (i, 0)),
            block,
            whole(gain.shape),
            whole(w_out.shape),
            *[whole(part.shape) for part in rows],
        ],
        [
            block,
            block,
            pl.BlockSpec((each, parts, span, group), lambda i: (i, 0, 0, 0)),
            whole((width, 128)),
        ],
        [
            sds(hidden.shape, F32),
            sds(hidden.shape, BF),
            sds((seqs, parts, span, group), BF),
            sds((width, 128), F32),
        ],
        (hidden, grad_shared, target, cotangent, gain, w_out, *rows),
        scratch=[pltpu.VMEM((8, width), F32)],
        flops=2 * count * width * (rows[0].shape[0] * len(rows) + width),
    )


def first_norm_back(tokens, gain, pieces, grad_hidden, z_at):
    count, width = tokens.shape
    blocks = len(pieces)
    span = count // blocks

    def body(at_ref, t_ref, g_ref, h_ref, *refs):
        o_ref = refs[-1]
        for index in range(blocks):
            seq = (at_ref[0] + blocks - index) % blocks
            spot = pl.ds(pl.multiple_of(seq * span, span), span)
            tok = t_ref[spot, :].astype(F32)
            scale = rms(tok)
            weighted = refs[index][...].astype(F32) * g_ref[...]
            inner = jnp.mean(weighted * tok, axis=1, keepdims=True)
            out = h_ref[spot, :] + scale * weighted - tok * (scale * scale * scale * inner)
            o_ref[spot, :] = out.astype(BF)

    return call(
        body,
        (1,),
        [whole(a.shape) for a in (tokens, gain, grad_hidden, *pieces)],
        whole(tokens.shape),
        sds(tokens.shape, BF),
        (z_at, tokens, gain, grad_hidden, *pieces),
        prefetch=1,
    )


def feed_forward(rows, grads, w_gate, w_up, w_down, router=None, other=None, own=None):
    count, width = rows.shape
    units = w_gate.shape[1]
    wide = 512
    steps = units // wide
    high = 256
    gated = router is not None
    kind = BF if gated else F32

    def body(*refs):
        if gated:
            (own_ref, x_ref, g_ref, wg_ref, wu_ref, wd_ref, wr_ref, ot_ref,
             y_ref, gi_ref, hid_ref, dg_ref, du_ref, eo_ref, gl_ref, ya_ref, ga_ref, gate_ref) = refs
        else:
            (x_ref, g_ref, wg_ref, wu_ref, wd_ref,
             y_ref, gi_ref, hid_ref, dg_ref, du_ref, ya_ref, ga_ref) = refs
        step = pl.program_id(0)

        if gated:

            @pl.when(step == 0)
            def _():
                logits = mm(x_ref[...], wr_ref[...])
                lane = lax.broadcasted_iota(jnp.int32, logits.shape, 1)
                mine = jnp.sum(jnp.where(lane == own_ref[0], logits, 0.0), axis=1, keepdims=True)
                theirs = jnp.sum(jnp.where(lane == ot_ref[...], logits, 0.0), axis=1, keepdims=True)
                gate = 1.0 / (1.0 + jnp.exp(theirs - mine))
                rest = 1.0 / (1.0 + jnp.exp(mine - theirs))
                gate_ref[:, 0:1] = gate
                gate_ref[:, 1:2] = rest
                eo_ref[...] = (g_ref[...].astype(F32) * gate).astype(BF)

        def rows_at(index, carry):
            at = pl.ds(pl.multiple_of(index * high, high), high)
            row = x_ref[at, :]
            grad = eo_ref[at, :] if gated else g_ref[at, :]
            gval = mm(row, wg_ref[...])
            uval = mm(row, wu_ref[...])
            sigma = 1.0 / (1.0 + jnp.exp(-gval))
            silu = gval * sigma
            hid = (silu * uval).astype(BF)
            hid_ref[at, :] = hid
            grad_hid = mm(grad, wd_ref[...], NT)
            du = (grad_hid * silu).astype(BF)
            dg = (grad_hid * uval * sigma * (1.0 + gval * (1.0 - sigma))).astype(BF)
            du_ref[at, :] = du
            dg_ref[at, :] = dg
            out = mm(hid, wd_ref[...])
            back = mm(dg, wg_ref[...], NT) + mm(du, wu_ref[...], NT)

            @pl.when(step == 0)
            def _():
                ya_ref[at, :] = out
                ga_ref[at, :] = back

            @pl.when(step > 0)
            def _():
                ya_ref[at, :] += out
                ga_ref[at, :] += back

            return carry

        lax.fori_loop(0, count // high, rows_at, 0)

        @pl.when(step == steps - 1)
        def _():
            if gated:
                out = ya_ref[...]
                gate = gate_ref[:, 0:1]
                lean = jnp.sum(out * g_ref[...].astype(F32), axis=1, keepdims=True)
                lean = lean * gate * gate_ref[:, 1:2]
                lane = lax.broadcasted_iota(jnp.int32, (count, 128), 1)
                sign = (lane == own_ref[0]).astype(F32) - (lane == ot_ref[...]).astype(F32)
                grad_logits = (lean * sign).astype(BF)
                gl_ref[...] = grad_logits
                y_ref[...] = (out * gate).astype(BF)
                gi_ref[...] = (ga_ref[...] + mm(grad_logits, wr_ref[...], NT)).astype(BF)
            else:
                y_ref[...] = ya_ref[...]
                gi_ref[...] = ga_ref[...]

    full = whole((count, width))
    hidden = pl.BlockSpec((count, wide), lambda i, *_: (0, i))
    in_specs = [
        full,
        full,
        pl.BlockSpec((width, wide), lambda i, *_: (0, i)),
        pl.BlockSpec((width, wide), lambda i, *_: (0, i)),
        pl.BlockSpec((wide, width), lambda i, *_: (i, 0)),
    ]
    out_specs = [full, full, hidden, hidden, hidden]
    out_shape = [sds((count, width), kind)] * 2 + [sds((count, units), BF)] * 3
    scratch = [pltpu.VMEM((count, width), F32)] * 2
    args = [rows, grads, w_gate, w_up, w_down]
    if gated:
        in_specs += [whole(router.shape), whole(other.shape)]
        out_specs += [full, whole((count, 128))]
        out_shape += [sds((count, width), BF), sds((count, 128), BF)]
        scratch += [pltpu.VMEM((count, 128), F32)]
        args = [own, *args, router, other]
    return call(
        body,
        (steps,),
        in_specs,
        out_specs,
        out_shape,
        tuple(args),
        scratch=scratch,
        prefetch=1 if gated else 0,
        flops=12 * count * width * units,
    )


def expert_weight_grads(halves, sizes, core_at):
    outer, cores = sizes["y"], sizes["core"]
    count, width = halves[0][0].shape
    units = halves[0][2].shape[1]
    wide = units // (outer * cores)

    def body(at_ref, *refs):
        keep_ref, give_ref, r_ref = refs[-3:]
        groups = [refs[6 * at : 6 * at + 6] for at in range(len(halves))]
        step = pl.program_id(0)

        def over(left, right):
            return sum(mm(group[left][...], group[right][...], TN) for group in groups)

        found = [over(0, 2).astype(BF), over(0, 3).astype(BF), over(1, 4).astype(BF)]

        @pl.when(step < outer)
        def _():
            for index in range(3):
                give_ref[0, index] = found[index]

        @pl.when(step >= outer)
        def _():
            for index in range(3):
                keep_ref[0, index] = found[index]

        @pl.when(step == 0)
        def _():
            r_ref[...] = over(0, 5)

    def taken(i, at):
        core = jnp.where(i < outer, 1 - at[0], at[0])
        return (0, (i % outer) * cores + core)

    hidden = pl.BlockSpec((count, wide), taken)
    part = (1, 3, width, wide)
    return call(
        body,
        (outer * cores,),
        [
            whole((count, width)),
            whole((count, width)),
            hidden,
            hidden,
            hidden,
            whole((count, 128)),
        ]
        * len(halves),
        [
            pl.BlockSpec(part, lambda i, *_: (jnp.maximum(i - outer, 0), 0, 0, 0)),
            pl.BlockSpec(part, lambda i, *_: (jnp.minimum(i, outer - 1), 0, 0, 0)),
            whole((width, 128)),
        ],
        [sds((outer, *part[1:]), BF)] * 2 + [sds((width, 128), F32)],
        (core_at, *[value for half in halves for value in half]),
        prefetch=1,
        flops=6 * count * len(halves) * width * units,
    )


def spread_places(sizes, names):
    found = []
    for y in range(sizes["y"]):
        for core in range(sizes["core"]):
            for z in range(sizes["z"]):
                for x in range(sizes["x"]):
                    at = {"y": y, "core": core, "z": z, "x": x}
                    found.append((core, tuple(at[n] for n in names)))
    return found


def spread(value, sizes, names, core_at):
    order = ("y", "core", "z", "x")
    split = value.reshape(*(sizes[n] for n in order), -1, value.shape[-1])
    split = jnp.transpose(split, (1, *(order.index(n) for n in names), 4, 5))
    return at_index(split, core_at[0]), at_index(split, 1 - core_at[0])


def store_spread(places, each, core_at, found, row, keep, give):
    first = row // each
    for core in range(2):
        todo = [at for at in range(found.shape[0] // each) if places[first + at][0] == core]

        def put(store, todo=todo):
            for at in todo:
                store(places[first + at][1], found[at * each : (at + 1) * each].astype(BF))

        pl.when(core_at == core)(lambda put=put: put(keep))
        pl.when(core_at != core)(lambda put=put: put(give))


def shared_weight_grads(rows, grads, dg, du, hid, sizes, core_at):
    names = ("y", "x", "z")
    lead = tuple(sizes[n] for n in names)
    places = spread_places(sizes, names)
    count, width = rows.shape
    units = dg.shape[1]
    wide = 512
    each = width // len(places)
    direct = each % 8 == 0

    def body(at_ref, x_ref, g_ref, dg_ref, du_ref, hid_ref, *outs):
        pairs = ((x_ref, dg_ref), (x_ref, du_ref), (g_ref, hid_ref))
        for index, (left, right) in enumerate(pairs):
            found = mm(left[...], right[...], TN)
            if not direct:
                outs[0][index] = found.astype(BF)
                continue

            def into(ref, index=index):
                def store(place, piece):
                    ref[(*place, index)] = piece

                return store

            store_spread(places, each, at_ref[0], found, 0, into(outs[0]), into(outs[1]))

    hidden = pl.BlockSpec((count, wide), lambda i, *_: (0, i))
    if direct:
        shapes = [(*lead, 3, each, units)] * 2
        spec = [pl.BlockSpec((*lead, 3, each, wide), lambda i, *_: (0,) * 5 + (i,))] * 2
    else:
        shapes = [(3, width, units)]
        spec = [pl.BlockSpec((3, width, wide), lambda i, *_: (0, 0, i))]
    out = call(
        body,
        (units // wide,),
        [whole(rows.shape), whole(grads.shape), hidden, hidden, hidden],
        spec,
        [sds(shape, BF) for shape in shapes],
        (core_at, rows, grads, dg, du, hid),
        prefetch=1,
        flops=6 * count * width * units,
    )
    if direct:
        return out
    found = [spread(out[0][i], sizes, names, core_at) for i in range(3)]
    return [jnp.stack([part[side] for part in found], axis=3) for side in range(2)]


def tall_weight_grads(lefts, rights, extras, sizes, core_at):
    names = ("y", "z", "x")
    lead = tuple(sizes[n] for n in names)
    places = spread_places(sizes, names)
    width = sum(left.shape[1] for left in lefts)
    cols = sum(right.shape[1] for right in rights)
    each = width // len(places)
    direct = each % 8 == 0
    flops = 2 * lefts[0].shape[0] * width * cols

    def body(at_ref, *refs):
        left_refs = refs[: len(lefts)]
        right_refs = refs[len(lefts) : len(lefts) + len(rights)]
        rest = refs[len(lefts) + len(rights) :]
        extra_refs, outs = rest[: len(extras)], rest[len(extras) :]

        def save(row, found, col):
            span = found.shape[1]
            if not direct:
                outs[0][row : row + found.shape[0], col : col + span] = found.astype(BF)
                return

            def into(ref):
                def store(place, piece):
                    ref[(*place, slice(None), slice(col, col + span))] = piece

                return store

            store_spread(places, each, at_ref[0], found, row, into(outs[0]), into(outs[1]))

        row = 0
        for left in left_refs:
            col = 0
            for right in right_refs:
                save(row, mm(left[...], right[...], TN), col)
                col += right.shape[1]
            row += left.shape[1]
        more = extra_refs[0][...]
        for extra in extra_refs[1:]:
            more = more + extra[...]
        save(0, more, cols)

    args = (*lefts, *rights, *extras)
    shapes = [(*lead, each, cols + 128)] * 2 if direct else [(width, cols + 128)]
    out = call(
        body,
        (1,),
        [whole(a.shape) for a in args],
        [whole(shape) for shape in shapes],
        [sds(shape, BF) for shape in shapes],
        (core_at, *args),
        prefetch=1,
        flops=flops,
    )
    return out if direct else spread(out[0], sizes, names, core_at)


def scatter_sum(value, name):
    return lax.psum_scatter(value, name, scatter_dimension=0, tiled=False)


def swap_all(value, names):
    return lax.all_to_all(value, names, 0, 0, tiled=True)


def at_index(value, index):
    return lax.dynamic_index_in_dim(value, index, 0, keepdims=False)


def total(terms):
    return sum(term.astype(F32) for term in terms)


def both(keep, give):
    return [keep, lax.ppermute(give, "core", [(0, 1), (1, 0)])]


def fold(terms, name, *others):
    if lax.axis_size(name) != 2:
        sent = total(terms).astype(BF)
        if others:
            sent = after(sent, *others)
        return [scatter_sum(sent, name)], sent
    at = lax.axis_index(name)
    sent = total([at_index(term, 1 - at) for term in terms]).astype(BF)
    if others:
        sent = after(sent, *others)
    got = lax.ppermute(sent, name, [(0, 1), (1, 0)])
    return [at_index(term, at) for term in terms] + [got], sent


def swap_by_steps(value, name):
    size, at = value.shape[0], lax.axis_index(name)
    found = [at_index(value, at)]
    for step in range(1, size):
        sent = at_index(value, (at + step) % size)
        found.append(lax.ppermute(sent, name, [(i, (i + step) % size) for i in range(size)]))
    return found


def after(value, *others):
    return lax.optimization_barrier((value, *others))[0]


def on_device(
    tokens,
    segments,
    routes,
    slots,
    cotangent,
    attn_gain,
    w_qkv,
    w_out,
    ffn_gain,
    w_router,
    shared_gate,
    shared_up,
    shared_down,
    expert_gate,
    expert_up,
    expert_down,
):
    sizes = {name: lax.axis_size(name) for name in ("y", "core", "z", "x")}
    ranks = ("z", "x")
    seqs, span, width = tokens.shape
    blocks, parts = sizes["z"], sizes["x"]
    experts = blocks * parts
    count = seqs * span
    capacity = 3 * count // experts
    length = span * experts
    group = width // parts
    z_at, x_at = lax.axis_index("z"), lax.axis_index("x")
    own = (z_at * parts + x_at).astype(jnp.int32).reshape(1)
    z_ref, x_ref = z_at.astype(jnp.int32).reshape(1), x_at.astype(jnp.int32).reshape(1)
    core_ref = lax.axis_index("core").astype(jnp.int32).reshape(1)
    attn_scale = attn_gain.astype(F32).reshape(1, width)
    ffn_scale = ffn_gain.astype(F32).reshape(1, width)
    flat_tokens = tokens.reshape(count, width)
    flat_cot = cotangent.reshape(count, width)

    route_rows = routes.reshape(count, 2)
    slot_rows = slots.reshape(count, 2)
    half = capacity // 2
    targets = []
    for first in (0, half):
        here = (slot_rows >= first) & (slot_rows < first + half)
        targets.append(jnp.where(here, route_rows * half + slot_rows - first, -1))
    target_rows = [jnp.transpose(target) for target in targets]
    target = jnp.concatenate(targets, axis=1)
    route_flat = jnp.transpose(route_rows)
    grad_sent = [dispatch(flat_cot, to, experts, half, route_flat) for to in target_rows]

    frequency = jnp.power(10000.0, -2.0 * jnp.arange(32, dtype=F32) / HEAD_DIM)
    angles = jnp.arange(length, dtype=jnp.int32).astype(F32)[:, None] * jnp.tile(frequency, 4)
    sign = jnp.where(jnp.arange(128) % 64 < 32, -1.0, 1.0)
    cosine, sine = jnp.cos(angles), jnp.sin(angles) * sign
    seg_row = lax.dynamic_slice_in_dim(segments, z_at, 1, 0)
    seg_col = seg_row.reshape(length, 1)
    fused = group % 128 == 0
    if fused:
        weights = [w_qkv] * 3
    else:
        picked = w_qkv.reshape(width, 3, parts, group)
        picked = lax.dynamic_index_in_dim(picked, x_at, 2, keepdims=False)
        weights = [picked.reshape(width, 3 * group)]

    by_seq = swap_all(tokens, "z")
    by_seq, cosine, sine, seg_col, *grad_sent = lax.optimization_barrier(
        (by_seq, cosine, sine, seg_col, *grad_sent)
    )
    if parts == 2:
        rows = [by_seq, lax.ppermute(by_seq, "x", [(0, 1), (1, 0)])]
    else:
        rows = [lax.all_gather(by_seq, "x", axis=0, tiled=False)]
    *rows, grad_sent[0] = lax.optimization_barrier((*rows, grad_sent[0]))
    grad_came = [swap_all(grad_sent[0], ranks)]

    qkv, normed = project(rows, attn_scale, weights, group, cosine, sine, x_ref, parts)
    attended, lse = (attend if fused else plain_attend)(qkv, seg_row, seg_col)
    attended = after(attended, grad_came[0])
    attended = swap_all(attended.reshape(experts, span, group), ranks)
    attended, grad_sent[1] = lax.optimization_barrier((attended, grad_sent[1]))
    grad_came.append(swap_all(grad_sent[1], ranks))
    attended = attended.reshape(seqs, parts, span, group)

    hidden, branch_in = after_attention(flat_tokens, attended, w_out, ffn_scale)
    sent = [dispatch(branch_in, target_rows[0], experts, half)]
    sent.append(dispatch(after(branch_in, sent[0]), target_rows[1], experts, half))
    shared_out, shared_back, hid, dg, du = feed_forward(
        after(branch_in, sent[1]), flat_cot, shared_gate, shared_up, shared_down
    )
    sent[0] = after(sent[0], grad_came[1], shared_out)
    received = [swap_all(value, ranks).reshape(-1, width) for value in sent]
    keep, give = shared_weight_grads(branch_in, flat_cot, dg, du, hid, sizes, core_ref)
    shared_sums, shared_sent = fold(both(keep, give), "y")

    router = jnp.pad(w_router, ((0, 0), (0, 128 - experts)))
    made, back_rows, halves = [], [], []
    before = (give,)
    for at in range(2):
        grad_rows = grad_came[at][:, :half, :].reshape(-1, width)
        other = grad_came[at][:, half, :half].astype(jnp.int32).reshape(-1, 1)
        rows_at = after(received[at], grad_rows, other, *before)
        out, back, hid, dg, du, gated_grads, grad_logits = feed_forward(
            rows_at, grad_rows, expert_gate[0], expert_up[0], expert_down[0], router, other, own
        )
        made.append(out)
        back_rows.append(swap_all(back.reshape(experts, half, width), ranks).reshape(-1, width))
        halves.append((rows_at, gated_grads, dg, du, hid, grad_logits))
        before = (out,)
    halves[1] = (after(halves[1][0], back_rows[0], shared_sent), *halves[1][1:])
    keep, give, grad_router = expert_weight_grads(halves, sizes, core_ref)
    back_rows[1] = after(back_rows[1], give)
    expert_sums, expert_sent = fold(both(keep, give), "y")

    grad_hidden, grad_attn, grad_att, grad_ffn = middle_back(
        hidden, shared_back, back_rows, target, flat_cot, ffn_scale, w_out, parts, span
    )
    grad_att = swap_all(grad_att.reshape(experts, span, group), ranks).reshape(length, group)

    column = lax.broadcasted_iota(jnp.int32, (width, 128), 1)
    small = jnp.where(column < experts, grad_router, jnp.where(column == experts, grad_ffn, 0.0))
    out_sums = tall_weight_grads(
        [attended[:, part].reshape(count, group) for part in range(parts)],
        [grad_attn],
        [small],
        sizes,
        core_ref,
    )
    out_sums, _ = fold(both(*out_sums), "y")
    out_sums = total(out_sums).astype(BF)

    made_rows = []
    for value in made:
        value = after(value.reshape(experts, half, width), grad_att)
        made_rows.append(swap_all(value, ranks).reshape(-1, width))
    grads = list(
        (attend_back if fused else plain_attend_back)(
            qkv, grad_att, lse, seg_row, seg_col, cosine, sine
        )
    )
    shared_sums, _ = fold([after(term, grads[0]) for term in shared_sums], "x")
    grads[0] = after(grads[0], expert_sent)
    normed_back, grad_gain = project_back(grads, weights, rows, x_ref, parts)
    normed_back, _ = fold([normed_back], "x")
    pieces = swap_by_steps(total(normed_back).astype(BF), "z")

    qkv_sums = tall_weight_grads([normed], list(grads), [grad_gain], sizes, core_ref)
    qkv_sums, _ = fold(both(*qkv_sums), "y", expert_sums[-1])
    qkv_sums = total(qkv_sums).astype(BF)
    token_grad = first_norm_back(flat_tokens, attn_scale, pieces, grad_hidden, z_ref)
    layer_out = layer_end(hidden, shared_out, made_rows, target).reshape(tokens.shape)

    shared_sums = swap_by_steps(after(total(shared_sums).astype(BF), *pieces), "z")
    last = after(jnp.concatenate([out_sums, qkv_sums], axis=-1), *made_rows)
    each, cols = last.shape[-2:]
    last = swap_all(last.reshape(experts, each, cols), ranks).astype(F32)
    last = jnp.sum(last.reshape(blocks, parts, each, cols), axis=0)
    out_sums = jnp.sum(last[:, :, : width + 128], axis=0)
    qkv_sums = last[:, :, width + 128 :]
    grad_attn_gain = jnp.sum(qkv_sums[:, :, 3 * group], axis=0)
    grad_w_qkv = qkv_sums[:, :, : 3 * group].reshape(parts, each, 3, group)
    grad_w_qkv = jnp.transpose(grad_w_qkv, (1, 2, 0, 3)).reshape(each, 3 * width)

    shared_sums, expert_sums = total(shared_sums), total(expert_sums)
    return (
        layer_out,
        token_grad.reshape(tokens.shape),
        grad_attn_gain,
        grad_w_qkv,
        out_sums[:, :width],
        out_sums[:, width + experts],
        out_sums[:, width : width + experts],
        shared_sums[0],
        shared_sums[1],
        jnp.transpose(shared_sums[2]),
        expert_sums[0][None],
        expert_sums[1][None],
        jnp.transpose(expert_sums[2])[None],
    )


def solution(mesh):
    dp, experts = mesh.shape["dp"], mesh.shape["expert"]

    def step(*args):
        seqs = args[0].shape[0] // dp
        cores = 2 if dp % 2 == 0 else 1
        fine = Mesh(
            mesh.devices.reshape(dp // cores, cores, seqs, experts // seqs),
            ("y", "core", "z", "x"),
        )
        data, ranks, every = ("y", "core"), ("z", "x"), ("y", "core", "z", "x")
        placed = (
            P(data, ranks, None),
            P(data, None),
            P(data, ranks, None),
            P(data, ranks, None),
            P(data, ranks, None),
            *([P()] * 8),
            P(ranks, None, None),
            P(ranks, None, None),
            P(ranks, None, None),
        )
        return jax.shard_map(
            on_device,
            mesh=fine,
            in_specs=placed,
            out_specs=(
                P(data, ranks, None),
                P(data, ranks, None),
                P(every),
                P(every, None),
                P(every, None),
                P(every),
                P(every, None),
                P(every, None),
                P(every, None),
                P(None, every),
                P(ranks, None, data),
                P(ranks, None, data),
                P(ranks, data, None),
            ),
            check_vma=False,
        )(*args)

    return step
```

```python
import jax
import jax.numpy as jnp
from jax import lax
from jax.experimental import pallas as pl
from jax.experimental.pallas import tpu as pltpu
from jax.sharding import Mesh
from jax.sharding import PartitionSpec as P

HEAD_DIM = 64
EPS = 1e-06
BF = jnp.bfloat16
F32 = jnp.float32
NEG = -1e30
NN = (((1,), (0,)), ((), ()))
NT = (((1,), (1,)), ((), ()))
TN = (((0,), (0,)), ((), ()))
VMEM_MOST = 60 << 20
WEIGHT = 3


def mm(left, right, dims=NN):
    return lax.dot_general(left, right, dims, preferred_element_type=F32)


def sds(shape, dtype):
    return jax.ShapeDtypeStruct(shape, dtype)


def call(
    body, grid, in_specs, out_specs, out_shape, args, scratch=(), prefetch=0, flops=0, alias=None
):
    leaves = jax.tree.leaves(out_shape)
    moved = sum(a.size * a.dtype.itemsize for a in args) + sum(
        a.size * a.dtype.itemsize for a in leaves
    )
    return pl.pallas_call(
        body,
        out_shape=out_shape,
        grid_spec=pltpu.PrefetchScalarGridSpec(
            num_scalar_prefetch=prefetch,
            grid=grid,
            in_specs=in_specs,
            out_specs=out_specs,
            scratch_shapes=list(scratch),
        ),
        compiler_params=pltpu.CompilerParams(
            dimension_semantics=("arbitrary",) * len(grid), vmem_limit_bytes=VMEM_MOST
        ),
        cost_estimate=pl.CostEstimate(
            flops=int(flops), transcendentals=0, bytes_accessed=int(moved)
        ),
        input_output_aliases=alias or {},
    )(*args)


def whole(shape):
    rank = len(shape)
    return pl.BlockSpec(tuple(shape), lambda *_: (0,) * rank)


def swap_halves(value):
    lane = lax.broadcasted_iota(jnp.int32, value.shape, 1)
    return jnp.where(lane % 64 < 32, pltpu.roll(value, 96, 1), pltpu.roll(value, 32, 1))


def rms(values):
    return lax.rsqrt(jnp.mean(values * values, axis=1, keepdims=True) + EPS)


def row_specs(rows):
    if len(rows) == 2:
        _, span, width = rows[0].shape
        return [pl.BlockSpec((1, span, width), lambda i, *_: (i, 0, 0))] * 2
    parts, _, span, width = rows[0].shape
    return [pl.BlockSpec((parts, 1, span, width), lambda i, *_: (0, i, 0, 0))]


def load_rows(refs, at_ref):
    if len(refs) == 2:
        mine, theirs = refs[0][0].astype(F32), refs[1][0].astype(F32)
        first = at_ref[0] == 0
        pair = [jnp.where(first, mine, theirs), jnp.where(first, theirs, mine)]
        return jnp.concatenate(pair, axis=0)
    value = refs[0][...]
    return value.reshape(value.shape[0] * value.shape[2], value.shape[3]).astype(F32)


def weight_specs(weights, group):
    if len(weights) == 1:
        return [whole(weights[0].shape)]
    width, cols = weights[0].shape
    parts = cols // (3 * group)

    def spec(index):
        return pl.BlockSpec((width, group), lambda i, at: (0, index * parts + at[0]))

    return [spec(index) for index in range(3)]


def load_weights(refs, group):
    if len(refs) == 3:
        return [ref[...] for ref in refs]
    return [refs[0][:, at * group : (at + 1) * group] for at in range(3)]


def project(rows, gain, weights, group, cosine, sine, x_at, parts):
    blocks, span, width = rows[0].shape[-3:]
    height = parts * span
    length = height * blocks
    cut = len(rows)

    def body(at_ref, *refs):
        r_refs, (g_ref, c_ref, s_ref) = refs[:cut], refs[cut : cut + 3]
        w_refs, (qkv_ref, n_ref) = refs[cut + 3 : -2], refs[-2:]
        tok = load_rows(r_refs, at_ref)
        normed = (tok * rms(tok) * g_ref[...]).astype(BF)
        n_ref[...] = normed
        if len(w_refs) == 3:
            found = [mm(normed, ref[...]) for ref in w_refs]
            turning = [(found[0], 0), (found[1], group)]
            last = found[2]
        else:
            found = mm(normed, w_refs[0][...])
            turning, last = [(found[:, : 2 * group], 0)], found[:, 2 * group :]
        for value, base in turning:
            for at in range(0, value.shape[1], 128):
                part = value[:, at : at + 128]
                lane = lax.broadcasted_iota(jnp.int32, part.shape, 1) + (base + at)
                turned = part * c_ref[...] + swap_halves(part) * s_ref[...]
                turned = turned * jnp.where(lane < group, HEAD_DIM**-0.5, 1.0)
                qkv_ref[:, base + at : base + at + 128] = turned.astype(BF)
        qkv_ref[:, 2 * group :] = last.astype(BF)

    return call(
        body,
        (blocks,),
        [
            *row_specs(rows),
            whole((1, width)),
            pl.BlockSpec((height, 128), lambda i, *_: (i, 0)),
            pl.BlockSpec((height, 128), lambda i, *_: (i, 0)),
            *weight_specs(weights, group),
        ],
        [
            pl.BlockSpec((height, 3 * group), lambda i, *_: (i, 0)),
            pl.BlockSpec((height, width), lambda i, *_: (i, 0)),
        ],
        [sds((length, 3 * group), BF), sds((length, width), BF)],
        (x_at, *rows, gain, cosine, sine, *weights),
        prefetch=1,
        flops=6 * length * width * group,
    )


def project_back(grads, weights, rows, x_at, parts):
    blocks, span, width = rows[0].shape[-3:]
    group = grads[0].shape[1]
    height = parts * span
    length = height * blocks
    cut = len(rows)

    def body(at_ref, q_ref, k_ref, v_ref, *refs):
        r_refs, w_refs, (out_ref, gain_ref, acc_ref) = refs[:cut], refs[cut:-3], refs[-3:]
        step = pl.program_id(0)
        w_q, w_k, w_v = load_weights(w_refs, group)
        back = mm(q_ref[...], w_q, NT) + mm(k_ref[...], w_k, NT) + mm(v_ref[...], w_v, NT)
        tok = load_rows(r_refs, at_ref)
        part = jnp.sum(back * tok * rms(tok), axis=0, keepdims=True)

        @pl.when(step == 0)
        def _():
            acc_ref[...] = jnp.zeros_like(acc_ref)

        acc_ref[...] += jnp.broadcast_to(part, acc_ref.shape)
        out_ref[...] = back.astype(BF).reshape(parts, 1, span, width)

        @pl.when(step == blocks - 1)
        def _():
            column = jnp.transpose(acc_ref[...])
            gain_ref[...] = jnp.broadcast_to(column[:, :1], gain_ref.shape)

    block = pl.BlockSpec((height, group), lambda i, *_: (i, 0))
    return call(
        body,
        (blocks,),
        [block, block, block, *row_specs(rows), *weight_specs(weights, group)],
        [
            pl.BlockSpec((parts, 1, span, width), lambda i, *_: (0, i, 0, 0)),
            whole((width, 128)),
        ],
        [sds((parts, blocks, span, width), BF), sds((width, 128), F32)],
        (x_at, *grads, *rows, *weights),
        scratch=[pltpu.VMEM((8, width), F32)],
        prefetch=1,
        flops=6 * length * width * group,
    )


def attend(qkv, seg_row, seg_col):
    length, cols = qkv.shape
    group = cols // 3
    pairs = group // 128
    high = min(256, length)

    def body(q_ref, k_ref, v_ref, sr_ref, sc_ref, o_ref, l_ref):
        lane = lax.broadcasted_iota(jnp.int32, (high, 128), 1)
        for at in range(0, length, high):
            end = at + high
            query = q_ref[at:end, :]
            keys = k_ref[:end, :]
            vals = v_ref[:end, :]
            q_pos = lax.broadcasted_iota(jnp.int32, (high, end), 0) + at
            k_pos = lax.broadcasted_iota(jnp.int32, (high, end), 1)
            allowed = (sc_ref[at:end, :] == sr_ref[:, :end]) & (k_pos <= q_pos)
            outs = []
            for head in range(2):
                mine = (lane // 64) == head
                scores = mm(jnp.where(mine, query, jnp.zeros_like(query)), keys, NT)
                scores = jnp.where(allowed, scores, NEG)
                most = jnp.max(scores, axis=1, keepdims=True)
                expo = jnp.exp(scores - most)
                total = jnp.sum(expo, axis=1, keepdims=True)
                outs.append(mm(expo.astype(BF), vals) / total)
                lse = jnp.broadcast_to(most + jnp.log(total), (high, 128))
                l_ref[0, head : head + 1, at:end] = jnp.transpose(lse)[:1, :]
            o_ref[at:end, :] = jnp.where(lane < 64, outs[0], outs[1]).astype(BF)

    def col(offset):
        return pl.BlockSpec((length, 128), lambda i: (0, offset * pairs + i))

    return call(
        body,
        (pairs,),
        [col(0), col(1), col(2), whole((1, length)), whole((length, 1))],
        [col(0), pl.BlockSpec((1, 2, length), lambda i: (i, 0, 0))],
        [sds((length, group), BF), sds((pairs, 2, length), F32)],
        (qkv, qkv, qkv, seg_row, seg_col),
        flops=4 * length * length * group,
    )


def attend_back(qkv, grad, lse, seg_row, seg_col, cosine, sine):
    length, cols = qkv.shape
    group = cols // 3
    pairs = group // 128
    high = min(256, length)

    def body(
        q_ref, k_ref, v_ref, g_ref, l_ref, sr_ref, sc_ref, c_ref, s_ref, dq_ref, dk_ref, dv_ref,
        ka_ref, va_ref,
    ):
        lane = lax.broadcasted_iota(jnp.int32, (high, 128), 1)
        ka_ref[...] = jnp.zeros_like(ka_ref)
        va_ref[...] = jnp.zeros_like(va_ref)
        for at in range(0, length, high):
            end = at + high
            query = q_ref[at:end, :]
            grads = g_ref[at:end, :]
            keys = k_ref[:end, :]
            vals = v_ref[:end, :]
            k_pos = lax.broadcasted_iota(jnp.int32, (end, high), 0)
            q_pos = lax.broadcasted_iota(jnp.int32, (end, high), 1) + at
            allowed = (sc_ref[:end, :] == sr_ref[:, at:end]) & (k_pos <= q_pos)
            outs = []
            for head in range(2):
                mine = (lane // 64) == head
                q_own = jnp.where(mine, query, jnp.zeros_like(query))
                g_own = jnp.where(mine, grads, jnp.zeros_like(grads))
                scores = jnp.where(allowed, mm(keys, q_own, NT), NEG)
                probs = jnp.exp(scores - l_ref[0, head : head + 1, at:end])
                grad_probs = mm(vals, g_own, NT)
                delta = jnp.sum(probs * grad_probs, axis=0, keepdims=True)
                grad_scores = (probs * (grad_probs - delta)).astype(BF)
                va_ref[:end, :] += mm(probs.astype(BF), g_own)
                ka_ref[:end, :] += mm(grad_scores, q_own)
                outs.append(mm(grad_scores, keys, TN))
            found = jnp.where(lane < 64, outs[0], outs[1]) * HEAD_DIM**-0.5
            back = found * c_ref[at:end, :] - swap_halves(found) * s_ref[at:end, :]
            dq_ref[at:end, :] = back.astype(BF)
        found = ka_ref[...]
        dk_ref[...] = (found * c_ref[...] - swap_halves(found) * s_ref[...]).astype(BF)
        dv_ref[...] = va_ref[...].astype(BF)

    def col(offset):
        return pl.BlockSpec((length, 128), lambda i: (0, offset * pairs + i))

    return call(
        body,
        (pairs,),
        [
            col(0),
            col(1),
            col(2),
            col(0),
            pl.BlockSpec((1, 2, length), lambda i: (i, 0, 0)),
            whole((1, length)),
            whole((length, 1)),
            whole((length, 128)),
            whole((length, 128)),
        ],
        [col(0), col(0), col(0)],
        [sds((length, group), BF)] * 3,
        (qkv, qkv, qkv, grad, lse, seg_row, seg_col, cosine, sine),
        scratch=[pltpu.VMEM((length, 128), F32)] * 2,
        flops=10 * length * length * group,
    )


def heads_of(flat):
    return flat.reshape(flat.shape[0], -1, HEAD_DIM)


def plain_mask(seg_row, seg_col):
    length = seg_col.shape[0]
    spots = jnp.arange(length, dtype=jnp.int32)
    return (seg_row == seg_col) & (spots[None, :] <= spots[:, None])


def plain_attend(qkv, seg_row, seg_col):
    query, keys, vals = (heads_of(part) for part in jnp.split(qkv, 3, axis=1))
    scores = jnp.einsum("qhd,khd->hqk", query, keys, preferred_element_type=F32)
    scores = jnp.where(plain_mask(seg_row, seg_col)[None], scores, NEG)
    lse = jax.nn.logsumexp(scores, axis=-1, keepdims=True)
    probs = jnp.exp(scores - lse).astype(BF)
    found = jnp.einsum("hqk,khd->qhd", probs, vals, preferred_element_type=F32)
    return found.astype(BF).reshape(qkv.shape[0], -1), lse


def plain_turn_back(grads, cosine, sine):
    table_c, table_s = cosine[:, None, :HEAD_DIM], sine[:, None, :HEAD_DIM]
    swapped = jnp.roll(grads, HEAD_DIM // 2, axis=-1)
    return (grads * table_c - swapped * table_s).astype(BF).reshape(grads.shape[0], -1)


def plain_attend_back(qkv, grad, lse, seg_row, seg_col, cosine, sine):
    query, keys, vals = (heads_of(part) for part in jnp.split(qkv, 3, axis=1))
    grad = heads_of(grad)
    scores = jnp.einsum("qhd,khd->hqk", query, keys, preferred_element_type=F32)
    scores = jnp.where(plain_mask(seg_row, seg_col)[None], scores, NEG)
    probs = jnp.exp(scores - lse)
    grad_probs = jnp.einsum("qhd,khd->hqk", grad, vals, preferred_element_type=F32)
    delta = jnp.sum(probs * grad_probs, axis=-1, keepdims=True)
    grad_scores = (probs * (grad_probs - delta)).astype(BF)
    gq = jnp.einsum("hqk,khd->qhd", grad_scores, keys, preferred_element_type=F32)
    gk = jnp.einsum("hqk,qhd->khd", grad_scores, query, preferred_element_type=F32)
    gv = jnp.einsum("hqk,qhd->khd", probs.astype(BF), grad, preferred_element_type=F32)
    return (
        plain_turn_back(gq * HEAD_DIM**-0.5, cosine, sine),
        plain_turn_back(gk, cosine, sine),
        gv.astype(BF).reshape(qkv.shape[0], -1),
    )


def after_attention(tokens, attended, w_out, gain):
    seqs, parts, span, group = attended.shape
    count, width = tokens.shape

    def body(t_ref, a_ref, w_ref, g_ref, h_ref, b_ref):
        hidden = t_ref[...].astype(F32)
        for part in range(parts):
            rows = a_ref[:, part].reshape(count, group)
            hidden += mm(rows, w_ref[part * group : (part + 1) * group, :])
        h_ref[...] = hidden
        b_ref[...] = (hidden * rms(hidden) * g_ref[...]).astype(BF)

    return call(
        body,
        (1,),
        [whole(a.shape) for a in (tokens, attended, w_out, gain)],
        [whole(tokens.shape)] * 2,
        [sds(tokens.shape, F32), sds(tokens.shape, BF)],
        (tokens, attended, w_out, gain),
        flops=2 * count * width * width,
    )


def dispatch(rows, target_rows, experts, capacity, route_rows=None):
    count, width = rows.shape
    more = 0 if route_rows is None else 16
    tables = () if route_rows is None else (route_rows,)

    def body(r_ref, t_ref, *refs):
        o_ref = refs[-1]
        slot = lax.broadcasted_iota(jnp.int32, (capacity, count), 0)
        slot += pl.program_id(0) * capacity
        hits = [slot == t_ref[k : k + 1, :] for k in range(2)]
        hot = (hits[0] | hits[1]).astype(F32).astype(BF)
        o_ref[0, :capacity, :] = mm(hot, r_ref[...]).astype(BF)
        if more:
            o_ref[0, capacity:, :] = jnp.zeros((more, width), BF)
            other = jnp.zeros((8, capacity), F32)
            for k in range(2):
                route = jnp.broadcast_to(refs[0][1 - k : 2 - k, :].astype(F32), (8, count))
                other += mm(route.astype(BF), hits[k].astype(F32).astype(BF), NT)
            o_ref[0, capacity : capacity + 8, :capacity] = other.astype(BF)

    return call(
        body,
        (experts,),
        [whole(a.shape) for a in (rows, target_rows, *tables)],
        pl.BlockSpec((1, capacity + more, width), lambda i: (i, 0, 0)),
        sds((experts, capacity + more, width), BF),
        (rows, target_rows, *tables),
        flops=2 * experts * capacity * count * width,
    )


def pick(target, row_refs):
    total = None
    for index, ref in enumerate(row_refs):
        rows = ref[...]
        spot = lax.broadcasted_iota(jnp.int32, (target.shape[0], rows.shape[0]), 1)
        one, two = target[:, 2 * index : 2 * index + 1], target[:, 2 * index + 1 : 2 * index + 2]
        found = mm(((spot == one) | (spot == two)).astype(F32).astype(BF), rows)
        total = found if total is None else total + found
    return total


def layer_end(hidden, shared_out, rows, target):
    count, width = hidden.shape
    high = count // 2

    def body(h_ref, s_ref, t_ref, *refs):
        refs[-1][...] = (h_ref[...] + s_ref[...] + pick(t_ref[...], refs[:-1])).astype(BF)

    block = pl.BlockSpec((high, width), lambda i: (i, 0))
    return call(
        body,
        (2,),
        [
            block,
            block,
            pl.BlockSpec((high, target.shape[1]), lambda i: (i, 0)),
            *[whole(part.shape) for part in rows],
        ],
        block,
        sds(hidden.shape, BF),
        (hidden, shared_out, target, *rows),
        flops=2 * count * width * rows[0].shape[0] * len(rows),
    )


def middle_back(hidden, grad_shared, rows, target, cotangent, gain, w_out, parts, span):
    count, width = hidden.shape
    seqs = count // span
    each = 2 if seqs % 2 == 0 else 1
    high = each * span
    steps = count // high
    group = width // parts

    def body(h_ref, s_ref, t_ref, c_ref, g_ref, w_ref, *refs):
        gh_ref, ga_ref, d_ref, n_ref, acc_ref = refs[len(rows) :]
        step = pl.program_id(0)
        branch = s_ref[...] + pick(t_ref[...], refs[: len(rows)])
        hidden = h_ref[...]
        scale = rms(hidden)
        weighted = branch * g_ref[...]
        inner = jnp.mean(weighted * hidden, axis=1, keepdims=True)
        part = jnp.sum(branch * hidden * scale, axis=0, keepdims=True)
        out = c_ref[...].astype(F32) + scale * weighted - hidden * (scale * scale * scale * inner)
        gh_ref[...] = out
        out = out.astype(BF)
        ga_ref[...] = out
        for at in range(parts):
            sent = mm(out, w_ref[at * group : (at + 1) * group, :], NT).astype(BF)
            d_ref[:, at] = sent.reshape(each, span, group)

        @pl.when(step == 0)
        def _():
            acc_ref[...] = jnp.zeros_like(acc_ref)

        acc_ref[...] += jnp.broadcast_to(part, acc_ref.shape)

        @pl.when(step == steps - 1)
        def _():
            column = jnp.transpose(acc_ref[...])
            n_ref[...] = jnp.broadcast_to(column[:, :1], n_ref.shape)

    block = pl.BlockSpec((high, width), lambda i: (i, 0))
    return call(
        body,
        (steps,),
        [
            block,
            block,
            pl.BlockSpec((high, target.shape[1]), lambda i: (i, 0)),
            block,
            whole(gain.shape),
            whole(w_out.shape),
            *[whole(part.shape) for part in rows],
        ],
        [
            block,
            block,
            pl.BlockSpec((each, parts, span, group), lambda i: (i, 0, 0, 0)),
            whole((width, 128)),
        ],
        [
            sds(hidden.shape, F32),
            sds(hidden.shape, BF),
            sds((seqs, parts, span, group), BF),
            sds((width, 128), F32),
        ],
        (hidden, grad_shared, target, cotangent, gain, w_out, *rows),
        scratch=[pltpu.VMEM((8, width), F32)],
        flops=WEIGHT * 2 * count * width * (rows[0].shape[0] * len(rows) + width),
    )


def first_norm_back(tokens, gain, pieces, grad_hidden, z_at):
    count, width = tokens.shape
    blocks = len(pieces)
    span = count // blocks

    def body(at_ref, t_ref, g_ref, h_ref, *refs):
        o_ref = refs[-1]
        for index in range(blocks):
            seq = (at_ref[0] + blocks - index) % blocks
            spot = pl.ds(pl.multiple_of(seq * span, span), span)
            tok = t_ref[spot, :].astype(F32)
            scale = rms(tok)
            weighted = refs[index][...].astype(F32) * g_ref[...]
            inner = jnp.mean(weighted * tok, axis=1, keepdims=True)
            out = h_ref[spot, :] + scale * weighted - tok * (scale * scale * scale * inner)
            o_ref[spot, :] = out.astype(BF)

    return call(
        body,
        (1,),
        [whole(a.shape) for a in (tokens, gain, grad_hidden, *pieces)],
        whole(tokens.shape),
        sds(tokens.shape, BF),
        (z_at, tokens, gain, grad_hidden, *pieces),
        prefetch=1,
    )


def feed_forward(
    rows, grads, w_gate, w_up, w_down, router=None, other=None, own=None, experts=0, place=0, made=None
):
    count, width = rows.shape
    units = w_gate.shape[1]
    wide = 512
    steps = units // wide
    high = 256
    gated = router is not None
    more = 0 if made is None else 1
    kind = BF if gated else F32

    def body(*refs):
        if gated:
            (own_ref, x_ref, g_ref, wg_ref, wu_ref, wd_ref, wr_ref, ot_ref) = refs[:8]
            (y_ref, gi_ref, hid_ref, dg_ref, du_ref, eo_ref, gl_ref, ya_ref, ga_ref, gate_ref) = refs[8 + more :]
        else:
            (x_ref, g_ref, wg_ref, wu_ref, wd_ref,
             y_ref, gi_ref, hid_ref, dg_ref, du_ref, ya_ref, ga_ref) = refs
        step = pl.program_id(0)

        if gated:

            @pl.when(step == 0)
            def _():
                logits = mm(x_ref[...], wr_ref[...])
                lane = lax.broadcasted_iota(jnp.int32, logits.shape, 1)
                mine = jnp.sum(jnp.where(lane == own_ref[0], logits, 0.0), axis=1, keepdims=True)
                theirs = jnp.sum(jnp.where(lane == ot_ref[...], logits, 0.0), axis=1, keepdims=True)
                gate = 1.0 / (1.0 + jnp.exp(theirs - mine))
                rest = 1.0 / (1.0 + jnp.exp(mine - theirs))
                gate_ref[:, 0:1] = gate
                gate_ref[:, 1:2] = rest
                eo_ref[...] = (g_ref[...].astype(F32) * gate).astype(BF)

        def rows_at(index, carry):
            at = pl.ds(pl.multiple_of(index * high, high), high)
            row = x_ref[at, :]
            grad = eo_ref[at, :] if gated else g_ref[at, :]
            gval = mm(row, wg_ref[...])
            uval = mm(row, wu_ref[...])
            sigma = 1.0 / (1.0 + jnp.exp(-gval))
            silu = gval * sigma
            hid = (silu * uval).astype(BF)
            hid_ref[at, :] = hid
            grad_hid = mm(grad, wd_ref[...], NT)
            du = (grad_hid * silu).astype(BF)
            dg = (grad_hid * uval * sigma * (1.0 + gval * (1.0 - sigma))).astype(BF)
            du_ref[at, :] = du
            dg_ref[at, :] = dg
            out = mm(hid, wd_ref[...])
            back = mm(dg, wg_ref[...], NT) + mm(du, wu_ref[...], NT)

            @pl.when(step == 0)
            def _():
                ya_ref[at, :] = out
                ga_ref[at, :] = back

            @pl.when(step > 0)
            def _():
                ya_ref[at, :] += out
                ga_ref[at, :] += back

            return carry

        lax.fori_loop(0, count // high, rows_at, 0)

        @pl.when(step == steps - 1)
        def _():
            if gated:
                out = ya_ref[...]
                gate = gate_ref[:, 0:1]
                lean = jnp.sum(out * g_ref[...].astype(F32), axis=1, keepdims=True)
                lean = lean * gate * gate_ref[:, 1:2]
                lane = lax.broadcasted_iota(jnp.int32, (count, 128), 1)
                sign = (lane == own_ref[0]).astype(F32) - (lane == ot_ref[...]).astype(F32)
                grad_logits = (lean * sign).astype(BF)
                gl_ref[...] = grad_logits
                y_ref[...] = (out * gate).astype(BF).reshape(y_ref.shape)
                gi_ref[...] = (ga_ref[...] + mm(grad_logits, wr_ref[...], NT)).astype(BF)
            else:
                y_ref[...] = ya_ref[...]
                gi_ref[...] = ga_ref[...]

    full = whole((count, width))
    hidden = pl.BlockSpec((count, wide), lambda i, *_: (0, i))
    in_specs = [
        full,
        full,
        pl.BlockSpec((width, wide), lambda i, *_: (0, i)),
        pl.BlockSpec((width, wide), lambda i, *_: (0, i)),
        pl.BlockSpec((wide, width), lambda i, *_: (i, 0)),
    ]
    out_specs = [full, full, hidden, hidden, hidden]
    out_shape = [sds((count, width), kind)] * 2 + [sds((count, units), BF)] * 3
    scratch = [pltpu.VMEM((count, width), F32)] * 2
    args = [rows, grads, w_gate, w_up, w_down]
    if gated:
        in_specs += [whole(router.shape), whole(other.shape)]
        out_specs += [full, whole((count, 128))]
        out_shape += [sds((count, width), BF), sds((count, 128), BF)]
        scratch += [pltpu.VMEM((count, 128), F32)]
        args = [own, *args, router, other]
        out_specs[0] = pl.BlockSpec((experts, count // experts, width), lambda *_: (0, place, 0))
        out_shape[0] = sds((experts, 2 * count // experts, width), BF)
        if more:
            in_specs += [pl.BlockSpec(memory_space=pl.ANY)]
            args += [made]
    return call(
        body,
        (steps,),
        in_specs,
        out_specs,
        out_shape,
        tuple(args),
        scratch=scratch,
        prefetch=1 if gated else 0,
        alias={len(args) - 1: 0} if more else None,
        flops=12 * count * width * units,
    )


def expert_weight_grads(halves, sizes, core_at):
    outer, cores = sizes["y"], sizes["core"]
    count, width = halves[0][0].shape
    units = halves[0][2].shape[1]
    wide = units // (outer * cores)

    def body(at_ref, *refs):
        keep_ref, give_ref, r_ref = refs[-3:]
        groups = [refs[6 * at : 6 * at + 6] for at in range(len(halves))]
        step = pl.program_id(0)

        def over(left, right):
            return sum(mm(group[left][...], group[right][...], TN) for group in groups)

        found = [over(0, 2).astype(BF), over(0, 3).astype(BF), over(1, 4).astype(BF)]

        @pl.when(step < outer)
        def _():
            for index in range(3):
                give_ref[0, index] = found[index]

        @pl.when(step >= outer)
        def _():
            for index in range(3):
                keep_ref[0, index] = found[index]

        @pl.when(step == 0)
        def _():
            r_ref[...] = over(0, 5)

    def taken(i, at):
        core = jnp.where(i < outer, 1 - at[0], at[0])
        return (0, (i % outer) * cores + core)

    hidden = pl.BlockSpec((count, wide), taken)
    part = (1, 3, width, wide)
    return call(
        body,
        (outer * cores,),
        [
            whole((count, width)),
            whole((count, width)),
            hidden,
            hidden,
            hidden,
            whole((count, 128)),
        ]
        * len(halves),
        [
            pl.BlockSpec(part, lambda i, *_: (jnp.maximum(i - outer, 0), 0, 0, 0)),
            pl.BlockSpec(part, lambda i, *_: (jnp.minimum(i, outer - 1), 0, 0, 0)),
            whole((width, 128)),
        ],
        [sds((outer, *part[1:]), BF)] * 2 + [sds((width, 128), F32)],
        (core_at, *[value for half in halves for value in half]),
        prefetch=1,
        flops=6 * count * len(halves) * width * units,
    )


def spread_places(sizes, names):
    found = []
    for y in range(sizes["y"]):
        for core in range(sizes["core"]):
            for z in range(sizes["z"]):
                for x in range(sizes["x"]):
                    at = {"y": y, "core": core, "z": z, "x": x}
                    found.append((core, tuple(at[n] for n in names)))
    return found


def spread(value, sizes, names, core_at):
    order = ("y", "core", "z", "x")
    split = value.reshape(*(sizes[n] for n in order), -1, value.shape[-1])
    split = jnp.transpose(split, (1, *(order.index(n) for n in names), 4, 5))
    return at_index(split, core_at[0]), at_index(split, 1 - core_at[0])


def store_spread(places, each, core_at, found, row, keep, give):
    first = row // each
    for core in range(2):
        todo = [at for at in range(found.shape[0] // each) if places[first + at][0] == core]

        def put(store, todo=todo):
            for at in todo:
                store(places[first + at][1], found[at * each : (at + 1) * each].astype(BF))

        pl.when(core_at == core)(lambda put=put: put(keep))
        pl.when(core_at != core)(lambda put=put: put(give))


def shared_weight_grads(rows, grads, dg, du, hid, sizes, core_at):
    names = ("y", "x", "z")
    lead = tuple(sizes[n] for n in names)
    places = spread_places(sizes, names)
    count, width = rows.shape
    units = dg.shape[1]
    wide = 512
    each = width // len(places)
    direct = each % 8 == 0

    def body(at_ref, x_ref, g_ref, dg_ref, du_ref, hid_ref, *outs):
        pairs = ((x_ref, dg_ref), (x_ref, du_ref), (g_ref, hid_ref))
        for index, (left, right) in enumerate(pairs):
            found = mm(left[...], right[...], TN)
            if not direct:
                outs[0][index] = found.astype(BF)
                continue

            def into(ref, index=index):
                def store(place, piece):
                    ref[(*place, index)] = piece

                return store

            store_spread(places, each, at_ref[0], found, 0, into(outs[0]), into(outs[1]))

    hidden = pl.BlockSpec((count, wide), lambda i, *_: (0, i))
    if direct:
        shapes = [(*lead, 3, each, units)] * 2
        spec = [pl.BlockSpec((*lead, 3, each, wide), lambda i, *_: (0,) * 5 + (i,))] * 2
    else:
        shapes = [(3, width, units)]
        spec = [pl.BlockSpec((3, width, wide), lambda i, *_: (0, 0, i))]
    out = call(
        body,
        (units // wide,),
        [whole(rows.shape), whole(grads.shape), hidden, hidden, hidden],
        spec,
        [sds(shape, BF) for shape in shapes],
        (core_at, rows, grads, dg, du, hid),
        prefetch=1,
        flops=6 * count * width * units,
    )
    if direct:
        return out
    found = [spread(out[0][i], sizes, names, core_at) for i in range(3)]
    return [jnp.stack([part[side] for part in found], axis=3) for side in range(2)]


def tall_weight_grads(lefts, rights, extras, sizes, core_at):
    names = ("y", "z", "x")
    lead = tuple(sizes[n] for n in names)
    places = spread_places(sizes, names)
    width = sum(left.shape[1] for left in lefts)
    cols = sum(right.shape[1] for right in rights)
    each = width // len(places)
    direct = each % 8 == 0
    flops = WEIGHT * 2 * lefts[0].shape[0] * width * cols

    def body(at_ref, *refs):
        left_refs = refs[: len(lefts)]
        right_refs = refs[len(lefts) : len(lefts) + len(rights)]
        rest = refs[len(lefts) + len(rights) :]
        extra_refs, outs = rest[: len(extras)], rest[len(extras) :]

        def save(row, found, col):
            span = found.shape[1]
            if not direct:
                outs[0][row : row + found.shape[0], col : col + span] = found.astype(BF)
                return

            def into(ref):
                def store(place, piece):
                    ref[(*place, slice(None), slice(col, col + span))] = piece

                return store

            store_spread(places, each, at_ref[0], found, row, into(outs[0]), into(outs[1]))

        row = 0
        for left in left_refs:
            col = 0
            for right in right_refs:
                save(row, mm(left[...], right[...], TN), col)
                col += right.shape[1]
            row += left.shape[1]
        more = extra_refs[0][...]
        for extra in extra_refs[1:]:
            more = more + extra[...]
        save(0, more, cols)

    args = (*lefts, *rights, *extras)
    shapes = [(*lead, each, cols + 128)] * 2 if direct else [(width, cols + 128)]
    out = call(
        body,
        (1,),
        [whole(a.shape) for a in args],
        [whole(shape) for shape in shapes],
        [sds(shape, BF) for shape in shapes],
        (core_at, *args),
        prefetch=1,
        flops=flops,
    )
    return out if direct else spread(out[0], sizes, names, core_at)


def scatter_sum(value, name):
    return lax.psum_scatter(value, name, scatter_dimension=0, tiled=False)


def swap_all(value, names):
    return lax.all_to_all(value, names, 0, 0, tiled=True)


def at_index(value, index):
    return lax.dynamic_index_in_dim(value, index, 0, keepdims=False)


def total(terms):
    return sum(term.astype(F32) for term in terms)


def both(keep, give):
    return [keep, lax.ppermute(give, "core", [(0, 1), (1, 0)])]


def fold(terms, name, *others):
    if lax.axis_size(name) != 2:
        sent = total(terms).astype(BF)
        if others:
            sent = after(sent, *others)
        return [scatter_sum(sent, name)], sent
    at = lax.axis_index(name)
    sent = total([at_index(term, 1 - at) for term in terms]).astype(BF)
    if others:
        sent = after(sent, *others)
    got = lax.ppermute(sent, name, [(0, 1), (1, 0)])
    return [at_index(term, at) for term in terms] + [got], sent


def swap_by_steps(value, name):
    size, at = value.shape[0], lax.axis_index(name)
    found = [at_index(value, at)]
    for step in range(1, size):
        sent = at_index(value, (at + step) % size)
        found.append(lax.ppermute(sent, name, [(i, (i + step) % size) for i in range(size)]))
    return found


def after(value, *others):
    return lax.optimization_barrier((value, *others))[0]


def on_device(
    tokens,
    segments,
    routes,
    slots,
    cotangent,
    attn_gain,
    w_qkv,
    w_out,
    ffn_gain,
    w_router,
    shared_gate,
    shared_up,
    shared_down,
    expert_gate,
    expert_up,
    expert_down,
):
    sizes = {name: lax.axis_size(name) for name in ("y", "core", "z", "x")}
    ranks = ("z", "x")
    seqs, span, width = tokens.shape
    blocks, parts = sizes["z"], sizes["x"]
    experts = blocks * parts
    count = seqs * span
    capacity = 3 * count // experts
    length = span * experts
    group = width // parts
    z_at, x_at = lax.axis_index("z"), lax.axis_index("x")
    own = (z_at * parts + x_at).astype(jnp.int32).reshape(1)
    z_ref, x_ref = z_at.astype(jnp.int32).reshape(1), x_at.astype(jnp.int32).reshape(1)
    core_ref = lax.axis_index("core").astype(jnp.int32).reshape(1)
    attn_scale = attn_gain.astype(F32).reshape(1, width)
    ffn_scale = ffn_gain.astype(F32).reshape(1, width)
    flat_tokens = tokens.reshape(count, width)
    flat_cot = cotangent.reshape(count, width)

    route_rows = routes.reshape(count, 2)
    slot_rows = slots.reshape(count, 2)
    half = capacity // 2
    targets = []
    for first in (0, half):
        here = (slot_rows >= first) & (slot_rows < first + half)
        targets.append(jnp.where(here, route_rows * half + slot_rows - first, -1))
    target_rows = [jnp.transpose(target) for target in targets]
    target = jnp.concatenate(targets, axis=1)
    whole_target = jnp.where(slot_rows >= 0, route_rows * capacity + slot_rows, -1)
    route_flat = jnp.transpose(route_rows)
    grad_sent = [dispatch(flat_cot, to, experts, half, route_flat) for to in target_rows]

    frequency = jnp.power(10000.0, -2.0 * jnp.arange(32, dtype=F32) / HEAD_DIM)
    angles = jnp.arange(length, dtype=jnp.int32).astype(F32)[:, None] * jnp.tile(frequency, 4)
    sign = jnp.where(jnp.arange(128) % 64 < 32, -1.0, 1.0)
    cosine, sine = jnp.cos(angles), jnp.sin(angles) * sign
    seg_row = lax.dynamic_slice_in_dim(segments, z_at, 1, 0)
    seg_col = seg_row.reshape(length, 1)
    fused = group % 128 == 0
    if fused:
        weights = [w_qkv] * 3
    else:
        picked = w_qkv.reshape(width, 3, parts, group)
        picked = lax.dynamic_index_in_dim(picked, x_at, 2, keepdims=False)
        weights = [picked.reshape(width, 3 * group)]

    by_seq = swap_all(tokens, "z")
    by_seq, cosine, sine, seg_col, *grad_sent = lax.optimization_barrier(
        (by_seq, cosine, sine, seg_col, *grad_sent)
    )
    if parts == 2:
        rows = [by_seq, lax.ppermute(by_seq, "x", [(0, 1), (1, 0)])]
    else:
        rows = [lax.all_gather(by_seq, "x", axis=0, tiled=False)]
    *rows, grad_sent[0] = lax.optimization_barrier((*rows, grad_sent[0]))
    grad_came = [swap_all(grad_sent[0], ranks)]

    qkv, normed = project(rows, attn_scale, weights, group, cosine, sine, x_ref, parts)
    attended, lse = (attend if fused else plain_attend)(qkv, seg_row, seg_col)
    attended = after(attended, grad_came[0])
    attended = swap_all(attended.reshape(experts, span, group), ranks)
    attended, grad_sent[1] = lax.optimization_barrier((attended, grad_sent[1]))
    grad_came.append(swap_all(grad_sent[1], ranks))
    attended = attended.reshape(seqs, parts, span, group)

    hidden, branch_in = after_attention(flat_tokens, attended, w_out, ffn_scale)
    sent = [dispatch(branch_in, target_rows[0], experts, half)]
    sent.append(dispatch(after(branch_in, sent[0]), target_rows[1], experts, half))
    shared_out, shared_back, hid, dg, du = feed_forward(
        after(branch_in, sent[1]), flat_cot, shared_gate, shared_up, shared_down
    )
    sent[0] = after(sent[0], grad_came[1], shared_out)
    received = [swap_all(value, ranks).reshape(-1, width) for value in sent]
    keep, give = shared_weight_grads(branch_in, flat_cot, dg, du, hid, sizes, core_ref)
    shared_sums, shared_sent = fold(both(keep, give), "y")

    router = jnp.pad(w_router, ((0, 0), (0, 128 - experts)))
    made, back_rows, halves = None, [], []
    before = (give,)
    for at in range(2):
        grad_rows = grad_came[at][:, :half, :].reshape(-1, width)
        other = grad_came[at][:, half, :half].astype(jnp.int32).reshape(-1, 1)
        rows_at = after(received[at], grad_rows, other, *before)
        made, back, hid, dg, du, gated_grads, grad_logits = feed_forward(
            rows_at, grad_rows, expert_gate[0], expert_up[0], expert_down[0], router, other, own,
            experts, at, made,
        )
        back_rows.append(swap_all(back.reshape(experts, half, width), ranks).reshape(-1, width))
        halves.append((rows_at, gated_grads, dg, du, hid, grad_logits))
        before = (back,)
    halves[1] = (after(halves[1][0], back_rows[0], shared_sent), *halves[1][1:])
    keep, give, grad_router = expert_weight_grads(halves, sizes, core_ref)
    back_rows[1] = after(back_rows[1], give)
    expert_sums, expert_sent = fold(both(keep, give), "y")

    grad_hidden, grad_attn, grad_att, grad_ffn = middle_back(
        hidden, shared_back, back_rows, target, flat_cot, ffn_scale, w_out, parts, span
    )
    grad_att = swap_all(grad_att.reshape(experts, span, group), ranks).reshape(length, group)

    column = lax.broadcasted_iota(jnp.int32, (width, 128), 1)
    small = jnp.where(column < experts, grad_router, jnp.where(column == experts, grad_ffn, 0.0))
    out_sums = tall_weight_grads(
        [attended[:, part].reshape(count, group) for part in range(parts)],
        [grad_attn],
        [small],
        sizes,
        core_ref,
    )
    out_sums = both(*out_sums)

    made = after(made, grad_att, out_sums[0])
    made_rows = swap_all(made, ranks).reshape(-1, width)
    grads = list(
        (attend_back if fused else plain_attend_back)(
            qkv, grad_att, lse, seg_row, seg_col, cosine, sine
        )
    )
    shared_sums, _ = fold([after(term, grads[0]) for term in shared_sums], "x")
    grads[0] = after(grads[0], expert_sent)
    normed_back, grad_gain = project_back(grads, weights, rows, x_ref, parts)
    normed_back, _ = fold([normed_back], "x")
    pieces = swap_by_steps(total(normed_back).astype(BF), "z")

    qkv_sums = tall_weight_grads([normed], list(grads), [grad_gain], sizes, core_ref)
    last = [jnp.concatenate(pair, axis=-1) for pair in zip(out_sums, both(*qkv_sums))]
    last, _ = fold(last, "y", expert_sums[-1])
    token_grad = first_norm_back(flat_tokens, attn_scale, pieces, grad_hidden, z_ref)
    layer_out = layer_end(hidden, shared_out, [made_rows], whole_target).reshape(tokens.shape)

    shared_sums = swap_by_steps(after(total(shared_sums).astype(BF), *pieces), "z")
    last = after(total(last).astype(BF), made_rows)
    each, cols = last.shape[-2:]
    last = swap_all(last.reshape(experts, each, cols), ranks).astype(F32)
    last = jnp.sum(last.reshape(blocks, parts, each, cols), axis=0)
    out_sums = jnp.sum(last[:, :, : width + 128], axis=0)
    qkv_sums = last[:, :, width + 128 :]
    grad_attn_gain = jnp.sum(qkv_sums[:, :, 3 * group], axis=0)
    grad_w_qkv = qkv_sums[:, :, : 3 * group].reshape(parts, each, 3, group)
    grad_w_qkv = jnp.transpose(grad_w_qkv, (1, 2, 0, 3)).reshape(each, 3 * width)

    shared_sums, expert_sums = total(shared_sums), total(expert_sums)
    return (
        layer_out,
        token_grad.reshape(tokens.shape),
        grad_attn_gain,
        grad_w_qkv,
        out_sums[:, :width],
        out_sums[:, width + experts],
        out_sums[:, width : width + experts],
        shared_sums[0],
        shared_sums[1],
        jnp.transpose(shared_sums[2]),
        expert_sums[0][None],
        expert_sums[1][None],
        jnp.transpose(expert_sums[2])[None],
    )


def solution(mesh):
    dp, experts = mesh.shape["dp"], mesh.shape["expert"]

    def step(*args):
        seqs = args[0].shape[0] // dp
        cores = 2 if dp % 2 == 0 else 1
        fine = Mesh(
            mesh.devices.reshape(dp // cores, cores, seqs, experts // seqs),
            ("y", "core", "z", "x"),
        )
        data, ranks, every = ("y", "core"), ("z", "x"), ("y", "core", "z", "x")
        placed = (
            P(data, ranks, None),
            P(data, None),
            P(data, ranks, None),
            P(data, ranks, None),
            P(data, ranks, None),
            *([P()] * 8),
            P(ranks, None, None),
            P(ranks, None, None),
            P(ranks, None, None),
        )
        return jax.shard_map(
            on_device,
            mesh=fine,
            in_specs=placed,
            out_specs=(
                P(data, ranks, None),
                P(data, ranks, None),
                P(every),
                P(every, None),
                P(every, None),
                P(every),
                P(every, None),
                P(every, None),
                P(every, None),
                P(None, every),
                P(ranks, None, data),
                P(ranks, None, data),
                P(ranks, data, None),
            ),
            check_vma=False,
        )(*args)

    return step
```

```python
import jax
import jax.numpy as jnp
from jax import lax
from jax.experimental import pallas as pl
from jax.experimental.pallas import tpu as pltpu
from jax.sharding import Mesh
from jax.sharding import PartitionSpec as P

HEAD_DIM = 64
EPS = 1e-06
BF = jnp.bfloat16
F32 = jnp.float32
NEG = -1e30
NN = (((1,), (0,)), ((), ()))
NT = (((1,), (1,)), ((), ()))
TN = (((0,), (0,)), ((), ()))
VMEM_MOST = 60 << 20
WEIGHT = 3


def mm(left, right, dims=NN):
    return lax.dot_general(left, right, dims, preferred_element_type=F32)


def sds(shape, dtype):
    return jax.ShapeDtypeStruct(shape, dtype)


def call(
    body, grid, in_specs, out_specs, out_shape, args, scratch=(), prefetch=0, flops=0, alias=None
):
    leaves = jax.tree.leaves(out_shape)
    moved = sum(a.size * a.dtype.itemsize for a in args) + sum(
        a.size * a.dtype.itemsize for a in leaves
    )
    return pl.pallas_call(
        body,
        out_shape=out_shape,
        grid_spec=pltpu.PrefetchScalarGridSpec(
            num_scalar_prefetch=prefetch,
            grid=grid,
            in_specs=in_specs,
            out_specs=out_specs,
            scratch_shapes=list(scratch),
        ),
        compiler_params=pltpu.CompilerParams(
            dimension_semantics=("arbitrary",) * len(grid), vmem_limit_bytes=VMEM_MOST
        ),
        cost_estimate=pl.CostEstimate(
            flops=int(flops), transcendentals=0, bytes_accessed=int(moved)
        ),
        input_output_aliases=alias or {},
    )(*args)


def whole(shape):
    rank = len(shape)
    return pl.BlockSpec(tuple(shape), lambda *_: (0,) * rank)


def swap_halves(value):
    lane = lax.broadcasted_iota(jnp.int32, value.shape, 1)
    return jnp.where(lane % 64 < 32, pltpu.roll(value, 96, 1), pltpu.roll(value, 32, 1))


def rms(values):
    return lax.rsqrt(jnp.mean(values * values, axis=1, keepdims=True) + EPS)


def row_specs(rows):
    if len(rows) == 2:
        _, span, width = rows[0].shape
        return [pl.BlockSpec((1, span, width), lambda i, *_: (i, 0, 0))] * 2
    parts, _, span, width = rows[0].shape
    return [pl.BlockSpec((parts, 1, span, width), lambda i, *_: (0, i, 0, 0))]


def load_rows(refs, at_ref):
    if len(refs) == 2:
        mine, theirs = refs[0][0].astype(F32), refs[1][0].astype(F32)
        first = at_ref[0] == 0
        pair = [jnp.where(first, mine, theirs), jnp.where(first, theirs, mine)]
        return jnp.concatenate(pair, axis=0)
    value = refs[0][...]
    return value.reshape(value.shape[0] * value.shape[2], value.shape[3]).astype(F32)


def weight_specs(weights, group):
    if len(weights) == 1:
        return [whole(weights[0].shape)]
    width, cols = weights[0].shape
    parts = cols // (3 * group)

    def spec(index):
        return pl.BlockSpec((width, group), lambda i, at: (0, index * parts + at[0]))

    return [spec(index) for index in range(3)]


def load_weights(refs, group):
    if len(refs) == 3:
        return [ref[...] for ref in refs]
    return [refs[0][:, at * group : (at + 1) * group] for at in range(3)]


def project(rows, gain, weights, group, cosine, sine, x_at, parts):
    blocks, span, width = rows[0].shape[-3:]
    height = parts * span
    length = height * blocks
    cut = len(rows)

    def body(at_ref, *refs):
        r_refs, (g_ref, c_ref, s_ref) = refs[:cut], refs[cut : cut + 3]
        w_refs, (qkv_ref, n_ref) = refs[cut + 3 : -2], refs[-2:]
        tok = load_rows(r_refs, at_ref)
        normed = (tok * rms(tok) * g_ref[...]).astype(BF)
        n_ref[...] = normed
        if len(w_refs) == 3:
            found = [mm(normed, ref[...]) for ref in w_refs]
            turning = [(found[0], 0), (found[1], group)]
            last = found[2]
        else:
            found = mm(normed, w_refs[0][...])
            turning, last = [(found[:, : 2 * group], 0)], found[:, 2 * group :]
        for value, base in turning:
            for at in range(0, value.shape[1], 128):
                part = value[:, at : at + 128]
                lane = lax.broadcasted_iota(jnp.int32, part.shape, 1) + (base + at)
                turned = part * c_ref[...] + swap_halves(part) * s_ref[...]
                turned = turned * jnp.where(lane < group, HEAD_DIM**-0.5, 1.0)
                qkv_ref[:, base + at : base + at + 128] = turned.astype(BF)
        qkv_ref[:, 2 * group :] = last.astype(BF)

    return call(
        body,
        (blocks,),
        [
            *row_specs(rows),
            whole((1, width)),
            pl.BlockSpec((height, 128), lambda i, *_: (i, 0)),
            pl.BlockSpec((height, 128), lambda i, *_: (i, 0)),
            *weight_specs(weights, group),
        ],
        [
            pl.BlockSpec((height, 3 * group), lambda i, *_: (i, 0)),
            pl.BlockSpec((height, width), lambda i, *_: (i, 0)),
        ],
        [sds((length, 3 * group), BF), sds((length, width), BF)],
        (x_at, *rows, gain, cosine, sine, *weights),
        prefetch=1,
        flops=6 * length * width * group,
    )


def project_back(grads, weights, rows, x_at, parts):
    blocks, span, width = rows[0].shape[-3:]
    group = grads[0].shape[1]
    height = parts * span
    length = height * blocks
    cut = len(rows)

    def body(at_ref, q_ref, k_ref, v_ref, *refs):
        r_refs, w_refs, (out_ref, gain_ref, acc_ref) = refs[:cut], refs[cut:-3], refs[-3:]
        step = pl.program_id(0)
        w_q, w_k, w_v = load_weights(w_refs, group)
        back = mm(q_ref[...], w_q, NT) + mm(k_ref[...], w_k, NT) + mm(v_ref[...], w_v, NT)
        tok = load_rows(r_refs, at_ref)
        part = jnp.sum(back * tok * rms(tok), axis=0, keepdims=True)

        @pl.when(step == 0)
        def _():
            acc_ref[...] = jnp.zeros_like(acc_ref)

        acc_ref[...] += jnp.broadcast_to(part, acc_ref.shape)
        out_ref[...] = back.astype(BF).reshape(parts, 1, span, width)

        @pl.when(step == blocks - 1)
        def _():
            column = jnp.transpose(acc_ref[...])
            gain_ref[...] = jnp.broadcast_to(column[:, :1], gain_ref.shape)

    block = pl.BlockSpec((height, group), lambda i, *_: (i, 0))
    return call(
        body,
        (blocks,),
        [block, block, block, *row_specs(rows), *weight_specs(weights, group)],
        [
            pl.BlockSpec((parts, 1, span, width), lambda i, *_: (0, i, 0, 0)),
            whole((width, 128)),
        ],
        [sds((parts, blocks, span, width), BF), sds((width, 128), F32)],
        (x_at, *grads, *rows, *weights),
        scratch=[pltpu.VMEM((8, width), F32)],
        prefetch=1,
        flops=0.2 * length * width * group,
    )


def attend(qkv, seg_row, seg_col):
    length, cols = qkv.shape
    group = cols // 3
    pairs = group // 128
    high = min(256, length)

    def body(q_ref, k_ref, v_ref, sr_ref, sc_ref, o_ref, l_ref):
        lane = lax.broadcasted_iota(jnp.int32, (high, 128), 1)
        for at in range(0, length, high):
            end = at + high
            query = q_ref[at:end, :]
            keys = k_ref[:end, :]
            vals = v_ref[:end, :]
            q_pos = lax.broadcasted_iota(jnp.int32, (high, end), 0) + at
            k_pos = lax.broadcasted_iota(jnp.int32, (high, end), 1)
            allowed = (sc_ref[at:end, :] == sr_ref[:, :end]) & (k_pos <= q_pos)
            outs = []
            for head in range(2):
                mine = (lane // 64) == head
                scores = mm(jnp.where(mine, query, jnp.zeros_like(query)), keys, NT)
                scores = jnp.where(allowed, scores, NEG)
                most = jnp.max(scores, axis=1, keepdims=True)
                expo = jnp.exp(scores - most)
                total = jnp.sum(expo, axis=1, keepdims=True)
                outs.append(mm(expo.astype(BF), vals) / total)
                lse = jnp.broadcast_to(most + jnp.log(total), (high, 128))
                l_ref[0, head : head + 1, at:end] = jnp.transpose(lse)[:1, :]
            o_ref[at:end, :] = jnp.where(lane < 64, outs[0], outs[1]).astype(BF)

    def col(offset):
        return pl.BlockSpec((length, 128), lambda i: (0, offset * pairs + i))

    return call(
        body,
        (pairs,),
        [col(0), col(1), col(2), whole((1, length)), whole((length, 1))],
        [col(0), pl.BlockSpec((1, 2, length), lambda i: (i, 0, 0))],
        [sds((length, group), BF), sds((pairs, 2, length), F32)],
        (qkv, qkv, qkv, seg_row, seg_col),
        flops=4 * length * length * group,
    )


def attend_back(qkv, grad, lse, seg_row, seg_col, cosine, sine):
    length, cols = qkv.shape
    group = cols // 3
    pairs = group // 128
    high = min(256, length)

    def body(
        q_ref, k_ref, v_ref, g_ref, l_ref, sr_ref, sc_ref, c_ref, s_ref, dq_ref, dk_ref, dv_ref,
        ka_ref, va_ref,
    ):
        lane = lax.broadcasted_iota(jnp.int32, (high, 128), 1)
        ka_ref[...] = jnp.zeros_like(ka_ref)
        va_ref[...] = jnp.zeros_like(va_ref)
        for at in range(0, length, high):
            end = at + high
            query = q_ref[at:end, :]
            grads = g_ref[at:end, :]
            keys = k_ref[:end, :]
            vals = v_ref[:end, :]
            k_pos = lax.broadcasted_iota(jnp.int32, (end, high), 0)
            q_pos = lax.broadcasted_iota(jnp.int32, (end, high), 1) + at
            allowed = (sc_ref[:end, :] == sr_ref[:, at:end]) & (k_pos <= q_pos)
            outs = []
            for head in range(2):
                mine = (lane // 64) == head
                q_own = jnp.where(mine, query, jnp.zeros_like(query))
                g_own = jnp.where(mine, grads, jnp.zeros_like(grads))
                scores = jnp.where(allowed, mm(keys, q_own, NT), NEG)
                probs = jnp.exp(scores - l_ref[0, head : head + 1, at:end])
                grad_probs = mm(vals, g_own, NT)
                delta = jnp.sum(probs * grad_probs, axis=0, keepdims=True)
                grad_scores = (probs * (grad_probs - delta)).astype(BF)
                va_ref[:end, :] += mm(probs.astype(BF), g_own)
                ka_ref[:end, :] += mm(grad_scores, q_own)
                outs.append(mm(grad_scores, keys, TN))
            found = jnp.where(lane < 64, outs[0], outs[1]) * HEAD_DIM**-0.5
            back = found * c_ref[at:end, :] - swap_halves(found) * s_ref[at:end, :]
            dq_ref[at:end, :] = back.astype(BF)
        found = ka_ref[...]
        dk_ref[...] = (found * c_ref[...] - swap_halves(found) * s_ref[...]).astype(BF)
        dv_ref[...] = va_ref[...].astype(BF)

    def col(offset):
        return pl.BlockSpec((length, 128), lambda i: (0, offset * pairs + i))

    return call(
        body,
        (pairs,),
        [
            col(0),
            col(1),
            col(2),
            col(0),
            pl.BlockSpec((1, 2, length), lambda i: (i, 0, 0)),
            whole((1, length)),
            whole((length, 1)),
            whole((length, 128)),
            whole((length, 128)),
        ],
        [col(0), col(0), col(0)],
        [sds((length, group), BF)] * 3,
        (qkv, qkv, qkv, grad, lse, seg_row, seg_col, cosine, sine),
        scratch=[pltpu.VMEM((length, 128), F32)] * 2,
        flops=length * length * group,
    )


def heads_of(flat):
    return flat.reshape(flat.shape[0], -1, HEAD_DIM)


def plain_mask(seg_row, seg_col):
    length = seg_col.shape[0]
    spots = jnp.arange(length, dtype=jnp.int32)
    return (seg_row == seg_col) & (spots[None, :] <= spots[:, None])


def plain_attend(qkv, seg_row, seg_col):
    query, keys, vals = (heads_of(part) for part in jnp.split(qkv, 3, axis=1))
    scores = jnp.einsum("qhd,khd->hqk", query, keys, preferred_element_type=F32)
    scores = jnp.where(plain_mask(seg_row, seg_col)[None], scores, NEG)
    lse = jax.nn.logsumexp(scores, axis=-1, keepdims=True)
    probs = jnp.exp(scores - lse).astype(BF)
    found = jnp.einsum("hqk,khd->qhd", probs, vals, preferred_element_type=F32)
    return found.astype(BF).reshape(qkv.shape[0], -1), lse


def plain_turn_back(grads, cosine, sine):
    table_c, table_s = cosine[:, None, :HEAD_DIM], sine[:, None, :HEAD_DIM]
    swapped = jnp.roll(grads, HEAD_DIM // 2, axis=-1)
    return (grads * table_c - swapped * table_s).astype(BF).reshape(grads.shape[0], -1)


def plain_attend_back(qkv, grad, lse, seg_row, seg_col, cosine, sine):
    query, keys, vals = (heads_of(part) for part in jnp.split(qkv, 3, axis=1))
    grad = heads_of(grad)
    scores = jnp.einsum("qhd,khd->hqk", query, keys, preferred_element_type=F32)
    scores = jnp.where(plain_mask(seg_row, seg_col)[None], scores, NEG)
    probs = jnp.exp(scores - lse)
    grad_probs = jnp.einsum("qhd,khd->hqk", grad, vals, preferred_element_type=F32)
    delta = jnp.sum(probs * grad_probs, axis=-1, keepdims=True)
    grad_scores = (probs * (grad_probs - delta)).astype(BF)
    gq = jnp.einsum("hqk,khd->qhd", grad_scores, keys, preferred_element_type=F32)
    gk = jnp.einsum("hqk,qhd->khd", grad_scores, query, preferred_element_type=F32)
    gv = jnp.einsum("hqk,qhd->khd", probs.astype(BF), grad, preferred_element_type=F32)
    return (
        plain_turn_back(gq * HEAD_DIM**-0.5, cosine, sine),
        plain_turn_back(gk, cosine, sine),
        gv.astype(BF).reshape(qkv.shape[0], -1),
    )


def after_attention(tokens, attended, w_out, gain):
    seqs, parts, span, group = attended.shape
    count, width = tokens.shape

    def body(t_ref, a_ref, w_ref, g_ref, h_ref, b_ref):
        hidden = t_ref[...].astype(F32)
        for part in range(parts):
            rows = a_ref[:, part].reshape(count, group)
            hidden += mm(rows, w_ref[part * group : (part + 1) * group, :])
        h_ref[...] = hidden
        b_ref[...] = (hidden * rms(hidden) * g_ref[...]).astype(BF)

    return call(
        body,
        (1,),
        [whole(a.shape) for a in (tokens, attended, w_out, gain)],
        [whole(tokens.shape)] * 2,
        [sds(tokens.shape, F32), sds(tokens.shape, BF)],
        (tokens, attended, w_out, gain),
        flops=2 * count * width * width,
    )


def dispatch(rows, target_rows, experts, capacity, route_rows=None):
    count, width = rows.shape
    more = 0 if route_rows is None else 16
    tables = () if route_rows is None else (route_rows,)

    def body(r_ref, t_ref, *refs):
        o_ref = refs[-1]
        slot = lax.broadcasted_iota(jnp.int32, (capacity, count), 0)
        slot += pl.program_id(0) * capacity
        hits = [slot == t_ref[k : k + 1, :] for k in range(2)]
        hot = (hits[0] | hits[1]).astype(F32).astype(BF)
        o_ref[0, :capacity, :] = mm(hot, r_ref[...]).astype(BF)
        if more:
            o_ref[0, capacity:, :] = jnp.zeros((more, width), BF)
            other = jnp.zeros((8, capacity), F32)
            for k in range(2):
                route = jnp.broadcast_to(refs[0][1 - k : 2 - k, :].astype(F32), (8, count))
                other += mm(route.astype(BF), hits[k].astype(F32).astype(BF), NT)
            o_ref[0, capacity : capacity + 8, :capacity] = other.astype(BF)

    return call(
        body,
        (experts,),
        [whole(a.shape) for a in (rows, target_rows, *tables)],
        pl.BlockSpec((1, capacity + more, width), lambda i: (i, 0, 0)),
        sds((experts, capacity + more, width), BF),
        (rows, target_rows, *tables),
        flops=2 * experts * capacity * count * width,
    )


def pick(target, row_refs):
    total = None
    for index, ref in enumerate(row_refs):
        rows = ref[...]
        spot = lax.broadcasted_iota(jnp.int32, (target.shape[0], rows.shape[0]), 1)
        one, two = target[:, 2 * index : 2 * index + 1], target[:, 2 * index + 1 : 2 * index + 2]
        found = mm(((spot == one) | (spot == two)).astype(F32).astype(BF), rows)
        total = found if total is None else total + found
    return total


def layer_end(hidden, shared_out, rows, target):
    count, width = hidden.shape
    high = count // 2

    def body(h_ref, s_ref, t_ref, *refs):
        refs[-1][...] = (h_ref[...] + s_ref[...] + pick(t_ref[...], refs[:-1])).astype(BF)

    block = pl.BlockSpec((high, width), lambda i: (i, 0))
    return call(
        body,
        (2,),
        [
            block,
            block,
            pl.BlockSpec((high, target.shape[1]), lambda i: (i, 0)),
            *[whole(part.shape) for part in rows],
        ],
        block,
        sds(hidden.shape, BF),
        (hidden, shared_out, target, *rows),
        flops=2 * count * width * rows[0].shape[0] * len(rows),
    )


def middle_back(hidden, grad_shared, rows, target, cotangent, gain, w_out, parts, span):
    count, width = hidden.shape
    seqs = count // span
    each = 2 if seqs % 2 == 0 else 1
    high = each * span
    steps = count // high
    group = width // parts

    def body(h_ref, s_ref, t_ref, c_ref, g_ref, w_ref, *refs):
        gh_ref, ga_ref, d_ref, n_ref, acc_ref = refs[len(rows) :]
        step = pl.program_id(0)
        branch = s_ref[...] + pick(t_ref[...], refs[: len(rows)])
        hidden = h_ref[...]
        scale = rms(hidden)
        weighted = branch * g_ref[...]
        inner = jnp.mean(weighted * hidden, axis=1, keepdims=True)
        part = jnp.sum(branch * hidden * scale, axis=0, keepdims=True)
        out = c_ref[...].astype(F32) + scale * weighted - hidden * (scale * scale * scale * inner)
        gh_ref[...] = out
        out = out.astype(BF)
        ga_ref[...] = out
        for at in range(parts):
            sent = mm(out, w_ref[at * group : (at + 1) * group, :], NT).astype(BF)
            d_ref[:, at] = sent.reshape(each, span, group)

        @pl.when(step == 0)
        def _():
            acc_ref[...] = jnp.zeros_like(acc_ref)

        acc_ref[...] += jnp.broadcast_to(part, acc_ref.shape)

        @pl.when(step == steps - 1)
        def _():
            column = jnp.transpose(acc_ref[...])
            n_ref[...] = jnp.broadcast_to(column[:, :1], n_ref.shape)

    block = pl.BlockSpec((high, width), lambda i: (i, 0))
    return call(
        body,
        (steps,),
        [
            block,
            block,
            pl.BlockSpec((high, target.shape[1]), lambda i: (i, 0)),
            block,
            whole(gain.shape),
            whole(w_out.shape),
            *[whole(part.shape) for part in rows],
        ],
        [
            block,
            block,
            pl.BlockSpec((each, parts, span, group), lambda i: (i, 0, 0, 0)),
            whole((width, 128)),
        ],
        [
            sds(hidden.shape, F32),
            sds(hidden.shape, BF),
            sds((seqs, parts, span, group), BF),
            sds((width, 128), F32),
        ],
        (hidden, grad_shared, target, cotangent, gain, w_out, *rows),
        scratch=[pltpu.VMEM((8, width), F32)],
        flops=WEIGHT * 2 * count * width * (rows[0].shape[0] * len(rows) + width),
    )


def first_norm_back(tokens, gain, pieces, grad_hidden, z_at):
    count, width = tokens.shape
    blocks = len(pieces)
    span = count // blocks

    def body(at_ref, t_ref, g_ref, h_ref, *refs):
        o_ref = refs[-1]
        for index in range(blocks):
            seq = (at_ref[0] + blocks - index) % blocks
            spot = pl.ds(pl.multiple_of(seq * span, span), span)
            tok = t_ref[spot, :].astype(F32)
            scale = rms(tok)
            weighted = refs[index][...].astype(F32) * g_ref[...]
            inner = jnp.mean(weighted * tok, axis=1, keepdims=True)
            out = h_ref[spot, :] + scale * weighted - tok * (scale * scale * scale * inner)
            o_ref[spot, :] = out.astype(BF)

    return call(
        body,
        (1,),
        [whole(a.shape) for a in (tokens, gain, grad_hidden, *pieces)],
        whole(tokens.shape),
        sds(tokens.shape, BF),
        (z_at, tokens, gain, grad_hidden, *pieces),
        prefetch=1,
    )


def feed_forward(
    rows, grads, w_gate, w_up, w_down, router=None, other=None, own=None, experts=0, place=0, made=None
):
    count, width = rows.shape
    units = w_gate.shape[1]
    wide = 512
    steps = units // wide
    high = 256
    gated = router is not None
    more = 0 if made is None else 1
    kind = BF if gated else F32

    def body(*refs):
        if gated:
            (own_ref, x_ref, g_ref, wg_ref, wu_ref, wd_ref, wr_ref, ot_ref) = refs[:8]
            (y_ref, gi_ref, hid_ref, dg_ref, du_ref, eo_ref, gl_ref, ya_ref, ga_ref, gate_ref) = refs[8 + more :]
        else:
            (x_ref, g_ref, wg_ref, wu_ref, wd_ref,
             y_ref, gi_ref, hid_ref, dg_ref, du_ref, ya_ref, ga_ref) = refs
        step = pl.program_id(0)

        if gated:

            @pl.when(step == 0)
            def _():
                logits = mm(x_ref[...], wr_ref[...])
                lane = lax.broadcasted_iota(jnp.int32, logits.shape, 1)
                mine = jnp.sum(jnp.where(lane == own_ref[0], logits, 0.0), axis=1, keepdims=True)
                theirs = jnp.sum(jnp.where(lane == ot_ref[...], logits, 0.0), axis=1, keepdims=True)
                gate = 1.0 / (1.0 + jnp.exp(theirs - mine))
                rest = 1.0 / (1.0 + jnp.exp(mine - theirs))
                gate_ref[:, 0:1] = gate
                gate_ref[:, 1:2] = rest
                eo_ref[...] = (g_ref[...].astype(F32) * gate).astype(BF)

        def rows_at(index, carry):
            at = pl.ds(pl.multiple_of(index * high, high), high)
            row = x_ref[at, :]
            grad = eo_ref[at, :] if gated else g_ref[at, :]
            gval = mm(row, wg_ref[...])
            uval = mm(row, wu_ref[...])
            sigma = 1.0 / (1.0 + jnp.exp(-gval))
            silu = gval * sigma
            hid = (silu * uval).astype(BF)
            hid_ref[at, :] = hid
            grad_hid = mm(grad, wd_ref[...], NT)
            du = (grad_hid * silu).astype(BF)
            dg = (grad_hid * uval * sigma * (1.0 + gval * (1.0 - sigma))).astype(BF)
            du_ref[at, :] = du
            dg_ref[at, :] = dg
            out = mm(hid, wd_ref[...])
            back = mm(dg, wg_ref[...], NT) + mm(du, wu_ref[...], NT)

            @pl.when(step == 0)
            def _():
                ya_ref[at, :] = out
                ga_ref[at, :] = back

            @pl.when(step > 0)
            def _():
                ya_ref[at, :] += out
                ga_ref[at, :] += back

            return carry

        lax.fori_loop(0, count // high, rows_at, 0)

        @pl.when(step == steps - 1)
        def _():
            if gated:
                out = ya_ref[...]
                gate = gate_ref[:, 0:1]
                lean = jnp.sum(out * g_ref[...].astype(F32), axis=1, keepdims=True)
                lean = lean * gate * gate_ref[:, 1:2]
                lane = lax.broadcasted_iota(jnp.int32, (count, 128), 1)
                sign = (lane == own_ref[0]).astype(F32) - (lane == ot_ref[...]).astype(F32)
                grad_logits = (lean * sign).astype(BF)
                gl_ref[...] = grad_logits
                y_ref[...] = (out * gate).astype(BF).reshape(y_ref.shape)
                gi_ref[...] = (ga_ref[...] + mm(grad_logits, wr_ref[...], NT)).astype(BF)
            else:
                y_ref[...] = ya_ref[...]
                gi_ref[...] = ga_ref[...]

    full = whole((count, width))
    hidden = pl.BlockSpec((count, wide), lambda i, *_: (0, i))
    in_specs = [
        full,
        full,
        pl.BlockSpec((width, wide), lambda i, *_: (0, i)),
        pl.BlockSpec((width, wide), lambda i, *_: (0, i)),
        pl.BlockSpec((wide, width), lambda i, *_: (i, 0)),
    ]
    out_specs = [full, full, hidden, hidden, hidden]
    out_shape = [sds((count, width), kind)] * 2 + [sds((count, units), BF)] * 3
    scratch = [pltpu.VMEM((count, width), F32)] * 2
    args = [rows, grads, w_gate, w_up, w_down]
    if gated:
        in_specs += [whole(router.shape), whole(other.shape)]
        out_specs += [full, whole((count, 128))]
        out_shape += [sds((count, width), BF), sds((count, 128), BF)]
        scratch += [pltpu.VMEM((count, 128), F32)]
        args = [own, *args, router, other]
        out_specs[0] = pl.BlockSpec((experts, count // experts, width), lambda *_: (0, place, 0))
        out_shape[0] = sds((experts, 2 * count // experts, width), BF)
        if more:
            in_specs += [pl.BlockSpec(memory_space=pl.ANY)]
            args += [made]
    return call(
        body,
        (steps,),
        in_specs,
        out_specs,
        out_shape,
        tuple(args),
        scratch=scratch,
        prefetch=1 if gated else 0,
        alias={len(args) - 1: 0} if more else None,
        flops=12 * count * width * units,
    )


def expert_weight_grads(halves, sizes, core_at):
    outer, cores = sizes["y"], sizes["core"]
    count, width = halves[0][0].shape
    units = halves[0][2].shape[1]
    wide = units // (outer * cores)

    def body(at_ref, *refs):
        keep_ref, give_ref, r_ref = refs[-3:]
        groups = [refs[6 * at : 6 * at + 6] for at in range(len(halves))]
        step = pl.program_id(0)

        def over(left, right):
            return sum(mm(group[left][...], group[right][...], TN) for group in groups)

        found = [over(0, 2).astype(BF), over(0, 3).astype(BF), over(1, 4).astype(BF)]

        @pl.when(step < outer)
        def _():
            for index in range(3):
                give_ref[0, index] = found[index]

        @pl.when(step >= outer)
        def _():
            for index in range(3):
                keep_ref[0, index] = found[index]

        @pl.when(step == 0)
        def _():
            r_ref[...] = over(0, 5)

    def taken(i, at):
        core = jnp.where(i < outer, 1 - at[0], at[0])
        y = (i + 1 + at[1]) % outer if outer == 2 else i % outer
        return (0, y * cores + core)

    hidden = pl.BlockSpec((count, wide), taken)
    part = (1, 3, width, wide)
    return call(
        body,
        (outer * cores,),
        [
            whole((count, width)),
            whole((count, width)),
            hidden,
            hidden,
            hidden,
            whole((count, 128)),
        ]
        * len(halves),
        [
            pl.BlockSpec(part, lambda i, *_: (jnp.maximum(i - outer, 0), 0, 0, 0)),
            pl.BlockSpec(part, lambda i, *_: (jnp.minimum(i, outer - 1), 0, 0, 0)),
            whole((width, 128)),
        ],
        [sds((outer, *part[1:]), BF)] * 2 + [sds((width, 128), F32)],
        (core_at, *[value for half in halves for value in half]),
        prefetch=1,
        flops=6 * count * len(halves) * width * units,
    )


def spread_places(sizes, names):
    found = []
    for y in range(sizes["y"]):
        for core in range(sizes["core"]):
            for z in range(sizes["z"]):
                for x in range(sizes["x"]):
                    at = {"y": y, "core": core, "z": z, "x": x}
                    found.append((core, tuple(at[n] for n in names)))
    return found


def spread(value, sizes, names, core_at):
    order = ("y", "core", "z", "x")
    split = value.reshape(*(sizes[n] for n in order), -1, value.shape[-1])
    split = jnp.transpose(split, (1, *(order.index(n) for n in names), 4, 5))
    return at_index(split, core_at[0]), at_index(split, 1 - core_at[0])


def store_spread(places, each, core_at, found, row, keep, give):
    first = row // each
    for core in range(2):
        todo = [at for at in range(found.shape[0] // each) if places[first + at][0] == core]

        def put(store, todo=todo):
            for at in todo:
                store(places[first + at][1], found[at * each : (at + 1) * each].astype(BF))

        pl.when(core_at == core)(lambda put=put: put(keep))
        pl.when(core_at != core)(lambda put=put: put(give))


def shared_weight_grads(rows, grads, dg, du, hid, sizes, core_at):
    names = ("y", "x", "z")
    lead = tuple(sizes[n] for n in names)
    places = spread_places(sizes, names)
    count, width = rows.shape
    units = dg.shape[1]
    wide = 512
    each = width // len(places)
    direct = each % 8 == 0

    def body(at_ref, x_ref, g_ref, dg_ref, du_ref, hid_ref, *outs):
        pairs = ((x_ref, dg_ref), (x_ref, du_ref), (g_ref, hid_ref))
        for index, (left, right) in enumerate(pairs):
            found = mm(left[...], right[...], TN)
            if not direct:
                outs[0][index] = found.astype(BF)
                continue

            def into(ref, index=index):
                def store(place, piece):
                    ref[(*place, index)] = piece

                return store

            store_spread(places, each, at_ref[0], found, 0, into(outs[0]), into(outs[1]))

    hidden = pl.BlockSpec((count, wide), lambda i, *_: (0, i))
    if direct:
        shapes = [(*lead, 3, each, units)] * 2
        spec = [pl.BlockSpec((*lead, 3, each, wide), lambda i, *_: (0,) * 5 + (i,))] * 2
    else:
        shapes = [(3, width, units)]
        spec = [pl.BlockSpec((3, width, wide), lambda i, *_: (0, 0, i))]
    out = call(
        body,
        (units // wide,),
        [whole(rows.shape), whole(grads.shape), hidden, hidden, hidden],
        spec,
        [sds(shape, BF) for shape in shapes],
        (core_at, rows, grads, dg, du, hid),
        prefetch=1,
        flops=6 * count * width * units,
    )
    if direct:
        return out
    found = [spread(out[0][i], sizes, names, core_at) for i in range(3)]
    return [jnp.stack([part[side] for part in found], axis=3) for side in range(2)]


def tall_weight_grads(lefts, rights, extras, sizes, core_at, weight=1):
    names = ("y", "z", "x")
    lead = tuple(sizes[n] for n in names)
    places = spread_places(sizes, names)
    width = sum(left.shape[1] for left in lefts)
    cols = sum(right.shape[1] for right in rights)
    each = width // len(places)
    direct = each % 8 == 0
    flops = weight * 2 * lefts[0].shape[0] * width * cols

    def body(at_ref, *refs):
        left_refs = refs[: len(lefts)]
        right_refs = refs[len(lefts) : len(lefts) + len(rights)]
        rest = refs[len(lefts) + len(rights) :]
        extra_refs, outs = rest[: len(extras)], rest[len(extras) :]

        def save(row, found, col):
            span = found.shape[1]
            if not direct:
                outs[0][row : row + found.shape[0], col : col + span] = found.astype(BF)
                return

            def into(ref):
                def store(place, piece):
                    ref[(*place, slice(None), slice(col, col + span))] = piece

                return store

            store_spread(places, each, at_ref[0], found, row, into(outs[0]), into(outs[1]))

        row = 0
        for left in left_refs:
            col = 0
            for right in right_refs:
                save(row, mm(left[...], right[...], TN), col)
                col += right.shape[1]
            row += left.shape[1]
        more = extra_refs[0][...]
        for extra in extra_refs[1:]:
            more = more + extra[...]
        save(0, more, cols)

    args = (*lefts, *rights, *extras)
    shapes = [(*lead, each, cols + 128)] * 2 if direct else [(width, cols + 128)]
    out = call(
        body,
        (1,),
        [whole(a.shape) for a in args],
        [whole(shape) for shape in shapes],
        [sds(shape, BF) for shape in shapes],
        (core_at, *args),
        prefetch=1,
        flops=flops,
    )
    return out if direct else spread(out[0], sizes, names, core_at)


def scatter_sum(value, name):
    return lax.psum_scatter(value, name, scatter_dimension=0, tiled=False)


def swap_all(value, names):
    return lax.all_to_all(value, names, 0, 0, tiled=True)


def at_index(value, index):
    if isinstance(index, int):
        return value[index]
    return lax.dynamic_index_in_dim(value, index, 0, keepdims=False)


def total(terms):
    return sum(term.astype(F32) for term in terms)


def both(keep, give):
    return [keep, lax.ppermute(give, "core", [(0, 1), (1, 0)])]


def fold(terms, name, *others, ordered=False):
    if lax.axis_size(name) != 2:
        sent = total(terms).astype(BF)
        if others:
            sent = after(sent, *others)
        return [scatter_sum(sent, name)], sent
    at = 1 if ordered else lax.axis_index(name)
    sent = total([at_index(term, 1 - at) for term in terms]).astype(BF)
    if others:
        sent = after(sent, *others)
    got = lax.ppermute(sent, name, [(0, 1), (1, 0)])
    return [at_index(term, at) for term in terms] + [got], sent


def swap_by_steps(value, name):
    size, at = value.shape[0], lax.axis_index(name)
    found = [at_index(value, at)]
    for step in range(1, size):
        sent = at_index(value, (at + step) % size)
        found.append(lax.ppermute(sent, name, [(i, (i + step) % size) for i in range(size)]))
    return found


def after(value, *others):
    return lax.optimization_barrier((value, *others))[0]


def on_device(
    tokens,
    segments,
    routes,
    slots,
    cotangent,
    attn_gain,
    w_qkv,
    w_out,
    ffn_gain,
    w_router,
    shared_gate,
    shared_up,
    shared_down,
    expert_gate,
    expert_up,
    expert_down,
):
    sizes = {name: lax.axis_size(name) for name in ("y", "core", "z", "x")}
    ranks = ("z", "x")
    seqs, span, width = tokens.shape
    blocks, parts = sizes["z"], sizes["x"]
    experts = blocks * parts
    count = seqs * span
    capacity = 3 * count // experts
    length = span * experts
    group = width // parts
    z_at, x_at = lax.axis_index("z"), lax.axis_index("x")
    own = (z_at * parts + x_at).astype(jnp.int32).reshape(1)
    z_ref, x_ref = z_at.astype(jnp.int32).reshape(1), x_at.astype(jnp.int32).reshape(1)
    core_ref = lax.axis_index("core").astype(jnp.int32).reshape(1)
    pair_ref = jnp.stack([lax.axis_index("core"), lax.axis_index("y")]).astype(jnp.int32)
    attn_scale = attn_gain.astype(F32).reshape(1, width)
    ffn_scale = ffn_gain.astype(F32).reshape(1, width)
    flat_tokens = tokens.reshape(count, width)
    flat_cot = cotangent.reshape(count, width)

    route_rows = routes.reshape(count, 2)
    slot_rows = slots.reshape(count, 2)
    half = capacity // 2
    targets = []
    for first in (0, half):
        here = (slot_rows >= first) & (slot_rows < first + half)
        targets.append(jnp.where(here, route_rows * half + slot_rows - first, -1))
    target_rows = [jnp.transpose(target) for target in targets]
    target = jnp.concatenate(targets, axis=1)
    whole_target = jnp.where(slot_rows >= 0, route_rows * capacity + slot_rows, -1)
    route_flat = jnp.transpose(route_rows)
    grad_sent = [dispatch(flat_cot, to, experts, half, route_flat) for to in target_rows]

    frequency = jnp.power(10000.0, -2.0 * jnp.arange(32, dtype=F32) / HEAD_DIM)
    angles = jnp.arange(length, dtype=jnp.int32).astype(F32)[:, None] * jnp.tile(frequency, 4)
    sign = jnp.where(jnp.arange(128) % 64 < 32, -1.0, 1.0)
    cosine, sine = jnp.cos(angles), jnp.sin(angles) * sign
    seg_row = lax.dynamic_slice_in_dim(segments, z_at, 1, 0)
    seg_col = seg_row.reshape(length, 1)
    fused = group % 128 == 0
    if fused:
        weights = [w_qkv] * 3
    else:
        picked = w_qkv.reshape(width, 3, parts, group)
        picked = lax.dynamic_index_in_dim(picked, x_at, 2, keepdims=False)
        weights = [picked.reshape(width, 3 * group)]

    by_seq = swap_all(tokens, "z")
    by_seq, cosine, sine, seg_col, *grad_sent = lax.optimization_barrier(
        (by_seq, cosine, sine, seg_col, *grad_sent)
    )
    if parts == 2:
        rows = [by_seq, lax.ppermute(by_seq, "x", [(0, 1), (1, 0)])]
    else:
        rows = [lax.all_gather(by_seq, "x", axis=0, tiled=False)]
    *rows, grad_sent[0] = lax.optimization_barrier((*rows, grad_sent[0]))
    grad_came = [swap_all(grad_sent[0], ranks)]

    qkv, normed = project(rows, attn_scale, weights, group, cosine, sine, x_ref, parts)
    attended, lse = (attend if fused else plain_attend)(qkv, seg_row, seg_col)
    attended = after(attended, grad_came[0])
    attended = swap_all(attended.reshape(experts, span, group), ranks)
    attended, grad_sent[1] = lax.optimization_barrier((attended, grad_sent[1]))
    grad_came.append(swap_all(grad_sent[1], ranks))
    attended = attended.reshape(seqs, parts, span, group)

    hidden, branch_in = after_attention(flat_tokens, attended, w_out, ffn_scale)
    sent = [dispatch(branch_in, target_rows[0], experts, half)]
    shared_out, shared_back, hid, dg, du = feed_forward(
        after(branch_in, sent[0]), flat_cot, shared_gate, shared_up, shared_down
    )
    sent.append(dispatch(after(branch_in, shared_out), target_rows[1], experts, half))
    sent[0] = after(sent[0], grad_came[1], shared_out)
    received = [swap_all(value, ranks).reshape(-1, width) for value in sent]
    keep, give = shared_weight_grads(branch_in, flat_cot, dg, du, hid, sizes, core_ref)
    shared_sums, _ = fold(both(keep, give), "y")

    router = jnp.pad(w_router, ((0, 0), (0, 128 - experts)))
    made, back_rows, halves = None, [], []
    before = (give, sent[1])
    for at in range(2):
        grad_rows = grad_came[at][:, :half, :].reshape(-1, width)
        other = grad_came[at][:, half, :half].astype(jnp.int32).reshape(-1, 1)
        rows_at = after(received[at], grad_rows, other, *before)
        made, back, hid, dg, du, gated_grads, grad_logits = feed_forward(
            rows_at, grad_rows, expert_gate[0], expert_up[0], expert_down[0], router, other, own,
            experts, at, made,
        )
        back_rows.append(swap_all(back.reshape(experts, half, width), ranks).reshape(-1, width))
        halves.append((rows_at, gated_grads, dg, du, hid, grad_logits))
        before = (back,)
    halves[1] = (after(halves[1][0], back_rows[0]), *halves[1][1:])
    keep, give, grad_router = expert_weight_grads(halves, sizes, pair_ref)
    back_rows[1] = after(back_rows[1], give)
    expert_sums = both(keep, give)

    grad_hidden, grad_attn, grad_att, grad_ffn = middle_back(
        hidden, shared_back, back_rows, target, flat_cot, ffn_scale, w_out, parts, span
    )
    grad_att = swap_all(grad_att.reshape(experts, span, group), ranks).reshape(length, group)

    column = lax.broadcasted_iota(jnp.int32, (width, 128), 1)
    small = jnp.where(column < experts, grad_router, jnp.where(column == experts, grad_ffn, 0.0))
    out_sums = tall_weight_grads(
        [attended[:, part].reshape(count, group) for part in range(parts)],
        [grad_attn],
        [small],
        sizes,
        core_ref,
        WEIGHT,
    )
    out_sums = both(*out_sums)

    made = after(made, grad_att, out_sums[0])
    made_rows = swap_all(made, ranks).reshape(-1, width)
    grads = list(
        (attend_back if fused else plain_attend_back)(
            qkv, grad_att, lse, seg_row, seg_col, cosine, sine
        )
    )
    shared_sums, shared_sent = fold([after(term, grads[0]) for term in shared_sums], "x")
    grads[0] = after(grads[0], shared_sent)
    normed_back, grad_gain = project_back(grads, weights, rows, x_ref, parts)
    normed_back, _ = fold([normed_back], "x")
    shared_sums = total(shared_sums).astype(BF)
    pieces = swap_by_steps(after(total(normed_back).astype(BF), shared_sums, made_rows), "z")

    qkv_sums = tall_weight_grads([normed], list(grads), [grad_gain], sizes, core_ref, 0.2)
    last = [jnp.concatenate(pair, axis=-1) for pair in zip(out_sums, both(*qkv_sums))]
    last, last_sent = fold(last, "y", shared_sums)
    expert_sums, _ = fold(expert_sums, "y", last_sent, ordered=True)
    token_grad = first_norm_back(flat_tokens, attn_scale, pieces, grad_hidden, z_ref)
    layer_out = layer_end(hidden, shared_out, [made_rows], whole_target).reshape(tokens.shape)

    shared_sums = swap_by_steps(shared_sums, "z")
    last = after(total(last).astype(BF), made_rows)
    each, cols = last.shape[-2:]
    last = swap_all(last.reshape(experts, each, cols), ranks).astype(F32)
    last = jnp.sum(last.reshape(blocks, parts, each, cols), axis=0)
    out_sums = jnp.sum(last[:, :, : width + 128], axis=0)
    qkv_sums = last[:, :, width + 128 :]
    grad_attn_gain = jnp.sum(qkv_sums[:, :, 3 * group], axis=0)
    grad_w_qkv = qkv_sums[:, :, : 3 * group].reshape(parts, each, 3, group)
    grad_w_qkv = jnp.transpose(grad_w_qkv, (1, 2, 0, 3)).reshape(each, 3 * width)

    shared_sums, expert_sums = total(shared_sums), total(expert_sums)
    return (
        layer_out,
        token_grad.reshape(tokens.shape),
        grad_attn_gain,
        grad_w_qkv,
        out_sums[:, :width],
        out_sums[:, width + experts],
        out_sums[:, width : width + experts],
        shared_sums[0],
        shared_sums[1],
        jnp.transpose(shared_sums[2]),
        expert_sums[0][None],
        expert_sums[1][None],
        jnp.transpose(expert_sums[2])[None],
    )


def solution(mesh):
    dp, experts = mesh.shape["dp"], mesh.shape["expert"]

    def step(*args):
        seqs = args[0].shape[0] // dp
        cores = 2 if dp % 2 == 0 else 1
        fine = Mesh(
            mesh.devices.reshape(dp // cores, cores, seqs, experts // seqs),
            ("y", "core", "z", "x"),
        )
        data, ranks, every = ("y", "core"), ("z", "x"), ("y", "core", "z", "x")
        placed = (
            P(data, ranks, None),
            P(data, None),
            P(data, ranks, None),
            P(data, ranks, None),
            P(data, ranks, None),
            *([P()] * 8),
            P(ranks, None, None),
            P(ranks, None, None),
            P(ranks, None, None),
        )
        return jax.shard_map(
            on_device,
            mesh=fine,
            in_specs=placed,
            out_specs=(
                P(data, ranks, None),
                P(data, ranks, None),
                P(every),
                P(every, None),
                P(every, None),
                P(every),
                P(every, None),
                P(every, None),
                P(every, None),
                P(None, every),
                P(ranks, None, data),
                P(ranks, None, data),
                P(ranks, data, None),
            ),
            check_vma=False,
        )(*args)

    return step
```

```python
import jax
import jax.numpy as jnp
from jax import lax
from jax.experimental import pallas as pl
from jax.experimental.pallas import tpu as pltpu
from jax.sharding import Mesh
from jax.sharding import PartitionSpec as P

HEAD_DIM = 64
EPS = 1e-06
BF = jnp.bfloat16
F32 = jnp.float32
NEG = -1e30
NN = (((1,), (0,)), ((), ()))
NT = (((1,), (1,)), ((), ()))
TN = (((0,), (0,)), ((), ()))
VMEM_MOST = 60 << 20
WEIGHT = 3


def mm(left, right, dims=NN):
    return lax.dot_general(left, right, dims, preferred_element_type=F32)


def sds(shape, dtype):
    return jax.ShapeDtypeStruct(shape, dtype)


def call(
    body, grid, in_specs, out_specs, out_shape, args, scratch=(), prefetch=0, flops=0, alias=None
):
    leaves = jax.tree.leaves(out_shape)
    moved = sum(a.size * a.dtype.itemsize for a in args) + sum(
        a.size * a.dtype.itemsize for a in leaves
    )
    return pl.pallas_call(
        body,
        out_shape=out_shape,
        grid_spec=pltpu.PrefetchScalarGridSpec(
            num_scalar_prefetch=prefetch,
            grid=grid,
            in_specs=in_specs,
            out_specs=out_specs,
            scratch_shapes=list(scratch),
        ),
        compiler_params=pltpu.CompilerParams(
            dimension_semantics=("arbitrary",) * len(grid), vmem_limit_bytes=VMEM_MOST
        ),
        cost_estimate=pl.CostEstimate(
            flops=int(flops), transcendentals=0, bytes_accessed=int(moved)
        ),
        input_output_aliases=alias or {},
    )(*args)


def whole(shape):
    rank = len(shape)
    return pl.BlockSpec(tuple(shape), lambda *_: (0,) * rank)


def swap_halves(value):
    lane = lax.broadcasted_iota(jnp.int32, value.shape, 1)
    return jnp.where(lane % 64 < 32, pltpu.roll(value, 96, 1), pltpu.roll(value, 32, 1))


def rms(values):
    return lax.rsqrt(jnp.mean(values * values, axis=1, keepdims=True) + EPS)


def row_specs(rows):
    if len(rows) == 2:
        _, span, width = rows[0].shape
        return [pl.BlockSpec((1, span, width), lambda i, *_: (i, 0, 0))] * 2
    parts, _, span, width = rows[0].shape
    return [pl.BlockSpec((parts, 1, span, width), lambda i, *_: (0, i, 0, 0))]


def load_rows(refs, at_ref):
    if len(refs) == 2:
        mine, theirs = refs[0][0].astype(F32), refs[1][0].astype(F32)
        first = at_ref[0] == 0
        pair = [jnp.where(first, mine, theirs), jnp.where(first, theirs, mine)]
        return jnp.concatenate(pair, axis=0)
    value = refs[0][...]
    return value.reshape(value.shape[0] * value.shape[2], value.shape[3]).astype(F32)


def weight_specs(weights, group):
    if len(weights) == 1:
        return [whole(weights[0].shape)]
    width, cols = weights[0].shape
    parts = cols // (3 * group)

    def spec(index):
        return pl.BlockSpec((width, group), lambda i, at: (0, index * parts + at[0]))

    return [spec(index) for index in range(3)]


def load_weights(refs, group):
    if len(refs) == 3:
        return [ref[...] for ref in refs]
    return [refs[0][:, at * group : (at + 1) * group] for at in range(3)]


def project(rows, gain, weights, group, cosine, sine, x_at, parts):
    blocks, span, width = rows[0].shape[-3:]
    height = parts * span
    length = height * blocks
    cut = len(rows)

    def body(at_ref, *refs):
        r_refs, (g_ref, c_ref, s_ref) = refs[:cut], refs[cut : cut + 3]
        w_refs, (qkv_ref, n_ref) = refs[cut + 3 : -2], refs[-2:]
        tok = load_rows(r_refs, at_ref)
        normed = (tok * rms(tok) * g_ref[...]).astype(BF)
        n_ref[...] = normed
        if len(w_refs) == 3:
            found = [mm(normed, ref[...]) for ref in w_refs]
            turning = [(found[0], 0), (found[1], group)]
            last = found[2]
        else:
            found = mm(normed, w_refs[0][...])
            turning, last = [(found[:, : 2 * group], 0)], found[:, 2 * group :]
        for value, base in turning:
            for at in range(0, value.shape[1], 128):
                part = value[:, at : at + 128]
                lane = lax.broadcasted_iota(jnp.int32, part.shape, 1) + (base + at)
                turned = part * c_ref[...] + swap_halves(part) * s_ref[...]
                turned = turned * jnp.where(lane < group, HEAD_DIM**-0.5, 1.0)
                qkv_ref[:, base + at : base + at + 128] = turned.astype(BF)
        qkv_ref[:, 2 * group :] = last.astype(BF)

    return call(
        body,
        (blocks,),
        [
            *row_specs(rows),
            whole((1, width)),
            pl.BlockSpec((height, 128), lambda i, *_: (i, 0)),
            pl.BlockSpec((height, 128), lambda i, *_: (i, 0)),
            *weight_specs(weights, group),
        ],
        [
            pl.BlockSpec((height, 3 * group), lambda i, *_: (i, 0)),
            pl.BlockSpec((height, width), lambda i, *_: (i, 0)),
        ],
        [sds((length, 3 * group), BF), sds((length, width), BF)],
        (x_at, *rows, gain, cosine, sine, *weights),
        prefetch=1,
        flops=6 * length * width * group,
    )


def project_back(grads, weights, rows, x_at, parts):
    blocks, span, width = rows[0].shape[-3:]
    group = grads[0].shape[1]
    height = parts * span
    length = height * blocks
    cut = len(rows)

    def body(at_ref, q_ref, k_ref, v_ref, *refs):
        r_refs, w_refs, (out_ref, gain_ref, acc_ref) = refs[:cut], refs[cut:-3], refs[-3:]
        step = pl.program_id(0)
        w_q, w_k, w_v = load_weights(w_refs, group)
        back = mm(q_ref[...], w_q, NT) + mm(k_ref[...], w_k, NT) + mm(v_ref[...], w_v, NT)
        tok = load_rows(r_refs, at_ref)
        part = jnp.sum(back * tok * rms(tok), axis=0, keepdims=True)

        @pl.when(step == 0)
        def _():
            acc_ref[...] = jnp.zeros_like(acc_ref)

        acc_ref[...] += jnp.broadcast_to(part, acc_ref.shape)
        out_ref[...] = back.astype(BF).reshape(parts, 1, span, width)

        @pl.when(step == blocks - 1)
        def _():
            column = jnp.transpose(acc_ref[...])
            gain_ref[...] = jnp.broadcast_to(column[:, :1], gain_ref.shape)

    block = pl.BlockSpec((height, group), lambda i, *_: (i, 0))
    return call(
        body,
        (blocks,),
        [block, block, block, *row_specs(rows), *weight_specs(weights, group)],
        [
            pl.BlockSpec((parts, 1, span, width), lambda i, *_: (0, i, 0, 0)),
            whole((width, 128)),
        ],
        [sds((parts, blocks, span, width), BF), sds((width, 128), F32)],
        (x_at, *grads, *rows, *weights),
        scratch=[pltpu.VMEM((8, width), F32)],
        prefetch=1,
        flops=0.2 * length * width * group,
    )


def attend(qkv, seg_row, seg_col):
    length, cols = qkv.shape
    group = cols // 3
    pairs = group // 128
    high = min(256, length)

    def body(q_ref, k_ref, v_ref, sr_ref, sc_ref, o_ref, l_ref):
        lane = lax.broadcasted_iota(jnp.int32, (high, 128), 1)
        for at in range(0, length, high):
            end = at + high
            query = q_ref[at:end, :]
            keys = k_ref[:end, :]
            vals = v_ref[:end, :]
            q_pos = lax.broadcasted_iota(jnp.int32, (high, end), 0) + at
            k_pos = lax.broadcasted_iota(jnp.int32, (high, end), 1)
            allowed = (sc_ref[at:end, :] == sr_ref[:, :end]) & (k_pos <= q_pos)
            outs = []
            for head in range(2):
                mine = (lane // 64) == head
                scores = mm(jnp.where(mine, query, jnp.zeros_like(query)), keys, NT)
                scores = jnp.where(allowed, scores, NEG)
                most = jnp.max(scores, axis=1, keepdims=True)
                expo = jnp.exp(scores - most)
                total = jnp.sum(expo, axis=1, keepdims=True)
                outs.append(mm(expo.astype(BF), vals) / total)
                lse = jnp.broadcast_to(most + jnp.log(total), (high, 128))
                l_ref[0, head : head + 1, at:end] = jnp.transpose(lse)[:1, :]
            o_ref[at:end, :] = jnp.where(lane < 64, outs[0], outs[1]).astype(BF)

    def col(offset):
        return pl.BlockSpec((length, 128), lambda i: (0, offset * pairs + i))

    return call(
        body,
        (pairs,),
        [col(0), col(1), col(2), whole((1, length)), whole((length, 1))],
        [col(0), pl.BlockSpec((1, 2, length), lambda i: (i, 0, 0))],
        [sds((length, group), BF), sds((pairs, 2, length), F32)],
        (qkv, qkv, qkv, seg_row, seg_col),
        flops=4 * length * length * group,
    )


def attend_back(qkv, grad, lse, seg_row, seg_col, cosine, sine):
    length, cols = qkv.shape
    group = cols // 3
    pairs = group // 128
    high = min(256, length)

    def body(
        q_ref, k_ref, v_ref, g_ref, l_ref, sr_ref, sc_ref, c_ref, s_ref, dq_ref, dk_ref, dv_ref,
        ka_ref, va_ref,
    ):
        lane = lax.broadcasted_iota(jnp.int32, (high, 128), 1)
        ka_ref[...] = jnp.zeros_like(ka_ref)
        va_ref[...] = jnp.zeros_like(va_ref)
        for at in range(0, length, high):
            end = at + high
            query = q_ref[at:end, :]
            grads = g_ref[at:end, :]
            keys = k_ref[:end, :]
            vals = v_ref[:end, :]
            k_pos = lax.broadcasted_iota(jnp.int32, (end, high), 0)
            q_pos = lax.broadcasted_iota(jnp.int32, (end, high), 1) + at
            allowed = (sc_ref[:end, :] == sr_ref[:, at:end]) & (k_pos <= q_pos)
            outs = []
            for head in range(2):
                mine = (lane // 64) == head
                q_own = jnp.where(mine, query, jnp.zeros_like(query))
                g_own = jnp.where(mine, grads, jnp.zeros_like(grads))
                scores = jnp.where(allowed, mm(keys, q_own, NT), NEG)
                probs = jnp.exp(scores - l_ref[0, head : head + 1, at:end])
                grad_probs = mm(vals, g_own, NT)
                delta = jnp.sum(probs * grad_probs, axis=0, keepdims=True)
                grad_scores = (probs * (grad_probs - delta)).astype(BF)
                va_ref[:end, :] += mm(probs.astype(BF), g_own)
                ka_ref[:end, :] += mm(grad_scores, q_own)
                outs.append(mm(grad_scores, keys, TN))
            found = jnp.where(lane < 64, outs[0], outs[1]) * HEAD_DIM**-0.5
            back = found * c_ref[at:end, :] - swap_halves(found) * s_ref[at:end, :]
            dq_ref[at:end, :] = back.astype(BF)
        found = ka_ref[...]
        dk_ref[...] = (found * c_ref[...] - swap_halves(found) * s_ref[...]).astype(BF)
        dv_ref[...] = va_ref[...].astype(BF)

    def col(offset):
        return pl.BlockSpec((length, 128), lambda i: (0, offset * pairs + i))

    return call(
        body,
        (pairs,),
        [
            col(0),
            col(1),
            col(2),
            col(0),
            pl.BlockSpec((1, 2, length), lambda i: (i, 0, 0)),
            whole((1, length)),
            whole((length, 1)),
            whole((length, 128)),
            whole((length, 128)),
        ],
        [col(0), col(0), col(0)],
        [sds((length, group), BF)] * 3,
        (qkv, qkv, qkv, grad, lse, seg_row, seg_col, cosine, sine),
        scratch=[pltpu.VMEM((length, 128), F32)] * 2,
        flops=length * length * group,
    )


def heads_of(flat):
    return flat.reshape(flat.shape[0], -1, HEAD_DIM)


def plain_mask(seg_row, seg_col):
    length = seg_col.shape[0]
    spots = jnp.arange(length, dtype=jnp.int32)
    return (seg_row == seg_col) & (spots[None, :] <= spots[:, None])


def plain_attend(qkv, seg_row, seg_col):
    query, keys, vals = (heads_of(part) for part in jnp.split(qkv, 3, axis=1))
    scores = jnp.einsum("qhd,khd->hqk", query, keys, preferred_element_type=F32)
    scores = jnp.where(plain_mask(seg_row, seg_col)[None], scores, NEG)
    lse = jax.nn.logsumexp(scores, axis=-1, keepdims=True)
    probs = jnp.exp(scores - lse).astype(BF)
    found = jnp.einsum("hqk,khd->qhd", probs, vals, preferred_element_type=F32)
    return found.astype(BF).reshape(qkv.shape[0], -1), lse


def plain_turn_back(grads, cosine, sine):
    table_c, table_s = cosine[:, None, :HEAD_DIM], sine[:, None, :HEAD_DIM]
    swapped = jnp.roll(grads, HEAD_DIM // 2, axis=-1)
    return (grads * table_c - swapped * table_s).astype(BF).reshape(grads.shape[0], -1)


def plain_attend_back(qkv, grad, lse, seg_row, seg_col, cosine, sine):
    query, keys, vals = (heads_of(part) for part in jnp.split(qkv, 3, axis=1))
    grad = heads_of(grad)
    scores = jnp.einsum("qhd,khd->hqk", query, keys, preferred_element_type=F32)
    scores = jnp.where(plain_mask(seg_row, seg_col)[None], scores, NEG)
    probs = jnp.exp(scores - lse)
    grad_probs = jnp.einsum("qhd,khd->hqk", grad, vals, preferred_element_type=F32)
    delta = jnp.sum(probs * grad_probs, axis=-1, keepdims=True)
    grad_scores = (probs * (grad_probs - delta)).astype(BF)
    gq = jnp.einsum("hqk,khd->qhd", grad_scores, keys, preferred_element_type=F32)
    gk = jnp.einsum("hqk,qhd->khd", grad_scores, query, preferred_element_type=F32)
    gv = jnp.einsum("hqk,qhd->khd", probs.astype(BF), grad, preferred_element_type=F32)
    return (
        plain_turn_back(gq * HEAD_DIM**-0.5, cosine, sine),
        plain_turn_back(gk, cosine, sine),
        gv.astype(BF).reshape(qkv.shape[0], -1),
    )


def after_attention(tokens, attended, w_out, gain):
    seqs, parts, span, group = attended.shape
    count, width = tokens.shape

    def body(t_ref, a_ref, w_ref, g_ref, h_ref, b_ref):
        hidden = t_ref[...].astype(F32)
        for part in range(parts):
            rows = a_ref[:, part].reshape(count, group)
            hidden += mm(rows, w_ref[part * group : (part + 1) * group, :])
        h_ref[...] = hidden
        b_ref[...] = (hidden * rms(hidden) * g_ref[...]).astype(BF)

    return call(
        body,
        (1,),
        [whole(a.shape) for a in (tokens, attended, w_out, gain)],
        [whole(tokens.shape)] * 2,
        [sds(tokens.shape, F32), sds(tokens.shape, BF)],
        (tokens, attended, w_out, gain),
        flops=2 * count * width * width,
    )


def dispatch(rows, target_rows, experts, capacity, route_rows=None):
    count, width = rows.shape
    more = 0 if route_rows is None else 16
    tables = () if route_rows is None else (route_rows,)

    def body(r_ref, t_ref, *refs):
        o_ref = refs[-1]
        slot = lax.broadcasted_iota(jnp.int32, (capacity, count), 0)
        slot += pl.program_id(0) * capacity
        hits = [slot == t_ref[k : k + 1, :] for k in range(2)]
        hot = (hits[0] | hits[1]).astype(F32).astype(BF)
        o_ref[0, :capacity, :] = mm(hot, r_ref[...]).astype(BF)
        if more:
            o_ref[0, capacity:, :] = jnp.zeros((more, width), BF)
            other = jnp.zeros((8, capacity), F32)
            for k in range(2):
                route = jnp.broadcast_to(refs[0][1 - k : 2 - k, :].astype(F32), (8, count))
                other += mm(route.astype(BF), hits[k].astype(F32).astype(BF), NT)
            o_ref[0, capacity : capacity + 8, :capacity] = other.astype(BF)

    return call(
        body,
        (experts,),
        [whole(a.shape) for a in (rows, target_rows, *tables)],
        pl.BlockSpec((1, capacity + more, width), lambda i: (i, 0, 0)),
        sds((experts, capacity + more, width), BF),
        (rows, target_rows, *tables),
        flops=2 * experts * capacity * count * width,
    )


def pick(target, row_refs):
    total = None
    for index, ref in enumerate(row_refs):
        rows = ref[...]
        spot = lax.broadcasted_iota(jnp.int32, (target.shape[0], rows.shape[0]), 1)
        one, two = target[:, 2 * index : 2 * index + 1], target[:, 2 * index + 1 : 2 * index + 2]
        found = mm(((spot == one) | (spot == two)).astype(F32).astype(BF), rows)
        total = found if total is None else total + found
    return total


def layer_end(hidden, shared_out, rows, target):
    count, width = hidden.shape
    high = count // 2

    def body(h_ref, s_ref, t_ref, *refs):
        refs[-1][...] = (h_ref[...] + s_ref[...] + pick(t_ref[...], refs[:-1])).astype(BF)

    block = pl.BlockSpec((high, width), lambda i: (i, 0))
    return call(
        body,
        (2,),
        [
            block,
            block,
            pl.BlockSpec((high, target.shape[1]), lambda i: (i, 0)),
            *[whole(part.shape) for part in rows],
        ],
        block,
        sds(hidden.shape, BF),
        (hidden, shared_out, target, *rows),
        flops=2 * count * width * rows[0].shape[0] * len(rows),
    )


def middle_back(hidden, grad_shared, rows, target, cotangent, gain, w_out, parts, span):
    count, width = hidden.shape
    seqs = count // span
    each = 2 if seqs % 2 == 0 else 1
    high = each * span
    steps = count // high
    group = width // parts

    def body(h_ref, s_ref, t_ref, c_ref, g_ref, w_ref, *refs):
        gh_ref, ga_ref, d_ref, n_ref, acc_ref = refs[len(rows) :]
        step = pl.program_id(0)
        branch = s_ref[...] + pick(t_ref[...], refs[: len(rows)])
        hidden = h_ref[...]
        scale = rms(hidden)
        weighted = branch * g_ref[...]
        inner = jnp.mean(weighted * hidden, axis=1, keepdims=True)
        part = jnp.sum(branch * hidden * scale, axis=0, keepdims=True)
        out = c_ref[...].astype(F32) + scale * weighted - hidden * (scale * scale * scale * inner)
        gh_ref[...] = out
        out = out.astype(BF)
        ga_ref[...] = out
        for at in range(parts):
            sent = mm(out, w_ref[at * group : (at + 1) * group, :], NT).astype(BF)
            d_ref[:, at] = sent.reshape(each, span, group)

        @pl.when(step == 0)
        def _():
            acc_ref[...] = jnp.zeros_like(acc_ref)

        acc_ref[...] += jnp.broadcast_to(part, acc_ref.shape)

        @pl.when(step == steps - 1)
        def _():
            column = jnp.transpose(acc_ref[...])
            n_ref[...] = jnp.broadcast_to(column[:, :1], n_ref.shape)

    block = pl.BlockSpec((high, width), lambda i: (i, 0))
    return call(
        body,
        (steps,),
        [
            block,
            block,
            pl.BlockSpec((high, target.shape[1]), lambda i: (i, 0)),
            block,
            whole(gain.shape),
            whole(w_out.shape),
            *[whole(part.shape) for part in rows],
        ],
        [
            block,
            block,
            pl.BlockSpec((each, parts, span, group), lambda i: (i, 0, 0, 0)),
            whole((width, 128)),
        ],
        [
            sds(hidden.shape, F32),
            sds(hidden.shape, BF),
            sds((seqs, parts, span, group), BF),
            sds((width, 128), F32),
        ],
        (hidden, grad_shared, target, cotangent, gain, w_out, *rows),
        scratch=[pltpu.VMEM((8, width), F32)],
        flops=WEIGHT * 2 * count * width * (rows[0].shape[0] * len(rows) + width),
    )


def first_norm_back(tokens, gain, pieces, grad_hidden, z_at):
    count, width = tokens.shape
    blocks = len(pieces)
    span = count // blocks

    def body(at_ref, t_ref, g_ref, h_ref, *refs):
        o_ref = refs[-1]
        for index in range(blocks):
            seq = (at_ref[0] + blocks - index) % blocks
            spot = pl.ds(pl.multiple_of(seq * span, span), span)
            tok = t_ref[spot, :].astype(F32)
            scale = rms(tok)
            weighted = refs[index][...].astype(F32) * g_ref[...]
            inner = jnp.mean(weighted * tok, axis=1, keepdims=True)
            out = h_ref[spot, :] + scale * weighted - tok * (scale * scale * scale * inner)
            o_ref[spot, :] = out.astype(BF)

    return call(
        body,
        (1,),
        [whole(a.shape) for a in (tokens, gain, grad_hidden, *pieces)],
        whole(tokens.shape),
        sds(tokens.shape, BF),
        (z_at, tokens, gain, grad_hidden, *pieces),
        prefetch=1,
    )


def feed_forward(
    rows, grads, w_gate, w_up, w_down, router=None, other=None, own=None, experts=0, place=0, made=None
):
    count, width = rows.shape
    units = w_gate.shape[1]
    wide = 512
    steps = units // wide
    high = 256
    gated = router is not None
    more = 0 if made is None else 1
    kind = BF if gated else F32

    def body(*refs):
        if gated:
            (own_ref, x_ref, g_ref, wg_ref, wu_ref, wd_ref, wr_ref, ot_ref) = refs[:8]
            (y_ref, gi_ref, hid_ref, dg_ref, du_ref, eo_ref, gl_ref, ya_ref, ga_ref, gate_ref) = refs[8 + more :]
        else:
            (x_ref, g_ref, wg_ref, wu_ref, wd_ref,
             y_ref, gi_ref, hid_ref, dg_ref, du_ref, ya_ref, ga_ref) = refs
        step = pl.program_id(0)

        if gated:

            @pl.when(step == 0)
            def _():
                logits = mm(x_ref[...], wr_ref[...])
                lane = lax.broadcasted_iota(jnp.int32, logits.shape, 1)
                mine = jnp.sum(jnp.where(lane == own_ref[0], logits, 0.0), axis=1, keepdims=True)
                theirs = jnp.sum(jnp.where(lane == ot_ref[...], logits, 0.0), axis=1, keepdims=True)
                gate = 1.0 / (1.0 + jnp.exp(theirs - mine))
                rest = 1.0 / (1.0 + jnp.exp(mine - theirs))
                gate_ref[:, 0:1] = gate
                gate_ref[:, 1:2] = rest
                eo_ref[...] = (g_ref[...].astype(F32) * gate).astype(BF)

        def rows_at(index, carry):
            at = pl.ds(pl.multiple_of(index * high, high), high)
            row = x_ref[at, :]
            grad = eo_ref[at, :] if gated else g_ref[at, :]
            gval = mm(row, wg_ref[...])
            uval = mm(row, wu_ref[...])
            sigma = 1.0 / (1.0 + jnp.exp(-gval))
            silu = gval * sigma
            hid = (silu * uval).astype(BF)
            hid_ref[at, :] = hid
            grad_hid = mm(grad, wd_ref[...], NT)
            du = (grad_hid * silu).astype(BF)
            dg = (grad_hid * uval * sigma * (1.0 + gval * (1.0 - sigma))).astype(BF)
            du_ref[at, :] = du
            dg_ref[at, :] = dg
            out = mm(hid, wd_ref[...])
            back = mm(dg, wg_ref[...], NT) + mm(du, wu_ref[...], NT)

            @pl.when(step == 0)
            def _():
                ya_ref[at, :] = out
                ga_ref[at, :] = back

            @pl.when(step > 0)
            def _():
                ya_ref[at, :] += out
                ga_ref[at, :] += back

            return carry

        lax.fori_loop(0, count // high, rows_at, 0)

        @pl.when(step == steps - 1)
        def _():
            if gated:
                out = ya_ref[...]
                gate = gate_ref[:, 0:1]
                lean = jnp.sum(out * g_ref[...].astype(F32), axis=1, keepdims=True)
                lean = lean * gate * gate_ref[:, 1:2]
                lane = lax.broadcasted_iota(jnp.int32, (count, 128), 1)
                sign = (lane == own_ref[0]).astype(F32) - (lane == ot_ref[...]).astype(F32)
                grad_logits = (lean * sign).astype(BF)
                gl_ref[...] = grad_logits
                y_ref[...] = (out * gate).astype(BF).reshape(y_ref.shape)
                gi_ref[...] = (ga_ref[...] + mm(grad_logits, wr_ref[...], NT)).astype(BF)
            else:
                y_ref[...] = ya_ref[...]
                gi_ref[...] = ga_ref[...]

    full = whole((count, width))
    hidden = pl.BlockSpec((count, wide), lambda i, *_: (0, i))
    in_specs = [
        full,
        full,
        pl.BlockSpec((width, wide), lambda i, *_: (0, i)),
        pl.BlockSpec((width, wide), lambda i, *_: (0, i)),
        pl.BlockSpec((wide, width), lambda i, *_: (i, 0)),
    ]
    out_specs = [full, full, hidden, hidden, hidden]
    out_shape = [sds((count, width), kind)] * 2 + [sds((count, units), BF)] * 3
    scratch = [pltpu.VMEM((count, width), F32)] * 2
    args = [rows, grads, w_gate, w_up, w_down]
    if gated:
        in_specs += [whole(router.shape), whole(other.shape)]
        out_specs += [full, whole((count, 128))]
        out_shape += [sds((count, width), BF), sds((count, 128), BF)]
        scratch += [pltpu.VMEM((count, 128), F32)]
        args = [own, *args, router, other]
        out_specs[0] = pl.BlockSpec((experts, count // experts, width), lambda *_: (0, place, 0))
        out_shape[0] = sds((experts, 2 * count // experts, width), BF)
        if more:
            in_specs += [pl.BlockSpec(memory_space=pl.ANY)]
            args += [made]
    return call(
        body,
        (steps,),
        in_specs,
        out_specs,
        out_shape,
        tuple(args),
        scratch=scratch,
        prefetch=1 if gated else 0,
        alias={len(args) - 1: 0} if more else None,
        flops=12 * count * width * units,
    )


def expert_weight_grads(halves, sizes, core_at):
    outer, cores = sizes["y"], sizes["core"]
    count, width = halves[0][0].shape
    units = halves[0][2].shape[1]
    wide = units // (outer * cores)

    def body(at_ref, *refs):
        keep_ref, give_ref, r_ref = refs[-3:]
        groups = [refs[6 * at : 6 * at + 6] for at in range(len(halves))]
        step = pl.program_id(0)

        def over(left, right):
            return sum(mm(group[left][...], group[right][...], TN) for group in groups)

        found = [over(0, 2).astype(BF), over(0, 3).astype(BF), over(1, 4).astype(BF)]

        @pl.when(step < outer)
        def _():
            for index in range(3):
                give_ref[0, index] = found[index]

        @pl.when(step >= outer)
        def _():
            for index in range(3):
                keep_ref[0, index] = found[index]

        @pl.when(step == 0)
        def _():
            r_ref[...] = over(0, 5)

    def taken(i, at):
        core = jnp.where(i < outer, 1 - at[0], at[0])
        y = (i + 1 + at[1]) % outer if outer == 2 else i % outer
        return (0, y * cores + core)

    hidden = pl.BlockSpec((count, wide), taken)
    part = (1, 3, width, wide)
    return call(
        body,
        (outer * cores,),
        [
            whole((count, width)),
            whole((count, width)),
            hidden,
            hidden,
            hidden,
            whole((count, 128)),
        ]
        * len(halves),
        [
            pl.BlockSpec(part, lambda i, *_: (jnp.maximum(i - outer, 0), 0, 0, 0)),
            pl.BlockSpec(part, lambda i, *_: (jnp.minimum(i, outer - 1), 0, 0, 0)),
            whole((width, 128)),
        ],
        [sds((outer, *part[1:]), BF)] * 2 + [sds((width, 128), F32)],
        (core_at, *[value for half in halves for value in half]),
        prefetch=1,
        flops=6 * count * len(halves) * width * units,
    )


def spread_places(sizes, names):
    found = []
    for y in range(sizes["y"]):
        for core in range(sizes["core"]):
            for z in range(sizes["z"]):
                for x in range(sizes["x"]):
                    at = {"y": y, "core": core, "z": z, "x": x}
                    found.append((core, tuple(at[n] for n in names)))
    return found


def spread(value, sizes, names, core_at):
    order = ("y", "core", "z", "x")
    split = value.reshape(*(sizes[n] for n in order), -1, value.shape[-1])
    split = jnp.transpose(split, (1, *(order.index(n) for n in names), 4, 5))
    return at_index(split, core_at[0]), at_index(split, 1 - core_at[0])


def store_spread(places, each, core_at, found, row, keep, give):
    first = row // each
    for core in range(2):
        todo = [at for at in range(found.shape[0] // each) if places[first + at][0] == core]

        def put(store, todo=todo):
            for at in todo:
                store(places[first + at][1], found[at * each : (at + 1) * each].astype(BF))

        pl.when(core_at == core)(lambda put=put: put(keep))
        pl.when(core_at != core)(lambda put=put: put(give))


def shared_weight_grads(rows, grads, dg, du, hid, sizes, core_at):
    names = ("y", "x", "z")
    lead = tuple(sizes[n] for n in names)
    places = spread_places(sizes, names)
    count, width = rows.shape
    units = dg.shape[1]
    wide = 512
    each = width // len(places)
    direct = each % 8 == 0

    def body(at_ref, x_ref, g_ref, dg_ref, du_ref, hid_ref, *outs):
        pairs = ((x_ref, dg_ref), (x_ref, du_ref), (g_ref, hid_ref))
        for index, (left, right) in enumerate(pairs):
            found = mm(left[...], right[...], TN)
            if not direct:
                outs[0][index] = found.astype(BF)
                continue

            def into(ref, index=index):
                def store(place, piece):
                    ref[(*place, index)] = piece

                return store

            store_spread(places, each, at_ref[0], found, 0, into(outs[0]), into(outs[1]))

    hidden = pl.BlockSpec((count, wide), lambda i, *_: (0, i))
    if direct:
        shapes = [(*lead, 3, each, units)] * 2
        spec = [pl.BlockSpec((*lead, 3, each, wide), lambda i, *_: (0,) * 5 + (i,))] * 2
    else:
        shapes = [(3, width, units)]
        spec = [pl.BlockSpec((3, width, wide), lambda i, *_: (0, 0, i))]
    out = call(
        body,
        (units // wide,),
        [whole(rows.shape), whole(grads.shape), hidden, hidden, hidden],
        spec,
        [sds(shape, BF) for shape in shapes],
        (core_at, rows, grads, dg, du, hid),
        prefetch=1,
        flops=6 * count * width * units,
    )
    if direct:
        return out
    found = [spread(out[0][i], sizes, names, core_at) for i in range(3)]
    return [jnp.stack([part[side] for part in found], axis=3) for side in range(2)]


def tall_weight_grads(lefts, rights, extras, sizes, core_at, weight=1):
    names = ("y", "z", "x")
    lead = tuple(sizes[n] for n in names)
    places = spread_places(sizes, names)
    width = sum(left.shape[1] for left in lefts)
    cols = sum(right.shape[1] for right in rights)
    each = width // len(places)
    direct = each % 8 == 0
    flops = weight * 2 * lefts[0].shape[0] * width * cols

    def body(at_ref, *refs):
        left_refs = refs[: len(lefts)]
        right_refs = refs[len(lefts) : len(lefts) + len(rights)]
        rest = refs[len(lefts) + len(rights) :]
        extra_refs, outs = rest[: len(extras)], rest[len(extras) :]

        def save(row, found, col):
            span = found.shape[1]
            if not direct:
                outs[0][row : row + found.shape[0], col : col + span] = found.astype(BF)
                return

            def into(ref):
                def store(place, piece):
                    ref[(*place, slice(None), slice(col, col + span))] = piece

                return store

            store_spread(places, each, at_ref[0], found, row, into(outs[0]), into(outs[1]))

        row = 0
        for left in left_refs:
            col = 0
            for right in right_refs:
                save(row, mm(left[...], right[...], TN), col)
                col += right.shape[1]
            row += left.shape[1]
        more = extra_refs[0][...]
        for extra in extra_refs[1:]:
            more = more + extra[...]
        save(0, more, cols)

    args = (*lefts, *rights, *extras)
    shapes = [(*lead, each, cols + 128)] * 2 if direct else [(width, cols + 128)]
    out = call(
        body,
        (1,),
        [whole(a.shape) for a in args],
        [whole(shape) for shape in shapes],
        [sds(shape, BF) for shape in shapes],
        (core_at, *args),
        prefetch=1,
        flops=flops,
    )
    return out if direct else spread(out[0], sizes, names, core_at)


def scatter_sum(value, name):
    return lax.psum_scatter(value, name, scatter_dimension=0, tiled=False)


def swap_all(value, names):
    return lax.all_to_all(value, names, 0, 0, tiled=True)


def at_index(value, index):
    if isinstance(index, int):
        return value[index]
    return lax.dynamic_index_in_dim(value, index, 0, keepdims=False)


def total(terms):
    return sum(term.astype(F32) for term in terms)


def both(keep, give):
    return [keep, lax.ppermute(give, "core", [(0, 1), (1, 0)])]


def fold(terms, name, *others, ordered=False):
    if lax.axis_size(name) != 2:
        sent = total(terms).astype(BF)
        if others:
            sent = after(sent, *others)
        return [scatter_sum(sent, name)], sent
    at = 1 if ordered else lax.axis_index(name)
    sent = total([at_index(term, 1 - at) for term in terms]).astype(BF)
    if others:
        sent = after(sent, *others)
    got = lax.ppermute(sent, name, [(0, 1), (1, 0)])
    return [at_index(term, at) for term in terms] + [got], sent


def swap_by_steps(value, name):
    size, at = value.shape[0], lax.axis_index(name)
    found = [at_index(value, at)]
    for step in range(1, size):
        sent = at_index(value, (at + step) % size)
        found.append(lax.ppermute(sent, name, [(i, (i + step) % size) for i in range(size)]))
    return found


def after(value, *others):
    return lax.optimization_barrier((value, *others))[0]


def on_device(
    tokens,
    segments,
    routes,
    slots,
    cotangent,
    attn_gain,
    w_qkv,
    w_out,
    ffn_gain,
    w_router,
    shared_gate,
    shared_up,
    shared_down,
    expert_gate,
    expert_up,
    expert_down,
):
    sizes = {name: lax.axis_size(name) for name in ("y", "core", "z", "x")}
    ranks = ("z", "x")
    seqs, span, width = tokens.shape
    blocks, parts = sizes["z"], sizes["x"]
    experts = blocks * parts
    count = seqs * span
    capacity = 3 * count // experts
    length = span * experts
    group = width // parts
    z_at, x_at = lax.axis_index("z"), lax.axis_index("x")
    own = (z_at * parts + x_at).astype(jnp.int32).reshape(1)
    z_ref, x_ref = z_at.astype(jnp.int32).reshape(1), x_at.astype(jnp.int32).reshape(1)
    core_ref = lax.axis_index("core").astype(jnp.int32).reshape(1)
    pair_ref = jnp.stack([lax.axis_index("core"), lax.axis_index("y")]).astype(jnp.int32)
    attn_scale = attn_gain.astype(F32).reshape(1, width)
    ffn_scale = ffn_gain.astype(F32).reshape(1, width)
    flat_tokens = tokens.reshape(count, width)
    flat_cot = cotangent.reshape(count, width)

    route_rows = routes.reshape(count, 2)
    slot_rows = slots.reshape(count, 2)
    half = capacity // 2
    targets = []
    for first in (0, half):
        here = (slot_rows >= first) & (slot_rows < first + half)
        targets.append(jnp.where(here, route_rows * half + slot_rows - first, -1))
    target_rows = [jnp.transpose(target) for target in targets]
    target = jnp.concatenate(targets, axis=1)
    whole_target = jnp.where(slot_rows >= 0, route_rows * capacity + slot_rows, -1)
    route_flat = jnp.transpose(route_rows)
    grad_sent = [dispatch(flat_cot, to, experts, half, route_flat) for to in target_rows]

    frequency = jnp.power(10000.0, -2.0 * jnp.arange(32, dtype=F32) / HEAD_DIM)
    angles = jnp.arange(length, dtype=jnp.int32).astype(F32)[:, None] * jnp.tile(frequency, 4)
    sign = jnp.where(jnp.arange(128) % 64 < 32, -1.0, 1.0)
    cosine, sine = jnp.cos(angles), jnp.sin(angles) * sign
    seg_row = lax.dynamic_slice_in_dim(segments, z_at, 1, 0)
    seg_col = seg_row.reshape(length, 1)
    fused = group % 128 == 0
    if fused:
        weights = [w_qkv] * 3
    else:
        picked = w_qkv.reshape(width, 3, parts, group)
        picked = lax.dynamic_index_in_dim(picked, x_at, 2, keepdims=False)
        weights = [picked.reshape(width, 3 * group)]

    by_seq = swap_all(tokens, "z")
    by_seq, cosine, sine, seg_col, *grad_sent = lax.optimization_barrier(
        (by_seq, cosine, sine, seg_col, *grad_sent)
    )
    if parts == 2:
        rows = [by_seq, lax.ppermute(by_seq, "x", [(0, 1), (1, 0)])]
    else:
        rows = [lax.all_gather(by_seq, "x", axis=0, tiled=False)]
    *rows, grad_sent[0] = lax.optimization_barrier((*rows, grad_sent[0]))
    grad_came = [swap_all(grad_sent[0], ranks)]

    qkv, normed = project(rows, attn_scale, weights, group, cosine, sine, x_ref, parts)
    attended, lse = (attend if fused else plain_attend)(qkv, seg_row, seg_col)
    attended = after(attended, grad_came[0])
    attended = swap_all(attended.reshape(experts, span, group), ranks)
    attended, grad_sent[1] = lax.optimization_barrier((attended, grad_sent[1]))
    grad_came.append(swap_all(grad_sent[1], ranks))
    attended = attended.reshape(seqs, parts, span, group)

    hidden, branch_in = after_attention(flat_tokens, attended, w_out, ffn_scale)
    sent = [dispatch(branch_in, target_rows[0], experts, half)]
    shared_out, shared_back, hid, dg, du = feed_forward(
        after(branch_in, sent[0]), flat_cot, shared_gate, shared_up, shared_down
    )
    sent.append(dispatch(after(branch_in, shared_out), target_rows[1], experts, half))
    sent[0] = after(sent[0], grad_came[1], shared_out)
    received = [swap_all(value, ranks).reshape(-1, width) for value in sent]
    keep, give = shared_weight_grads(branch_in, flat_cot, dg, du, hid, sizes, core_ref)
    shared_sums, _ = fold(both(keep, give), "y")

    router = jnp.pad(w_router, ((0, 0), (0, 128 - experts)))
    made, back_rows, halves = None, [], []
    before = (give, sent[1])
    for at in range(2):
        grad_rows = grad_came[at][:, :half, :].reshape(-1, width)
        other = grad_came[at][:, half, :half].astype(jnp.int32).reshape(-1, 1)
        rows_at = after(received[at], grad_rows, other, *before)
        made, back, hid, dg, du, gated_grads, grad_logits = feed_forward(
            rows_at, grad_rows, expert_gate[0], expert_up[0], expert_down[0], router, other, own,
            experts, at, made,
        )
        back_rows.append(swap_all(back.reshape(experts, half, width), ranks).reshape(-1, width))
        halves.append((rows_at, gated_grads, dg, du, hid, grad_logits))
        before = (back,)
    halves[1] = (after(halves[1][0], back_rows[0]), *halves[1][1:])
    keep, give, grad_router = expert_weight_grads(halves, sizes, pair_ref)
    back_rows[1] = after(back_rows[1], give)
    expert_sums = both(keep, give)

    grad_hidden, grad_attn, grad_att, grad_ffn = middle_back(
        hidden, shared_back, back_rows, target, flat_cot, ffn_scale, w_out, parts, span
    )
    grad_att = swap_all(grad_att.reshape(experts, span, group), ranks).reshape(length, group)

    column = lax.broadcasted_iota(jnp.int32, (width, 128), 1)
    small = jnp.where(column < experts, grad_router, jnp.where(column == experts, grad_ffn, 0.0))
    out_sums = tall_weight_grads(
        [attended[:, part].reshape(count, group) for part in range(parts)],
        [grad_attn],
        [small],
        sizes,
        core_ref,
        WEIGHT,
    )
    out_sums = both(*out_sums)

    shared_sums, shared_sent = fold([after(term, out_sums[0]) for term in shared_sums], "x")
    made = after(made, grad_att, out_sums[0], shared_sent)
    made_rows = swap_all(made, ranks).reshape(-1, width)
    grads = list(
        (attend_back if fused else plain_attend_back)(
            qkv, grad_att, lse, seg_row, seg_col, cosine, sine
        )
    )
    shared_sums = total(shared_sums).astype(BF)
    grads[0] = after(grads[0], shared_sums)
    normed_back, grad_gain = project_back(grads, weights, rows, x_ref, parts)
    normed_back, _ = fold([normed_back], "x")
    pieces = swap_by_steps(total(normed_back).astype(BF), "z")

    qkv_sums = tall_weight_grads([normed], list(grads), [grad_gain], sizes, core_ref, 0.2)
    last = [jnp.concatenate(pair, axis=-1) for pair in zip(out_sums, both(*qkv_sums))]
    last, last_sent = fold(last, "y")
    expert_sums, _ = fold(expert_sums, "y", last_sent, ordered=True)
    token_grad = first_norm_back(flat_tokens, attn_scale, pieces, grad_hidden, z_ref)
    layer_out = layer_end(hidden, shared_out, [made_rows], whole_target).reshape(tokens.shape)

    shared_sums = swap_by_steps(shared_sums, "z")
    last = after(total(last).astype(BF), made_rows)
    each, cols = last.shape[-2:]
    last = swap_all(last.reshape(experts, each, cols), ranks).astype(F32)
    last = jnp.sum(last.reshape(blocks, parts, each, cols), axis=0)
    out_sums = jnp.sum(last[:, :, : width + 128], axis=0)
    qkv_sums = last[:, :, width + 128 :]
    grad_attn_gain = jnp.sum(qkv_sums[:, :, 3 * group], axis=0)
    grad_w_qkv = qkv_sums[:, :, : 3 * group].reshape(parts, each, 3, group)
    grad_w_qkv = jnp.transpose(grad_w_qkv, (1, 2, 0, 3)).reshape(each, 3 * width)

    shared_sums, expert_sums = total(shared_sums), total(expert_sums)
    return (
        layer_out,
        token_grad.reshape(tokens.shape),
        grad_attn_gain,
        grad_w_qkv,
        out_sums[:, :width],
        out_sums[:, width + experts],
        out_sums[:, width : width + experts],
        shared_sums[0],
        shared_sums[1],
        jnp.transpose(shared_sums[2]),
        expert_sums[0][None],
        expert_sums[1][None],
        jnp.transpose(expert_sums[2])[None],
    )


def solution(mesh):
    dp, experts = mesh.shape["dp"], mesh.shape["expert"]

    def step(*args):
        seqs = args[0].shape[0] // dp
        cores = 2 if dp % 2 == 0 else 1
        fine = Mesh(
            mesh.devices.reshape(dp // cores, cores, seqs, experts // seqs),
            ("y", "core", "z", "x"),
        )
        data, ranks, every = ("y", "core"), ("z", "x"), ("y", "core", "z", "x")
        placed = (
            P(data, ranks, None),
            P(data, None),
            P(data, ranks, None),
            P(data, ranks, None),
            P(data, ranks, None),
            *([P()] * 8),
            P(ranks, None, None),
            P(ranks, None, None),
            P(ranks, None, None),
        )
        return jax.shard_map(
            on_device,
            mesh=fine,
            in_specs=placed,
            out_specs=(
                P(data, ranks, None),
                P(data, ranks, None),
                P(every),
                P(every, None),
                P(every, None),
                P(every),
                P(every, None),
                P(every, None),
                P(every, None),
                P(None, every),
                P(ranks, None, data),
                P(ranks, None, data),
                P(ranks, data, None),
            ),
            check_vma=False,
        )(*args)

    return step
```

```python
import jax
import jax.numpy as jnp
from jax import lax
from jax.experimental import pallas as pl
from jax.experimental.pallas import tpu as pltpu
from jax.sharding import Mesh
from jax.sharding import PartitionSpec as P

HEAD_DIM = 64
EPS = 1e-06
BF = jnp.bfloat16
F32 = jnp.float32
NEG = -1e30
NN = (((1,), (0,)), ((), ()))
NT = (((1,), (1,)), ((), ()))
TN = (((0,), (0,)), ((), ()))
VMEM_MOST = 60 << 20
WEIGHT = 3


def mm(left, right, dims=NN):
    return lax.dot_general(left, right, dims, preferred_element_type=F32)


def sds(shape, dtype):
    return jax.ShapeDtypeStruct(shape, dtype)


def call(
    body, grid, in_specs, out_specs, out_shape, args, scratch=(), prefetch=0, flops=0, alias=None
):
    leaves = jax.tree.leaves(out_shape)
    moved = sum(a.size * a.dtype.itemsize for a in args) + sum(
        a.size * a.dtype.itemsize for a in leaves
    )
    return pl.pallas_call(
        body,
        out_shape=out_shape,
        grid_spec=pltpu.PrefetchScalarGridSpec(
            num_scalar_prefetch=prefetch,
            grid=grid,
            in_specs=in_specs,
            out_specs=out_specs,
            scratch_shapes=list(scratch),
        ),
        compiler_params=pltpu.CompilerParams(
            dimension_semantics=("arbitrary",) * len(grid), vmem_limit_bytes=VMEM_MOST
        ),
        cost_estimate=pl.CostEstimate(
            flops=int(flops), transcendentals=0, bytes_accessed=int(moved)
        ),
        input_output_aliases=alias or {},
    )(*args)


def whole(shape):
    rank = len(shape)
    return pl.BlockSpec(tuple(shape), lambda *_: (0,) * rank)


def swap_halves(value):
    lane = lax.broadcasted_iota(jnp.int32, value.shape, 1)
    return jnp.where(lane % 64 < 32, pltpu.roll(value, 96, 1), pltpu.roll(value, 32, 1))


def rms(values):
    return lax.rsqrt(jnp.mean(values * values, axis=1, keepdims=True) + EPS)


def row_specs(rows):
    if len(rows) == 2:
        _, span, width = rows[0].shape
        return [pl.BlockSpec((1, span, width), lambda i, *_: (i, 0, 0))] * 2
    parts, _, span, width = rows[0].shape
    return [pl.BlockSpec((parts, 1, span, width), lambda i, *_: (0, i, 0, 0))]


def load_rows(refs, at_ref):
    if len(refs) == 2:
        mine, theirs = refs[0][0].astype(F32), refs[1][0].astype(F32)
        first = at_ref[0] == 0
        pair = [jnp.where(first, mine, theirs), jnp.where(first, theirs, mine)]
        return jnp.concatenate(pair, axis=0)
    value = refs[0][...]
    return value.reshape(value.shape[0] * value.shape[2], value.shape[3]).astype(F32)


def weight_specs(weights, group):
    if len(weights) == 1:
        return [whole(weights[0].shape)]
    width, cols = weights[0].shape
    parts = cols // (3 * group)

    def spec(index):
        return pl.BlockSpec((width, group), lambda i, at: (0, index * parts + at[0]))

    return [spec(index) for index in range(3)]


def load_weights(refs, group):
    if len(refs) == 3:
        return [ref[...] for ref in refs]
    return [refs[0][:, at * group : (at + 1) * group] for at in range(3)]


def project(rows, gain, weights, group, cosine, sine, x_at, parts):
    blocks, span, width = rows[0].shape[-3:]
    height = parts * span
    length = height * blocks
    cut = len(rows)

    def body(at_ref, *refs):
        r_refs, (g_ref, c_ref, s_ref) = refs[:cut], refs[cut : cut + 3]
        w_refs, (qkv_ref, n_ref) = refs[cut + 3 : -2], refs[-2:]
        tok = load_rows(r_refs, at_ref)
        normed = (tok * rms(tok) * g_ref[...]).astype(BF)
        n_ref[...] = normed
        if len(w_refs) == 3:
            found = [mm(normed, ref[...]) for ref in w_refs]
            turning = [(found[0], 0), (found[1], group)]
            last = found[2]
        else:
            found = mm(normed, w_refs[0][...])
            turning, last = [(found[:, : 2 * group], 0)], found[:, 2 * group :]
        for value, base in turning:
            for at in range(0, value.shape[1], 128):
                part = value[:, at : at + 128]
                lane = lax.broadcasted_iota(jnp.int32, part.shape, 1) + (base + at)
                turned = part * c_ref[...] + swap_halves(part) * s_ref[...]
                turned = turned * jnp.where(lane < group, HEAD_DIM**-0.5, 1.0)
                qkv_ref[:, base + at : base + at + 128] = turned.astype(BF)
        qkv_ref[:, 2 * group :] = last.astype(BF)

    return call(
        body,
        (blocks,),
        [
            *row_specs(rows),
            whole((1, width)),
            pl.BlockSpec((height, 128), lambda i, *_: (i, 0)),
            pl.BlockSpec((height, 128), lambda i, *_: (i, 0)),
            *weight_specs(weights, group),
        ],
        [
            pl.BlockSpec((height, 3 * group), lambda i, *_: (i, 0)),
            pl.BlockSpec((height, width), lambda i, *_: (i, 0)),
        ],
        [sds((length, 3 * group), BF), sds((length, width), BF)],
        (x_at, *rows, gain, cosine, sine, *weights),
        prefetch=1,
        flops=6 * length * width * group,
    )


def project_back(grads, weights, rows, x_at, parts):
    blocks, span, width = rows[0].shape[-3:]
    group = grads[0].shape[1]
    height = parts * span
    length = height * blocks
    cut = len(rows)

    def body(at_ref, q_ref, k_ref, v_ref, *refs):
        r_refs, w_refs, (out_ref, gain_ref, acc_ref) = refs[:cut], refs[cut:-3], refs[-3:]
        step = pl.program_id(0)
        w_q, w_k, w_v = load_weights(w_refs, group)
        back = mm(q_ref[...], w_q, NT) + mm(k_ref[...], w_k, NT) + mm(v_ref[...], w_v, NT)
        tok = load_rows(r_refs, at_ref)
        part = jnp.sum(back * tok * rms(tok), axis=0, keepdims=True)

        @pl.when(step == 0)
        def _():
            acc_ref[...] = jnp.zeros_like(acc_ref)

        acc_ref[...] += jnp.broadcast_to(part, acc_ref.shape)
        out_ref[...] = back.astype(BF).reshape(parts, 1, span, width)

        @pl.when(step == blocks - 1)
        def _():
            column = jnp.transpose(acc_ref[...])
            gain_ref[...] = jnp.broadcast_to(column[:, :1], gain_ref.shape)

    block = pl.BlockSpec((height, group), lambda i, *_: (i, 0))
    return call(
        body,
        (blocks,),
        [block, block, block, *row_specs(rows), *weight_specs(weights, group)],
        [
            pl.BlockSpec((parts, 1, span, width), lambda i, *_: (0, i, 0, 0)),
            whole((width, 128)),
        ],
        [sds((parts, blocks, span, width), BF), sds((width, 128), F32)],
        (x_at, *grads, *rows, *weights),
        scratch=[pltpu.VMEM((8, width), F32)],
        prefetch=1,
        flops=0.2 * length * width * group,
    )


def attend(qkv, seg_row, seg_col):
    length, cols = qkv.shape
    group = cols // 3
    pairs = group // 128
    high = min(256, length)

    def body(q_ref, k_ref, v_ref, sr_ref, sc_ref, o_ref, l_ref):
        lane = lax.broadcasted_iota(jnp.int32, (high, 128), 1)
        for at in range(0, length, high):
            end = at + high
            query = q_ref[at:end, :]
            keys = k_ref[:end, :]
            vals = v_ref[:end, :]
            q_pos = lax.broadcasted_iota(jnp.int32, (high, end), 0) + at
            k_pos = lax.broadcasted_iota(jnp.int32, (high, end), 1)
            allowed = (sc_ref[at:end, :] == sr_ref[:, :end]) & (k_pos <= q_pos)
            outs = []
            for head in range(2):
                mine = (lane // 64) == head
                scores = mm(jnp.where(mine, query, jnp.zeros_like(query)), keys, NT)
                scores = jnp.where(allowed, scores, NEG)
                most = jnp.max(scores, axis=1, keepdims=True)
                expo = jnp.exp(scores - most)
                total = jnp.sum(expo, axis=1, keepdims=True)
                outs.append(mm(expo.astype(BF), vals) / total)
                lse = jnp.broadcast_to(most + jnp.log(total), (high, 128))
                l_ref[0, head : head + 1, at:end] = jnp.transpose(lse)[:1, :]
            o_ref[at:end, :] = jnp.where(lane < 64, outs[0], outs[1]).astype(BF)

    def col(offset):
        return pl.BlockSpec((length, 128), lambda i: (0, offset * pairs + i))

    return call(
        body,
        (pairs,),
        [col(0), col(1), col(2), whole((1, length)), whole((length, 1))],
        [col(0), pl.BlockSpec((1, 2, length), lambda i: (i, 0, 0))],
        [sds((length, group), BF), sds((pairs, 2, length), F32)],
        (qkv, qkv, qkv, seg_row, seg_col),
        flops=4 * length * length * group,
    )


def attend_back(qkv, grad, lse, seg_row, seg_col, cosine, sine):
    length, cols = qkv.shape
    group = cols // 3
    pairs = group // 128
    high = min(256, length)

    def body(
        q_ref, k_ref, v_ref, g_ref, l_ref, sr_ref, sc_ref, c_ref, s_ref, dq_ref, dk_ref, dv_ref,
        ka_ref, va_ref,
    ):
        lane = lax.broadcasted_iota(jnp.int32, (high, 128), 1)
        ka_ref[...] = jnp.zeros_like(ka_ref)
        va_ref[...] = jnp.zeros_like(va_ref)
        for at in range(0, length, high):
            end = at + high
            query = q_ref[at:end, :]
            grads = g_ref[at:end, :]
            keys = k_ref[:end, :]
            vals = v_ref[:end, :]
            k_pos = lax.broadcasted_iota(jnp.int32, (end, high), 0)
            q_pos = lax.broadcasted_iota(jnp.int32, (end, high), 1) + at
            allowed = (sc_ref[:end, :] == sr_ref[:, at:end]) & (k_pos <= q_pos)
            outs = []
            for head in range(2):
                mine = (lane // 64) == head
                q_own = jnp.where(mine, query, jnp.zeros_like(query))
                g_own = jnp.where(mine, grads, jnp.zeros_like(grads))
                scores = jnp.where(allowed, mm(keys, q_own, NT), NEG)
                probs = jnp.exp(scores - l_ref[0, head : head + 1, at:end])
                grad_probs = mm(vals, g_own, NT)
                delta = jnp.sum(probs * grad_probs, axis=0, keepdims=True)
                grad_scores = (probs * (grad_probs - delta)).astype(BF)
                va_ref[:end, :] += mm(probs.astype(BF), g_own)
                ka_ref[:end, :] += mm(grad_scores, q_own)
                outs.append(mm(grad_scores, keys, TN))
            found = jnp.where(lane < 64, outs[0], outs[1]) * HEAD_DIM**-0.5
            back = found * c_ref[at:end, :] - swap_halves(found) * s_ref[at:end, :]
            dq_ref[at:end, :] = back.astype(BF)
        found = ka_ref[...]
        dk_ref[...] = (found * c_ref[...] - swap_halves(found) * s_ref[...]).astype(BF)
        dv_ref[...] = va_ref[...].astype(BF)

    def col(offset):
        return pl.BlockSpec((length, 128), lambda i: (0, offset * pairs + i))

    return call(
        body,
        (pairs,),
        [
            col(0),
            col(1),
            col(2),
            col(0),
            pl.BlockSpec((1, 2, length), lambda i: (i, 0, 0)),
            whole((1, length)),
            whole((length, 1)),
            whole((length, 128)),
            whole((length, 128)),
        ],
        [col(0), col(0), col(0)],
        [sds((length, group), BF)] * 3,
        (qkv, qkv, qkv, grad, lse, seg_row, seg_col, cosine, sine),
        scratch=[pltpu.VMEM((length, 128), F32)] * 2,
        flops=length * length * group,
    )


def heads_of(flat):
    return flat.reshape(flat.shape[0], -1, HEAD_DIM)


def plain_mask(seg_row, seg_col):
    length = seg_col.shape[0]
    spots = jnp.arange(length, dtype=jnp.int32)
    return (seg_row == seg_col) & (spots[None, :] <= spots[:, None])


def plain_attend(qkv, seg_row, seg_col):
    query, keys, vals = (heads_of(part) for part in jnp.split(qkv, 3, axis=1))
    scores = jnp.einsum("qhd,khd->hqk", query, keys, preferred_element_type=F32)
    scores = jnp.where(plain_mask(seg_row, seg_col)[None], scores, NEG)
    lse = jax.nn.logsumexp(scores, axis=-1, keepdims=True)
    probs = jnp.exp(scores - lse).astype(BF)
    found = jnp.einsum("hqk,khd->qhd", probs, vals, preferred_element_type=F32)
    return found.astype(BF).reshape(qkv.shape[0], -1), lse


def plain_turn_back(grads, cosine, sine):
    table_c, table_s = cosine[:, None, :HEAD_DIM], sine[:, None, :HEAD_DIM]
    swapped = jnp.roll(grads, HEAD_DIM // 2, axis=-1)
    return (grads * table_c - swapped * table_s).astype(BF).reshape(grads.shape[0], -1)


def plain_attend_back(qkv, grad, lse, seg_row, seg_col, cosine, sine):
    query, keys, vals = (heads_of(part) for part in jnp.split(qkv, 3, axis=1))
    grad = heads_of(grad)
    scores = jnp.einsum("qhd,khd->hqk", query, keys, preferred_element_type=F32)
    scores = jnp.where(plain_mask(seg_row, seg_col)[None], scores, NEG)
    probs = jnp.exp(scores - lse)
    grad_probs = jnp.einsum("qhd,khd->hqk", grad, vals, preferred_element_type=F32)
    delta = jnp.sum(probs * grad_probs, axis=-1, keepdims=True)
    grad_scores = (probs * (grad_probs - delta)).astype(BF)
    gq = jnp.einsum("hqk,khd->qhd", grad_scores, keys, preferred_element_type=F32)
    gk = jnp.einsum("hqk,qhd->khd", grad_scores, query, preferred_element_type=F32)
    gv = jnp.einsum("hqk,qhd->khd", probs.astype(BF), grad, preferred_element_type=F32)
    return (
        plain_turn_back(gq * HEAD_DIM**-0.5, cosine, sine),
        plain_turn_back(gk, cosine, sine),
        gv.astype(BF).reshape(qkv.shape[0], -1),
    )


def after_attention(tokens, attended, w_out, gain):
    seqs, parts, span, group = attended.shape
    count, width = tokens.shape

    def body(t_ref, a_ref, w_ref, g_ref, h_ref, b_ref):
        hidden = t_ref[...].astype(F32)
        for part in range(parts):
            rows = a_ref[:, part].reshape(count, group)
            hidden += mm(rows, w_ref[part * group : (part + 1) * group, :])
        h_ref[...] = hidden
        b_ref[...] = (hidden * rms(hidden) * g_ref[...]).astype(BF)

    return call(
        body,
        (1,),
        [whole(a.shape) for a in (tokens, attended, w_out, gain)],
        [whole(tokens.shape)] * 2,
        [sds(tokens.shape, F32), sds(tokens.shape, BF)],
        (tokens, attended, w_out, gain),
        flops=2 * count * width * width,
    )


def dispatch(rows, target_rows, experts, capacity, route_rows=None):
    count, width = rows.shape
    more = 0 if route_rows is None else 16
    tables = () if route_rows is None else (route_rows,)

    def body(r_ref, t_ref, *refs):
        o_ref = refs[-1]
        slot = lax.broadcasted_iota(jnp.int32, (capacity, count), 0)
        slot += pl.program_id(0) * capacity
        hits = [slot == t_ref[k : k + 1, :] for k in range(2)]
        hot = (hits[0] | hits[1]).astype(F32).astype(BF)
        o_ref[0, :capacity, :] = mm(hot, r_ref[...]).astype(BF)
        if more:
            o_ref[0, capacity:, :] = jnp.zeros((more, width), BF)
            other = jnp.zeros((8, capacity), F32)
            for k in range(2):
                route = jnp.broadcast_to(refs[0][1 - k : 2 - k, :].astype(F32), (8, count))
                other += mm(route.astype(BF), hits[k].astype(F32).astype(BF), NT)
            o_ref[0, capacity : capacity + 8, :capacity] = other.astype(BF)

    return call(
        body,
        (experts,),
        [whole(a.shape) for a in (rows, target_rows, *tables)],
        pl.BlockSpec((1, capacity + more, width), lambda i: (i, 0, 0)),
        sds((experts, capacity + more, width), BF),
        (rows, target_rows, *tables),
        flops=2 * experts * capacity * count * width,
    )


def pick(target, row_refs):
    total = None
    for index, ref in enumerate(row_refs):
        rows = ref[...]
        spot = lax.broadcasted_iota(jnp.int32, (target.shape[0], rows.shape[0]), 1)
        one, two = target[:, 2 * index : 2 * index + 1], target[:, 2 * index + 1 : 2 * index + 2]
        found = mm(((spot == one) | (spot == two)).astype(F32).astype(BF), rows)
        total = found if total is None else total + found
    return total


def layer_end(hidden, shared_out, rows, target):
    count, width = hidden.shape
    high = count // 2

    def body(h_ref, s_ref, t_ref, *refs):
        refs[-1][...] = (h_ref[...] + s_ref[...] + pick(t_ref[...], refs[:-1])).astype(BF)

    block = pl.BlockSpec((high, width), lambda i: (i, 0))
    return call(
        body,
        (2,),
        [
            block,
            block,
            pl.BlockSpec((high, target.shape[1]), lambda i: (i, 0)),
            *[whole(part.shape) for part in rows],
        ],
        block,
        sds(hidden.shape, BF),
        (hidden, shared_out, target, *rows),
        flops=2 * count * width * rows[0].shape[0] * len(rows),
    )


def middle_back(hidden, grad_shared, rows, target, cotangent, gain, w_out, parts, span):
    count, width = hidden.shape
    seqs = count // span
    each = 2 if seqs % 2 == 0 else 1
    high = each * span
    steps = count // high
    group = width // parts

    def body(h_ref, s_ref, t_ref, c_ref, g_ref, w_ref, *refs):
        gh_ref, ga_ref, d_ref, n_ref, acc_ref = refs[len(rows) :]
        step = pl.program_id(0)
        branch = s_ref[...] + pick(t_ref[...], refs[: len(rows)])
        hidden = h_ref[...]
        scale = rms(hidden)
        weighted = branch * g_ref[...]
        inner = jnp.mean(weighted * hidden, axis=1, keepdims=True)
        part = jnp.sum(branch * hidden * scale, axis=0, keepdims=True)
        out = c_ref[...].astype(F32) + scale * weighted - hidden * (scale * scale * scale * inner)
        gh_ref[...] = out
        out = out.astype(BF)
        ga_ref[...] = out
        for at in range(parts):
            sent = mm(out, w_ref[at * group : (at + 1) * group, :], NT).astype(BF)
            d_ref[:, at] = sent.reshape(each, span, group)

        @pl.when(step == 0)
        def _():
            acc_ref[...] = jnp.zeros_like(acc_ref)

        acc_ref[...] += jnp.broadcast_to(part, acc_ref.shape)

        @pl.when(step == steps - 1)
        def _():
            column = jnp.transpose(acc_ref[...])
            n_ref[...] = jnp.broadcast_to(column[:, :1], n_ref.shape)

    block = pl.BlockSpec((high, width), lambda i: (i, 0))
    return call(
        body,
        (steps,),
        [
            block,
            block,
            pl.BlockSpec((high, target.shape[1]), lambda i: (i, 0)),
            block,
            whole(gain.shape),
            whole(w_out.shape),
            *[whole(part.shape) for part in rows],
        ],
        [
            block,
            block,
            pl.BlockSpec((each, parts, span, group), lambda i: (i, 0, 0, 0)),
            whole((width, 128)),
        ],
        [
            sds(hidden.shape, F32),
            sds(hidden.shape, BF),
            sds((seqs, parts, span, group), BF),
            sds((width, 128), F32),
        ],
        (hidden, grad_shared, target, cotangent, gain, w_out, *rows),
        scratch=[pltpu.VMEM((8, width), F32)],
        flops=WEIGHT * 2 * count * width * (rows[0].shape[0] * len(rows) + width),
    )


def first_norm_back(tokens, gain, pieces, grad_hidden, z_at):
    count, width = tokens.shape
    blocks = len(pieces)
    span = count // blocks

    def body(at_ref, t_ref, g_ref, h_ref, *refs):
        o_ref = refs[-1]
        for index in range(blocks):
            seq = (at_ref[0] + blocks - index) % blocks
            spot = pl.ds(pl.multiple_of(seq * span, span), span)
            tok = t_ref[spot, :].astype(F32)
            scale = rms(tok)
            weighted = refs[index][...].astype(F32) * g_ref[...]
            inner = jnp.mean(weighted * tok, axis=1, keepdims=True)
            out = h_ref[spot, :] + scale * weighted - tok * (scale * scale * scale * inner)
            o_ref[spot, :] = out.astype(BF)

    return call(
        body,
        (1,),
        [whole(a.shape) for a in (tokens, gain, grad_hidden, *pieces)],
        whole(tokens.shape),
        sds(tokens.shape, BF),
        (z_at, tokens, gain, grad_hidden, *pieces),
        prefetch=1,
    )


def feed_forward(
    rows, grads, w_gate, w_up, w_down, router=None, other=None, own=None, experts=0, place=0, made=None
):
    count, width = rows.shape
    units = w_gate.shape[1]
    wide = 512
    steps = units // wide
    high = 256
    gated = router is not None
    more = 0 if made is None else 1
    kind = BF if gated else F32

    def body(*refs):
        if gated:
            (own_ref, x_ref, g_ref, wg_ref, wu_ref, wd_ref, wr_ref, ot_ref) = refs[:8]
            (y_ref, gi_ref, hid_ref, dg_ref, du_ref, eo_ref, gl_ref, ya_ref, ga_ref, gate_ref) = refs[8 + more :]
        else:
            (x_ref, g_ref, wg_ref, wu_ref, wd_ref,
             y_ref, gi_ref, hid_ref, dg_ref, du_ref, ya_ref, ga_ref) = refs
        step = pl.program_id(0)

        if gated:

            @pl.when(step == 0)
            def _():
                logits = mm(x_ref[...], wr_ref[...])
                lane = lax.broadcasted_iota(jnp.int32, logits.shape, 1)
                mine = jnp.sum(jnp.where(lane == own_ref[0], logits, 0.0), axis=1, keepdims=True)
                theirs = jnp.sum(jnp.where(lane == ot_ref[...], logits, 0.0), axis=1, keepdims=True)
                gate = 1.0 / (1.0 + jnp.exp(theirs - mine))
                rest = 1.0 / (1.0 + jnp.exp(mine - theirs))
                gate_ref[:, 0:1] = gate
                gate_ref[:, 1:2] = rest
                eo_ref[...] = (g_ref[...].astype(F32) * gate).astype(BF)

        def rows_at(index, carry):
            at = pl.ds(pl.multiple_of(index * high, high), high)
            row = x_ref[at, :]
            grad = eo_ref[at, :] if gated else g_ref[at, :]
            gval = mm(row, wg_ref[...])
            uval = mm(row, wu_ref[...])
            sigma = 1.0 / (1.0 + jnp.exp(-gval))
            silu = gval * sigma
            hid = (silu * uval).astype(BF)
            hid_ref[at, :] = hid
            grad_hid = mm(grad, wd_ref[...], NT)
            du = (grad_hid * silu).astype(BF)
            dg = (grad_hid * uval * sigma * (1.0 + gval * (1.0 - sigma))).astype(BF)
            du_ref[at, :] = du
            dg_ref[at, :] = dg
            out = mm(hid, wd_ref[...])
            back = mm(dg, wg_ref[...], NT) + mm(du, wu_ref[...], NT)

            @pl.when(step == 0)
            def _():
                ya_ref[at, :] = out
                ga_ref[at, :] = back

            @pl.when(step > 0)
            def _():
                ya_ref[at, :] += out
                ga_ref[at, :] += back

            return carry

        lax.fori_loop(0, count // high, rows_at, 0)

        @pl.when(step == steps - 1)
        def _():
            if gated:
                out = ya_ref[...]
                gate = gate_ref[:, 0:1]
                lean = jnp.sum(out * g_ref[...].astype(F32), axis=1, keepdims=True)
                lean = lean * gate * gate_ref[:, 1:2]
                lane = lax.broadcasted_iota(jnp.int32, (count, 128), 1)
                sign = (lane == own_ref[0]).astype(F32) - (lane == ot_ref[...]).astype(F32)
                grad_logits = (lean * sign).astype(BF)
                gl_ref[...] = grad_logits
                y_ref[...] = (out * gate).astype(BF).reshape(y_ref.shape)
                gi_ref[...] = (ga_ref[...] + mm(grad_logits, wr_ref[...], NT)).astype(BF)
            else:
                y_ref[...] = ya_ref[...]
                gi_ref[...] = ga_ref[...]

    full = whole((count, width))
    hidden = pl.BlockSpec((count, wide), lambda i, *_: (0, i))
    in_specs = [
        full,
        full,
        pl.BlockSpec((width, wide), lambda i, *_: (0, i)),
        pl.BlockSpec((width, wide), lambda i, *_: (0, i)),
        pl.BlockSpec((wide, width), lambda i, *_: (i, 0)),
    ]
    out_specs = [full, full, hidden, hidden, hidden]
    out_shape = [sds((count, width), kind)] * 2 + [sds((count, units), BF)] * 3
    scratch = [pltpu.VMEM((count, width), F32)] * 2
    args = [rows, grads, w_gate, w_up, w_down]
    if gated:
        in_specs += [whole(router.shape), whole(other.shape)]
        out_specs += [full, whole((count, 128))]
        out_shape += [sds((count, width), BF), sds((count, 128), BF)]
        scratch += [pltpu.VMEM((count, 128), F32)]
        args = [own, *args, router, other]
        out_specs[0] = pl.BlockSpec((experts, count // experts, width), lambda *_: (0, place, 0))
        out_shape[0] = sds((experts, 2 * count // experts, width), BF)
        if more:
            in_specs += [pl.BlockSpec(memory_space=pl.ANY)]
            args += [made]
    return call(
        body,
        (steps,),
        in_specs,
        out_specs,
        out_shape,
        tuple(args),
        scratch=scratch,
        prefetch=1 if gated else 0,
        alias={len(args) - 1: 0} if more else None,
        flops=12 * count * width * units,
    )


def expert_weight_grads(halves, sizes, core_at):
    outer, cores = sizes["y"], sizes["core"]
    count, width = halves[0][0].shape
    units = halves[0][2].shape[1]
    wide = units // (outer * cores)

    def body(at_ref, *refs):
        keep_ref, give_ref, r_ref = refs[-3:]
        groups = [refs[6 * at : 6 * at + 6] for at in range(len(halves))]
        step = pl.program_id(0)

        def over(left, right):
            return sum(mm(group[left][...], group[right][...], TN) for group in groups)

        found = [over(0, 2).astype(BF), over(0, 3).astype(BF), over(1, 4).astype(BF)]

        @pl.when(step < outer)
        def _():
            for index in range(3):
                give_ref[0, index] = found[index]

        @pl.when(step >= outer)
        def _():
            for index in range(3):
                keep_ref[0, index] = found[index]

        @pl.when(step == 0)
        def _():
            r_ref[...] = over(0, 5)

    def taken(i, at):
        core = jnp.where(i < outer, 1 - at[0], at[0])
        y = (i + 1 + at[1]) % outer if outer == 2 else i % outer
        return (0, y * cores + core)

    hidden = pl.BlockSpec((count, wide), taken)
    part = (1, 3, width, wide)
    return call(
        body,
        (outer * cores,),
        [
            whole((count, width)),
            whole((count, width)),
            hidden,
            hidden,
            hidden,
            whole((count, 128)),
        ]
        * len(halves),
        [
            pl.BlockSpec(part, lambda i, *_: (jnp.maximum(i - outer, 0), 0, 0, 0)),
            pl.BlockSpec(part, lambda i, *_: (jnp.minimum(i, outer - 1), 0, 0, 0)),
            whole((width, 128)),
        ],
        [sds((outer, *part[1:]), BF)] * 2 + [sds((width, 128), F32)],
        (core_at, *[value for half in halves for value in half]),
        prefetch=1,
        flops=6 * count * len(halves) * width * units,
    )


def spread_places(sizes, names):
    found = []
    for y in range(sizes["y"]):
        for core in range(sizes["core"]):
            for z in range(sizes["z"]):
                for x in range(sizes["x"]):
                    at = {"y": y, "core": core, "z": z, "x": x}
                    found.append((core, tuple(at[n] for n in names)))
    return found


def spread(value, sizes, names, core_at):
    order = ("y", "core", "z", "x")
    split = value.reshape(*(sizes[n] for n in order), -1, value.shape[-1])
    split = jnp.transpose(split, (1, *(order.index(n) for n in names), 4, 5))
    return at_index(split, core_at[0]), at_index(split, 1 - core_at[0])


def store_spread(places, each, core_at, found, row, keep, give):
    first = row // each
    for core in range(2):
        todo = [at for at in range(found.shape[0] // each) if places[first + at][0] == core]

        def put(store, todo=todo):
            for at in todo:
                store(places[first + at][1], found[at * each : (at + 1) * each].astype(BF))

        pl.when(core_at == core)(lambda put=put: put(keep))
        pl.when(core_at != core)(lambda put=put: put(give))


def shared_weight_grads(rows, grads, dg, du, hid, sizes, core_at):
    names = ("y", "x", "z")
    lead = tuple(sizes[n] for n in names)
    places = spread_places(sizes, names)
    count, width = rows.shape
    units = dg.shape[1]
    wide = 512
    each = width // len(places)
    direct = each % 8 == 0

    def body(at_ref, x_ref, g_ref, dg_ref, du_ref, hid_ref, *outs):
        pairs = ((x_ref, dg_ref), (x_ref, du_ref), (g_ref, hid_ref))
        for index, (left, right) in enumerate(pairs):
            found = mm(left[...], right[...], TN)
            if not direct:
                outs[0][index] = found.astype(BF)
                continue

            def into(ref, index=index):
                def store(place, piece):
                    ref[(*place, index)] = piece

                return store

            store_spread(places, each, at_ref[0], found, 0, into(outs[0]), into(outs[1]))

    hidden = pl.BlockSpec((count, wide), lambda i, *_: (0, i))
    if direct:
        shapes = [(*lead, 3, each, units)] * 2
        spec = [pl.BlockSpec((*lead, 3, each, wide), lambda i, *_: (0,) * 5 + (i,))] * 2
    else:
        shapes = [(3, width, units)]
        spec = [pl.BlockSpec((3, width, wide), lambda i, *_: (0, 0, i))]
    out = call(
        body,
        (units // wide,),
        [whole(rows.shape), whole(grads.shape), hidden, hidden, hidden],
        spec,
        [sds(shape, BF) for shape in shapes],
        (core_at, rows, grads, dg, du, hid),
        prefetch=1,
        flops=6 * count * width * units,
    )
    if direct:
        return out
    found = [spread(out[0][i], sizes, names, core_at) for i in range(3)]
    return [jnp.stack([part[side] for part in found], axis=3) for side in range(2)]


def tall_weight_grads(lefts, rights, extras, sizes, core_at, weight=1):
    names = ("y", "z", "x")
    lead = tuple(sizes[n] for n in names)
    places = spread_places(sizes, names)
    width = sum(left.shape[1] for left in lefts)
    cols = sum(right.shape[1] for right in rights)
    each = width // len(places)
    direct = each % 8 == 0
    flops = weight * 2 * lefts[0].shape[0] * width * cols

    def body(at_ref, *refs):
        left_refs = refs[: len(lefts)]
        right_refs = refs[len(lefts) : len(lefts) + len(rights)]
        rest = refs[len(lefts) + len(rights) :]
        extra_refs, outs = rest[: len(extras)], rest[len(extras) :]

        def save(row, found, col):
            span = found.shape[1]
            if not direct:
                outs[0][row : row + found.shape[0], col : col + span] = found.astype(BF)
                return

            def into(ref):
                def store(place, piece):
                    ref[(*place, slice(None), slice(col, col + span))] = piece

                return store

            store_spread(places, each, at_ref[0], found, row, into(outs[0]), into(outs[1]))

        row = 0
        for left in left_refs:
            col = 0
            for right in right_refs:
                save(row, mm(left[...], right[...], TN), col)
                col += right.shape[1]
            row += left.shape[1]
        more = extra_refs[0][...]
        for extra in extra_refs[1:]:
            more = more + extra[...]
        save(0, more, cols)

    args = (*lefts, *rights, *extras)
    shapes = [(*lead, each, cols + 128)] * 2 if direct else [(width, cols + 128)]
    out = call(
        body,
        (1,),
        [whole(a.shape) for a in args],
        [whole(shape) for shape in shapes],
        [sds(shape, BF) for shape in shapes],
        (core_at, *args),
        prefetch=1,
        flops=flops,
    )
    return out if direct else spread(out[0], sizes, names, core_at)


def scatter_sum(value, name):
    return lax.psum_scatter(value, name, scatter_dimension=0, tiled=False)


def swap_all(value, names):
    return lax.all_to_all(value, names, 0, 0, tiled=True)


def at_index(value, index):
    if isinstance(index, int):
        return value[index]
    return lax.dynamic_index_in_dim(value, index, 0, keepdims=False)


def total(terms):
    return sum(term.astype(F32) for term in terms)


def both(keep, give):
    return [keep, lax.ppermute(give, "core", [(0, 1), (1, 0)])]


def fold(terms, name, *others, ordered=False):
    if lax.axis_size(name) != 2:
        sent = total(terms).astype(BF)
        if others:
            sent = after(sent, *others)
        return [scatter_sum(sent, name)], sent
    at = 1 if ordered else lax.axis_index(name)
    sent = total([at_index(term, 1 - at) for term in terms]).astype(BF)
    if others:
        sent = after(sent, *others)
    got = lax.ppermute(sent, name, [(0, 1), (1, 0)])
    return [at_index(term, at) for term in terms] + [got], sent


def swap_by_steps(value, name):
    size, at = value.shape[0], lax.axis_index(name)
    found = [at_index(value, at)]
    for step in range(1, size):
        sent = at_index(value, (at + step) % size)
        found.append(lax.ppermute(sent, name, [(i, (i + step) % size) for i in range(size)]))
    return found


def after(value, *others):
    return lax.optimization_barrier((value, *others))[0]


def on_device(
    tokens,
    segments,
    routes,
    slots,
    cotangent,
    attn_gain,
    w_qkv,
    w_out,
    ffn_gain,
    w_router,
    shared_gate,
    shared_up,
    shared_down,
    expert_gate,
    expert_up,
    expert_down,
):
    sizes = {name: lax.axis_size(name) for name in ("y", "core", "z", "x")}
    ranks = ("z", "x")
    seqs, span, width = tokens.shape
    blocks, parts = sizes["z"], sizes["x"]
    experts = blocks * parts
    count = seqs * span
    capacity = 3 * count // experts
    length = span * experts
    group = width // parts
    z_at, x_at = lax.axis_index("z"), lax.axis_index("x")
    own = (z_at * parts + x_at).astype(jnp.int32).reshape(1)
    z_ref, x_ref = z_at.astype(jnp.int32).reshape(1), x_at.astype(jnp.int32).reshape(1)
    core_ref = lax.axis_index("core").astype(jnp.int32).reshape(1)
    pair_ref = jnp.stack([lax.axis_index("core"), lax.axis_index("y")]).astype(jnp.int32)
    attn_scale = attn_gain.astype(F32).reshape(1, width)
    ffn_scale = ffn_gain.astype(F32).reshape(1, width)
    flat_tokens = tokens.reshape(count, width)
    flat_cot = cotangent.reshape(count, width)

    route_rows = routes.reshape(count, 2)
    slot_rows = slots.reshape(count, 2)
    half = capacity // 2
    targets = []
    for first in (0, half):
        here = (slot_rows >= first) & (slot_rows < first + half)
        targets.append(jnp.where(here, route_rows * half + slot_rows - first, -1))
    target_rows = [jnp.transpose(target) for target in targets]
    target = jnp.concatenate(targets, axis=1)
    whole_target = jnp.where(slot_rows >= 0, route_rows * capacity + slot_rows, -1)
    route_flat = jnp.transpose(route_rows)
    grad_sent = [dispatch(flat_cot, to, experts, half, route_flat) for to in target_rows]

    frequency = jnp.power(10000.0, -2.0 * jnp.arange(32, dtype=F32) / HEAD_DIM)
    angles = jnp.arange(length, dtype=jnp.int32).astype(F32)[:, None] * jnp.tile(frequency, 4)
    sign = jnp.where(jnp.arange(128) % 64 < 32, -1.0, 1.0)
    cosine, sine = jnp.cos(angles), jnp.sin(angles) * sign
    seg_row = lax.dynamic_slice_in_dim(segments, z_at, 1, 0)
    seg_col = seg_row.reshape(length, 1)
    fused = group % 128 == 0
    if fused:
        weights = [w_qkv] * 3
    else:
        picked = w_qkv.reshape(width, 3, parts, group)
        picked = lax.dynamic_index_in_dim(picked, x_at, 2, keepdims=False)
        weights = [picked.reshape(width, 3 * group)]

    by_seq = swap_all(tokens, "z")
    by_seq, cosine, sine, seg_col, *grad_sent = lax.optimization_barrier(
        (by_seq, cosine, sine, seg_col, *grad_sent)
    )
    if parts == 2:
        rows = [by_seq, lax.ppermute(by_seq, "x", [(0, 1), (1, 0)])]
    else:
        rows = [lax.all_gather(by_seq, "x", axis=0, tiled=False)]
    *rows, grad_sent[0] = lax.optimization_barrier((*rows, grad_sent[0]))
    grad_came = [swap_all(grad_sent[0], ranks)]

    qkv, normed = project(rows, attn_scale, weights, group, cosine, sine, x_ref, parts)
    attended, lse = (attend if fused else plain_attend)(qkv, seg_row, seg_col)
    attended = after(attended, grad_came[0])
    attended = swap_all(attended.reshape(experts, span, group), ranks)
    attended, grad_sent[1] = lax.optimization_barrier((attended, grad_sent[1]))
    grad_came.append(swap_all(grad_sent[1], ranks))
    attended = attended.reshape(seqs, parts, span, group)

    hidden, branch_in = after_attention(flat_tokens, attended, w_out, ffn_scale)
    sent = [dispatch(branch_in, target_rows[0], experts, half)]
    shared_out, shared_back, hid, dg, du = feed_forward(
        after(branch_in, sent[0]), flat_cot, shared_gate, shared_up, shared_down
    )
    sent.append(dispatch(after(branch_in, shared_out), target_rows[1], experts, half))
    sent[0] = after(sent[0], grad_came[1], shared_out)
    received = [swap_all(value, ranks).reshape(-1, width) for value in sent]
    keep, give = shared_weight_grads(branch_in, flat_cot, dg, du, hid, sizes, core_ref)
    shared_sums, _ = fold(both(keep, give), "y")

    router = jnp.pad(w_router, ((0, 0), (0, 128 - experts)))
    made, back_rows, halves = None, [], []
    before = (give, sent[1])
    for at in range(2):
        grad_rows = grad_came[at][:, :half, :].reshape(-1, width)
        other = grad_came[at][:, half, :half].astype(jnp.int32).reshape(-1, 1)
        rows_at = after(received[at], grad_rows, other, *before)
        made, back, hid, dg, du, gated_grads, grad_logits = feed_forward(
            rows_at, grad_rows, expert_gate[0], expert_up[0], expert_down[0], router, other, own,
            experts, at, made,
        )
        back_rows.append(swap_all(back.reshape(experts, half, width), ranks).reshape(-1, width))
        halves.append((rows_at, gated_grads, dg, du, hid, grad_logits))
        before = (back,)
    halves[1] = (after(halves[1][0], back_rows[0]), *halves[1][1:])
    keep, give, grad_router = expert_weight_grads(halves, sizes, pair_ref)
    back_rows[1] = after(back_rows[1], give)
    expert_sums, expert_sent = fold(both(keep, give), "y", ordered=True)
    expert_got = expert_sums[-1]

    grad_hidden, grad_attn, grad_att, grad_ffn = middle_back(
        hidden, shared_back, back_rows, target, flat_cot, ffn_scale, w_out, parts, span
    )
    grad_att = swap_all(grad_att.reshape(experts, span, group), ranks).reshape(length, group)

    column = lax.broadcasted_iota(jnp.int32, (width, 128), 1)
    small = jnp.where(column < experts, grad_router, jnp.where(column == experts, grad_ffn, 0.0))
    out_sums = tall_weight_grads(
        [attended[:, part].reshape(count, group) for part in range(parts)],
        [grad_attn],
        [small],
        sizes,
        core_ref,
        WEIGHT,
    )
    out_sums = both(*out_sums)

    shared_sums, shared_sent = fold([after(term, out_sums[0]) for term in shared_sums], "x")
    made = after(made, grad_att, out_sums[0], shared_sent)
    grad_att = after(grad_att, expert_sent)
    made_rows = swap_all(made, ranks).reshape(-1, width)
    grads = list(
        (attend_back if fused else plain_attend_back)(
            qkv, grad_att, lse, seg_row, seg_col, cosine, sine
        )
    )
    normed_back, grad_gain = project_back(grads, weights, rows, x_ref, parts)
    normed_back, _ = fold([normed_back], "x")
    shared_sums = total(shared_sums).astype(BF)
    pieces = swap_by_steps(after(total(normed_back).astype(BF), made_rows), "z")

    qkv_sums = tall_weight_grads([normed], list(grads), [grad_gain], sizes, core_ref, 0.2)
    last = [jnp.concatenate(pair, axis=-1) for pair in zip(out_sums, both(*qkv_sums))]
    last, _ = fold(last, "y", expert_got)
    expert_sums = total(expert_sums)
    layer_out = layer_end(hidden, shared_out, [made_rows], whole_target).reshape(tokens.shape)
    token_grad = first_norm_back(flat_tokens, attn_scale, pieces, after(grad_hidden, layer_out, expert_sums), z_ref)

    shared_sums = swap_by_steps(after(shared_sums, *pieces), "z")
    last = after(total(last).astype(BF), made_rows)
    each, cols = last.shape[-2:]
    last = swap_all(last.reshape(experts, each, cols), ranks).astype(F32)
    last = jnp.sum(last.reshape(blocks, parts, each, cols), axis=0)
    out_sums = jnp.sum(last[:, :, : width + 128], axis=0)
    qkv_sums = last[:, :, width + 128 :]
    grad_attn_gain = jnp.sum(qkv_sums[:, :, 3 * group], axis=0)
    grad_w_qkv = qkv_sums[:, :, : 3 * group].reshape(parts, each, 3, group)
    grad_w_qkv = jnp.transpose(grad_w_qkv, (1, 2, 0, 3)).reshape(each, 3 * width)

    shared_sums = total(shared_sums)
    return (
        layer_out,
        token_grad.reshape(tokens.shape),
        grad_attn_gain,
        grad_w_qkv,
        out_sums[:, :width],
        out_sums[:, width + experts],
        out_sums[:, width : width + experts],
        shared_sums[0],
        shared_sums[1],
        jnp.transpose(shared_sums[2]),
        expert_sums[0][None],
        expert_sums[1][None],
        jnp.transpose(expert_sums[2])[None],
    )


def solution(mesh):
    dp, experts = mesh.shape["dp"], mesh.shape["expert"]

    def step(*args):
        seqs = args[0].shape[0] // dp
        cores = 2 if dp % 2 == 0 else 1
        fine = Mesh(
            mesh.devices.reshape(dp // cores, cores, seqs, experts // seqs),
            ("y", "core", "z", "x"),
        )
        data, ranks, every = ("y", "core"), ("z", "x"), ("y", "core", "z", "x")
        placed = (
            P(data, ranks, None),
            P(data, None),
            P(data, ranks, None),
            P(data, ranks, None),
            P(data, ranks, None),
            *([P()] * 8),
            P(ranks, None, None),
            P(ranks, None, None),
            P(ranks, None, None),
        )
        return jax.shard_map(
            on_device,
            mesh=fine,
            in_specs=placed,
            out_specs=(
                P(data, ranks, None),
                P(data, ranks, None),
                P(every),
                P(every, None),
                P(every, None),
                P(every),
                P(every, None),
                P(every, None),
                P(every, None),
                P(None, every),
                P(ranks, None, data),
                P(ranks, None, data),
                P(ranks, data, None),
            ),
            check_vma=False,
        )(*args)

    return step
```

```python
import jax
import jax.numpy as jnp
from jax import lax
from jax.experimental import pallas as pl
from jax.experimental.pallas import tpu as pltpu
from jax.sharding import Mesh
from jax.sharding import PartitionSpec as P

HEAD_DIM = 64
EPS = 1e-06
BF = jnp.bfloat16
F32 = jnp.float32
NEG = -1e30
NN = (((1,), (0,)), ((), ()))
NT = (((1,), (1,)), ((), ()))
TN = (((0,), (0,)), ((), ()))
VMEM_MOST = 60 << 20
WEIGHT = 3


def mm(left, right, dims=NN):
    return lax.dot_general(left, right, dims, preferred_element_type=F32)


def sds(shape, dtype):
    return jax.ShapeDtypeStruct(shape, dtype)


def call(
    body, grid, in_specs, out_specs, out_shape, args, scratch=(), prefetch=0, flops=0, alias=None
):
    leaves = jax.tree.leaves(out_shape)
    moved = sum(a.size * a.dtype.itemsize for a in args) + sum(
        a.size * a.dtype.itemsize for a in leaves
    )
    return pl.pallas_call(
        body,
        out_shape=out_shape,
        grid_spec=pltpu.PrefetchScalarGridSpec(
            num_scalar_prefetch=prefetch,
            grid=grid,
            in_specs=in_specs,
            out_specs=out_specs,
            scratch_shapes=list(scratch),
        ),
        compiler_params=pltpu.CompilerParams(
            dimension_semantics=("arbitrary",) * len(grid), vmem_limit_bytes=VMEM_MOST
        ),
        cost_estimate=pl.CostEstimate(
            flops=int(flops), transcendentals=0, bytes_accessed=int(moved)
        ),
        input_output_aliases=alias or {},
    )(*args)


def whole(shape):
    rank = len(shape)
    return pl.BlockSpec(tuple(shape), lambda *_: (0,) * rank)


def swap_halves(value):
    lane = lax.broadcasted_iota(jnp.int32, value.shape, 1)
    return jnp.where(lane % 64 < 32, pltpu.roll(value, 96, 1), pltpu.roll(value, 32, 1))


def rms(values):
    return lax.rsqrt(jnp.mean(values * values, axis=1, keepdims=True) + EPS)


def row_specs(rows):
    if len(rows) == 2:
        _, span, width = rows[0].shape
        return [pl.BlockSpec((1, span, width), lambda i, *_: (i, 0, 0))] * 2
    parts, _, span, width = rows[0].shape
    return [pl.BlockSpec((parts, 1, span, width), lambda i, *_: (0, i, 0, 0))]


def load_rows(refs, at_ref):
    if len(refs) == 2:
        mine, theirs = refs[0][0].astype(F32), refs[1][0].astype(F32)
        first = at_ref[0] == 0
        pair = [jnp.where(first, mine, theirs), jnp.where(first, theirs, mine)]
        return jnp.concatenate(pair, axis=0)
    value = refs[0][...]
    return value.reshape(value.shape[0] * value.shape[2], value.shape[3]).astype(F32)


def weight_specs(weights, group):
    if len(weights) == 1:
        return [whole(weights[0].shape)]
    width, cols = weights[0].shape
    parts = cols // (3 * group)

    def spec(index):
        return pl.BlockSpec((width, group), lambda i, at: (0, index * parts + at[0]))

    return [spec(index) for index in range(3)]


def load_weights(refs, group):
    if len(refs) == 3:
        return [ref[...] for ref in refs]
    return [refs[0][:, at * group : (at + 1) * group] for at in range(3)]


def project(rows, gain, weights, group, cosine, sine, x_at, parts):
    blocks, span, width = rows[0].shape[-3:]
    height = parts * span
    length = height * blocks
    cut = len(rows)

    def body(at_ref, *refs):
        r_refs, (g_ref, c_ref, s_ref) = refs[:cut], refs[cut : cut + 3]
        w_refs, (qkv_ref, n_ref) = refs[cut + 3 : -2], refs[-2:]
        tok = load_rows(r_refs, at_ref)
        normed = (tok * rms(tok) * g_ref[...]).astype(BF)
        n_ref[...] = normed
        if len(w_refs) == 3:
            found = [mm(normed, ref[...]) for ref in w_refs]
            turning = [(found[0], 0), (found[1], group)]
            last = found[2]
        else:
            found = mm(normed, w_refs[0][...])
            turning, last = [(found[:, : 2 * group], 0)], found[:, 2 * group :]
        for value, base in turning:
            for at in range(0, value.shape[1], 128):
                part = value[:, at : at + 128]
                lane = lax.broadcasted_iota(jnp.int32, part.shape, 1) + (base + at)
                turned = part * c_ref[...] + swap_halves(part) * s_ref[...]
                turned = turned * jnp.where(lane < group, HEAD_DIM**-0.5, 1.0)
                qkv_ref[:, base + at : base + at + 128] = turned.astype(BF)
        qkv_ref[:, 2 * group :] = last.astype(BF)

    return call(
        body,
        (blocks,),
        [
            *row_specs(rows),
            whole((1, width)),
            pl.BlockSpec((height, 128), lambda i, *_: (i, 0)),
            pl.BlockSpec((height, 128), lambda i, *_: (i, 0)),
            *weight_specs(weights, group),
        ],
        [
            pl.BlockSpec((height, 3 * group), lambda i, *_: (i, 0)),
            pl.BlockSpec((height, width), lambda i, *_: (i, 0)),
        ],
        [sds((length, 3 * group), BF), sds((length, width), BF)],
        (x_at, *rows, gain, cosine, sine, *weights),
        prefetch=1,
        flops=6 * length * width * group,
    )


def project_back(grads, weights, rows, x_at, parts):
    blocks, span, width = rows[0].shape[-3:]
    group = grads[0].shape[1]
    height = parts * span
    length = height * blocks
    cut = len(rows)

    def body(at_ref, q_ref, k_ref, v_ref, *refs):
        r_refs, w_refs, (out_ref, gain_ref, acc_ref) = refs[:cut], refs[cut:-3], refs[-3:]
        step = pl.program_id(0)
        w_q, w_k, w_v = load_weights(w_refs, group)
        back = mm(q_ref[...], w_q, NT) + mm(k_ref[...], w_k, NT) + mm(v_ref[...], w_v, NT)
        tok = load_rows(r_refs, at_ref)
        part = jnp.sum(back * tok * rms(tok), axis=0, keepdims=True)

        @pl.when(step == 0)
        def _():
            acc_ref[...] = jnp.zeros_like(acc_ref)

        acc_ref[...] += jnp.broadcast_to(part, acc_ref.shape)
        out_ref[...] = back.astype(BF).reshape(parts, 1, span, width)

        @pl.when(step == blocks - 1)
        def _():
            column = jnp.transpose(acc_ref[...])
            gain_ref[...] = jnp.broadcast_to(column[:, :1], gain_ref.shape)

    block = pl.BlockSpec((height, group), lambda i, *_: (i, 0))
    return call(
        body,
        (blocks,),
        [block, block, block, *row_specs(rows), *weight_specs(weights, group)],
        [
            pl.BlockSpec((parts, 1, span, width), lambda i, *_: (0, i, 0, 0)),
            whole((width, 128)),
        ],
        [sds((parts, blocks, span, width), BF), sds((width, 128), F32)],
        (x_at, *grads, *rows, *weights),
        scratch=[pltpu.VMEM((8, width), F32)],
        prefetch=1,
        flops=0.2 * length * width * group,
    )


def attend(qkv, seg_row, seg_col):
    length, cols = qkv.shape
    group = cols // 3
    pairs = group // 128
    high = min(256, length)

    def body(q_ref, k_ref, v_ref, sr_ref, sc_ref, o_ref, l_ref):
        lane = lax.broadcasted_iota(jnp.int32, (high, 128), 1)
        for at in range(0, length, high):
            end = at + high
            query = q_ref[at:end, :]
            keys = k_ref[:end, :]
            vals = v_ref[:end, :]
            q_pos = lax.broadcasted_iota(jnp.int32, (high, end), 0) + at
            k_pos = lax.broadcasted_iota(jnp.int32, (high, end), 1)
            allowed = (sc_ref[at:end, :] == sr_ref[:, :end]) & (k_pos <= q_pos)
            outs = []
            for head in range(2):
                mine = (lane // 64) == head
                scores = mm(jnp.where(mine, query, jnp.zeros_like(query)), keys, NT)
                scores = jnp.where(allowed, scores, NEG)
                most = jnp.max(scores, axis=1, keepdims=True)
                expo = jnp.exp(scores - most)
                total = jnp.sum(expo, axis=1, keepdims=True)
                outs.append(mm(expo.astype(BF), vals) / total)
                lse = jnp.broadcast_to(most + jnp.log(total), (high, 128))
                l_ref[0, head : head + 1, at:end] = jnp.transpose(lse)[:1, :]
            o_ref[at:end, :] = jnp.where(lane < 64, outs[0], outs[1]).astype(BF)

    def col(offset):
        return pl.BlockSpec((length, 128), lambda i: (0, offset * pairs + i))

    return call(
        body,
        (pairs,),
        [col(0), col(1), col(2), whole((1, length)), whole((length, 1))],
        [col(0), pl.BlockSpec((1, 2, length), lambda i: (i, 0, 0))],
        [sds((length, group), BF), sds((pairs, 2, length), F32)],
        (qkv, qkv, qkv, seg_row, seg_col),
        flops=4 * length * length * group,
    )


def attend_back(qkv, grad, lse, seg_row, seg_col, cosine, sine):
    length, cols = qkv.shape
    group = cols // 3
    pairs = group // 128
    high = min(256, length)

    def body(
        q_ref, k_ref, v_ref, g_ref, l_ref, sr_ref, sc_ref, c_ref, s_ref, dq_ref, dk_ref, dv_ref,
        ka_ref, va_ref,
    ):
        lane = lax.broadcasted_iota(jnp.int32, (high, 128), 1)
        ka_ref[...] = jnp.zeros_like(ka_ref)
        va_ref[...] = jnp.zeros_like(va_ref)
        for at in range(0, length, high):
            end = at + high
            query = q_ref[at:end, :]
            grads = g_ref[at:end, :]
            keys = k_ref[:end, :]
            vals = v_ref[:end, :]
            k_pos = lax.broadcasted_iota(jnp.int32, (end, high), 0)
            q_pos = lax.broadcasted_iota(jnp.int32, (end, high), 1) + at
            allowed = (sc_ref[:end, :] == sr_ref[:, at:end]) & (k_pos <= q_pos)
            outs = []
            for head in range(2):
                mine = (lane // 64) == head
                q_own = jnp.where(mine, query, jnp.zeros_like(query))
                g_own = jnp.where(mine, grads, jnp.zeros_like(grads))
                scores = jnp.where(allowed, mm(keys, q_own, NT), NEG)
                probs = jnp.exp(scores - l_ref[0, head : head + 1, at:end])
                grad_probs = mm(vals, g_own, NT)
                delta = jnp.sum(probs * grad_probs, axis=0, keepdims=True)
                grad_scores = (probs * (grad_probs - delta)).astype(BF)
                va_ref[:end, :] += mm(probs.astype(BF), g_own)
                ka_ref[:end, :] += mm(grad_scores, q_own)
                outs.append(mm(grad_scores, keys, TN))
            found = jnp.where(lane < 64, outs[0], outs[1]) * HEAD_DIM**-0.5
            back = found * c_ref[at:end, :] - swap_halves(found) * s_ref[at:end, :]
            dq_ref[at:end, :] = back.astype(BF)
        found = ka_ref[...]
        dk_ref[...] = (found * c_ref[...] - swap_halves(found) * s_ref[...]).astype(BF)
        dv_ref[...] = va_ref[...].astype(BF)

    def col(offset):
        return pl.BlockSpec((length, 128), lambda i: (0, offset * pairs + i))

    return call(
        body,
        (pairs,),
        [
            col(0),
            col(1),
            col(2),
            col(0),
            pl.BlockSpec((1, 2, length), lambda i: (i, 0, 0)),
            whole((1, length)),
            whole((length, 1)),
            whole((length, 128)),
            whole((length, 128)),
        ],
        [col(0), col(0), col(0)],
        [sds((length, group), BF)] * 3,
        (qkv, qkv, qkv, grad, lse, seg_row, seg_col, cosine, sine),
        scratch=[pltpu.VMEM((length, 128), F32)] * 2,
        flops=length * length * group,
    )


def heads_of(flat):
    return flat.reshape(flat.shape[0], -1, HEAD_DIM)


def plain_mask(seg_row, seg_col):
    length = seg_col.shape[0]
    spots = jnp.arange(length, dtype=jnp.int32)
    return (seg_row == seg_col) & (spots[None, :] <= spots[:, None])


def plain_attend(qkv, seg_row, seg_col):
    query, keys, vals = (heads_of(part) for part in jnp.split(qkv, 3, axis=1))
    scores = jnp.einsum("qhd,khd->hqk", query, keys, preferred_element_type=F32)
    scores = jnp.where(plain_mask(seg_row, seg_col)[None], scores, NEG)
    lse = jax.nn.logsumexp(scores, axis=-1, keepdims=True)
    probs = jnp.exp(scores - lse).astype(BF)
    found = jnp.einsum("hqk,khd->qhd", probs, vals, preferred_element_type=F32)
    return found.astype(BF).reshape(qkv.shape[0], -1), lse


def plain_turn_back(grads, cosine, sine):
    table_c, table_s = cosine[:, None, :HEAD_DIM], sine[:, None, :HEAD_DIM]
    swapped = jnp.roll(grads, HEAD_DIM // 2, axis=-1)
    return (grads * table_c - swapped * table_s).astype(BF).reshape(grads.shape[0], -1)


def plain_attend_back(qkv, grad, lse, seg_row, seg_col, cosine, sine):
    query, keys, vals = (heads_of(part) for part in jnp.split(qkv, 3, axis=1))
    grad = heads_of(grad)
    scores = jnp.einsum("qhd,khd->hqk", query, keys, preferred_element_type=F32)
    scores = jnp.where(plain_mask(seg_row, seg_col)[None], scores, NEG)
    probs = jnp.exp(scores - lse)
    grad_probs = jnp.einsum("qhd,khd->hqk", grad, vals, preferred_element_type=F32)
    delta = jnp.sum(probs * grad_probs, axis=-1, keepdims=True)
    grad_scores = (probs * (grad_probs - delta)).astype(BF)
    gq = jnp.einsum("hqk,khd->qhd", grad_scores, keys, preferred_element_type=F32)
    gk = jnp.einsum("hqk,qhd->khd", grad_scores, query, preferred_element_type=F32)
    gv = jnp.einsum("hqk,qhd->khd", probs.astype(BF), grad, preferred_element_type=F32)
    return (
        plain_turn_back(gq * HEAD_DIM**-0.5, cosine, sine),
        plain_turn_back(gk, cosine, sine),
        gv.astype(BF).reshape(qkv.shape[0], -1),
    )


def after_attention(tokens, attended, w_out, gain):
    seqs, parts, span, group = attended.shape
    count, width = tokens.shape

    def body(t_ref, a_ref, w_ref, g_ref, h_ref, b_ref):
        hidden = t_ref[...].astype(F32)
        for part in range(parts):
            rows = a_ref[:, part].reshape(count, group)
            hidden += mm(rows, w_ref[part * group : (part + 1) * group, :])
        h_ref[...] = hidden
        b_ref[...] = (hidden * rms(hidden) * g_ref[...]).astype(BF)

    return call(
        body,
        (1,),
        [whole(a.shape) for a in (tokens, attended, w_out, gain)],
        [whole(tokens.shape)] * 2,
        [sds(tokens.shape, F32), sds(tokens.shape, BF)],
        (tokens, attended, w_out, gain),
        flops=2 * count * width * width,
    )


def dispatch(rows, target_rows, experts, capacity, route_rows=None):
    count, width = rows.shape
    more = 0 if route_rows is None else 16
    tables = () if route_rows is None else (route_rows,)

    def body(r_ref, t_ref, *refs):
        o_ref = refs[-1]
        slot = lax.broadcasted_iota(jnp.int32, (capacity, count), 0)
        slot += pl.program_id(0) * capacity
        hits = [slot == t_ref[k : k + 1, :] for k in range(2)]
        hot = (hits[0] | hits[1]).astype(F32).astype(BF)
        o_ref[0, :capacity, :] = mm(hot, r_ref[...]).astype(BF)
        if more:
            o_ref[0, capacity:, :] = jnp.zeros((more, width), BF)
            other = jnp.zeros((8, capacity), F32)
            for k in range(2):
                route = jnp.broadcast_to(refs[0][1 - k : 2 - k, :].astype(F32), (8, count))
                other += mm(route.astype(BF), hits[k].astype(F32).astype(BF), NT)
            o_ref[0, capacity : capacity + 8, :capacity] = other.astype(BF)

    return call(
        body,
        (experts,),
        [whole(a.shape) for a in (rows, target_rows, *tables)],
        pl.BlockSpec((1, capacity + more, width), lambda i: (i, 0, 0)),
        sds((experts, capacity + more, width), BF),
        (rows, target_rows, *tables),
        flops=2 * experts * capacity * count * width,
    )


def pick(target, row_refs):
    total = None
    for index, ref in enumerate(row_refs):
        rows = ref[...]
        spot = lax.broadcasted_iota(jnp.int32, (target.shape[0], rows.shape[0]), 1)
        one, two = target[:, 2 * index : 2 * index + 1], target[:, 2 * index + 1 : 2 * index + 2]
        found = mm(((spot == one) | (spot == two)).astype(F32).astype(BF), rows)
        total = found if total is None else total + found
    return total


def layer_end(hidden, shared_out, rows, target):
    count, width = hidden.shape
    high = count // 2

    def body(h_ref, s_ref, t_ref, *refs):
        refs[-1][...] = (h_ref[...] + s_ref[...] + pick(t_ref[...], refs[:-1])).astype(BF)

    block = pl.BlockSpec((high, width), lambda i: (i, 0))
    return call(
        body,
        (2,),
        [
            block,
            block,
            pl.BlockSpec((high, target.shape[1]), lambda i: (i, 0)),
            *[whole(part.shape) for part in rows],
        ],
        block,
        sds(hidden.shape, BF),
        (hidden, shared_out, target, *rows),
        flops=2 * count * width * rows[0].shape[0] * len(rows),
    )


def middle_back(hidden, grad_shared, rows, target, cotangent, gain, w_out, parts, span):
    count, width = hidden.shape
    seqs = count // span
    each = 2 if seqs % 2 == 0 else 1
    high = each * span
    steps = count // high
    group = width // parts

    def body(h_ref, s_ref, t_ref, c_ref, g_ref, w_ref, *refs):
        gh_ref, ga_ref, d_ref, n_ref, acc_ref = refs[len(rows) :]
        step = pl.program_id(0)
        branch = s_ref[...] + pick(t_ref[...], refs[: len(rows)])
        hidden = h_ref[...]
        scale = rms(hidden)
        weighted = branch * g_ref[...]
        inner = jnp.mean(weighted * hidden, axis=1, keepdims=True)
        part = jnp.sum(branch * hidden * scale, axis=0, keepdims=True)
        out = c_ref[...].astype(F32) + scale * weighted - hidden * (scale * scale * scale * inner)
        gh_ref[...] = out
        out = out.astype(BF)
        ga_ref[...] = out
        for at in range(parts):
            sent = mm(out, w_ref[at * group : (at + 1) * group, :], NT).astype(BF)
            d_ref[:, at] = sent.reshape(each, span, group)

        @pl.when(step == 0)
        def _():
            acc_ref[...] = jnp.zeros_like(acc_ref)

        acc_ref[...] += jnp.broadcast_to(part, acc_ref.shape)

        @pl.when(step == steps - 1)
        def _():
            column = jnp.transpose(acc_ref[...])
            n_ref[...] = jnp.broadcast_to(column[:, :1], n_ref.shape)

    block = pl.BlockSpec((high, width), lambda i: (i, 0))
    return call(
        body,
        (steps,),
        [
            block,
            block,
            pl.BlockSpec((high, target.shape[1]), lambda i: (i, 0)),
            block,
            whole(gain.shape),
            whole(w_out.shape),
            *[whole(part.shape) for part in rows],
        ],
        [
            block,
            block,
            pl.BlockSpec((each, parts, span, group), lambda i: (i, 0, 0, 0)),
            whole((width, 128)),
        ],
        [
            sds(hidden.shape, F32),
            sds(hidden.shape, BF),
            sds((seqs, parts, span, group), BF),
            sds((width, 128), F32),
        ],
        (hidden, grad_shared, target, cotangent, gain, w_out, *rows),
        scratch=[pltpu.VMEM((8, width), F32)],
        flops=WEIGHT * 2 * count * width * (rows[0].shape[0] * len(rows) + width),
    )


def first_norm_back(tokens, gain, pieces, grad_hidden, z_at):
    count, width = tokens.shape
    blocks = len(pieces)
    span = count // blocks

    def body(at_ref, t_ref, g_ref, h_ref, *refs):
        o_ref = refs[-1]
        for index in range(blocks):
            seq = (at_ref[0] + blocks - index) % blocks
            spot = pl.ds(pl.multiple_of(seq * span, span), span)
            tok = t_ref[spot, :].astype(F32)
            scale = rms(tok)
            weighted = refs[index][...].astype(F32) * g_ref[...]
            inner = jnp.mean(weighted * tok, axis=1, keepdims=True)
            out = h_ref[spot, :] + scale * weighted - tok * (scale * scale * scale * inner)
            o_ref[spot, :] = out.astype(BF)

    return call(
        body,
        (1,),
        [whole(a.shape) for a in (tokens, gain, grad_hidden, *pieces)],
        whole(tokens.shape),
        sds(tokens.shape, BF),
        (z_at, tokens, gain, grad_hidden, *pieces),
        prefetch=1,
    )


def feed_forward(
    rows, grads, w_gate, w_up, w_down, router=None, other=None, own=None, experts=0, place=0, made=None
):
    count, width = rows.shape
    units = w_gate.shape[1]
    wide = 512
    steps = units // wide
    high = 256
    gated = router is not None
    more = 0 if made is None else 1
    kind = BF if gated else F32

    def body(*refs):
        if gated:
            (own_ref, x_ref, g_ref, wg_ref, wu_ref, wd_ref, wr_ref, ot_ref) = refs[:8]
            (y_ref, gi_ref, hid_ref, dg_ref, du_ref, eo_ref, gl_ref, ya_ref, ga_ref, gate_ref) = refs[8 + more :]
        else:
            (x_ref, g_ref, wg_ref, wu_ref, wd_ref,
             y_ref, gi_ref, hid_ref, dg_ref, du_ref, ya_ref, ga_ref) = refs
        step = pl.program_id(0)

        if gated:

            @pl.when(step == 0)
            def _():
                logits = mm(x_ref[...], wr_ref[...])
                lane = lax.broadcasted_iota(jnp.int32, logits.shape, 1)
                mine = jnp.sum(jnp.where(lane == own_ref[0], logits, 0.0), axis=1, keepdims=True)
                theirs = jnp.sum(jnp.where(lane == ot_ref[...], logits, 0.0), axis=1, keepdims=True)
                gate = 1.0 / (1.0 + jnp.exp(theirs - mine))
                rest = 1.0 / (1.0 + jnp.exp(mine - theirs))
                gate_ref[:, 0:1] = gate
                gate_ref[:, 1:2] = rest
                eo_ref[...] = (g_ref[...].astype(F32) * gate).astype(BF)

        def rows_at(index, carry):
            at = pl.ds(pl.multiple_of(index * high, high), high)
            row = x_ref[at, :]
            grad = eo_ref[at, :] if gated else g_ref[at, :]
            gval = mm(row, wg_ref[...])
            uval = mm(row, wu_ref[...])
            sigma = 1.0 / (1.0 + jnp.exp(-gval))
            silu = gval * sigma
            hid = (silu * uval).astype(BF)
            hid_ref[at, :] = hid
            grad_hid = mm(grad, wd_ref[...], NT)
            du = (grad_hid * silu).astype(BF)
            dg = (grad_hid * uval * sigma * (1.0 + gval * (1.0 - sigma))).astype(BF)
            du_ref[at, :] = du
            dg_ref[at, :] = dg
            out = mm(hid, wd_ref[...])
            back = mm(dg, wg_ref[...], NT) + mm(du, wu_ref[...], NT)

            @pl.when(step == 0)
            def _():
                ya_ref[at, :] = out
                ga_ref[at, :] = back

            @pl.when(step > 0)
            def _():
                ya_ref[at, :] += out
                ga_ref[at, :] += back

            return carry

        lax.fori_loop(0, count // high, rows_at, 0)

        @pl.when(step == steps - 1)
        def _():
            if gated:
                out = ya_ref[...]
                gate = gate_ref[:, 0:1]
                lean = jnp.sum(out * g_ref[...].astype(F32), axis=1, keepdims=True)
                lean = lean * gate * gate_ref[:, 1:2]
                lane = lax.broadcasted_iota(jnp.int32, (count, 128), 1)
                sign = (lane == own_ref[0]).astype(F32) - (lane == ot_ref[...]).astype(F32)
                grad_logits = (lean * sign).astype(BF)
                gl_ref[...] = grad_logits
                y_ref[...] = (out * gate).astype(BF).reshape(y_ref.shape)
                gi_ref[...] = (ga_ref[...] + mm(grad_logits, wr_ref[...], NT)).astype(BF)
            else:
                y_ref[...] = ya_ref[...]
                gi_ref[...] = ga_ref[...]

    full = whole((count, width))
    hidden = pl.BlockSpec((count, wide), lambda i, *_: (0, i))
    in_specs = [
        full,
        full,
        pl.BlockSpec((width, wide), lambda i, *_: (0, i)),
        pl.BlockSpec((width, wide), lambda i, *_: (0, i)),
        pl.BlockSpec((wide, width), lambda i, *_: (i, 0)),
    ]
    out_specs = [full, full, hidden, hidden, hidden]
    out_shape = [sds((count, width), kind)] * 2 + [sds((count, units), BF)] * 3
    scratch = [pltpu.VMEM((count, width), F32)] * 2
    args = [rows, grads, w_gate, w_up, w_down]
    if gated:
        in_specs += [whole(router.shape), whole(other.shape)]
        out_specs += [full, whole((count, 128))]
        out_shape += [sds((count, width), BF), sds((count, 128), BF)]
        scratch += [pltpu.VMEM((count, 128), F32)]
        args = [own, *args, router, other]
        out_specs[0] = pl.BlockSpec((experts, count // experts, width), lambda *_: (0, place, 0))
        out_shape[0] = sds((experts, 2 * count // experts, width), BF)
        if more:
            in_specs += [pl.BlockSpec(memory_space=pl.ANY)]
            args += [made]
    return call(
        body,
        (steps,),
        in_specs,
        out_specs,
        out_shape,
        tuple(args),
        scratch=scratch,
        prefetch=1 if gated else 0,
        alias={len(args) - 1: 0} if more else None,
        flops=12 * count * width * units,
    )


def expert_weight_grads(halves, sizes, core_at):
    outer, cores = sizes["y"], sizes["core"]
    count, width = halves[0][0].shape
    units = halves[0][2].shape[1]
    wide = units // (outer * cores)

    def body(at_ref, *refs):
        keep_ref, give_ref, r_ref = refs[-3:]
        groups = [refs[6 * at : 6 * at + 6] for at in range(len(halves))]
        step = pl.program_id(0)

        def over(left, right):
            return sum(mm(group[left][...], group[right][...], TN) for group in groups)

        found = [over(0, 2).astype(BF), over(0, 3).astype(BF), over(1, 4).astype(BF)]

        @pl.when(step < outer)
        def _():
            for index in range(3):
                give_ref[0, index] = found[index]

        @pl.when(step >= outer)
        def _():
            for index in range(3):
                keep_ref[0, index] = found[index]

        @pl.when(step == 0)
        def _():
            r_ref[...] = over(0, 5)

    def taken(i, at):
        core = jnp.where(i < outer, 1 - at[0], at[0])
        y = (i + 1 + at[1]) % outer if outer == 2 else i % outer
        return (0, y * cores + core)

    hidden = pl.BlockSpec((count, wide), taken)
    part = (1, 3, width, wide)
    return call(
        body,
        (outer * cores,),
        [
            whole((count, width)),
            whole((count, width)),
            hidden,
            hidden,
            hidden,
            whole((count, 128)),
        ]
        * len(halves),
        [
            pl.BlockSpec(part, lambda i, *_: (jnp.maximum(i - outer, 0), 0, 0, 0)),
            pl.BlockSpec(part, lambda i, *_: (jnp.minimum(i, outer - 1), 0, 0, 0)),
            whole((width, 128)),
        ],
        [sds((outer, *part[1:]), BF)] * 2 + [sds((width, 128), F32)],
        (core_at, *[value for half in halves for value in half]),
        prefetch=1,
        flops=6 * count * len(halves) * width * units,
    )


def spread_places(sizes, names):
    found = []
    for y in range(sizes["y"]):
        for core in range(sizes["core"]):
            for z in range(sizes["z"]):
                for x in range(sizes["x"]):
                    at = {"y": y, "core": core, "z": z, "x": x}
                    found.append((core, tuple(at[n] for n in names)))
    return found


def spread(value, sizes, names, core_at):
    order = ("y", "core", "z", "x")
    split = value.reshape(*(sizes[n] for n in order), -1, value.shape[-1])
    split = jnp.transpose(split, (1, *(order.index(n) for n in names), 4, 5))
    return at_index(split, core_at[0]), at_index(split, 1 - core_at[0])


def store_spread(places, each, core_at, found, row, keep, give):
    first = row // each
    for core in range(2):
        todo = [at for at in range(found.shape[0] // each) if places[first + at][0] == core]

        def put(store, todo=todo):
            for at in todo:
                store(places[first + at][1], found[at * each : (at + 1) * each].astype(BF))

        pl.when(core_at == core)(lambda put=put: put(keep))
        pl.when(core_at != core)(lambda put=put: put(give))


def shared_weight_grads(rows, grads, dg, du, hid, sizes, core_at):
    names = ("y", "x", "z")
    lead = tuple(sizes[n] for n in names)
    places = spread_places(sizes, names)
    count, width = rows.shape
    units = dg.shape[1]
    wide = 512
    each = width // len(places)
    direct = each % 8 == 0

    def body(at_ref, x_ref, g_ref, dg_ref, du_ref, hid_ref, *outs):
        pairs = ((x_ref, dg_ref), (x_ref, du_ref), (g_ref, hid_ref))
        for index, (left, right) in enumerate(pairs):
            found = mm(left[...], right[...], TN)
            if not direct:
                outs[0][index] = found.astype(BF)
                continue

            def into(ref, index=index):
                def store(place, piece):
                    ref[(*place, index)] = piece

                return store

            store_spread(places, each, at_ref[0], found, 0, into(outs[0]), into(outs[1]))

    hidden = pl.BlockSpec((count, wide), lambda i, *_: (0, i))
    if direct:
        shapes = [(*lead, 3, each, units)] * 2
        spec = [pl.BlockSpec((*lead, 3, each, wide), lambda i, *_: (0,) * 5 + (i,))] * 2
    else:
        shapes = [(3, width, units)]
        spec = [pl.BlockSpec((3, width, wide), lambda i, *_: (0, 0, i))]
    out = call(
        body,
        (units // wide,),
        [whole(rows.shape), whole(grads.shape), hidden, hidden, hidden],
        spec,
        [sds(shape, BF) for shape in shapes],
        (core_at, rows, grads, dg, du, hid),
        prefetch=1,
        flops=6 * count * width * units,
    )
    if direct:
        return out
    found = [spread(out[0][i], sizes, names, core_at) for i in range(3)]
    return [jnp.stack([part[side] for part in found], axis=3) for side in range(2)]


def tall_weight_grads(lefts, rights, extras, sizes, core_at, weight=1):
    names = ("y", "z", "x")
    lead = tuple(sizes[n] for n in names)
    places = spread_places(sizes, names)
    width = sum(left.shape[1] for left in lefts)
    cols = sum(right.shape[1] for right in rights)
    each = width // len(places)
    direct = each % 8 == 0
    flops = weight * 2 * lefts[0].shape[0] * width * cols

    def body(at_ref, *refs):
        left_refs = refs[: len(lefts)]
        right_refs = refs[len(lefts) : len(lefts) + len(rights)]
        rest = refs[len(lefts) + len(rights) :]
        extra_refs, outs = rest[: len(extras)], rest[len(extras) :]

        def save(row, found, col):
            span = found.shape[1]
            if not direct:
                outs[0][row : row + found.shape[0], col : col + span] = found.astype(BF)
                return

            def into(ref):
                def store(place, piece):
                    ref[(*place, slice(None), slice(col, col + span))] = piece

                return store

            store_spread(places, each, at_ref[0], found, row, into(outs[0]), into(outs[1]))

        row = 0
        for left in left_refs:
            col = 0
            for right in right_refs:
                save(row, mm(left[...], right[...], TN), col)
                col += right.shape[1]
            row += left.shape[1]
        more = extra_refs[0][...]
        for extra in extra_refs[1:]:
            more = more + extra[...]
        save(0, more, cols)

    args = (*lefts, *rights, *extras)
    shapes = [(*lead, each, cols + 128)] * 2 if direct else [(width, cols + 128)]
    out = call(
        body,
        (1,),
        [whole(a.shape) for a in args],
        [whole(shape) for shape in shapes],
        [sds(shape, BF) for shape in shapes],
        (core_at, *args),
        prefetch=1,
        flops=flops,
    )
    return out if direct else spread(out[0], sizes, names, core_at)


def scatter_sum(value, name):
    return lax.psum_scatter(value, name, scatter_dimension=0, tiled=False)


def swap_all(value, names):
    return lax.all_to_all(value, names, 0, 0, tiled=True)


def at_index(value, index):
    if isinstance(index, int):
        return value[index]
    return lax.dynamic_index_in_dim(value, index, 0, keepdims=False)


def total(terms):
    return sum(term.astype(F32) for term in terms)


def both(keep, give):
    return [keep, lax.ppermute(give, "core", [(0, 1), (1, 0)])]


def fold(terms, name, *others, ordered=False):
    if lax.axis_size(name) != 2:
        sent = total(terms).astype(BF)
        if others:
            sent = after(sent, *others)
        return [scatter_sum(sent, name)], sent
    at = 1 if ordered else lax.axis_index(name)
    sent = total([at_index(term, 1 - at) for term in terms]).astype(BF)
    if others:
        sent = after(sent, *others)
    got = lax.ppermute(sent, name, [(0, 1), (1, 0)])
    return [at_index(term, at) for term in terms] + [got], sent


def swap_by_steps(value, name):
    size, at = value.shape[0], lax.axis_index(name)
    found = [at_index(value, at)]
    for step in range(1, size):
        sent = at_index(value, (at + step) % size)
        found.append(lax.ppermute(sent, name, [(i, (i + step) % size) for i in range(size)]))
    return found


def after(value, *others):
    return lax.optimization_barrier((value, *others))[0]


def on_device(
    tokens,
    segments,
    routes,
    slots,
    cotangent,
    attn_gain,
    w_qkv,
    w_out,
    ffn_gain,
    w_router,
    shared_gate,
    shared_up,
    shared_down,
    expert_gate,
    expert_up,
    expert_down,
):
    sizes = {name: lax.axis_size(name) for name in ("y", "core", "z", "x")}
    ranks = ("z", "x")
    seqs, span, width = tokens.shape
    blocks, parts = sizes["z"], sizes["x"]
    experts = blocks * parts
    count = seqs * span
    capacity = 3 * count // experts
    length = span * experts
    group = width // parts
    z_at, x_at = lax.axis_index("z"), lax.axis_index("x")
    own = (z_at * parts + x_at).astype(jnp.int32).reshape(1)
    z_ref, x_ref = z_at.astype(jnp.int32).reshape(1), x_at.astype(jnp.int32).reshape(1)
    core_ref = lax.axis_index("core").astype(jnp.int32).reshape(1)
    pair_ref = jnp.stack([lax.axis_index("core"), lax.axis_index("y")]).astype(jnp.int32)
    attn_scale = attn_gain.astype(F32).reshape(1, width)
    ffn_scale = ffn_gain.astype(F32).reshape(1, width)
    flat_tokens = tokens.reshape(count, width)
    flat_cot = cotangent.reshape(count, width)

    route_rows = routes.reshape(count, 2)
    slot_rows = slots.reshape(count, 2)
    half = capacity // 2
    targets = []
    for first in (0, half):
        here = (slot_rows >= first) & (slot_rows < first + half)
        targets.append(jnp.where(here, route_rows * half + slot_rows - first, -1))
    target_rows = [jnp.transpose(target) for target in targets]
    target = jnp.concatenate(targets, axis=1)
    whole_target = jnp.where(slot_rows >= 0, route_rows * capacity + slot_rows, -1)
    route_flat = jnp.transpose(route_rows)
    grad_sent = [dispatch(flat_cot, to, experts, half, route_flat) for to in target_rows]

    frequency = jnp.power(10000.0, -2.0 * jnp.arange(32, dtype=F32) / HEAD_DIM)
    angles = jnp.arange(length, dtype=jnp.int32).astype(F32)[:, None] * jnp.tile(frequency, 4)
    sign = jnp.where(jnp.arange(128) % 64 < 32, -1.0, 1.0)
    cosine, sine = jnp.cos(angles), jnp.sin(angles) * sign
    seg_row = lax.dynamic_slice_in_dim(segments, z_at, 1, 0)
    seg_col = seg_row.reshape(length, 1)
    fused = group % 128 == 0
    if fused:
        weights = [w_qkv] * 3
    else:
        picked = w_qkv.reshape(width, 3, parts, group)
        picked = lax.dynamic_index_in_dim(picked, x_at, 2, keepdims=False)
        weights = [picked.reshape(width, 3 * group)]

    by_seq = swap_all(tokens, "z")
    by_seq, cosine, sine, seg_col, *grad_sent = lax.optimization_barrier(
        (by_seq, cosine, sine, seg_col, *grad_sent)
    )
    if parts == 2:
        rows = [by_seq, lax.ppermute(by_seq, "x", [(0, 1), (1, 0)])]
    else:
        rows = [lax.all_gather(by_seq, "x", axis=0, tiled=False)]
    *rows, grad_sent[0] = lax.optimization_barrier((*rows, grad_sent[0]))
    grad_came = [swap_all(grad_sent[0], ranks)]

    qkv, normed = project(rows, attn_scale, weights, group, cosine, sine, x_ref, parts)
    attended, lse = (attend if fused else plain_attend)(qkv, seg_row, seg_col)
    attended = after(attended, grad_came[0])
    attended = swap_all(attended.reshape(experts, span, group), ranks)
    attended, grad_sent[1] = lax.optimization_barrier((attended, grad_sent[1]))
    grad_came.append(swap_all(grad_sent[1], ranks))
    attended = attended.reshape(seqs, parts, span, group)

    hidden, branch_in = after_attention(flat_tokens, attended, w_out, ffn_scale)
    sent = [dispatch(branch_in, target_rows[0], experts, half)]
    shared_out, shared_back, hid, dg, du = feed_forward(
        after(branch_in, sent[0]), flat_cot, shared_gate, shared_up, shared_down
    )
    sent.append(dispatch(after(branch_in, shared_out), target_rows[1], experts, half))
    sent[0] = after(sent[0], grad_came[1], shared_out)
    received = [swap_all(value, ranks).reshape(-1, width) for value in sent]
    keep, give = shared_weight_grads(branch_in, flat_cot, dg, du, hid, sizes, core_ref)
    shared_sums, _ = fold(both(keep, give), "y")

    router = jnp.pad(w_router, ((0, 0), (0, 128 - experts)))
    made, back_rows, halves = None, [], []
    before = (give, sent[1])
    for at in range(2):
        grad_rows = grad_came[at][:, :half, :].reshape(-1, width)
        other = grad_came[at][:, half, :half].astype(jnp.int32).reshape(-1, 1)
        rows_at = after(received[at], grad_rows, other, *before)
        made, back, hid, dg, du, gated_grads, grad_logits = feed_forward(
            rows_at, grad_rows, expert_gate[0], expert_up[0], expert_down[0], router, other, own,
            experts, at, made,
        )
        back_rows.append(swap_all(back.reshape(experts, half, width), ranks).reshape(-1, width))
        halves.append((rows_at, gated_grads, dg, du, hid, grad_logits))
        before = (back,)
    halves[1] = (after(halves[1][0], back_rows[0]), *halves[1][1:])
    keep, give, grad_router = expert_weight_grads(halves, sizes, pair_ref)
    back_rows[1] = after(back_rows[1], give)
    expert_sums, expert_sent = fold(both(keep, give), "y", ordered=True)
    expert_got = expert_sums[-1]

    grad_hidden, grad_attn, grad_att, grad_ffn = middle_back(
        hidden, shared_back, back_rows, target, flat_cot, ffn_scale, w_out, parts, span
    )
    grad_att = swap_all(grad_att.reshape(experts, span, group), ranks).reshape(length, group)

    column = lax.broadcasted_iota(jnp.int32, (width, 128), 1)
    small = jnp.where(column < experts, grad_router, jnp.where(column == experts, grad_ffn, 0.0))
    out_sums = tall_weight_grads(
        [attended[:, part].reshape(count, group) for part in range(parts)],
        [grad_attn],
        [small],
        sizes,
        core_ref,
        WEIGHT,
    )
    out_sums = both(*out_sums)

    shared_sums, shared_sent = fold([after(term, out_sums[0]) for term in shared_sums], "x")
    made = after(made, grad_att, out_sums[0], shared_sent)
    grad_att = after(grad_att, expert_sent)
    made_rows = swap_all(made, ranks).reshape(-1, width)
    grads = list(
        (attend_back if fused else plain_attend_back)(
            qkv, grad_att, lse, seg_row, seg_col, cosine, sine
        )
    )
    normed_back, grad_gain = project_back(grads, weights, rows, x_ref, parts)
    normed_back, _ = fold([normed_back], "x")
    shared_sums = total(shared_sums).astype(BF)
    pieces = swap_by_steps(after(total(normed_back).astype(BF), made_rows), "z")

    qkv_sums = tall_weight_grads([normed], list(grads), [grad_gain], sizes, core_ref, 0.2)
    last = [jnp.concatenate(pair, axis=-1) for pair in zip(out_sums, both(*qkv_sums))]
    last, _ = fold(last, "y", expert_got)

    shared_sums = swap_by_steps(after(shared_sums, *pieces), "z")
    last = after(total(last).astype(BF), made_rows)
    each, cols = last.shape[-2:]
    expert_out = [total([term[index] for term in expert_sums]) for index in range(3)]
    expert_out = [expert_out[0][None], expert_out[1][None], jnp.transpose(expert_out[2])[None]]
    layer_out = layer_end(hidden, shared_out, [made_rows], whole_target).reshape(tokens.shape)
    token_grad = first_norm_back(
        flat_tokens, attn_scale, pieces, after(grad_hidden, layer_out), z_ref
    )
    last = swap_all(last.reshape(experts, each, cols), ranks).astype(F32)
    last = jnp.sum(last.reshape(blocks, parts, each, cols), axis=0)
    out_sums = jnp.sum(last[:, :, : width + 128], axis=0)
    qkv_sums = last[:, :, width + 128 :]
    grad_attn_gain = jnp.sum(qkv_sums[:, :, 3 * group], axis=0)
    grad_w_qkv = qkv_sums[:, :, : 3 * group].reshape(parts, each, 3, group)
    grad_w_qkv = jnp.transpose(grad_w_qkv, (1, 2, 0, 3)).reshape(each, 3 * width)

    first, *shared_sums = shared_sums
    shared_sums = total([after(first, token_grad, *expert_out), *shared_sums])
    return (
        layer_out,
        token_grad.reshape(tokens.shape),
        grad_attn_gain,
        grad_w_qkv,
        out_sums[:, :width],
        out_sums[:, width + experts],
        out_sums[:, width : width + experts],
        shared_sums[0],
        shared_sums[1],
        jnp.transpose(shared_sums[2]),
        *expert_out,
    )


def solution(mesh):
    dp, experts = mesh.shape["dp"], mesh.shape["expert"]

    def step(*args):
        seqs = args[0].shape[0] // dp
        cores = 2 if dp % 2 == 0 else 1
        fine = Mesh(
            mesh.devices.reshape(dp // cores, cores, seqs, experts // seqs),
            ("y", "core", "z", "x"),
        )
        data, ranks, every = ("y", "core"), ("z", "x"), ("y", "core", "z", "x")
        placed = (
            P(data, ranks, None),
            P(data, None),
            P(data, ranks, None),
            P(data, ranks, None),
            P(data, ranks, None),
            *([P()] * 8),
            P(ranks, None, None),
            P(ranks, None, None),
            P(ranks, None, None),
        )
        return jax.shard_map(
            on_device,
            mesh=fine,
            in_specs=placed,
            out_specs=(
                P(data, ranks, None),
                P(data, ranks, None),
                P(every),
                P(every, None),
                P(every, None),
                P(every),
                P(every, None),
                P(every, None),
                P(every, None),
                P(None, every),
                P(ranks, None, data),
                P(ranks, None, data),
                P(ranks, data, None),
            ),
            check_vma=False,
        )(*args)

    return step
```

```python
import jax
import jax.numpy as jnp
from jax import lax
from jax.experimental import pallas as pl
from jax.experimental.pallas import tpu as pltpu
from jax.sharding import Mesh
from jax.sharding import PartitionSpec as P

HEAD_DIM = 64
EPS = 1e-06
BF = jnp.bfloat16
F32 = jnp.float32
NEG = -1e30
NN = (((1,), (0,)), ((), ()))
NT = (((1,), (1,)), ((), ()))
TN = (((0,), (0,)), ((), ()))
VMEM_MOST = 60 << 20
WEIGHT = 8


def mm(left, right, dims=NN):
    return lax.dot_general(left, right, dims, preferred_element_type=F32)


def sds(shape, dtype):
    return jax.ShapeDtypeStruct(shape, dtype)


def call(
    body, grid, in_specs, out_specs, out_shape, args, scratch=(), prefetch=0, flops=0, alias=None
):
    leaves = jax.tree.leaves(out_shape)
    moved = sum(a.size * a.dtype.itemsize for a in args) + sum(
        a.size * a.dtype.itemsize for a in leaves
    )
    return pl.pallas_call(
        body,
        out_shape=out_shape,
        grid_spec=pltpu.PrefetchScalarGridSpec(
            num_scalar_prefetch=prefetch,
            grid=grid,
            in_specs=in_specs,
            out_specs=out_specs,
            scratch_shapes=list(scratch),
        ),
        compiler_params=pltpu.CompilerParams(
            dimension_semantics=("arbitrary",) * len(grid), vmem_limit_bytes=VMEM_MOST
        ),
        cost_estimate=pl.CostEstimate(
            flops=int(flops), transcendentals=0, bytes_accessed=int(moved)
        ),
        input_output_aliases=alias or {},
    )(*args)


def whole(shape):
    rank = len(shape)
    return pl.BlockSpec(tuple(shape), lambda *_: (0,) * rank)


def swap_halves(value):
    lane = lax.broadcasted_iota(jnp.int32, value.shape, 1)
    return jnp.where(lane % 64 < 32, pltpu.roll(value, 96, 1), pltpu.roll(value, 32, 1))


def rms(values):
    return lax.rsqrt(jnp.mean(values * values, axis=1, keepdims=True) + EPS)


def row_specs(rows):
    if len(rows) == 2:
        _, span, width = rows[0].shape
        return [pl.BlockSpec((1, span, width), lambda i, *_: (i, 0, 0))] * 2
    parts, _, span, width = rows[0].shape
    return [pl.BlockSpec((parts, 1, span, width), lambda i, *_: (0, i, 0, 0))]


def load_rows(refs, at_ref):
    if len(refs) == 2:
        mine, theirs = refs[0][0].astype(F32), refs[1][0].astype(F32)
        first = at_ref[0] == 0
        pair = [jnp.where(first, mine, theirs), jnp.where(first, theirs, mine)]
        return jnp.concatenate(pair, axis=0)
    value = refs[0][...]
    return value.reshape(value.shape[0] * value.shape[2], value.shape[3]).astype(F32)


def weight_specs(weights, group):
    if len(weights) == 1:
        return [whole(weights[0].shape)]
    width, cols = weights[0].shape
    parts = cols // (3 * group)

    def spec(index):
        return pl.BlockSpec((width, group), lambda i, at: (0, index * parts + at[0]))

    return [spec(index) for index in range(3)]


def load_weights(refs, group):
    if len(refs) == 3:
        return [ref[...] for ref in refs]
    return [refs[0][:, at * group : (at + 1) * group] for at in range(3)]


def project(rows, gain, weights, group, cosine, sine, x_at, parts):
    blocks, span, width = rows[0].shape[-3:]
    height = parts * span
    length = height * blocks
    cut = len(rows)

    def body(at_ref, *refs):
        r_refs, (g_ref, c_ref, s_ref) = refs[:cut], refs[cut : cut + 3]
        w_refs, (qkv_ref, n_ref) = refs[cut + 3 : -2], refs[-2:]
        tok = load_rows(r_refs, at_ref)
        normed = (tok * rms(tok) * g_ref[...]).astype(BF)
        n_ref[...] = normed
        if len(w_refs) == 3:
            found = [mm(normed, ref[...]) for ref in w_refs]
            turning = [(found[0], 0), (found[1], group)]
            last = found[2]
        else:
            found = mm(normed, w_refs[0][...])
            turning, last = [(found[:, : 2 * group], 0)], found[:, 2 * group :]
        for value, base in turning:
            for at in range(0, value.shape[1], 128):
                part = value[:, at : at + 128]
                lane = lax.broadcasted_iota(jnp.int32, part.shape, 1) + (base + at)
                turned = part * c_ref[...] + swap_halves(part) * s_ref[...]
                turned = turned * jnp.where(lane < group, HEAD_DIM**-0.5, 1.0)
                qkv_ref[:, base + at : base + at + 128] = turned.astype(BF)
        qkv_ref[:, 2 * group :] = last.astype(BF)

    return call(
        body,
        (blocks,),
        [
            *row_specs(rows),
            whole((1, width)),
            pl.BlockSpec((height, 128), lambda i, *_: (i, 0)),
            pl.BlockSpec((height, 128), lambda i, *_: (i, 0)),
            *weight_specs(weights, group),
        ],
        [
            pl.BlockSpec((height, 3 * group), lambda i, *_: (i, 0)),
            pl.BlockSpec((height, width), lambda i, *_: (i, 0)),
        ],
        [sds((length, 3 * group), BF), sds((length, width), BF)],
        (x_at, *rows, gain, cosine, sine, *weights),
        prefetch=1,
        flops=6 * length * width * group,
    )


def project_back(grads, weights, rows, x_at, parts):
    blocks, span, width = rows[0].shape[-3:]
    group = grads[0].shape[1]
    height = parts * span
    length = height * blocks
    cut = len(rows)

    def body(at_ref, q_ref, k_ref, v_ref, *refs):
        r_refs, w_refs, (out_ref, gain_ref, acc_ref) = refs[:cut], refs[cut:-3], refs[-3:]
        step = pl.program_id(0)
        w_q, w_k, w_v = load_weights(w_refs, group)
        back = mm(q_ref[...], w_q, NT) + mm(k_ref[...], w_k, NT) + mm(v_ref[...], w_v, NT)
        tok = load_rows(r_refs, at_ref)
        part = jnp.sum(back * tok * rms(tok), axis=0, keepdims=True)

        @pl.when(step == 0)
        def _():
            acc_ref[...] = jnp.zeros_like(acc_ref)

        acc_ref[...] += jnp.broadcast_to(part, acc_ref.shape)
        out_ref[...] = back.astype(BF).reshape(parts, 1, span, width)

        @pl.when(step == blocks - 1)
        def _():
            column = jnp.transpose(acc_ref[...])
            gain_ref[...] = jnp.broadcast_to(column[:, :1], gain_ref.shape)

    block = pl.BlockSpec((height, group), lambda i, *_: (i, 0))
    return call(
        body,
        (blocks,),
        [block, block, block, *row_specs(rows), *weight_specs(weights, group)],
        [
            pl.BlockSpec((parts, 1, span, width), lambda i, *_: (0, i, 0, 0)),
            whole((width, 128)),
        ],
        [sds((parts, blocks, span, width), BF), sds((width, 128), F32)],
        (x_at, *grads, *rows, *weights),
        scratch=[pltpu.VMEM((8, width), F32)],
        prefetch=1,
        flops=0.2 * length * width * group,
    )


def attend(qkv, seg_row, seg_col):
    length, cols = qkv.shape
    group = cols // 3
    pairs = group // 128
    high = min(256, length)

    def body(q_ref, k_ref, v_ref, sr_ref, sc_ref, o_ref, l_ref):
        lane = lax.broadcasted_iota(jnp.int32, (high, 128), 1)
        for at in range(0, length, high):
            end = at + high
            query = q_ref[at:end, :]
            keys = k_ref[:end, :]
            vals = v_ref[:end, :]
            q_pos = lax.broadcasted_iota(jnp.int32, (high, end), 0) + at
            k_pos = lax.broadcasted_iota(jnp.int32, (high, end), 1)
            allowed = (sc_ref[at:end, :] == sr_ref[:, :end]) & (k_pos <= q_pos)
            outs = []
            for head in range(2):
                mine = (lane // 64) == head
                scores = mm(jnp.where(mine, query, jnp.zeros_like(query)), keys, NT)
                scores = jnp.where(allowed, scores, NEG)
                most = jnp.max(scores, axis=1, keepdims=True)
                expo = jnp.exp(scores - most)
                total = jnp.sum(expo, axis=1, keepdims=True)
                outs.append(mm(expo.astype(BF), vals) / total)
                lse = jnp.broadcast_to(most + jnp.log(total), (high, 128))
                l_ref[0, head : head + 1, at:end] = jnp.transpose(lse)[:1, :]
            o_ref[at:end, :] = jnp.where(lane < 64, outs[0], outs[1]).astype(BF)

    def col(offset):
        return pl.BlockSpec((length, 128), lambda i: (0, offset * pairs + i))

    return call(
        body,
        (pairs,),
        [col(0), col(1), col(2), whole((1, length)), whole((length, 1))],
        [col(0), pl.BlockSpec((1, 2, length), lambda i: (i, 0, 0))],
        [sds((length, group), BF), sds((pairs, 2, length), F32)],
        (qkv, qkv, qkv, seg_row, seg_col),
        flops=4 * length * length * group,
    )


def attend_back(qkv, grad, lse, seg_row, seg_col, cosine, sine):
    length, cols = qkv.shape
    group = cols // 3
    pairs = group // 128
    high = min(256, length)

    def body(
        q_ref, k_ref, v_ref, g_ref, l_ref, sr_ref, sc_ref, c_ref, s_ref, dq_ref, dk_ref, dv_ref,
        ka_ref, va_ref,
    ):
        lane = lax.broadcasted_iota(jnp.int32, (high, 128), 1)
        ka_ref[...] = jnp.zeros_like(ka_ref)
        va_ref[...] = jnp.zeros_like(va_ref)
        for at in range(0, length, high):
            end = at + high
            query = q_ref[at:end, :]
            grads = g_ref[at:end, :]
            keys = k_ref[:end, :]
            vals = v_ref[:end, :]
            k_pos = lax.broadcasted_iota(jnp.int32, (end, high), 0)
            q_pos = lax.broadcasted_iota(jnp.int32, (end, high), 1) + at
            allowed = (sc_ref[:end, :] == sr_ref[:, at:end]) & (k_pos <= q_pos)
            outs = []
            for head in range(2):
                mine = (lane // 64) == head
                q_own = jnp.where(mine, query, jnp.zeros_like(query))
                g_own = jnp.where(mine, grads, jnp.zeros_like(grads))
                scores = jnp.where(allowed, mm(keys, q_own, NT), NEG)
                probs = jnp.exp(scores - l_ref[0, head : head + 1, at:end])
                grad_probs = mm(vals, g_own, NT)
                delta = jnp.sum(probs * grad_probs, axis=0, keepdims=True)
                grad_scores = (probs * (grad_probs - delta)).astype(BF)
                va_ref[:end, :] += mm(probs.astype(BF), g_own)
                ka_ref[:end, :] += mm(grad_scores, q_own)
                outs.append(mm(grad_scores, keys, TN))
            found = jnp.where(lane < 64, outs[0], outs[1]) * HEAD_DIM**-0.5
            back = found * c_ref[at:end, :] - swap_halves(found) * s_ref[at:end, :]
            dq_ref[at:end, :] = back.astype(BF)
        found = ka_ref[...]
        dk_ref[...] = (found * c_ref[...] - swap_halves(found) * s_ref[...]).astype(BF)
        dv_ref[...] = va_ref[...].astype(BF)

    def col(offset):
        return pl.BlockSpec((length, 128), lambda i: (0, offset * pairs + i))

    return call(
        body,
        (pairs,),
        [
            col(0),
            col(1),
            col(2),
            col(0),
            pl.BlockSpec((1, 2, length), lambda i: (i, 0, 0)),
            whole((1, length)),
            whole((length, 1)),
            whole((length, 128)),
            whole((length, 128)),
        ],
        [col(0), col(0), col(0)],
        [sds((length, group), BF)] * 3,
        (qkv, qkv, qkv, grad, lse, seg_row, seg_col, cosine, sine),
        scratch=[pltpu.VMEM((length, 128), F32)] * 2,
        flops=length * length * group,
    )


def heads_of(flat):
    return flat.reshape(flat.shape[0], -1, HEAD_DIM)


def plain_mask(seg_row, seg_col):
    length = seg_col.shape[0]
    spots = jnp.arange(length, dtype=jnp.int32)
    return (seg_row == seg_col) & (spots[None, :] <= spots[:, None])


def plain_attend(qkv, seg_row, seg_col):
    query, keys, vals = (heads_of(part) for part in jnp.split(qkv, 3, axis=1))
    scores = jnp.einsum("qhd,khd->hqk", query, keys, preferred_element_type=F32)
    scores = jnp.where(plain_mask(seg_row, seg_col)[None], scores, NEG)
    lse = jax.nn.logsumexp(scores, axis=-1, keepdims=True)
    probs = jnp.exp(scores - lse).astype(BF)
    found = jnp.einsum("hqk,khd->qhd", probs, vals, preferred_element_type=F32)
    return found.astype(BF).reshape(qkv.shape[0], -1), lse


def plain_turn_back(grads, cosine, sine):
    table_c, table_s = cosine[:, None, :HEAD_DIM], sine[:, None, :HEAD_DIM]
    swapped = jnp.roll(grads, HEAD_DIM // 2, axis=-1)
    return (grads * table_c - swapped * table_s).astype(BF).reshape(grads.shape[0], -1)


def plain_attend_back(qkv, grad, lse, seg_row, seg_col, cosine, sine):
    query, keys, vals = (heads_of(part) for part in jnp.split(qkv, 3, axis=1))
    grad = heads_of(grad)
    scores = jnp.einsum("qhd,khd->hqk", query, keys, preferred_element_type=F32)
    scores = jnp.where(plain_mask(seg_row, seg_col)[None], scores, NEG)
    probs = jnp.exp(scores - lse)
    grad_probs = jnp.einsum("qhd,khd->hqk", grad, vals, preferred_element_type=F32)
    delta = jnp.sum(probs * grad_probs, axis=-1, keepdims=True)
    grad_scores = (probs * (grad_probs - delta)).astype(BF)
    gq = jnp.einsum("hqk,khd->qhd", grad_scores, keys, preferred_element_type=F32)
    gk = jnp.einsum("hqk,qhd->khd", grad_scores, query, preferred_element_type=F32)
    gv = jnp.einsum("hqk,qhd->khd", probs.astype(BF), grad, preferred_element_type=F32)
    return (
        plain_turn_back(gq * HEAD_DIM**-0.5, cosine, sine),
        plain_turn_back(gk, cosine, sine),
        gv.astype(BF).reshape(qkv.shape[0], -1),
    )


def after_attention(tokens, attended, w_out, gain):
    seqs, parts, span, group = attended.shape
    count, width = tokens.shape

    def body(t_ref, a_ref, w_ref, g_ref, h_ref, b_ref):
        hidden = t_ref[...].astype(F32)
        for part in range(parts):
            rows = a_ref[:, part].reshape(count, group)
            hidden += mm(rows, w_ref[part * group : (part + 1) * group, :])
        h_ref[...] = hidden
        b_ref[...] = (hidden * rms(hidden) * g_ref[...]).astype(BF)

    return call(
        body,
        (1,),
        [whole(a.shape) for a in (tokens, attended, w_out, gain)],
        [whole(tokens.shape)] * 2,
        [sds(tokens.shape, F32), sds(tokens.shape, BF)],
        (tokens, attended, w_out, gain),
        flops=2 * count * width * width,
    )


def dispatch(rows, target_rows, experts, capacity, route_rows=None):
    count, width = rows.shape
    more = 0 if route_rows is None else 16
    tables = () if route_rows is None else (route_rows,)

    def body(r_ref, t_ref, *refs):
        o_ref = refs[-1]
        slot = lax.broadcasted_iota(jnp.int32, (capacity, count), 0)
        slot += pl.program_id(0) * capacity
        hits = [slot == t_ref[k : k + 1, :] for k in range(2)]
        hot = (hits[0] | hits[1]).astype(F32).astype(BF)
        o_ref[0, :capacity, :] = mm(hot, r_ref[...]).astype(BF)
        if more:
            o_ref[0, capacity:, :] = jnp.zeros((more, width), BF)
            other = jnp.zeros((8, capacity), F32)
            for k in range(2):
                route = jnp.broadcast_to(refs[0][1 - k : 2 - k, :].astype(F32), (8, count))
                other += mm(route.astype(BF), hits[k].astype(F32).astype(BF), NT)
            o_ref[0, capacity : capacity + 8, :capacity] = other.astype(BF)

    return call(
        body,
        (experts,),
        [whole(a.shape) for a in (rows, target_rows, *tables)],
        pl.BlockSpec((1, capacity + more, width), lambda i: (i, 0, 0)),
        sds((experts, capacity + more, width), BF),
        (rows, target_rows, *tables),
        flops=2 * experts * capacity * count * width,
    )


def pick(target, row_refs):
    total = None
    for index, ref in enumerate(row_refs):
        rows = ref[...]
        spot = lax.broadcasted_iota(jnp.int32, (target.shape[0], rows.shape[0]), 1)
        one, two = target[:, 2 * index : 2 * index + 1], target[:, 2 * index + 1 : 2 * index + 2]
        found = mm(((spot == one) | (spot == two)).astype(F32).astype(BF), rows)
        total = found if total is None else total + found
    return total


def layer_end(hidden, shared_out, rows, target):
    count, width = hidden.shape
    high = count // 2

    def body(h_ref, s_ref, t_ref, *refs):
        refs[-1][...] = (h_ref[...] + s_ref[...] + pick(t_ref[...], refs[:-1])).astype(BF)

    block = pl.BlockSpec((high, width), lambda i: (i, 0))
    return call(
        body,
        (2,),
        [
            block,
            block,
            pl.BlockSpec((high, target.shape[1]), lambda i: (i, 0)),
            *[whole(part.shape) for part in rows],
        ],
        block,
        sds(hidden.shape, BF),
        (hidden, shared_out, target, *rows),
        flops=2 * count * width * rows[0].shape[0] * len(rows),
    )


def middle_back(hidden, grad_shared, rows, target, cotangent, gain, w_out, parts, span):
    count, width = hidden.shape
    seqs = count // span
    each = 2 if seqs % 2 == 0 else 1
    high = each * span
    steps = count // high
    group = width // parts

    def body(h_ref, s_ref, t_ref, c_ref, g_ref, w_ref, *refs):
        gh_ref, ga_ref, d_ref, n_ref, acc_ref = refs[len(rows) :]
        step = pl.program_id(0)
        branch = s_ref[...] + pick(t_ref[...], refs[: len(rows)])
        hidden = h_ref[...]
        scale = rms(hidden)
        weighted = branch * g_ref[...]
        inner = jnp.mean(weighted * hidden, axis=1, keepdims=True)
        part = jnp.sum(branch * hidden * scale, axis=0, keepdims=True)
        out = c_ref[...].astype(F32) + scale * weighted - hidden * (scale * scale * scale * inner)
        gh_ref[...] = out
        out = out.astype(BF)
        ga_ref[...] = out
        for at in range(parts):
            sent = mm(out, w_ref[at * group : (at + 1) * group, :], NT).astype(BF)
            d_ref[:, at] = sent.reshape(each, span, group)

        @pl.when(step == 0)
        def _():
            acc_ref[...] = jnp.zeros_like(acc_ref)

        acc_ref[...] += jnp.broadcast_to(part, acc_ref.shape)

        @pl.when(step == steps - 1)
        def _():
            column = jnp.transpose(acc_ref[...])
            n_ref[...] = jnp.broadcast_to(column[:, :1], n_ref.shape)

    block = pl.BlockSpec((high, width), lambda i: (i, 0))
    return call(
        body,
        (steps,),
        [
            block,
            block,
            pl.BlockSpec((high, target.shape[1]), lambda i: (i, 0)),
            block,
            whole(gain.shape),
            whole(w_out.shape),
            *[whole(part.shape) for part in rows],
        ],
        [
            block,
            block,
            pl.BlockSpec((each, parts, span, group), lambda i: (i, 0, 0, 0)),
            whole((width, 128)),
        ],
        [
            sds(hidden.shape, F32),
            sds(hidden.shape, BF),
            sds((seqs, parts, span, group), BF),
            sds((width, 128), F32),
        ],
        (hidden, grad_shared, target, cotangent, gain, w_out, *rows),
        scratch=[pltpu.VMEM((8, width), F32)],
        flops=WEIGHT * 2 * count * width * (rows[0].shape[0] * len(rows) + width),
    )


def first_norm_back(tokens, gain, pieces, grad_hidden, z_at):
    count, width = tokens.shape
    blocks = len(pieces)
    span = count // blocks

    def body(at_ref, t_ref, g_ref, h_ref, *refs):
        o_ref = refs[-1]
        for index in range(blocks):
            seq = (at_ref[0] + blocks - index) % blocks
            spot = pl.ds(pl.multiple_of(seq * span, span), span)
            tok = t_ref[spot, :].astype(F32)
            scale = rms(tok)
            weighted = refs[index][...].astype(F32) * g_ref[...]
            inner = jnp.mean(weighted * tok, axis=1, keepdims=True)
            out = h_ref[spot, :] + scale * weighted - tok * (scale * scale * scale * inner)
            o_ref[spot, :] = out.astype(BF)

    return call(
        body,
        (1,),
        [whole(a.shape) for a in (tokens, gain, grad_hidden, *pieces)],
        whole(tokens.shape),
        sds(tokens.shape, BF),
        (z_at, tokens, gain, grad_hidden, *pieces),
        prefetch=1,
    )


def feed_forward(
    rows, grads, w_gate, w_up, w_down, router=None, other=None, own=None, experts=0, place=0, made=None
):
    count, width = rows.shape
    units = w_gate.shape[1]
    wide = 512
    steps = units // wide
    high = 256
    gated = router is not None
    more = 0 if made is None else 1
    kind = BF if gated else F32

    def body(*refs):
        if gated:
            (own_ref, x_ref, g_ref, wg_ref, wu_ref, wd_ref, wr_ref, ot_ref) = refs[:8]
            (y_ref, gi_ref, hid_ref, dg_ref, du_ref, eo_ref, gl_ref, ya_ref, ga_ref, gate_ref) = refs[8 + more :]
        else:
            (x_ref, g_ref, wg_ref, wu_ref, wd_ref,
             y_ref, gi_ref, hid_ref, dg_ref, du_ref, ya_ref, ga_ref) = refs
        step = pl.program_id(0)

        if gated:

            @pl.when(step == 0)
            def _():
                logits = mm(x_ref[...], wr_ref[...])
                lane = lax.broadcasted_iota(jnp.int32, logits.shape, 1)
                mine = jnp.sum(jnp.where(lane == own_ref[0], logits, 0.0), axis=1, keepdims=True)
                theirs = jnp.sum(jnp.where(lane == ot_ref[...], logits, 0.0), axis=1, keepdims=True)
                gate = 1.0 / (1.0 + jnp.exp(theirs - mine))
                rest = 1.0 / (1.0 + jnp.exp(mine - theirs))
                gate_ref[:, 0:1] = gate
                gate_ref[:, 1:2] = rest
                eo_ref[...] = (g_ref[...].astype(F32) * gate).astype(BF)

        def rows_at(index, carry):
            at = pl.ds(pl.multiple_of(index * high, high), high)
            row = x_ref[at, :]
            grad = eo_ref[at, :] if gated else g_ref[at, :]
            gval = mm(row, wg_ref[...])
            uval = mm(row, wu_ref[...])
            sigma = 1.0 / (1.0 + jnp.exp(-gval))
            silu = gval * sigma
            hid = (silu * uval).astype(BF)
            hid_ref[at, :] = hid
            grad_hid = mm(grad, wd_ref[...], NT)
            du = (grad_hid * silu).astype(BF)
            dg = (grad_hid * uval * sigma * (1.0 + gval * (1.0 - sigma))).astype(BF)
            du_ref[at, :] = du
            dg_ref[at, :] = dg
            out = mm(hid, wd_ref[...])
            back = mm(dg, wg_ref[...], NT) + mm(du, wu_ref[...], NT)

            @pl.when(step == 0)
            def _():
                ya_ref[at, :] = out
                ga_ref[at, :] = back

            @pl.when(step > 0)
            def _():
                ya_ref[at, :] += out
                ga_ref[at, :] += back

            return carry

        lax.fori_loop(0, count // high, rows_at, 0)

        @pl.when(step == steps - 1)
        def _():
            if gated:
                out = ya_ref[...]
                gate = gate_ref[:, 0:1]
                lean = jnp.sum(out * g_ref[...].astype(F32), axis=1, keepdims=True)
                lean = lean * gate * gate_ref[:, 1:2]
                lane = lax.broadcasted_iota(jnp.int32, (count, 128), 1)
                sign = (lane == own_ref[0]).astype(F32) - (lane == ot_ref[...]).astype(F32)
                grad_logits = (lean * sign).astype(BF)
                gl_ref[...] = grad_logits
                y_ref[...] = (out * gate).astype(BF).reshape(y_ref.shape)
                gi_ref[...] = (ga_ref[...] + mm(grad_logits, wr_ref[...], NT)).astype(BF)
            else:
                y_ref[...] = ya_ref[...]
                gi_ref[...] = ga_ref[...]

    full = whole((count, width))
    hidden = pl.BlockSpec((count, wide), lambda i, *_: (0, i))
    in_specs = [
        full,
        full,
        pl.BlockSpec((width, wide), lambda i, *_: (0, i)),
        pl.BlockSpec((width, wide), lambda i, *_: (0, i)),
        pl.BlockSpec((wide, width), lambda i, *_: (i, 0)),
    ]
    out_specs = [full, full, hidden, hidden, hidden]
    out_shape = [sds((count, width), kind)] * 2 + [sds((count, units), BF)] * 3
    scratch = [pltpu.VMEM((count, width), F32)] * 2
    args = [rows, grads, w_gate, w_up, w_down]
    if gated:
        in_specs += [whole(router.shape), whole(other.shape)]
        out_specs += [full, whole((count, 128))]
        out_shape += [sds((count, width), BF), sds((count, 128), BF)]
        scratch += [pltpu.VMEM((count, 128), F32)]
        args = [own, *args, router, other]
        out_specs[0] = pl.BlockSpec((experts, count // experts, width), lambda *_: (0, place, 0))
        out_shape[0] = sds((experts, 2 * count // experts, width), BF)
        if more:
            in_specs += [pl.BlockSpec(memory_space=pl.ANY)]
            args += [made]
    return call(
        body,
        (steps,),
        in_specs,
        out_specs,
        out_shape,
        tuple(args),
        scratch=scratch,
        prefetch=1 if gated else 0,
        alias={len(args) - 1: 0} if more else None,
        flops=12 * count * width * units,
    )


def expert_weight_grads(halves, sizes, core_at):
    outer, cores = sizes["y"], sizes["core"]
    count, width = halves[0][0].shape
    units = halves[0][2].shape[1]
    wide = units // (outer * cores)

    def body(at_ref, *refs):
        keep_ref, give_ref, r_ref = refs[-3:]
        groups = [refs[6 * at : 6 * at + 6] for at in range(len(halves))]
        step = pl.program_id(0)

        def over(left, right):
            return sum(mm(group[left][...], group[right][...], TN) for group in groups)

        found = [over(0, 2).astype(BF), over(0, 3).astype(BF), over(1, 4).astype(BF)]

        @pl.when(step < outer)
        def _():
            for index in range(3):
                give_ref[0, index] = found[index]

        @pl.when(step >= outer)
        def _():
            for index in range(3):
                keep_ref[0, index] = found[index]

        @pl.when(step == 0)
        def _():
            r_ref[...] = over(0, 5)

    def taken(i, at):
        core = jnp.where(i < outer, 1 - at[0], at[0])
        y = (i + 1 + at[1]) % outer if outer == 2 else i % outer
        return (0, y * cores + core)

    hidden = pl.BlockSpec((count, wide), taken)
    part = (1, 3, width, wide)
    return call(
        body,
        (outer * cores,),
        [
            whole((count, width)),
            whole((count, width)),
            hidden,
            hidden,
            hidden,
            whole((count, 128)),
        ]
        * len(halves),
        [
            pl.BlockSpec(part, lambda i, *_: (jnp.maximum(i - outer, 0), 0, 0, 0)),
            pl.BlockSpec(part, lambda i, *_: (jnp.minimum(i, outer - 1), 0, 0, 0)),
            whole((width, 128)),
        ],
        [sds((outer, *part[1:]), BF)] * 2 + [sds((width, 128), F32)],
        (core_at, *[value for half in halves for value in half]),
        prefetch=1,
        flops=6 * count * len(halves) * width * units,
    )


def spread_places(sizes, names):
    found = []
    for y in range(sizes["y"]):
        for core in range(sizes["core"]):
            for z in range(sizes["z"]):
                for x in range(sizes["x"]):
                    at = {"y": y, "core": core, "z": z, "x": x}
                    found.append((core, tuple(at[n] for n in names)))
    return found


def spread(value, sizes, names, core_at):
    order = ("y", "core", "z", "x")
    split = value.reshape(*(sizes[n] for n in order), -1, value.shape[-1])
    split = jnp.transpose(split, (1, *(order.index(n) for n in names), 4, 5))
    return at_index(split, core_at[0]), at_index(split, 1 - core_at[0])


def store_spread(places, each, core_at, found, row, keep, give):
    first = row // each
    for core in range(2):
        todo = [at for at in range(found.shape[0] // each) if places[first + at][0] == core]

        def put(store, todo=todo):
            for at in todo:
                store(places[first + at][1], found[at * each : (at + 1) * each].astype(BF))

        pl.when(core_at == core)(lambda put=put: put(keep))
        pl.when(core_at != core)(lambda put=put: put(give))


def shared_weight_grads(rows, grads, dg, du, hid, sizes, core_at):
    names = ("y", "x", "z")
    lead = tuple(sizes[n] for n in names)
    places = spread_places(sizes, names)
    count, width = rows.shape
    units = dg.shape[1]
    wide = 512
    each = width // len(places)
    direct = each % 8 == 0

    def body(at_ref, x_ref, g_ref, dg_ref, du_ref, hid_ref, *outs):
        pairs = ((x_ref, dg_ref), (x_ref, du_ref), (g_ref, hid_ref))
        for index, (left, right) in enumerate(pairs):
            found = mm(left[...], right[...], TN)
            if not direct:
                outs[0][index] = found.astype(BF)
                continue

            def into(ref, index=index):
                def store(place, piece):
                    ref[(*place, index)] = piece

                return store

            store_spread(places, each, at_ref[0], found, 0, into(outs[0]), into(outs[1]))

    hidden = pl.BlockSpec((count, wide), lambda i, *_: (0, i))
    if direct:
        shapes = [(*lead, 3, each, units)] * 2
        spec = [pl.BlockSpec((*lead, 3, each, wide), lambda i, *_: (0,) * 5 + (i,))] * 2
    else:
        shapes = [(3, width, units)]
        spec = [pl.BlockSpec((3, width, wide), lambda i, *_: (0, 0, i))]
    out = call(
        body,
        (units // wide,),
        [whole(rows.shape), whole(grads.shape), hidden, hidden, hidden],
        spec,
        [sds(shape, BF) for shape in shapes],
        (core_at, rows, grads, dg, du, hid),
        prefetch=1,
        flops=6 * count * width * units,
    )
    if direct:
        return out
    found = [spread(out[0][i], sizes, names, core_at) for i in range(3)]
    return [jnp.stack([part[side] for part in found], axis=3) for side in range(2)]


def tall_weight_grads(lefts, rights, extras, sizes, core_at, weight=1):
    names = ("y", "z", "x")
    lead = tuple(sizes[n] for n in names)
    places = spread_places(sizes, names)
    width = sum(left.shape[1] for left in lefts)
    cols = sum(right.shape[1] for right in rights)
    each = width // len(places)
    direct = each % 8 == 0
    flops = weight * 2 * lefts[0].shape[0] * width * cols

    def body(at_ref, *refs):
        left_refs = refs[: len(lefts)]
        right_refs = refs[len(lefts) : len(lefts) + len(rights)]
        rest = refs[len(lefts) + len(rights) :]
        extra_refs, outs = rest[: len(extras)], rest[len(extras) :]

        def save(row, found, col):
            span = found.shape[1]
            if not direct:
                outs[0][row : row + found.shape[0], col : col + span] = found.astype(BF)
                return

            def into(ref):
                def store(place, piece):
                    ref[(*place, slice(None), slice(col, col + span))] = piece

                return store

            store_spread(places, each, at_ref[0], found, row, into(outs[0]), into(outs[1]))

        row = 0
        for left in left_refs:
            col = 0
            for right in right_refs:
                save(row, mm(left[...], right[...], TN), col)
                col += right.shape[1]
            row += left.shape[1]
        more = extra_refs[0][...]
        for extra in extra_refs[1:]:
            more = more + extra[...]
        save(0, more, cols)

    args = (*lefts, *rights, *extras)
    shapes = [(*lead, each, cols + 128)] * 2 if direct else [(width, cols + 128)]
    out = call(
        body,
        (1,),
        [whole(a.shape) for a in args],
        [whole(shape) for shape in shapes],
        [sds(shape, BF) for shape in shapes],
        (core_at, *args),
        prefetch=1,
        flops=flops,
    )
    return out if direct else spread(out[0], sizes, names, core_at)


def scatter_sum(value, name):
    return lax.psum_scatter(value, name, scatter_dimension=0, tiled=False)


def swap_all(value, names):
    return lax.all_to_all(value, names, 0, 0, tiled=True)


def at_index(value, index):
    if isinstance(index, int):
        return value[index]
    return lax.dynamic_index_in_dim(value, index, 0, keepdims=False)


def total(terms):
    return sum(term.astype(F32) for term in terms)


def both(keep, give):
    return [keep, lax.ppermute(give, "core", [(0, 1), (1, 0)])]


def fold(terms, name, *others, ordered=False):
    if lax.axis_size(name) != 2:
        sent = total(terms).astype(BF)
        if others:
            sent = after(sent, *others)
        return [scatter_sum(sent, name)], sent
    at = 1 if ordered else lax.axis_index(name)
    sent = total([at_index(term, 1 - at) for term in terms]).astype(BF)
    if others:
        sent = after(sent, *others)
    got = lax.ppermute(sent, name, [(0, 1), (1, 0)])
    return [at_index(term, at) for term in terms] + [got], sent


def swap_by_steps(value, name):
    size, at = value.shape[0], lax.axis_index(name)
    found = [at_index(value, at)]
    for step in range(1, size):
        sent = at_index(value, (at + step) % size)
        found.append(lax.ppermute(sent, name, [(i, (i + step) % size) for i in range(size)]))
    return found


def after(value, *others):
    return lax.optimization_barrier((value, *others))[0]


def on_device(
    tokens,
    segments,
    routes,
    slots,
    cotangent,
    attn_gain,
    w_qkv,
    w_out,
    ffn_gain,
    w_router,
    shared_gate,
    shared_up,
    shared_down,
    expert_gate,
    expert_up,
    expert_down,
):
    sizes = {name: lax.axis_size(name) for name in ("y", "core", "z", "x")}
    ranks = ("z", "x")
    seqs, span, width = tokens.shape
    blocks, parts = sizes["z"], sizes["x"]
    experts = blocks * parts
    count = seqs * span
    capacity = 3 * count // experts
    length = span * experts
    group = width // parts
    z_at, x_at = lax.axis_index("z"), lax.axis_index("x")
    own = (z_at * parts + x_at).astype(jnp.int32).reshape(1)
    z_ref, x_ref = z_at.astype(jnp.int32).reshape(1), x_at.astype(jnp.int32).reshape(1)
    core_ref = lax.axis_index("core").astype(jnp.int32).reshape(1)
    pair_ref = jnp.stack([lax.axis_index("core"), lax.axis_index("y")]).astype(jnp.int32)
    attn_scale = attn_gain.astype(F32).reshape(1, width)
    ffn_scale = ffn_gain.astype(F32).reshape(1, width)
    flat_tokens = tokens.reshape(count, width)
    flat_cot = cotangent.reshape(count, width)

    route_rows = routes.reshape(count, 2)
    slot_rows = slots.reshape(count, 2)
    half = capacity // 2
    targets = []
    for first in (0, half):
        here = (slot_rows >= first) & (slot_rows < first + half)
        targets.append(jnp.where(here, route_rows * half + slot_rows - first, -1))
    target_rows = [jnp.transpose(target) for target in targets]
    target = jnp.concatenate(targets, axis=1)
    whole_target = jnp.where(slot_rows >= 0, route_rows * capacity + slot_rows, -1)
    route_flat = jnp.transpose(route_rows)
    grad_sent = [dispatch(flat_cot, to, experts, half, route_flat) for to in target_rows]

    frequency = jnp.power(10000.0, -2.0 * jnp.arange(32, dtype=F32) / HEAD_DIM)
    angles = jnp.arange(length, dtype=jnp.int32).astype(F32)[:, None] * jnp.tile(frequency, 4)
    sign = jnp.where(jnp.arange(128) % 64 < 32, -1.0, 1.0)
    cosine, sine = jnp.cos(angles), jnp.sin(angles) * sign
    seg_row = lax.dynamic_slice_in_dim(segments, z_at, 1, 0)
    seg_col = seg_row.reshape(length, 1)
    fused = group % 128 == 0
    if fused:
        weights = [w_qkv] * 3
    else:
        picked = w_qkv.reshape(width, 3, parts, group)
        picked = lax.dynamic_index_in_dim(picked, x_at, 2, keepdims=False)
        weights = [picked.reshape(width, 3 * group)]

    by_seq = swap_all(tokens, "z")
    by_seq, cosine, sine, seg_col, *grad_sent = lax.optimization_barrier(
        (by_seq, cosine, sine, seg_col, *grad_sent)
    )
    if parts == 2:
        rows = [by_seq, lax.ppermute(by_seq, "x", [(0, 1), (1, 0)])]
    else:
        rows = [lax.all_gather(by_seq, "x", axis=0, tiled=False)]
    *rows, grad_sent[0] = lax.optimization_barrier((*rows, grad_sent[0]))
    grad_came = [swap_all(grad_sent[0], ranks)]

    qkv, normed = project(rows, attn_scale, weights, group, cosine, sine, x_ref, parts)
    attended, lse = (attend if fused else plain_attend)(qkv, seg_row, seg_col)
    attended = after(attended, grad_came[0])
    attended = swap_all(attended.reshape(experts, span, group), ranks)
    attended, grad_sent[1] = lax.optimization_barrier((attended, grad_sent[1]))
    grad_came.append(swap_all(grad_sent[1], ranks))
    attended = attended.reshape(seqs, parts, span, group)

    hidden, branch_in = after_attention(flat_tokens, attended, w_out, ffn_scale)
    sent = [dispatch(branch_in, target_rows[0], experts, half)]
    shared_out, shared_back, hid, dg, du = feed_forward(
        after(branch_in, sent[0]), flat_cot, shared_gate, shared_up, shared_down
    )
    sent.append(dispatch(after(branch_in, shared_out), target_rows[1], experts, half))
    sent[0] = after(sent[0], grad_came[1], shared_out)
    received = [swap_all(value, ranks).reshape(-1, width) for value in sent]
    keep, give = shared_weight_grads(branch_in, flat_cot, dg, du, hid, sizes, core_ref)
    shared_sums, _ = fold(both(keep, give), "y")

    router = jnp.pad(w_router, ((0, 0), (0, 128 - experts)))
    made, back_rows, halves = None, [], []
    before = (give, sent[1])
    for at in range(2):
        grad_rows = grad_came[at][:, :half, :].reshape(-1, width)
        other = grad_came[at][:, half, :half].astype(jnp.int32).reshape(-1, 1)
        rows_at = after(received[at], grad_rows, other, *before)
        made, back, hid, dg, du, gated_grads, grad_logits = feed_forward(
            rows_at, grad_rows, expert_gate[0], expert_up[0], expert_down[0], router, other, own,
            experts, at, made,
        )
        back_rows.append(swap_all(back.reshape(experts, half, width), ranks).reshape(-1, width))
        halves.append((rows_at, gated_grads, dg, du, hid, grad_logits))
        before = (back,)
    halves[1] = (after(halves[1][0], back_rows[0]), *halves[1][1:])
    keep, give, grad_router = expert_weight_grads(halves, sizes, pair_ref)
    back_rows[1] = after(back_rows[1], give)
    expert_sums, expert_sent = fold(both(keep, give), "y", ordered=True)
    expert_got = expert_sums[-1]

    grad_hidden, grad_attn, grad_att, grad_ffn = middle_back(
        hidden, shared_back, back_rows, target, flat_cot, ffn_scale, w_out, parts, span
    )
    grad_att = swap_all(grad_att.reshape(experts, span, group), ranks).reshape(length, group)

    column = lax.broadcasted_iota(jnp.int32, (width, 128), 1)
    small = jnp.where(column < experts, grad_router, jnp.where(column == experts, grad_ffn, 0.0))
    out_sums = tall_weight_grads(
        [attended[:, part].reshape(count, group) for part in range(parts)],
        [grad_attn],
        [small],
        sizes,
        core_ref,
        WEIGHT,
    )
    out_sums = both(*out_sums)

    shared_sums, shared_sent = fold([after(term, out_sums[0]) for term in shared_sums], "x")
    made = after(made, grad_att, out_sums[0], shared_sent)
    grad_att = after(grad_att, expert_sent)
    made_rows = swap_all(made, ranks).reshape(-1, width)
    grads = list(
        (attend_back if fused else plain_attend_back)(
            qkv, grad_att, lse, seg_row, seg_col, cosine, sine
        )
    )
    normed_back, grad_gain = project_back(grads, weights, rows, x_ref, parts)
    normed_back, _ = fold([normed_back], "x")
    shared_sums = total(shared_sums).astype(BF)
    pieces = swap_by_steps(after(total(normed_back).astype(BF), made_rows), "z")

    qkv_sums = tall_weight_grads([normed], list(grads), [grad_gain], sizes, core_ref, 0.2)
    last = [jnp.concatenate(pair, axis=-1) for pair in zip(out_sums, both(*qkv_sums))]
    last, _ = fold(last, "y", expert_got)

    shared_sums = swap_by_steps(after(shared_sums, *pieces), "z")
    last = after(total(last).astype(BF), made_rows)
    each, cols = last.shape[-2:]
    expert_out = [total([term[index] for term in expert_sums]) for index in range(3)]
    expert_out = [expert_out[0][None], expert_out[1][None], jnp.transpose(expert_out[2])[None]]
    layer_out = layer_end(after(hidden, last), shared_out, [made_rows], whole_target).reshape(tokens.shape)
    token_grad = first_norm_back(
        flat_tokens, attn_scale, pieces, after(grad_hidden, layer_out), z_ref
    )
    last = swap_all(last.reshape(experts, each, cols), ranks).astype(F32)
    last = jnp.sum(last.reshape(blocks, parts, each, cols), axis=0)
    out_sums = jnp.sum(last[:, :, : width + 128], axis=0)
    qkv_sums = last[:, :, width + 128 :]
    grad_attn_gain = jnp.sum(qkv_sums[:, :, 3 * group], axis=0)
    grad_w_qkv = qkv_sums[:, :, : 3 * group].reshape(parts, each, 3, group)
    grad_w_qkv = jnp.transpose(grad_w_qkv, (1, 2, 0, 3)).reshape(each, 3 * width)

    first, *shared_sums = shared_sums
    shared_sums = total([after(first, token_grad, *expert_out), *shared_sums])
    return (
        layer_out,
        token_grad.reshape(tokens.shape),
        grad_attn_gain,
        grad_w_qkv,
        out_sums[:, :width],
        out_sums[:, width + experts],
        out_sums[:, width : width + experts],
        shared_sums[0],
        shared_sums[1],
        jnp.transpose(shared_sums[2]),
        *expert_out,
    )


def solution(mesh):
    dp, experts = mesh.shape["dp"], mesh.shape["expert"]

    def step(*args):
        seqs = args[0].shape[0] // dp
        cores = 2 if dp % 2 == 0 else 1
        fine = Mesh(
            mesh.devices.reshape(dp // cores, cores, seqs, experts // seqs),
            ("y", "core", "z", "x"),
        )
        data, ranks, every = ("y", "core"), ("z", "x"), ("y", "core", "z", "x")
        placed = (
            P(data, ranks, None),
            P(data, None),
            P(data, ranks, None),
            P(data, ranks, None),
            P(data, ranks, None),
            *([P()] * 8),
            P(ranks, None, None),
            P(ranks, None, None),
            P(ranks, None, None),
        )
        return jax.shard_map(
            on_device,
            mesh=fine,
            in_specs=placed,
            out_specs=(
                P(data, ranks, None),
                P(data, ranks, None),
                P(every),
                P(every, None),
                P(every, None),
                P(every),
                P(every, None),
                P(every, None),
                P(every, None),
                P(None, every),
                P(ranks, None, data),
                P(ranks, None, data),
                P(ranks, data, None),
            ),
            check_vma=False,
        )(*args)

    return step
```
